32 devices in a mesh: ctx: 16 (over z, y, core), wsh: 2 (over x).
Axes of the slice: x: 2, y: 2, z: 4, core: 2. Of those that a mesh axis runs over, the one named last changes fastest.
Arguments:
- tokens: bfloat16 [4, 2048, 1152], P('wsh', 'ctx'), may hold values from -6 to 6
- block_order: int32 [16], replicated, may hold values from 0 to 15, each once
- gain_attn_pre: bfloat16 [1152], P('wsh'), may hold values from 0.25 to 1.75
- gain_query: bfloat16 [256], P('wsh'), may hold values from 0.25 to 1.75
- gain_key: bfloat16 [256], P('wsh'), may hold values from 0.25 to 1.75
- gain_attn_post: bfloat16 [1152], P('wsh'), may hold values from 0.25 to 1.75
- gain_ff_pre: bfloat16 [1152], P('wsh'), may hold values from 0.25 to 1.75
- gain_ff_post: bfloat16 [1152], P('wsh'), may hold values from 0.25 to 1.75
- weight_query: bfloat16 [1152, 1024], P(None, 'wsh'), may hold values from -0.1875 to 0.1875
- weight_key: bfloat16 [1152, 256], P(None, 'wsh'), may hold values from -0.1875 to 0.1875
- weight_value: bfloat16 [1152, 256], P(None, 'wsh'), may hold values from -0.1875 to 0.1875
- weight_out: bfloat16 [1024, 1152], P(None, 'wsh'), may hold values from -0.1875 to 0.1875
- weight_gate: bfloat16 [1152, 6912], P(None, 'wsh'), may hold values from -0.1875 to 0.1875
- weight_up: bfloat16 [1152, 6912], P(None, 'wsh'), may hold values from -0.1875 to 0.1875
- weight_down: bfloat16 [1152, 6912], P(None, 'wsh'), may hold values from -0.078125 to 0.078125
- cotangent: bfloat16 [4, 2048, 1152], P('wsh', 'ctx'), may hold values from -6 to 6
Outputs:
- output: bfloat16 [4, 2048, 1152], P('wsh', 'ctx')
- grad_tokens: float32 [4, 2048, 1152], P('wsh', 'ctx')
- grad_gain_attn_pre: float32 [1152], P(('ctx', 'wsh'))
- grad_gain_query: float32 [256], P(('ctx', 'wsh'))
- grad_gain_key: float32 [256], P(('ctx', 'wsh'))
- grad_gain_attn_post: float32 [1152], P(('ctx', 'wsh'))
- grad_gain_ff_pre: float32 [1152], P(('ctx', 'wsh'))
- grad_gain_ff_post: float32 [1152], P(('ctx', 'wsh'))
- grad_weight_query: float32 [1152, 1024], P('ctx', 'wsh')
- grad_weight_key: float32 [1152, 256], P('ctx', 'wsh')
- grad_weight_value: float32 [1152, 256], P('ctx', 'wsh')
- grad_weight_out: float32 [1024, 1152], P('ctx', 'wsh')
- grad_weight_gate: float32 [1152, 6912], P('ctx', 'wsh')
- grad_weight_up: float32 [1152, 6912], P('ctx', 'wsh')
- grad_weight_down: float32 [1152, 6912], P('ctx', 'wsh')
The draws below stay inside these ranges and needn't reach their ends.
Inputs may be any that keep to these rules, and one draw needn't show every extreme that they name: block_order is a permutation of 0 to 15.
All inputs are finite; a program needn't handle non-finite values.
Results may differ from the reference program's by a relative error of at most 0.025.
Values may be sent and summed in bfloat16 or wider, within the bound.
A program may use at most 384 MiB of HBM per device.

```python
import math
import jax
import jax.numpy as jnp
from jax import lax

D = 1152
HEADS = 4
HEAD_DIM = 256
FF = 6912
BLK = 64
SEQS = 4
SEQLEN = 2048
N_CTX = 16


def strengthened(array, stream_key, source, target, blocks, factor):
    owner, partner = [(jnp.arange(array.shape[dim]) // (array.shape[dim] // blocks)).reshape([-1 if axis == dim else 1 for axis in range(array.ndim)]) for dim in (source, target)]
    chosen = jax.random.permutation(stream_key, blocks)[partner]
    strong = (owner == chosen) | (owner == (partner + blocks // 2) % blocks)
    return jnp.where(strong, factor * array, array)


def levels(rng, extent, split, smallest, largest):
    loudness = 1.0
    for dim, shards_of in split:
        steps = jax.random.uniform(jax.random.fold_in(jax.random.fold_in(rng, 6), dim), (shards_of,), jnp.float32, smallest / len(split), largest / len(split))
        loudness = loudness * jnp.repeat(jnp.exp(steps), extent[dim] // shards_of).reshape((-1,) + (1,) * (len(extent) - 1 - dim))
    return loudness


def bell_draw(stream_key, shape, scale, most, pieces=(), held_as=jnp.bfloat16):
    values = jax.random.normal(stream_key, shape, jnp.float32) * scale
    if len(pieces) > 0:
        values = levels(stream_key, shape, pieces, -0.22, 0.18) * values
    return jnp.clip(values, min=-most, max=most).astype(held_as)


def heavy_noise(key, dims, deviation, reach, split, heavy, kind=jnp.bfloat16):
    values = deviation * jax.random.normal(key, dims, jnp.float32)
    if split:
        values = values * levels(key, dims, split, -0.22, 0.18)
    return jnp.clip(strengthened(values, jax.random.fold_in(key, 3), *heavy), -reach, reach).astype(kind)


def setup_inputs(seed: int = 0) -> dict:
    splits = jax.random.split(jax.random.key(seed), 17)
    tokens = heavy_noise(splits[0], (SEQS, SEQLEN, D), 1.0, 6.0, ((0, 2), (1, 16)), (1, 2, 16, 2.0))
    block_order = jax.random.permutation(splits[1], N_CTX).astype(jnp.int32)
    gain_attn_pre = jnp.clip(1.0 + 0.15 * jax.random.normal(splits[2], (D,), jnp.float32), 0.25, 1.75).astype(jnp.bfloat16)
    gain_query = jnp.clip(1.0 + 0.15 * jax.random.normal(splits[3], (HEAD_DIM,), jnp.float32), 0.25, 1.75).astype(jnp.bfloat16)
    gain_key = jnp.clip(1.0 + 0.15 * jax.random.normal(splits[4], (HEAD_DIM,), jnp.float32), 0.25, 1.75).astype(jnp.bfloat16)
    gain_attn_post = jnp.clip(1.0 + 0.15 * jax.random.normal(splits[5], (D,), jnp.float32), 0.25, 1.75).astype(jnp.bfloat16)
    gain_ff_pre = jnp.clip(1.0 + 0.15 * jax.random.normal(splits[6], (D,), jnp.float32), 0.25, 1.75).astype(jnp.bfloat16)
    gain_ff_post = jnp.clip(1.0 + 0.15 * jax.random.normal(splits[7], (D,), jnp.float32), 0.25, 1.75).astype(jnp.bfloat16)
    weight_query = bell_draw(splits[8], (D, HEADS * HEAD_DIM), D ** -0.5, 0.1875, ((1, 2),))
    weight_key = bell_draw(splits[9], (D, HEAD_DIM), D ** -0.5, 0.1875, ((1, 2),))
    weight_value = bell_draw(splits[10], (D, HEAD_DIM), D ** -0.5, 0.1875, ((1, 2),))
    weight_out = bell_draw(splits[11], (HEADS * HEAD_DIM, D), (HEADS * HEAD_DIM) ** -0.5, 0.1875, ((1, 2),))
    weight_gate = bell_draw(splits[12], (D, FF), D ** -0.5, 0.1875, ((1, 2),))
    weight_up = bell_draw(splits[13], (D, FF), D ** -0.5, 0.1875, ((1, 2),))
    weight_down = bell_draw(splits[14], (D, FF), FF ** -0.5, 0.078125, ((1, 2),))
    cotangent = heavy_noise(splits[15], (SEQS, SEQLEN, D), 1.0, 6.0, ((0, 2), (1, 16)), (1, 2, 16, 2.0))
    return {"tokens": tokens, "block_order": block_order, "gain_attn_pre": gain_attn_pre, "gain_query": gain_query, "gain_key": gain_key, "gain_attn_post": gain_attn_post, "gain_ff_pre": gain_ff_pre, "gain_ff_post": gain_ff_post, "weight_query": weight_query, "weight_key": weight_key, "weight_value": weight_value, "weight_out": weight_out, "weight_gate": weight_gate, "weight_up": weight_up, "weight_down": weight_down, "cotangent": cotangent}


EPS = 1e-06
ROPE_BASE = 1000000.0
SCORE_SCALE = 0.0625
HIGH = lax.Precision.HIGHEST

@jax.custom_vjp
def low(v):
    return lax.optimization_barrier(v.astype(jnp.bfloat16)).astype(jnp.float32)

@jax.custom_vjp
def low_back(v):
    return v

def low_keep(v):
    return (low(v), None)

def low_pass(kept, grad):
    return (grad,)

def back_keep(v):
    return (v, None)

def back_low(kept, grad):
    return (low(grad),)
low.defvjp(low_keep, low_pass)
low_back.defvjp(back_keep, back_low)

def norm_gain(vector, gain):
    return vector * lax.rsqrt(lax.optimization_barrier(jnp.mean(vector * vector, -1, keepdims=True)) + EPS) * gain

def rotate(vector, cosine, sine):
    middle = vector.shape[-1] // 2
    first = vector[..., :middle]
    second = vector[..., middle:]
    return jnp.concatenate([first * cosine - second * sine, second * cosine + first * sine], -1)

def angle_tables(positions):
    middle = HEAD_DIM // 2
    inverse = jnp.exp(jnp.arange(middle, dtype=jnp.float32) * (-2.0 * math.log(ROPE_BASE) / HEAD_DIM))
    theta = positions.astype(jnp.float32)[:, None] * inverse[None, :]
    return (jnp.cos(theta), jnp.sin(theta))

def attend_block(query_block, query_pos, keys, values, key_pos):
    scores = low_back(jnp.einsum('qhd,kd->hqk', query_block, keys, precision=HIGH) * SCORE_SCALE)
    allowed = query_pos[None, :, None] >= key_pos[None, None, :]
    weights = low(jnp.where(allowed, jnp.exp(scores), 0.0))
    totals = lax.optimization_barrier(jnp.sum(weights, -1))
    summed = low_back(jnp.einsum('hqk,kd->qhd', weights, values, precision=HIGH))
    return summed / jnp.transpose(totals)[:, :, None]

def layer(params, sequence, positions):
    gain_attn_pre, gain_query, gain_key, gain_attn_post, gain_ff_pre, gain_ff_post, weight_query, weight_key, weight_value, weight_out, weight_gate, weight_up, weight_down = params
    length = sequence.shape[0]
    cosine, sine = angle_tables(positions)
    normed = low(norm_gain(sequence, gain_attn_pre))
    query_raw = low_back(jnp.dot(normed, weight_query, precision=HIGH)).reshape(length, HEADS, HEAD_DIM)
    key_raw = low_back(jnp.dot(normed, weight_key, precision=HIGH))
    value_low = low(low_back(jnp.dot(normed, weight_value, precision=HIGH)))
    query_low = low(rotate(norm_gain(query_raw, gain_query), cosine[:, None, :], sine[:, None, :]))
    key_low = low(rotate(norm_gain(key_raw, gain_key), cosine, sine))
    query_rows = min(512, length)
    blocks = length // query_rows
    query_blocks = query_low.reshape(blocks, query_rows, HEADS, HEAD_DIM)
    position_blocks = positions.reshape(blocks, query_rows)

    def one_block(pair):
        return attend_block(pair[0], pair[1], key_low, value_low, positions)
    mixed = lax.map(jax.checkpoint(one_block), (query_blocks, position_blocks))
    mixed = low(low_back(mixed.reshape(length, HEADS * HEAD_DIM)))
    attended = low_back(jnp.dot(mixed, weight_out, precision=HIGH))
    hidden_state = sequence + norm_gain(attended, gain_attn_post)
    ff_input = low(norm_gain(hidden_state, gain_ff_pre))
    gate = low_back(jnp.dot(ff_input, weight_gate, precision=HIGH))
    upward = low_back(jnp.dot(ff_input, weight_up, precision=HIGH))
    activated = low(jax.nn.gelu(gate, approximate=True) * upward)
    lowered = low_back(jnp.dot(activated, jnp.transpose(weight_down), precision=HIGH))
    return hidden_state + norm_gain(lowered, gain_ff_post)

def reference(tokens, block_order, gain_attn_pre, gain_query, gain_key, gain_attn_post, gain_ff_pre, gain_ff_post, weight_query, weight_key, weight_value, weight_out, weight_gate, weight_up, weight_down, cotangent):
    pairs = jnp.stack([block_order, 2 * N_CTX - 1 - block_order], 1).reshape(-1).astype(jnp.int32)
    positions = (pairs[:, None] * BLK + jnp.arange(BLK, dtype=jnp.int32)[None, :]).reshape(-1).astype(jnp.int32)
    params = tuple((member.astype(jnp.float32) for member in (gain_attn_pre, gain_query, gain_key, gain_attn_post, gain_ff_pre, gain_ff_post, weight_query, weight_key, weight_value, weight_out, weight_gate, weight_up, weight_down)))
    inputs = tokens.astype(jnp.float32)

    def forward(inputs, params):

        def scan_step(carry, sequence):
            return (carry, layer(params, sequence, positions))
        return lax.scan(scan_step, None, inputs)[1]
    result, back_fn = jax.vjp(forward, inputs, params)
    grad_inputs, grad_params = back_fn(cotangent.astype(jnp.float32))
    return (result.astype(jnp.bfloat16), grad_inputs, grad_params[0], grad_params[1], grad_params[2], grad_params[3], grad_params[4], grad_params[5], grad_params[6], grad_params[7], grad_params[8], grad_params[9], grad_params[10], grad_params[11], grad_params[12])
```

```python
import functools
import math

import jax
import jax.numpy as jnp
from jax import lax
from jax.experimental import pallas as pl
from jax.experimental.pallas import tpu as pltpu
from jax.sharding import PartitionSpec as P

EPS = 1e-06
ROPE_BASE = 1000000.0
SCORE_SCALE = 0.0625
F32 = jnp.float32
BF16 = jnp.bfloat16


def norm_gain(vector, gain):
    return vector * lax.rsqrt(jnp.mean(vector * vector, -1, keepdims=True) + EPS) * gain


def rotate(vector, cosine, sine):
    middle = vector.shape[-1] // 2
    first = vector[..., :middle]
    second = vector[..., middle:]
    return jnp.concatenate([first * cosine - second * sine, second * cosine + first * sine], -1)


def angle_tables(positions, head_size):
    middle = head_size // 2
    inverse = jnp.exp(
        jnp.arange(middle, dtype=F32) * (-2.0 * math.log(ROPE_BASE) / head_size)
    )
    theta = positions.astype(F32)[:, None] * inverse[None, :]
    return (jnp.cos(theta), jnp.sin(theta))


def gate_up(gate, upward):
    return jax.nn.gelu(gate, approximate=True) * upward


def swap(value):
    return lax.ppermute(value, "wsh", [(0, 1), (1, 0)])


def join_halves(mine, local, other):
    return jnp.where(
        mine == 0,
        jnp.concatenate([local, other], -1),
        jnp.concatenate([other, local], -1),
    )


def half_of(value, which):
    middle = value.shape[-1] // 2
    return jnp.where(which == 0, value[..., :middle], value[..., middle:])


def dot(left, right, dims):
    return lax.dot_general(left, right, (dims, ((), ())), preferred_element_type=F32)


def stack_heads(ref, half, block, heads, size):
    rows = slice(half * block, (half + 1) * block)
    return jnp.concatenate([ref[0, rows, h * size : (h + 1) * size] for h in range(heads)], 0)


def attend_forward_kernel(heads, chunk, q_ref, kv_ref, qpos_ref, kpos_ref, o_ref, mix_ref, tot_ref):
    shards, _, rows, pair = kv_ref.shape
    block, size = rows // 2, pair // 2
    queries = [stack_heads(q_ref, half, block, heads, size) for half in range(2)]
    stacked = heads * block
    sums = [jnp.zeros((stacked, size), F32) for _ in range(2)]
    totals = [jnp.zeros((stacked, 1), F32) for _ in range(2)]
    for first in range(0, shards, chunk):
        span = slice(first * block, (first + chunk) * block)
        for key_half in range(2):
            part = kv_ref[first : first + chunk, 0, key_half * block : (key_half + 1) * block, :]
            part = part.reshape(chunk * block, pair)
            keys, values = part[:, :size], part[:, size:]
            for half in range(key_half, 2):
                weights = jnp.exp(dot(queries[half], keys, ((1,), (1,))) * SCORE_SCALE)
                if half == key_half:
                    allowed = (
                        kpos_ref[key_half : key_half + 1, span]
                        <= qpos_ref[half * stacked : (half + 1) * stacked, :]
                    )
                    weights = jnp.where(allowed, weights, 0.0)
                low = weights.astype(BF16)
                totals[half] += jnp.sum(low.astype(F32), -1, keepdims=True)
                sums[half] += dot(low, values, ((1,), (0,)))
    for half in range(2):
        mixed = sums[half] / totals[half]
        mix_ref[0, half * stacked : (half + 1) * stacked, :] = mixed
        tot_ref[0, half * stacked : (half + 1) * stacked, :] = jnp.broadcast_to(
            totals[half], (stacked, tot_ref.shape[2])
        )
        for h in range(heads):
            o_ref[0, half * block : (half + 1) * block, h * size : (h + 1) * size] = mixed[
                h * block : (h + 1) * block
            ].astype(BF16)


def attend_backward_kernel(
    heads, chunk, q_ref, kv_ref, g_ref, mix_ref, tot_ref, qpos_ref, kpos_ref, dq_ref, dkv_ref
):
    shards, _, rows, pair = kv_ref.shape
    block, size = rows // 2, pair // 2
    stacked = heads * block
    queries, scaled, correction = [], [], []
    for half in range(2):
        queries.append(stack_heads(q_ref, half, block, heads, size))
        grad = stack_heads(g_ref, half, block, heads, size).astype(F32)
        span = slice(half * stacked, (half + 1) * stacked)
        total = tot_ref[0, span, :1]
        delta = jnp.sum(grad * mix_ref[0, span, :], -1, keepdims=True)
        scaled.append((grad / total).astype(BF16))
        correction.append(delta / total)
    grad_query = [jnp.zeros((stacked, size), F32) for _ in range(2)]
    for first in range(0, shards, chunk):
        span = slice(first * block, (first + chunk) * block)
        for key_half in range(2):
            part = kv_ref[first : first + chunk, 0, key_half * block : (key_half + 1) * block, :]
            part = part.reshape(chunk * block, pair)
            keys, values = part[:, :size], part[:, size:]
            grad_keys = jnp.zeros((chunk * block, size), F32)
            grad_values = jnp.zeros((chunk * block, size), F32)
            for half in range(key_half, 2):
                weights = jnp.exp(dot(queries[half], keys, ((1,), (1,))) * SCORE_SCALE)
                if half == key_half:
                    allowed = (
                        kpos_ref[key_half : key_half + 1, span]
                        <= qpos_ref[half * stacked : (half + 1) * stacked, :]
                    )
                    weights = jnp.where(allowed, weights, 0.0)
                low = weights.astype(BF16)
                grad_weights = dot(scaled[half], values, ((1,), (1,)))
                grad_scores = (weights * (grad_weights - correction[half])).astype(BF16)
                grad_query[half] += dot(grad_scores, keys, ((1,), (0,)))
                grad_keys += dot(grad_scores, queries[half], ((0,), (0,)))
                grad_values += dot(low, scaled[half], ((0,), (0,)))
            both = jnp.concatenate([grad_keys * SCORE_SCALE, grad_values], -1).astype(BF16)
            dkv_ref[first : first + chunk, 0, key_half * block : (key_half + 1) * block, :] = (
                both.reshape(chunk, block, pair)
            )
    for half in range(2):
        for h in range(heads):
            dq_ref[0, half * block : (half + 1) * block, h * size : (h + 1) * size] = (
                grad_query[half][h * block : (h + 1) * block] * SCORE_SCALE
            )


def whole(shape):
    return pl.BlockSpec(shape, lambda s: (0,) * len(shape))


def attend_forward(query_low, pairs, query_pos, key_pos, heads):
    sequences, rows, width = query_low.shape
    shards, _, _, pair = pairs.shape
    stacked = query_pos.shape[0]
    row = pl.BlockSpec((1, rows, width), lambda s: (s, 0, 0))
    stack = lambda last: pl.BlockSpec((1, stacked, last), lambda s: (s, 0, 0))
    return pl.pallas_call(
        functools.partial(attend_forward_kernel, heads, min(shards, 16)),
        grid=(sequences,),
        in_specs=[
            row,
            pl.BlockSpec((shards, 1, rows, pair), lambda s: (0, s, 0, 0)),
            whole(query_pos.shape),
            whole(key_pos.shape),
        ],
        out_specs=[row, stack(pair // 2), stack(128)],
        out_shape=[
            jax.ShapeDtypeStruct((sequences, rows, width), BF16),
            jax.ShapeDtypeStruct((sequences, stacked, pair // 2), F32),
            jax.ShapeDtypeStruct((sequences, stacked, 128), F32),
        ],
        name="attend_forward",
    )(query_low, pairs, query_pos, key_pos)


def attend_backward(query_low, pairs, grad_mixed, mixed, totals, query_pos, key_pos, heads):
    sequences, rows, width = query_low.shape
    shards, _, _, pair = pairs.shape
    stacked = query_pos.shape[0]
    row = pl.BlockSpec((1, rows, width), lambda s: (s, 0, 0))
    stack = lambda last: pl.BlockSpec((1, stacked, last), lambda s: (s, 0, 0))
    pairs_spec = pl.BlockSpec((shards, 1, rows, pair), lambda s: (0, s, 0, 0))
    return pl.pallas_call(
        functools.partial(attend_backward_kernel, heads, min(shards, 16)),
        grid=(sequences,),
        in_specs=[
            row,
            pairs_spec,
            row,
            stack(pair // 2),
            stack(128),
            whole(query_pos.shape),
            whole(key_pos.shape),
        ],
        out_specs=[row, pairs_spec],
        out_shape=[
            jax.ShapeDtypeStruct((sequences, rows, width), F32),
            jax.ShapeDtypeStruct(pairs.shape, BF16),
        ],
        name="attend_backward",
    )(query_low, pairs, grad_mixed, mixed, totals, query_pos, key_pos)


def body(
    tokens,
    block_order,
    gain_attn_pre,
    gain_query,
    gain_key,
    gain_attn_post,
    gain_ff_pre,
    gain_ff_post,
    weight_query,
    weight_key,
    weight_value,
    weight_out,
    weight_gate,
    weight_up,
    weight_down,
    cotangent,
):
    sequences, rows, width = tokens.shape
    count = sequences * rows
    block = rows // 2
    devices = lax.axis_size("ctx")
    me = lax.axis_index("ctx")
    mine = lax.axis_index("wsh")

    key_value_other = swap(jnp.concatenate([weight_key, weight_value], 1))
    local_size = weight_key.shape[1]
    gains = [gain_attn_pre, gain_query, gain_key, gain_attn_post, gain_ff_pre, gain_ff_post]
    gain_sizes = [g.shape[0] for g in gains]
    gains_other = swap(jnp.concatenate(gains))
    starts = [sum(gain_sizes[:i]) for i in range(len(gains))]
    attn_pre, query_gain, key_gain, attn_post, ff_pre, ff_post = [
        join_halves(mine, g, gains_other[s : s + n]).astype(F32)
        for g, s, n in zip(gains, starts, gain_sizes)
    ]
    pair_weight = jnp.concatenate(
        [
            join_halves(mine, weight_key, key_value_other[:, :local_size]),
            join_halves(mine, weight_value, key_value_other[:, local_size:]),
        ],
        1,
    )
    weight_query = join_halves(mine, weight_query, swap(weight_query))
    weight_out = join_halves(mine, weight_out, swap(weight_out))

    head_size = query_gain.shape[0]
    heads = weight_query.shape[1] // head_size

    lane = jnp.arange(block, dtype=jnp.int32)
    late_order = 2 * devices - 1 - block_order
    early_pos = (block_order[:, None] * block + lane[None]).reshape(-1)
    late_pos = (late_order[:, None] * block + lane[None]).reshape(-1)
    key_pos = jnp.stack([early_pos, late_pos], 0)
    own_first = lax.dynamic_slice_in_dim(block_order, me, 1)[0]
    own_early = own_first * block + lane
    own_late = (2 * devices - 1 - own_first) * block + lane
    own_pos = jnp.concatenate([own_early, own_late])
    query_pos = jnp.concatenate([jnp.tile(own_early, heads), jnp.tile(own_late, heads)])[:, None]

    inputs = tokens.astype(F32)
    normed, pre_back = jax.vjp(norm_gain, inputs, attn_pre)
    normed_low = normed.astype(BF16)
    key_value = jnp.einsum("srd,de->sre", normed_low, pair_weight, preferred_element_type=F32)
    key_raw = key_value[..., :head_size]
    value_low = key_value[..., head_size:].astype(BF16)
    cosine, sine = angle_tables(own_pos, head_size)

    def key_path(key_in, key_scale):
        return rotate(norm_gain(key_in, key_scale), cosine[None], sine[None])

    def query_path(query_in, query_scale):
        return rotate(
            norm_gain(query_in, query_scale), cosine[None, :, None, :], sine[None, :, None, :]
        )

    key_rot, key_back = jax.vjp(key_path, key_raw, key_gain)
    local_pair = jnp.concatenate([key_rot.astype(BF16), value_low], -1)
    pairs = lax.all_gather(local_pair, "ctx", axis=0, tiled=False)
    query_raw = jnp.einsum(
        "srd,de->sre", normed_low, weight_query, preferred_element_type=F32
    ).reshape(sequences, rows, heads, head_size)
    query_rot, query_back = jax.vjp(query_path, query_raw, query_gain)
    query_low = query_rot.astype(BF16).reshape(sequences, rows, heads * head_size)

    mixed_low, mixed, totals = attend_forward(query_low, pairs, query_pos, key_pos, heads)
    attended = jnp.einsum("sre,ed->srd", mixed_low, weight_out, preferred_element_type=F32)
    post_attn, post_attn_back = jax.vjp(norm_gain, attended, attn_post)
    hidden_state = inputs + post_attn
    ff_input, ff_pre_back = jax.vjp(norm_gain, hidden_state, ff_pre)
    ff_own = ff_input.astype(BF16).reshape(count, width)
    ff_other = swap(ff_own)

    def ff_forward(rows_in):
        gate = dot(rows_in, weight_gate, ((1,), (0,)))
        upward = dot(rows_in, weight_up, ((1,), (0,)))
        activated, gelu_back = jax.vjp(gate_up, gate, upward)
        activated_low = activated.astype(BF16)
        return activated_low, gelu_back, dot(activated_low, weight_down, ((1,), (1,)))

    act_own, gelu_own, lowered_own = ff_forward(ff_own)
    act_other, gelu_other, lowered_other = ff_forward(ff_other)
    lowered = lowered_own + swap(lowered_other.astype(BF16)).astype(F32)
    lowered = lowered.reshape(sequences, rows, width)
    post_ff, post_ff_back = jax.vjp(norm_gain, lowered, ff_post)
    output = (hidden_state + post_ff).astype(BF16)

    grad_output = cotangent.astype(F32)
    grad_lowered, grad_ff_post = post_ff_back(grad_output)
    low_own = grad_lowered.astype(BF16).reshape(count, width)
    low_other = swap(low_own)

    def ff_backward(rows_in, gelu_back):
        grad_gate, grad_up = gelu_back(dot(rows_in, weight_down, ((1,), (0,))))
        grad_gate, grad_up = grad_gate.astype(BF16), grad_up.astype(BF16)
        back = dot(grad_gate, weight_gate, ((1,), (1,))) + dot(grad_up, weight_up, ((1,), (1,)))
        return grad_gate, grad_up, back

    gate_own, up_own, back_own = ff_backward(low_own, gelu_own)
    gate_other, up_other, back_other = ff_backward(low_other, gelu_other)
    grad_ff_input = back_own + swap(back_other.astype(BF16)).astype(F32)
    grad_ff_input = grad_ff_input.reshape(sequences, rows, width)

    def both(own, other):
        return jnp.concatenate([own, other], 0)

    def weight_grad(left, right):
        return dot(left, right, ((0,), (0,))).astype(BF16)

    ff_rows = both(ff_own, ff_other)
    part_down = weight_grad(both(low_own, low_other), both(act_own, act_other))
    part_gate = weight_grad(ff_rows, both(gate_own, gate_other))
    part_up = weight_grad(ff_rows, both(up_own, up_other))

    grad_hidden, grad_ff_pre = ff_pre_back(grad_ff_input)
    grad_hidden = grad_hidden + grad_output
    grad_attended, grad_attn_post = post_attn_back(grad_hidden)
    attended_low = grad_attended.astype(BF16)
    grad_mixed = jnp.einsum(
        "srd,ed->sre", attended_low, weight_out, preferred_element_type=F32
    ).astype(BF16)
    attended_low = attended_low.reshape(count, width)
    mixed_rows = mixed_low.reshape(count, heads * head_size)
    part_out = weight_grad(
        both(mixed_rows, swap(mixed_rows)),
        both(half_of(attended_low, mine), swap(half_of(attended_low, 1 - mine))),
    )
    grad_query, grad_pairs = attend_backward(
        query_low, pairs, grad_mixed, mixed, totals, query_pos, key_pos, heads
    )
    own_grads = lax.psum_scatter(grad_pairs, "ctx", scatter_dimension=0, tiled=False).astype(F32)
    grad_key_raw, grad_key_gain = key_back(own_grads[..., :head_size])
    value_grad_low = own_grads[..., head_size:].astype(BF16)
    grad_query_raw, grad_query_gain = query_back(
        grad_query.reshape(sequences, rows, heads, head_size)
    )
    query_grad_low = grad_query_raw.reshape(count, heads * head_size).astype(BF16)
    key_grad_low = grad_key_raw.astype(BF16).reshape(count, head_size)
    value_grad_low = value_grad_low.reshape(count, head_size)
    grad_normed = (
        dot(query_grad_low, weight_query, ((1,), (1,)))
        + dot(jnp.concatenate([key_grad_low, value_grad_low], -1), pair_weight, ((1,), (1,)))
    ).reshape(sequences, rows, width)
    grad_inputs, grad_attn_pre = pre_back(grad_normed)
    grad_tokens = grad_inputs + grad_hidden

    def columns(which):
        return jnp.concatenate(
            [half_of(v, which) for v in (query_grad_low, key_grad_low, value_grad_low)], -1
        )

    normed_rows = normed_low.reshape(count, width)
    part_qkv = weight_grad(
        both(normed_rows, swap(normed_rows)), both(columns(mine), swap(columns(1 - mine)))
    )

    def reduce_rows(part):
        return lax.psum_scatter(part, "ctx", scatter_dimension=0, tiled=True).astype(F32)

    grad_down_w = reduce_rows(part_down)
    grad_gate_w = reduce_rows(part_gate)
    grad_up_w = reduce_rows(part_up)
    grad_out_w = reduce_rows(part_out)
    grad_qkv = reduce_rows(part_qkv)
    query_cols = query_grad_low.shape[1] // 2
    grad_query_w = grad_qkv[:, :query_cols]
    grad_key_w = grad_qkv[:, query_cols : query_cols + local_size]
    grad_value_w = grad_qkv[:, query_cols + local_size :]

    gain_grads = [
        grad_attn_pre,
        grad_query_gain,
        grad_key_gain,
        grad_attn_post,
        grad_ff_pre,
        grad_ff_post,
    ]
    packed = jnp.concatenate([g.reshape(devices, 2, -1) for g in gain_grads], -1)
    keep = jnp.where(mine == 0, packed[:, 0], packed[:, 1])
    send = jnp.where(mine == 0, packed[:, 1], packed[:, 0])
    packed = lax.psum_scatter(keep + swap(send), "ctx", scatter_dimension=0, tiled=False)
    outs, first = [], 0
    for g in gain_grads:
        size = g.shape[0] // (2 * devices)
        outs.append(packed[first : first + size])
        first += size
    return (
        output,
        grad_tokens,
        *outs,
        grad_query_w,
        grad_key_w,
        grad_value_w,
        grad_out_w,
        grad_gate_w,
        grad_up_w,
        grad_down_w,
    )


def solution(mesh):
    rows, vector, matrix = P("wsh", "ctx", None), P("wsh"), P(None, "wsh")
    in_specs = (rows, P()) + (vector,) * 6 + (matrix,) * 7 + (rows,)
    out_specs = (rows, rows) + (P(("ctx", "wsh")),) * 6 + (P("ctx", "wsh"),) * 7
    return jax.shard_map(body, mesh=mesh, in_specs=in_specs, out_specs=out_specs, check_vma=False)
```

```python
import functools
import math

import jax
import jax.numpy as jnp
from jax import lax
from jax.experimental import pallas as pl
from jax.experimental.pallas import tpu as pltpu
from jax.sharding import PartitionSpec as P

EPS = 1e-06
ROPE_BASE = 1000000.0
SCORE_SCALE = 0.0625
F32 = jnp.float32
BF16 = jnp.bfloat16
MESH = pl.DeviceIdType.MESH


def norm_gain(vector, gain):
    return vector * lax.rsqrt(jnp.mean(vector * vector, -1, keepdims=True) + EPS) * gain


def rotate(vector, cosine, sine):
    middle = vector.shape[-1] // 2
    first = vector[..., :middle]
    second = vector[..., middle:]
    return jnp.concatenate([first * cosine - second * sine, second * cosine + first * sine], -1)


def angle_tables(positions, head_size):
    middle = head_size // 2
    inverse = jnp.exp(
        jnp.arange(middle, dtype=F32) * (-2.0 * math.log(ROPE_BASE) / head_size)
    )
    theta = positions.astype(F32)[:, None] * inverse[None, :]
    return (jnp.cos(theta), jnp.sin(theta))


def gate_up(gate, upward):
    return jax.nn.gelu(gate, approximate=True) * upward


def swap(value):
    return lax.ppermute(value, "wsh", [(0, 1), (1, 0)])


def join_halves(mine, local, other):
    return jnp.where(
        mine == 0,
        jnp.concatenate([local, other], -1),
        jnp.concatenate([other, local], -1),
    )


def half_of(value, which):
    middle = value.shape[-1] // 2
    return jnp.where(which == 0, value[..., :middle], value[..., middle:])


def dot(left, right, dims):
    return lax.dot_general(left, right, (dims, ((), ())), preferred_element_type=F32)


def stack_heads(ref, half, block, heads, size):
    rows = slice(half * block, (half + 1) * block)
    return jnp.concatenate([ref[0, rows, h * size : (h + 1) * size] for h in range(heads)], 0)


def attend_forward_kernel(heads, chunk, q_ref, kv_ref, qpos_ref, kpos_ref, o_ref, mix_ref, tot_ref):
    shards, _, rows, pair = kv_ref.shape
    block, size = rows // 2, pair // 2
    queries = [stack_heads(q_ref, half, block, heads, size) for half in range(2)]
    stacked = heads * block
    sums = [jnp.zeros((stacked, size), F32) for _ in range(2)]
    totals = [jnp.zeros((stacked, 1), F32) for _ in range(2)]
    for first in range(0, shards, chunk):
        span = slice(first * block, (first + chunk) * block)
        for key_half in range(2):
            part = kv_ref[first : first + chunk, 0, key_half * block : (key_half + 1) * block, :]
            part = part.reshape(chunk * block, pair)
            keys, values = part[:, :size], part[:, size:]
            for half in range(key_half, 2):
                weights = jnp.exp(dot(queries[half], keys, ((1,), (1,))) * SCORE_SCALE)
                if half == key_half:
                    allowed = (
                        kpos_ref[key_half : key_half + 1, span]
                        <= qpos_ref[half * stacked : (half + 1) * stacked, :]
                    )
                    weights = jnp.where(allowed, weights, 0.0)
                low = weights.astype(BF16)
                totals[half] += jnp.sum(low.astype(F32), -1, keepdims=True)
                sums[half] += dot(low, values, ((1,), (0,)))
    for half in range(2):
        mixed = sums[half] / totals[half]
        mix_ref[0, half * stacked : (half + 1) * stacked, :] = mixed
        tot_ref[0, half * stacked : (half + 1) * stacked, :] = jnp.broadcast_to(
            totals[half], (stacked, tot_ref.shape[2])
        )
        for h in range(heads):
            o_ref[0, half * block : (half + 1) * block, h * size : (h + 1) * size] = mixed[
                h * block : (h + 1) * block
            ].astype(BF16)


def attend_backward_kernel(
    heads, chunk, q_ref, kv_ref, g_ref, mix_ref, tot_ref, qpos_ref, kpos_ref, dq_ref, dkv_ref
):
    shards, _, rows, pair = kv_ref.shape
    block, size = rows // 2, pair // 2
    stacked = heads * block
    queries, scaled, correction = [], [], []
    for half in range(2):
        queries.append(stack_heads(q_ref, half, block, heads, size))
        grad = stack_heads(g_ref, half, block, heads, size).astype(F32)
        span = slice(half * stacked, (half + 1) * stacked)
        total = tot_ref[0, span, :1]
        delta = jnp.sum(grad * mix_ref[0, span, :], -1, keepdims=True)
        scaled.append((grad / total).astype(BF16))
        correction.append(delta / total)
    grad_query = [jnp.zeros((stacked, size), F32) for _ in range(2)]
    for first in range(0, shards, chunk):
        span = slice(first * block, (first + chunk) * block)
        for key_half in range(2):
            part = kv_ref[first : first + chunk, 0, key_half * block : (key_half + 1) * block, :]
            part = part.reshape(chunk * block, pair)
            keys, values = part[:, :size], part[:, size:]
            grad_keys = jnp.zeros((chunk * block, size), F32)
            grad_values = jnp.zeros((chunk * block, size), F32)
            for half in range(key_half, 2):
                weights = jnp.exp(dot(queries[half], keys, ((1,), (1,))) * SCORE_SCALE)
                if half == key_half:
                    allowed = (
                        kpos_ref[key_half : key_half + 1, span]
                        <= qpos_ref[half * stacked : (half + 1) * stacked, :]
                    )
                    weights = jnp.where(allowed, weights, 0.0)
                low = weights.astype(BF16)
                grad_weights = dot(scaled[half], values, ((1,), (1,)))
                grad_scores = (weights * (grad_weights - correction[half])).astype(BF16)
                grad_query[half] += dot(grad_scores, keys, ((1,), (0,)))
                grad_keys += dot(grad_scores, queries[half], ((0,), (0,)))
                grad_values += dot(low, scaled[half], ((0,), (0,)))
            both = jnp.concatenate([grad_keys * SCORE_SCALE, grad_values], -1).astype(BF16)
            dkv_ref[first : first + chunk, 0, key_half * block : (key_half + 1) * block, :] = (
                both.reshape(chunk, block, pair)
            )
    for half in range(2):
        for h in range(heads):
            dq_ref[0, half * block : (half + 1) * block, h * size : (h + 1) * size] = (
                grad_query[half][h * block : (h + 1) * block] * SCORE_SCALE
            )


def whole(shape):
    return pl.BlockSpec(shape, lambda s: (0,) * len(shape))


def attend_forward(query_low, pairs, query_pos, key_pos, heads):
    sequences, rows, width = query_low.shape
    shards, _, _, pair = pairs.shape
    stacked = query_pos.shape[0]
    row = pl.BlockSpec((1, rows, width), lambda s: (s, 0, 0))
    stack = lambda last: pl.BlockSpec((1, stacked, last), lambda s: (s, 0, 0))
    return pl.pallas_call(
        functools.partial(attend_forward_kernel, heads, min(shards, 16)),
        grid=(sequences,),
        in_specs=[
            row,
            pl.BlockSpec((shards, 1, rows, pair), lambda s: (0, s, 0, 0)),
            whole(query_pos.shape),
            whole(key_pos.shape),
        ],
        out_specs=[row, stack(pair // 2), stack(128)],
        out_shape=[
            jax.ShapeDtypeStruct((sequences, rows, width), BF16),
            jax.ShapeDtypeStruct((sequences, stacked, pair // 2), F32),
            jax.ShapeDtypeStruct((sequences, stacked, 128), F32),
        ],
        name="attend_forward",
    )(query_low, pairs, query_pos, key_pos)


def attend_backward(query_low, pairs, grad_mixed, mixed, totals, query_pos, key_pos, heads):
    sequences, rows, width = query_low.shape
    shards, _, _, pair = pairs.shape
    stacked = query_pos.shape[0]
    row = pl.BlockSpec((1, rows, width), lambda s: (s, 0, 0))
    stack = lambda last: pl.BlockSpec((1, stacked, last), lambda s: (s, 0, 0))
    pairs_spec = pl.BlockSpec((shards, 1, rows, pair), lambda s: (0, s, 0, 0))
    return pl.pallas_call(
        functools.partial(attend_backward_kernel, heads, min(shards, 16)),
        grid=(sequences,),
        in_specs=[
            row,
            pairs_spec,
            row,
            stack(pair // 2),
            stack(128),
            whole(query_pos.shape),
            whole(key_pos.shape),
        ],
        out_specs=[row, pairs_spec],
        out_shape=[
            jax.ShapeDtypeStruct((sequences, rows, width), F32),
            jax.ShapeDtypeStruct(pairs.shape, BF16),
        ],
        name="attend_backward",
    )(query_low, pairs, grad_mixed, mixed, totals, query_pos, key_pos)


class Ring:
    def __init__(self, devices):
        self.chips = devices // 2
        me = lax.axis_index("ctx")
        self.core = me % 2
        chip = me // 2
        across = chip % 2
        deep = chip // 2
        self.place = deep + across * (self.chips - 1 - 2 * deep)
        self.partner = me + 1 - 2 * self.core
        self.right = self.device((self.place + 1) % self.chips, self.core)
        self.left = self.device((self.place + self.chips - 1) % self.chips, self.core)

    def device(self, place, core):
        side = place // (self.chips // 2)
        return 2 * (2 * (place + side * (self.chips - 1 - 2 * place)) + side) + core

    def enter(self):
        barrier = pltpu.get_barrier_semaphore()
        for other in (self.left, self.right, self.partner):
            pl.semaphore_signal(barrier, inc=1, device_id={"ctx": other}, device_id_type=MESH)
        pl.semaphore_wait(barrier, 3)


def ring_sum_kernel(devices, pieces, arrays, ahead, *refs):
    parts, outs = refs[:arrays], refs[arrays : 2 * arrays]
    own, other, flow = (refs[(2 + i) * arrays : (3 + i) * arrays] for i in range(3))
    own_sem, put_sem, got_sem, send_sem, recv_sem = refs[5 * arrays :]
    ring = Ring(devices)
    chips = ring.chips

    def region(p):
        array, _, first, rows, start, cols = pieces[p]
        return array, pl.ds(first, rows), pl.ds(start, cols)

    def chunk(p, step):
        way = pieces[p][1]
        return (ring.place + 2 * chips + way * (-1 - step)) % chips

    def load(p, step):
        array, rows, cols = region(p)
        source = ring.device(chunk(p, step), ring.core)
        return pltpu.make_async_copy(
            parts[array].at[source, rows, cols],
            own[array].at[step, rows, cols],
            own_sem.at[p, step],
        )

    def give(p, step):
        array, rows, cols = region(p)
        source = ring.device(chunk(p, step), 1 - ring.core)
        return pltpu.make_async_remote_copy(
            src_ref=parts[array].at[source, rows, cols],
            dst_ref=other[array].at[step, rows, cols],
            send_sem=put_sem.at[p, step],
            recv_sem=got_sem.at[p, step],
            device_id={"ctx": ring.partner},
            device_id_type=MESH,
        )

    def pass_on(p, step):
        array, rows, cols = region(p)
        way = pieces[p][1]
        return pltpu.make_async_remote_copy(
            src_ref=flow[array].at[step, rows, cols],
            dst_ref=flow[array].at[step + 1, rows, cols],
            send_sem=send_sem.at[p, step],
            recv_sem=recv_sem.at[p, step],
            device_id={"ctx": ring.right if way > 0 else ring.left},
            device_id_type=MESH,
        )

    def fetch(step):
        for p in range(len(pieces)):
            load(p, step).start()
            give(p, step).start()

    def add(p, step, first, last):
        array, _, row, rows, start, cols = pieces[p]
        width = 128 if cols % 128 == 0 else cols
        while width < 512 and cols % (2 * width) == 0:
            width *= 2
        rows = pl.ds(row, rows)

        def group(i, carry):
            at = start + i * width
            if cols > width:
                at = pl.multiple_of(at, 128)
            where = pl.ds(at, width)
            total = own[array][step, rows, where].astype(F32) + other[array][
                step, rows, where
            ].astype(F32)
            if not first:
                total += flow[array][step, rows, where].astype(F32)
            if last:
                outs[array][rows, where] = total.astype(outs[array].dtype)
            else:
                flow[array][step, rows, where] = total.astype(flow[array].dtype)
            return carry

        if cols == width:
            group(0, 0)
        else:
            lax.fori_loop(0, cols // width, group, 0)

    def work(step, first=False, last=False):
        for p in range(len(pieces)):
            load(p, step).wait()
            give(p, step).wait_recv()
            if not first:
                pass_on(p, step - 1).wait_recv()
            add(p, step, first, last)
            if not last:
                pass_on(p, step).start()

    for p in range(len(pieces)):
        load(p, 0).start()
    ring.enter()
    for p in range(len(pieces)):
        give(p, 0).start()
    for step in range(1, min(ahead, chips)):
        fetch(step)
    work(0, first=True)

    def middle(step, carry):
        @pl.when(step + ahead - 1 < chips)
        def _():
            fetch(step + ahead - 1)

        work(step)
        return carry

    lax.fori_loop(1, chips - 1, middle, 0)
    work(chips - 1, last=True)

    def drain(step, carry):
        for p in range(len(pieces)):
            give(p, step).wait_send()

            @pl.when(step < chips - 1)
            def _():
                pass_on(p, step).wait_send()

        return carry

    lax.fori_loop(0, chips, drain, 0)


def ring_sum(parts, pieces, devices, collective_id, ahead=3, name="ring_sum"):
    chips, count, arrays = devices // 2, len(pieces), len(parts)
    slots = [pltpu.VMEM((chips,) + p.shape[1:], p.dtype) for p in parts]
    return pl.pallas_call(
        functools.partial(ring_sum_kernel, devices, pieces, arrays, ahead),
        out_shape=[jax.ShapeDtypeStruct(p.shape[1:], F32) for p in parts],
        in_specs=[pl.BlockSpec(memory_space=pl.ANY)] * arrays,
        out_specs=[pl.BlockSpec(memory_space=pltpu.VMEM)] * arrays,
        scratch_shapes=slots * 3
        + [pltpu.SemaphoreType.DMA((count, chips))] * 3
        + [pltpu.SemaphoreType.DMA((count, chips - 1))] * 2,
        compiler_params=pltpu.CompilerParams(
            collective_id=collective_id, has_side_effects=True, vmem_limit_bytes=64000 * 1024
        ),
        name=name,
    )(*parts)


def split_ways(parts):
    pieces, lead = [], 1
    for i, p in enumerate(parts):
        _, rows, cols = p.shape
        tiles = cols // 128
        if cols % 128 == 0 and tiles > 1:
            left = (tiles + (1 if lead > 0 else 0)) // 2 * 128
            if tiles % 2:
                lead = -lead
            pieces.append((i, 1, 0, rows, 0, left))
            pieces.append((i, -1, 0, rows, left, cols - left))
        elif rows % 32 == 0:
            pieces.append((i, 1, 0, rows // 2, 0, cols))
            pieces.append((i, -1, rows // 2, rows // 2, 0, cols))
        else:
            pieces.append((i, 1, 0, rows, 0, cols))
    return tuple(pieces)


def sum_over_ctx(parts, pieces, devices, collective_id):
    if all(p.shape[1] % 8 == 0 for p in parts):
        return ring_sum(parts, pieces, devices, collective_id)
    return [
        lax.psum_scatter(p, "ctx", scatter_dimension=0, tiled=False).astype(F32) for p in parts
    ]


def body(
    tokens,
    block_order,
    gain_attn_pre,
    gain_query,
    gain_key,
    gain_attn_post,
    gain_ff_pre,
    gain_ff_post,
    weight_query,
    weight_key,
    weight_value,
    weight_out,
    weight_gate,
    weight_up,
    weight_down,
    cotangent,
):
    sequences, rows, width = tokens.shape
    count = sequences * rows
    block = rows // 2
    devices = lax.axis_size("ctx")
    me = lax.axis_index("ctx")
    mine = lax.axis_index("wsh")

    key_value_other = swap(jnp.concatenate([weight_key, weight_value], 1))
    local_size = weight_key.shape[1]
    gains = [gain_attn_pre, gain_query, gain_key, gain_attn_post, gain_ff_pre, gain_ff_post]
    gain_sizes = [g.shape[0] for g in gains]
    gains_other = swap(jnp.concatenate(gains))
    starts = [sum(gain_sizes[:i]) for i in range(len(gains))]
    attn_pre, query_gain, key_gain, attn_post, ff_pre, ff_post = [
        join_halves(mine, g, gains_other[s : s + n]).astype(F32)
        for g, s, n in zip(gains, starts, gain_sizes)
    ]
    pair_weight = jnp.concatenate(
        [
            join_halves(mine, weight_key, key_value_other[:, :local_size]),
            join_halves(mine, weight_value, key_value_other[:, local_size:]),
        ],
        1,
    )
    weight_query = join_halves(mine, weight_query, swap(weight_query))
    weight_out = join_halves(mine, weight_out, swap(weight_out))

    head_size = query_gain.shape[0]
    heads = weight_query.shape[1] // head_size

    lane = jnp.arange(block, dtype=jnp.int32)
    late_order = 2 * devices - 1 - block_order
    early_pos = (block_order[:, None] * block + lane[None]).reshape(-1)
    late_pos = (late_order[:, None] * block + lane[None]).reshape(-1)
    key_pos = jnp.stack([early_pos, late_pos], 0)
    own_first = lax.dynamic_slice_in_dim(block_order, me, 1)[0]
    own_early = own_first * block + lane
    own_late = (2 * devices - 1 - own_first) * block + lane
    own_pos = jnp.concatenate([own_early, own_late])
    query_pos = jnp.concatenate([jnp.tile(own_early, heads), jnp.tile(own_late, heads)])[:, None]

    inputs = tokens.astype(F32)
    normed, pre_back = jax.vjp(norm_gain, inputs, attn_pre)
    normed_low = normed.astype(BF16)
    key_value = jnp.einsum("srd,de->sre", normed_low, pair_weight, preferred_element_type=F32)
    key_raw = key_value[..., :head_size]
    value_low = key_value[..., head_size:].astype(BF16)
    cosine, sine = angle_tables(own_pos, head_size)

    def key_path(key_in, key_scale):
        return rotate(norm_gain(key_in, key_scale), cosine[None], sine[None])

    def query_path(query_in, query_scale):
        return rotate(
            norm_gain(query_in, query_scale), cosine[None, :, None, :], sine[None, :, None, :]
        )

    key_rot, key_back = jax.vjp(key_path, key_raw, key_gain)
    local_pair = jnp.concatenate([key_rot.astype(BF16), value_low], -1)
    pairs = lax.all_gather(local_pair, "ctx", axis=0, tiled=False)
    query_raw = jnp.einsum(
        "srd,de->sre", normed_low, weight_query, preferred_element_type=F32
    ).reshape(sequences, rows, heads, head_size)
    query_rot, query_back = jax.vjp(query_path, query_raw, query_gain)
    query_low = query_rot.astype(BF16).reshape(sequences, rows, heads * head_size)

    mixed_low, mixed, totals = attend_forward(query_low, pairs, query_pos, key_pos, heads)
    attended = jnp.einsum("sre,ed->srd", mixed_low, weight_out, preferred_element_type=F32)
    post_attn, post_attn_back = jax.vjp(norm_gain, attended, attn_post)
    hidden_state = inputs + post_attn
    ff_input, ff_pre_back = jax.vjp(norm_gain, hidden_state, ff_pre)
    ff_own = ff_input.astype(BF16).reshape(count, width)
    ff_other = swap(ff_own)

    def ff_forward(rows_in):
        gate = dot(rows_in, weight_gate, ((1,), (0,)))
        upward = dot(rows_in, weight_up, ((1,), (0,)))
        activated, gelu_back = jax.vjp(gate_up, gate, upward)
        activated_low = activated.astype(BF16)
        return activated_low, gelu_back, dot(activated_low, weight_down, ((1,), (1,)))

    act_own, gelu_own, lowered_own = ff_forward(ff_own)
    act_other, gelu_other, lowered_other = ff_forward(ff_other)
    lowered = lowered_own + swap(lowered_other.astype(BF16)).astype(F32)
    lowered = lowered.reshape(sequences, rows, width)
    post_ff, post_ff_back = jax.vjp(norm_gain, lowered, ff_post)
    output = (hidden_state + post_ff).astype(BF16)

    grad_output = cotangent.astype(F32)
    grad_lowered, grad_ff_post = post_ff_back(grad_output)
    low_own = grad_lowered.astype(BF16).reshape(count, width)
    low_other = swap(low_own)

    def ff_backward(rows_in, gelu_back):
        grad_gate, grad_up = gelu_back(dot(rows_in, weight_down, ((1,), (0,))))
        grad_gate, grad_up = grad_gate.astype(BF16), grad_up.astype(BF16)
        back = dot(grad_gate, weight_gate, ((1,), (1,))) + dot(grad_up, weight_up, ((1,), (1,)))
        return grad_gate, grad_up, back

    gate_own, up_own, back_own = ff_backward(low_own, gelu_own)
    gate_other, up_other, back_other = ff_backward(low_other, gelu_other)
    grad_ff_input = back_own + swap(back_other.astype(BF16)).astype(F32)
    grad_ff_input = grad_ff_input.reshape(sequences, rows, width)

    def both(own, other):
        return jnp.concatenate([own, other], 0)

    def weight_grad(left, right):
        return dot(left, right, ((0,), (0,))).astype(BF16)

    ff_rows = both(ff_own, ff_other)
    part_down = weight_grad(both(low_own, low_other), both(act_own, act_other))
    part_gate = weight_grad(ff_rows, both(gate_own, gate_other))
    part_up = weight_grad(ff_rows, both(up_own, up_other))

    grad_hidden, grad_ff_pre = ff_pre_back(grad_ff_input)
    grad_hidden = grad_hidden + grad_output
    grad_attended, grad_attn_post = post_attn_back(grad_hidden)
    attended_low = grad_attended.astype(BF16)
    grad_mixed = jnp.einsum(
        "srd,ed->sre", attended_low, weight_out, preferred_element_type=F32
    ).astype(BF16)
    attended_low = attended_low.reshape(count, width)
    mixed_rows = mixed_low.reshape(count, heads * head_size)
    part_out = weight_grad(
        both(mixed_rows, swap(mixed_rows)),
        both(half_of(attended_low, mine), swap(half_of(attended_low, 1 - mine))),
    )
    grad_query, grad_pairs = attend_backward(
        query_low, pairs, grad_mixed, mixed, totals, query_pos, key_pos, heads
    )
    pair_rows = sequences * rows
    slots = grad_pairs.reshape(devices, pair_rows, 2 * head_size)
    share = pair_rows // 8
    pieces = tuple((0, 1 - 2 * (i % 2), i * share, share, 0, 2 * head_size) for i in range(8))
    own_grads = sum_over_ctx([slots], pieces, devices, 0)[0]
    own_grads = own_grads.reshape(sequences, rows, 2 * head_size)
    grad_key_raw, grad_key_gain = key_back(own_grads[..., :head_size])
    value_grad_low = own_grads[..., head_size:].astype(BF16)
    grad_query_raw, grad_query_gain = query_back(
        grad_query.reshape(sequences, rows, heads, head_size)
    )
    query_grad_low = grad_query_raw.reshape(count, heads * head_size).astype(BF16)
    key_grad_low = grad_key_raw.astype(BF16).reshape(count, head_size)
    value_grad_low = value_grad_low.reshape(count, head_size)
    grad_normed = (
        dot(query_grad_low, weight_query, ((1,), (1,)))
        + dot(jnp.concatenate([key_grad_low, value_grad_low], -1), pair_weight, ((1,), (1,)))
    ).reshape(sequences, rows, width)
    grad_inputs, grad_attn_pre = pre_back(grad_normed)
    grad_tokens = grad_inputs + grad_hidden

    def columns(which):
        return jnp.concatenate(
            [half_of(v, which) for v in (query_grad_low, key_grad_low, value_grad_low)], -1
        )

    normed_rows = normed_low.reshape(count, width)
    part_qkv = weight_grad(
        both(normed_rows, swap(normed_rows)), both(columns(mine), swap(columns(1 - mine)))
    )

    gain_grads = [
        grad_attn_pre,
        grad_query_gain,
        grad_key_gain,
        grad_attn_post,
        grad_ff_pre,
        grad_ff_post,
    ]
    packed = jnp.concatenate([g.reshape(devices, 2, -1) for g in gain_grads], -1)
    keep = jnp.where(mine == 0, packed[:, 0], packed[:, 1])
    send = jnp.where(mine == 0, packed[:, 1], packed[:, 0])
    packed = keep + swap(send)
    gain_size = packed.shape[-1]
    packed = jnp.pad(packed, ((0, 0), (0, 1024 - gain_size))).reshape(devices, 8, 128)
    parts = [
        p.reshape(devices, p.shape[0] // devices, p.shape[1])
        for p in (part_down, part_gate, part_up, part_qkv, part_out)
    ] + [packed]
    grad_down_w, grad_gate_w, grad_up_w, grad_qkv, grad_out_w, packed = sum_over_ctx(
        parts, split_ways(parts), devices, 1
    )
    packed = packed.reshape(-1)
    query_cols = query_grad_low.shape[1] // 2
    grad_query_w = grad_qkv[:, :query_cols]
    grad_key_w = grad_qkv[:, query_cols : query_cols + local_size]
    grad_value_w = grad_qkv[:, query_cols + local_size :]
    outs, first = [], 0
    for g in gain_grads:
        size = g.shape[0] // (2 * devices)
        outs.append(packed[first : first + size])
        first += size
    return (
        output,
        grad_tokens,
        *outs,
        grad_query_w,
        grad_key_w,
        grad_value_w,
        grad_out_w,
        grad_gate_w,
        grad_up_w,
        grad_down_w,
    )


def solution(mesh):
    rows, vector, matrix = P("wsh", "ctx", None), P("wsh"), P(None, "wsh")
    in_specs = (rows, P()) + (vector,) * 6 + (matrix,) * 7 + (rows,)
    out_specs = (rows, rows) + (P(("ctx", "wsh")),) * 6 + (P("ctx", "wsh"),) * 7
    return jax.shard_map(body, mesh=mesh, in_specs=in_specs, out_specs=out_specs, check_vma=False)
```

```python
import functools
import math

import jax
import jax.numpy as jnp
from jax import lax
from jax.experimental import pallas as pl
from jax.experimental.pallas import tpu as pltpu
from jax.sharding import PartitionSpec as P

EPS = 1e-06
ROPE_BASE = 1000000.0
SCORE_SCALE = 0.0625
F32 = jnp.float32
BF16 = jnp.bfloat16
MESH = pl.DeviceIdType.MESH


def norm_gain(vector, gain):
    return vector * lax.rsqrt(jnp.mean(vector * vector, -1, keepdims=True) + EPS) * gain


def rotate(vector, cosine, sine):
    middle = vector.shape[-1] // 2
    first = vector[..., :middle]
    second = vector[..., middle:]
    return jnp.concatenate([first * cosine - second * sine, second * cosine + first * sine], -1)


def angle_tables(positions, head_size):
    middle = head_size // 2
    inverse = jnp.exp(
        jnp.arange(middle, dtype=F32) * (-2.0 * math.log(ROPE_BASE) / head_size)
    )
    theta = positions.astype(F32)[:, None] * inverse[None, :]
    return (jnp.cos(theta), jnp.sin(theta))


def gate_up(gate, upward):
    return jax.nn.gelu(gate, approximate=True) * upward


def swap(value):
    return lax.ppermute(value, "wsh", [(0, 1), (1, 0)])


def join_halves(mine, local, other):
    return jnp.where(
        mine == 0,
        jnp.concatenate([local, other], -1),
        jnp.concatenate([other, local], -1),
    )


def half_of(value, which):
    middle = value.shape[-1] // 2
    return jnp.where(which == 0, value[..., :middle], value[..., middle:])


def dot(left, right, dims):
    return lax.dot_general(left, right, (dims, ((), ())), preferred_element_type=F32)


def stack_heads(ref, half, block, heads, size):
    rows = slice(half * block, (half + 1) * block)
    return jnp.concatenate([ref[0, rows, h * size : (h + 1) * size] for h in range(heads)], 0)


def attend_forward_kernel(heads, chunk, q_ref, kv_ref, qpos_ref, kpos_ref, o_ref, mix_ref, tot_ref):
    shards, _, rows, pair = kv_ref.shape
    block, size = rows // 2, pair // 2
    queries = [stack_heads(q_ref, half, block, heads, size) for half in range(2)]
    stacked = heads * block
    sums = [jnp.zeros((stacked, size), F32) for _ in range(2)]
    totals = [jnp.zeros((stacked, 1), F32) for _ in range(2)]
    for first in range(0, shards, chunk):
        span = slice(first * block, (first + chunk) * block)
        for key_half in range(2):
            part = kv_ref[first : first + chunk, 0, key_half * block : (key_half + 1) * block, :]
            part = part.reshape(chunk * block, pair)
            keys, values = part[:, :size], part[:, size:]
            for half in range(key_half, 2):
                weights = jnp.exp(dot(queries[half], keys, ((1,), (1,))) * SCORE_SCALE)
                if half == key_half:
                    allowed = (
                        kpos_ref[key_half : key_half + 1, span]
                        <= qpos_ref[half * stacked : (half + 1) * stacked, :]
                    )
                    weights = jnp.where(allowed, weights, 0.0)
                low = weights.astype(BF16)
                totals[half] += jnp.sum(low.astype(F32), -1, keepdims=True)
                sums[half] += dot(low, values, ((1,), (0,)))
    for half in range(2):
        mixed = sums[half] / totals[half]
        mix_ref[0, half * stacked : (half + 1) * stacked, :] = mixed
        tot_ref[0, half * stacked : (half + 1) * stacked, :] = jnp.broadcast_to(
            totals[half], (stacked, tot_ref.shape[2])
        )
        for h in range(heads):
            o_ref[0, half * block : (half + 1) * block, h * size : (h + 1) * size] = mixed[
                h * block : (h + 1) * block
            ].astype(BF16)


def attend_backward_kernel(
    heads, chunk, q_ref, kv_ref, g_ref, mix_ref, tot_ref, qpos_ref, kpos_ref, dq_ref, dkv_ref
):
    shards, _, rows, pair = kv_ref.shape
    block, size = rows // 2, pair // 2
    stacked = heads * block
    queries, scaled, correction = [], [], []
    for half in range(2):
        queries.append(stack_heads(q_ref, half, block, heads, size))
        grad = stack_heads(g_ref, half, block, heads, size).astype(F32)
        span = slice(half * stacked, (half + 1) * stacked)
        total = tot_ref[0, span, :1]
        delta = jnp.sum(grad * mix_ref[0, span, :], -1, keepdims=True)
        scaled.append((grad / total).astype(BF16))
        correction.append(delta / total)
    grad_query = [jnp.zeros((stacked, size), F32) for _ in range(2)]
    for first in range(0, shards, chunk):
        span = slice(first * block, (first + chunk) * block)
        for key_half in range(2):
            part = kv_ref[first : first + chunk, 0, key_half * block : (key_half + 1) * block, :]
            part = part.reshape(chunk * block, pair)
            keys, values = part[:, :size], part[:, size:]
            grad_keys = jnp.zeros((chunk * block, size), F32)
            grad_values = jnp.zeros((chunk * block, size), F32)
            for half in range(key_half, 2):
                weights = jnp.exp(dot(queries[half], keys, ((1,), (1,))) * SCORE_SCALE)
                if half == key_half:
                    allowed = (
                        kpos_ref[key_half : key_half + 1, span]
                        <= qpos_ref[half * stacked : (half + 1) * stacked, :]
                    )
                    weights = jnp.where(allowed, weights, 0.0)
                low = weights.astype(BF16)
                grad_weights = dot(scaled[half], values, ((1,), (1,)))
                grad_scores = (weights * (grad_weights - correction[half])).astype(BF16)
                grad_query[half] += dot(grad_scores, keys, ((1,), (0,)))
                grad_keys += dot(grad_scores, queries[half], ((0,), (0,)))
                grad_values += dot(low, scaled[half], ((0,), (0,)))
            both = jnp.concatenate([grad_keys * SCORE_SCALE, grad_values], -1).astype(BF16)
            dkv_ref[first : first + chunk, 0, key_half * block : (key_half + 1) * block, :] = (
                both.reshape(chunk, block, pair)
            )
    for half in range(2):
        for h in range(heads):
            dq_ref[0, half * block : (half + 1) * block, h * size : (h + 1) * size] = (
                grad_query[half][h * block : (h + 1) * block] * SCORE_SCALE
            )


def whole(shape):
    return pl.BlockSpec(shape, lambda s: (0,) * len(shape))


def attend_forward(query_low, pairs, query_pos, key_pos, heads):
    sequences, rows, width = query_low.shape
    shards, _, _, pair = pairs.shape
    stacked = query_pos.shape[0]
    row = pl.BlockSpec((1, rows, width), lambda s: (s, 0, 0))
    stack = lambda last: pl.BlockSpec((1, stacked, last), lambda s: (s, 0, 0))
    return pl.pallas_call(
        functools.partial(attend_forward_kernel, heads, min(shards, 16)),
        grid=(sequences,),
        in_specs=[
            row,
            pl.BlockSpec((shards, 1, rows, pair), lambda s: (0, s, 0, 0)),
            whole(query_pos.shape),
            whole(key_pos.shape),
        ],
        out_specs=[row, stack(pair // 2), stack(128)],
        out_shape=[
            jax.ShapeDtypeStruct((sequences, rows, width), BF16),
            jax.ShapeDtypeStruct((sequences, stacked, pair // 2), F32),
            jax.ShapeDtypeStruct((sequences, stacked, 128), F32),
        ],
        name="attend_forward",
    )(query_low, pairs, query_pos, key_pos)


def attend_backward(query_low, pairs, grad_mixed, mixed, totals, query_pos, key_pos, heads):
    sequences, rows, width = query_low.shape
    shards, _, _, pair = pairs.shape
    stacked = query_pos.shape[0]
    row = pl.BlockSpec((1, rows, width), lambda s: (s, 0, 0))
    stack = lambda last: pl.BlockSpec((1, stacked, last), lambda s: (s, 0, 0))
    pairs_spec = pl.BlockSpec((shards, 1, rows, pair), lambda s: (0, s, 0, 0))
    return pl.pallas_call(
        functools.partial(attend_backward_kernel, heads, min(shards, 16)),
        grid=(sequences,),
        in_specs=[
            row,
            pairs_spec,
            row,
            stack(pair // 2),
            stack(128),
            whole(query_pos.shape),
            whole(key_pos.shape),
        ],
        out_specs=[row, pairs_spec],
        out_shape=[
            jax.ShapeDtypeStruct((sequences, rows, width), F32),
            jax.ShapeDtypeStruct(pairs.shape, BF16),
        ],
        name="attend_backward",
    )(query_low, pairs, grad_mixed, mixed, totals, query_pos, key_pos)


class Ring:
    def __init__(self, devices):
        self.chips = devices // 2
        me = lax.axis_index("ctx")
        self.core = me % 2
        chip = me // 2
        across = chip % 2
        deep = chip // 2
        self.place = deep + across * (self.chips - 1 - 2 * deep)
        self.partner = me + 1 - 2 * self.core
        self.right = self.device((self.place + 1) % self.chips, self.core)
        self.left = self.device((self.place + self.chips - 1) % self.chips, self.core)

    def device(self, place, core):
        side = place // (self.chips // 2)
        return 2 * (2 * (place + side * (self.chips - 1 - 2 * place)) + side) + core

    def enter(self, across=False):
        barrier = pltpu.get_barrier_semaphore()
        targets = [{"ctx": other} for other in (self.left, self.right, self.partner)]
        if across:
            targets.append({"wsh": 1 - lax.axis_index("wsh")})
        for target in targets:
            pl.semaphore_signal(barrier, inc=1, device_id=target, device_id_type=MESH)
        pl.semaphore_wait(barrier, len(targets))


def ring_sum_kernel(devices, pieces, arrays, ahead, *refs):
    parts, outs = refs[:arrays], refs[arrays : 2 * arrays]
    own, other, flow = (refs[(2 + i) * arrays : (3 + i) * arrays] for i in range(3))
    own_sem, put_sem, got_sem, send_sem, recv_sem = refs[5 * arrays :]
    ring = Ring(devices)
    chips = ring.chips

    def region(p):
        array, _, first, rows, start, cols = pieces[p]
        return array, pl.ds(first, rows), pl.ds(start, cols)

    def chunk(p, step):
        way = pieces[p][1]
        return (ring.place + 2 * chips + way * (-1 - step)) % chips

    def load(p, step):
        array, rows, cols = region(p)
        source = ring.device(chunk(p, step), ring.core)
        return pltpu.make_async_copy(
            parts[array].at[source, rows, cols],
            own[array].at[step, rows, cols],
            own_sem.at[p, step],
        )

    def give(p, step):
        array, rows, cols = region(p)
        source = ring.device(chunk(p, step), 1 - ring.core)
        return pltpu.make_async_remote_copy(
            src_ref=parts[array].at[source, rows, cols],
            dst_ref=other[array].at[step, rows, cols],
            send_sem=put_sem.at[p, step],
            recv_sem=got_sem.at[p, step],
            device_id={"ctx": ring.partner},
            device_id_type=MESH,
        )

    def pass_on(p, step):
        array, rows, cols = region(p)
        way = pieces[p][1]
        return pltpu.make_async_remote_copy(
            src_ref=flow[array].at[step, rows, cols],
            dst_ref=flow[array].at[step + 1, rows, cols],
            send_sem=send_sem.at[p, step],
            recv_sem=recv_sem.at[p, step],
            device_id={"ctx": ring.right if way > 0 else ring.left},
            device_id_type=MESH,
        )

    def fetch(step):
        for p in range(len(pieces)):
            load(p, step).start()
            give(p, step).start()

    def add(p, step, first, last):
        array, _, row, rows, start, cols = pieces[p]
        width = 128 if cols % 128 == 0 else cols
        while width < 512 and cols % (2 * width) == 0:
            width *= 2
        rows = pl.ds(row, rows)

        def group(i, carry):
            at = start + i * width
            if cols > width:
                at = pl.multiple_of(at, 128)
            where = pl.ds(at, width)
            total = own[array][step, rows, where].astype(F32) + other[array][
                step, rows, where
            ].astype(F32)
            if not first:
                total += flow[array][step, rows, where].astype(F32)
            if last:
                outs[array][rows, where] = total.astype(outs[array].dtype)
            else:
                flow[array][step, rows, where] = total.astype(flow[array].dtype)
            return carry

        if cols == width:
            group(0, 0)
        else:
            lax.fori_loop(0, cols // width, group, 0)

    def work(step, first=False, last=False):
        for p in range(len(pieces)):
            load(p, step).wait()
            give(p, step).wait_recv()
            if not first:
                pass_on(p, step - 1).wait_recv()
            add(p, step, first, last)
            if not last:
                pass_on(p, step).start()

    for p in range(len(pieces)):
        load(p, 0).start()
    ring.enter()
    for p in range(len(pieces)):
        give(p, 0).start()
    for step in range(1, min(ahead, chips)):
        fetch(step)
    work(0, first=True)

    def middle(step, carry):
        @pl.when(step + ahead - 1 < chips)
        def _():
            fetch(step + ahead - 1)

        work(step)
        return carry

    lax.fori_loop(1, chips - 1, middle, 0)
    work(chips - 1, last=True)

    def drain(step, carry):
        for p in range(len(pieces)):
            give(p, step).wait_send()

            @pl.when(step < chips - 1)
            def _():
                pass_on(p, step).wait_send()

        return carry

    lax.fori_loop(0, chips, drain, 0)


def ring_sum(parts, pieces, devices, collective_id, ahead=3, name="ring_sum"):
    chips, count, arrays = devices // 2, len(pieces), len(parts)
    slots = [pltpu.VMEM((chips,) + p.shape[1:], p.dtype) for p in parts]
    return pl.pallas_call(
        functools.partial(ring_sum_kernel, devices, pieces, arrays, ahead),
        out_shape=[jax.ShapeDtypeStruct(p.shape[1:], F32) for p in parts],
        in_specs=[pl.BlockSpec(memory_space=pl.ANY)] * arrays,
        out_specs=[pl.BlockSpec(memory_space=pltpu.VMEM)] * arrays,
        scratch_shapes=slots * 3
        + [pltpu.SemaphoreType.DMA((count, chips))] * 3
        + [pltpu.SemaphoreType.DMA((count, chips - 1))] * 2,
        compiler_params=pltpu.CompilerParams(
            collective_id=collective_id, has_side_effects=True, vmem_limit_bytes=64000 * 1024
        ),
        name=name,
    )(*parts)


def split_ways(parts):
    pieces, lead = [], 1
    for i, p in enumerate(parts):
        _, rows, cols = p.shape
        tiles = cols // 128
        if cols % 128 == 0 and tiles > 1:
            left = (tiles + (1 if lead > 0 else 0)) // 2 * 128
            if tiles % 2:
                lead = -lead
            pieces.append((i, 1, 0, rows, 0, left))
            pieces.append((i, -1, 0, rows, left, cols - left))
        elif rows % 32 == 0:
            pieces.append((i, 1, 0, rows // 2, 0, cols))
            pieces.append((i, -1, rows // 2, rows // 2, 0, cols))
        else:
            pieces.append((i, 1, 0, rows, 0, cols))
    return tuple(pieces)


def sum_over_ctx(parts, pieces, devices, collective_id):
    if all(p.shape[1] % 8 == 0 for p in parts):
        return ring_sum(parts, pieces, devices, collective_id)
    return [
        lax.psum_scatter(p, "ctx", scatter_dimension=0, tiled=False).astype(F32) for p in parts
    ]


def front_kernel(
    devices,
    tokens_ref,
    gains_ref,
    cos_ref,
    sin_ref,
    key_weight,
    value_weight,
    query_weight,
    out_weight,
    pairs_ref,
    normed_ref,
    key_ref,
    all_gains_ref,
    key_other,
    value_other,
    query_other,
    out_other,
    gains_other,
    cross_send,
    cross_recv,
    side_send,
    side_recv,
    flow_send,
    flow_recv,
    twin_send,
    twin_recv,
):
    ring = Ring(devices)
    chips, far = ring.chips, ring.chips // 2
    me = lax.axis_index("ctx")
    mine = lax.axis_index("wsh")
    sequences, rows, width = tokens_ref.shape
    count = sequences * rows
    weights = (
        (key_weight, key_other),
        (value_weight, value_other),
        (query_weight, query_other),
        (out_weight, out_other),
    )

    def cross(i):
        if i == len(weights):
            source, target = gains_ref, gains_other
        else:
            local, other = weights[i]
            half = local.shape[0] // 2
            part = pl.ds(pl.multiple_of(ring.core * half, 16), half)
            source, target = local.at[part], other.at[part]
        return pltpu.make_async_remote_copy(
            src_ref=source,
            dst_ref=target,
            send_sem=cross_send.at[i],
            recv_sem=cross_recv.at[i],
            device_id={"wsh": 1 - mine},
            device_id_type=MESH,
        )

    def side(i):
        other = weights[i][1]
        half = other.shape[0] // 2
        part = pl.ds(pl.multiple_of(ring.core * half, 16), half)
        return pltpu.make_async_remote_copy(
            src_ref=other.at[part],
            dst_ref=other.at[part],
            send_sem=side_send.at[i],
            recv_sem=side_recv.at[i],
            device_id={"ctx": ring.partner},
            device_id_type=MESH,
        )

    def flow(way, seq, hop):
        stream = (1 if way < 0 else 0) * sequences + seq
        place = (ring.place + chips - way * hop) % chips
        block = pairs_ref.at[ring.device(place, ring.core), seq]
        return pltpu.make_async_remote_copy(
            src_ref=block,
            dst_ref=block,
            send_sem=flow_send.at[stream, hop],
            recv_sem=flow_recv.at[stream, hop],
            device_id={"ctx": ring.right if way > 0 else ring.left},
            device_id_type=MESH,
        )

    def twin(way, seq, hop):
        stream = (1 if way < 0 else 0) * sequences + seq
        place = (ring.place + chips - way * hop) % chips
        block = pairs_ref.at[ring.device(place, ring.core), seq]
        return pltpu.make_async_remote_copy(
            src_ref=block,
            dst_ref=block,
            send_sem=twin_send.at[stream, hop],
            recv_sem=twin_recv.at[stream, hop],
            device_id={"ctx": ring.partner},
            device_id_type=MESH,
        )

    def hops(way, seq):
        return far if (seq % 2 == 0) == (way > 0) else far - 1

    ring.enter(across=True)
    order = (len(weights), 0, 1, 2, 3)
    for i in order:
        cross(i).start()
    inputs = tokens_ref[...].reshape(count, width).astype(F32)
    scale = lax.rsqrt(jnp.mean(inputs * inputs, -1, keepdims=True) + EPS)
    cross(len(weights)).wait_recv()
    all_gains_ref[...] = gains_ref[...] + gains_other[...]
    normed_ref[...] = (inputs * scale * all_gains_ref[0:1, :]).astype(BF16)
    for i in (0, 1):
        cross(i).wait_recv()
        side(i).start()
    key_here = dot(normed_ref[...], key_weight[...], ((1,), (0,)))
    value_here = dot(normed_ref[...], value_weight[...], ((1,), (0,)))
    for i in (0, 1):
        side(i).wait_recv()
    key_there = dot(normed_ref[...], key_other[...], ((1,), (0,)))
    value_there = dot(normed_ref[...], value_other[...], ((1,), (0,)))
    lower = mine == 0
    first = jnp.where(lower, key_here, key_there)
    second = jnp.where(lower, key_there, key_here)
    middle = first.shape[1]
    key_ref[:, :middle] = first
    key_ref[:, middle:] = second
    power = jnp.sum(first * first, -1, keepdims=True) + jnp.sum(second * second, -1, keepdims=True)
    scale = lax.rsqrt(power / (2 * middle) + EPS)
    gain = all_gains_ref[4:5, 2 * middle : 4 * middle]
    first = first * scale * gain[:, :middle]
    second = second * scale * gain[:, middle:]
    cosine, sine = cos_ref[...], sin_ref[...]
    value_first = jnp.where(lower, value_here, value_there).astype(BF16)
    value_second = jnp.where(lower, value_there, value_here).astype(BF16)
    for seq in range(sequences):
        span = slice(seq * rows, (seq + 1) * rows)
        head, tail = first[span], second[span]
        pairs_ref[me, seq, :, 0 * middle : 1 * middle] = (head * cosine - tail * sine).astype(BF16)
        pairs_ref[me, seq, :, 1 * middle : 2 * middle] = (tail * cosine + head * sine).astype(BF16)
        pairs_ref[me, seq, :, 2 * middle : 3 * middle] = value_first[span]
        pairs_ref[me, seq, :, 3 * middle : 4 * middle] = value_second[span]
    streams = [(way, seq) for seq in range(sequences) for way in (1, -1)]
    for hop in range(far + 1):
        for way, seq in streams:
            if hop > hops(way, seq):
                continue
            if hop > 0:
                flow(way, seq, hop - 1).wait_recv()
            if hop < hops(way, seq):
                flow(way, seq, hop).start()
            if hop > 0 or way > 0:
                twin(way, seq, hop).start()
    for i in (2, 3):
        cross(i).wait_recv()
        side(i).start()
    for hop in range(far + 1):
        for way, seq in streams:
            if hop > hops(way, seq):
                continue
            if hop > 0 or way > 0:
                twin(way, seq, hop).wait()
            if hop < hops(way, seq):
                flow(way, seq, hop).wait_send()
    for i in order:
        cross(i).wait_send()
    for i in (2, 3):
        side(i).wait()
    for i in (0, 1):
        side(i).wait_send()


def front(tokens, gains, cosine, sine, weights, devices, collective_id):
    sequences, rows, width = tokens.shape
    size = 2 * cosine.shape[1]
    far = devices // 4
    here, there = pl.BlockSpec(memory_space=pltpu.VMEM), pl.BlockSpec(memory_space=pl.ANY)
    streams = pltpu.SemaphoreType.DMA((2 * sequences, far + 1))
    like = lambda a: jax.ShapeDtypeStruct(a.shape, a.dtype)
    return pl.pallas_call(
        functools.partial(front_kernel, devices),
        in_specs=[here] * 6 + [there] * 2,
        out_specs=[here] * 6 + [there] * 2,
        out_shape=[
            jax.ShapeDtypeStruct((devices, sequences, rows, 2 * size), BF16),
            jax.ShapeDtypeStruct((sequences * rows, width), BF16),
            jax.ShapeDtypeStruct((sequences * rows, size), F32),
            like(gains),
        ]
        + [like(w) for w in weights],
        scratch_shapes=[pltpu.VMEM(gains.shape, gains.dtype)]
        + [pltpu.SemaphoreType.DMA((5,))] * 2
        + [pltpu.SemaphoreType.DMA((4,))] * 2
        + [streams] * 4,
        compiler_params=pltpu.CompilerParams(
            collective_id=collective_id, has_side_effects=True, vmem_limit_bytes=60000 * 1024
        ),
        name="front",
    )(tokens, gains, cosine, sine, *weights)


def body(
    tokens,
    block_order,
    gain_attn_pre,
    gain_query,
    gain_key,
    gain_attn_post,
    gain_ff_pre,
    gain_ff_post,
    weight_query,
    weight_key,
    weight_value,
    weight_out,
    weight_gate,
    weight_up,
    weight_down,
    cotangent,
):
    sequences, rows, width = tokens.shape
    count = sequences * rows
    block = rows // 2
    devices = lax.axis_size("ctx")
    me = lax.axis_index("ctx")
    mine = lax.axis_index("wsh")

    head_size = 2 * gain_key.shape[0]
    heads = 2 * weight_query.shape[1] // head_size

    lane = jnp.arange(block, dtype=jnp.int32)
    late_order = 2 * devices - 1 - block_order
    early_pos = (block_order[:, None] * block + lane[None]).reshape(-1)
    late_pos = (late_order[:, None] * block + lane[None]).reshape(-1)
    key_pos = jnp.stack([early_pos, late_pos], 0)
    own_first = lax.dynamic_slice_in_dim(block_order, me, 1)[0]
    own_early = own_first * block + lane
    own_late = (2 * devices - 1 - own_first) * block + lane
    own_pos = jnp.concatenate([own_early, own_late])
    query_pos = jnp.concatenate([jnp.tile(own_early, heads), jnp.tile(own_late, heads)])[:, None]

    cosine, sine = angle_tables(own_pos, head_size)

    def placed(gain):
        zeros = jnp.zeros_like(gain)
        return jnp.where(
            mine == 0, jnp.concatenate([gain, zeros]), jnp.concatenate([zeros, gain])
        ).astype(F32)

    own_gains = [placed(g) for g in (gain_attn_pre, gain_attn_post, gain_ff_pre, gain_ff_post)]
    small = [placed(gain_query), placed(gain_key)]
    own_gains.append(jnp.concatenate(small + [jnp.zeros((width - 2 * head_size,), F32)]))
    own_gains = jnp.stack(own_gains + [jnp.zeros((width,), F32)] * 3)
    pairs, normed_low, key_raw, all_gains, key_other, value_other, query_other, out_other = front(
        tokens,
        own_gains,
        cosine,
        sine,
        (weight_key, weight_value, weight_query, weight_out),
        devices,
        2,
    )
    attn_pre, attn_post, ff_pre, ff_post = (all_gains[i] for i in range(4))
    query_gain = all_gains[4, :head_size]
    key_gain = all_gains[4, head_size : 2 * head_size]
    normed_low = normed_low.reshape(sequences, rows, width)
    key_raw = key_raw.reshape(sequences, rows, head_size)
    pair_weight = jnp.concatenate(
        [join_halves(mine, weight_key, key_other), join_halves(mine, weight_value, value_other)], 1
    )
    weight_query = join_halves(mine, weight_query, query_other)
    weight_out = join_halves(mine, weight_out, out_other)
    local_size = weight_key.shape[1]
    inputs = tokens.astype(F32)

    def key_path(key_in, key_scale):
        return rotate(norm_gain(key_in, key_scale), cosine[None], sine[None])

    def query_path(query_in, query_scale):
        return rotate(
            norm_gain(query_in, query_scale), cosine[None, :, None, :], sine[None, :, None, :]
        )

    query_raw = jnp.einsum(
        "srd,de->sre", normed_low, weight_query, preferred_element_type=F32
    ).reshape(sequences, rows, heads, head_size)
    query_rot, query_back = jax.vjp(query_path, query_raw, query_gain)
    query_low = query_rot.astype(BF16).reshape(sequences, rows, heads * head_size)

    mixed_low, mixed, totals = attend_forward(query_low, pairs, query_pos, key_pos, heads)
    attended = jnp.einsum("sre,ed->srd", mixed_low, weight_out, preferred_element_type=F32)
    post_attn, post_attn_back = jax.vjp(norm_gain, attended, attn_post)
    hidden_state = inputs + post_attn
    ff_input, ff_pre_back = jax.vjp(norm_gain, hidden_state, ff_pre)
    ff_own = ff_input.astype(BF16).reshape(count, width)
    ff_other = swap(ff_own)

    def ff_forward(rows_in):
        gate = dot(rows_in, weight_gate, ((1,), (0,)))
        upward = dot(rows_in, weight_up, ((1,), (0,)))
        activated, gelu_back = jax.vjp(gate_up, gate, upward)
        activated_low = activated.astype(BF16)
        return activated_low, gelu_back, dot(activated_low, weight_down, ((1,), (1,)))

    act_own, gelu_own, lowered_own = ff_forward(ff_own)
    act_other, gelu_other, lowered_other = ff_forward(ff_other)
    lowered = lowered_own + swap(lowered_other.astype(BF16)).astype(F32)
    lowered = lowered.reshape(sequences, rows, width)
    post_ff, post_ff_back = jax.vjp(norm_gain, lowered, ff_post)
    output = (hidden_state + post_ff).astype(BF16)

    grad_output = cotangent.astype(F32)
    grad_lowered, grad_ff_post = post_ff_back(grad_output)
    low_own = grad_lowered.astype(BF16).reshape(count, width)
    low_other = swap(low_own)

    def ff_backward(rows_in, gelu_back):
        grad_gate, grad_up = gelu_back(dot(rows_in, weight_down, ((1,), (0,))))
        grad_gate, grad_up = grad_gate.astype(BF16), grad_up.astype(BF16)
        back = dot(grad_gate, weight_gate, ((1,), (1,))) + dot(grad_up, weight_up, ((1,), (1,)))
        return grad_gate, grad_up, back

    gate_own, up_own, back_own = ff_backward(low_own, gelu_own)
    gate_other, up_other, back_other = ff_backward(low_other, gelu_other)
    grad_ff_input = back_own + swap(back_other.astype(BF16)).astype(F32)
    grad_ff_input = grad_ff_input.reshape(sequences, rows, width)

    def both(own, other):
        return jnp.concatenate([own, other], 0)

    def weight_grad(left, right):
        return dot(left, right, ((0,), (0,))).astype(BF16)

    ff_rows = both(ff_own, ff_other)
    part_down = weight_grad(both(low_own, low_other), both(act_own, act_other))
    part_gate = weight_grad(ff_rows, both(gate_own, gate_other))
    part_up = weight_grad(ff_rows, both(up_own, up_other))

    grad_hidden, grad_ff_pre = ff_pre_back(grad_ff_input)
    grad_hidden = grad_hidden + grad_output
    grad_attended, grad_attn_post = post_attn_back(grad_hidden)
    attended_low = grad_attended.astype(BF16)
    grad_mixed = jnp.einsum(
        "srd,ed->sre", attended_low, weight_out, preferred_element_type=F32
    ).astype(BF16)
    attended_low = attended_low.reshape(count, width)
    mixed_rows = mixed_low.reshape(count, heads * head_size)
    part_out = weight_grad(
        both(mixed_rows, swap(mixed_rows)),
        both(half_of(attended_low, mine), swap(half_of(attended_low, 1 - mine))),
    )
    grad_query, grad_pairs = attend_backward(
        query_low, pairs, grad_mixed, mixed, totals, query_pos, key_pos, heads
    )
    pair_rows = sequences * rows
    slots = grad_pairs.reshape(devices, pair_rows, 2 * head_size)
    share = pair_rows // 8
    pieces = tuple((0, 1 - 2 * (i % 2), i * share, share, 0, 2 * head_size) for i in range(8))
    own_grads = sum_over_ctx([slots], pieces, devices, 0)[0]
    own_grads = own_grads.reshape(sequences, rows, 2 * head_size)
    grad_key_raw, grad_key_gain = jax.vjp(key_path, key_raw, key_gain)[1](own_grads[..., :head_size])
    value_grad_low = own_grads[..., head_size:].astype(BF16)
    grad_query_raw, grad_query_gain = query_back(
        grad_query.reshape(sequences, rows, heads, head_size)
    )
    query_grad_low = grad_query_raw.reshape(count, heads * head_size).astype(BF16)
    key_grad_low = grad_key_raw.astype(BF16).reshape(count, head_size)
    value_grad_low = value_grad_low.reshape(count, head_size)
    grad_normed = (
        dot(query_grad_low, weight_query, ((1,), (1,)))
        + dot(jnp.concatenate([key_grad_low, value_grad_low], -1), pair_weight, ((1,), (1,)))
    ).reshape(sequences, rows, width)
    grad_inputs, grad_attn_pre = jax.vjp(norm_gain, inputs, attn_pre)[1](grad_normed)
    grad_tokens = grad_inputs + grad_hidden

    def columns(which):
        return jnp.concatenate(
            [half_of(v, which) for v in (query_grad_low, key_grad_low, value_grad_low)], -1
        )

    normed_rows = normed_low.reshape(count, width)
    part_qkv = weight_grad(
        both(normed_rows, swap(normed_rows)), both(columns(mine), swap(columns(1 - mine)))
    )

    gain_grads = [
        grad_attn_pre,
        grad_query_gain,
        grad_key_gain,
        grad_attn_post,
        grad_ff_pre,
        grad_ff_post,
    ]
    packed = jnp.concatenate([g.reshape(devices, 2, -1) for g in gain_grads], -1)
    keep = jnp.where(mine == 0, packed[:, 0], packed[:, 1])
    send = jnp.where(mine == 0, packed[:, 1], packed[:, 0])
    packed = keep + swap(send)
    gain_size = packed.shape[-1]
    packed = jnp.pad(packed, ((0, 0), (0, 1024 - gain_size))).reshape(devices, 8, 128)
    parts = [
        p.reshape(devices, p.shape[0] // devices, p.shape[1])
        for p in (part_down, part_gate, part_up, part_qkv, part_out)
    ] + [packed]
    grad_down_w, grad_gate_w, grad_up_w, grad_qkv, grad_out_w, packed = sum_over_ctx(
        parts, split_ways(parts), devices, 1
    )
    packed = packed.reshape(-1)
    query_cols = query_grad_low.shape[1] // 2
    grad_query_w = grad_qkv[:, :query_cols]
    grad_key_w = grad_qkv[:, query_cols : query_cols + local_size]
    grad_value_w = grad_qkv[:, query_cols + local_size :]
    outs, first = [], 0
    for g in gain_grads:
        size = g.shape[0] // (2 * devices)
        outs.append(packed[first : first + size])
        first += size
    return (
        output,
        grad_tokens,
        *outs,
        grad_query_w,
        grad_key_w,
        grad_value_w,
        grad_out_w,
        grad_gate_w,
        grad_up_w,
        grad_down_w,
    )


def solution(mesh):
    rows, vector, matrix = P("wsh", "ctx", None), P("wsh"), P(None, "wsh")
    in_specs = (rows, P()) + (vector,) * 6 + (matrix,) * 7 + (rows,)
    out_specs = (rows, rows) + (P(("ctx", "wsh")),) * 6 + (P("ctx", "wsh"),) * 7
    return jax.shard_map(body, mesh=mesh, in_specs=in_specs, out_specs=out_specs, check_vma=False)
```

```python
import functools
import math

import jax
import jax.numpy as jnp
from jax import lax
from jax.experimental import pallas as pl
from jax.experimental.pallas import tpu as pltpu
from jax.sharding import PartitionSpec as P

EPS = 1e-06
ROPE_BASE = 1000000.0
SCORE_SCALE = 0.0625
F32 = jnp.float32
BF16 = jnp.bfloat16
MESH = pl.DeviceIdType.MESH


def norm_gain(vector, gain):
    return vector * lax.rsqrt(jnp.mean(vector * vector, -1, keepdims=True) + EPS) * gain


def rotate(vector, cosine, sine):
    middle = vector.shape[-1] // 2
    first = vector[..., :middle]
    second = vector[..., middle:]
    return jnp.concatenate([first * cosine - second * sine, second * cosine + first * sine], -1)


def angle_tables(positions, head_size):
    middle = head_size // 2
    inverse = jnp.exp(
        jnp.arange(middle, dtype=F32) * (-2.0 * math.log(ROPE_BASE) / head_size)
    )
    theta = positions.astype(F32)[:, None] * inverse[None, :]
    return (jnp.cos(theta), jnp.sin(theta))


def gate_up(gate, upward):
    return jax.nn.gelu(gate, approximate=True) * upward


def swap(value):
    return lax.ppermute(value, "wsh", [(0, 1), (1, 0)])


def join_halves(mine, local, other):
    return jnp.where(
        mine == 0,
        jnp.concatenate([local, other], -1),
        jnp.concatenate([other, local], -1),
    )


def half_of(value, which):
    middle = value.shape[-1] // 2
    return jnp.where(which == 0, value[..., :middle], value[..., middle:])


def dot(left, right, dims):
    return lax.dot_general(left, right, (dims, ((), ())), preferred_element_type=F32)


def stack_heads(ref, half, block, heads, size):
    rows = slice(half * block, (half + 1) * block)
    return jnp.concatenate([ref[0, rows, h * size : (h + 1) * size] for h in range(heads)], 0)


def attend_forward_kernel(heads, chunk, q_ref, kv_ref, qpos_ref, kpos_ref, o_ref, mix_ref, tot_ref):
    shards, _, rows, pair = kv_ref.shape
    block, size = rows // 2, pair // 2
    queries = [stack_heads(q_ref, half, block, heads, size) for half in range(2)]
    stacked = heads * block
    sums = [jnp.zeros((stacked, size), F32) for _ in range(2)]
    totals = [jnp.zeros((stacked, 1), F32) for _ in range(2)]
    for first in range(0, shards, chunk):
        span = slice(first * block, (first + chunk) * block)
        for key_half in range(2):
            part = kv_ref[first : first + chunk, 0, key_half * block : (key_half + 1) * block, :]
            part = part.reshape(chunk * block, pair)
            keys, values = part[:, :size], part[:, size:]
            for half in range(key_half, 2):
                weights = jnp.exp(dot(queries[half], keys, ((1,), (1,))) * SCORE_SCALE)
                if half == key_half:
                    allowed = (
                        kpos_ref[key_half : key_half + 1, span]
                        <= qpos_ref[half * stacked : (half + 1) * stacked, :]
                    )
                    weights = jnp.where(allowed, weights, 0.0)
                low = weights.astype(BF16)
                totals[half] += jnp.sum(low.astype(F32), -1, keepdims=True)
                sums[half] += dot(low, values, ((1,), (0,)))
    for half in range(2):
        mixed = sums[half] / totals[half]
        mix_ref[0, half * stacked : (half + 1) * stacked, :] = mixed
        tot_ref[0, half * stacked : (half + 1) * stacked, :] = jnp.broadcast_to(
            totals[half], (stacked, tot_ref.shape[2])
        )
        for h in range(heads):
            o_ref[0, half * block : (half + 1) * block, h * size : (h + 1) * size] = mixed[
                h * block : (h + 1) * block
            ].astype(BF16)


def attend_backward_kernel(
    heads, chunk, q_ref, kv_ref, g_ref, mix_ref, tot_ref, qpos_ref, kpos_ref, dq_ref, dkv_ref
):
    shards, _, rows, pair = kv_ref.shape
    block, size = rows // 2, pair // 2
    stacked = heads * block
    queries, scaled, correction = [], [], []
    for half in range(2):
        queries.append(stack_heads(q_ref, half, block, heads, size))
        grad = stack_heads(g_ref, half, block, heads, size).astype(F32)
        span = slice(half * stacked, (half + 1) * stacked)
        total = tot_ref[0, span, :1]
        delta = jnp.sum(grad * mix_ref[0, span, :], -1, keepdims=True)
        scaled.append((grad / total).astype(BF16))
        correction.append(delta / total)
    grad_query = [jnp.zeros((stacked, size), F32) for _ in range(2)]
    for first in range(0, shards, chunk):
        span = slice(first * block, (first + chunk) * block)
        for key_half in range(2):
            part = kv_ref[first : first + chunk, 0, key_half * block : (key_half + 1) * block, :]
            part = part.reshape(chunk * block, pair)
            keys, values = part[:, :size], part[:, size:]
            grad_keys = jnp.zeros((chunk * block, size), F32)
            grad_values = jnp.zeros((chunk * block, size), F32)
            for half in range(key_half, 2):
                weights = jnp.exp(dot(queries[half], keys, ((1,), (1,))) * SCORE_SCALE)
                if half == key_half:
                    allowed = (
                        kpos_ref[key_half : key_half + 1, span]
                        <= qpos_ref[half * stacked : (half + 1) * stacked, :]
                    )
                    weights = jnp.where(allowed, weights, 0.0)
                low = weights.astype(BF16)
                grad_weights = dot(scaled[half], values, ((1,), (1,)))
                grad_scores = (weights * (grad_weights - correction[half])).astype(BF16)
                grad_query[half] += dot(grad_scores, keys, ((1,), (0,)))
                grad_keys += dot(grad_scores, queries[half], ((0,), (0,)))
                grad_values += dot(low, scaled[half], ((0,), (0,)))
            both = jnp.concatenate([grad_keys * SCORE_SCALE, grad_values], -1).astype(BF16)
            dkv_ref[first : first + chunk, 0, key_half * block : (key_half + 1) * block, :] = (
                both.reshape(chunk, block, pair)
            )
    for half in range(2):
        for h in range(heads):
            dq_ref[0, half * block : (half + 1) * block, h * size : (h + 1) * size] = (
                grad_query[half][h * block : (h + 1) * block] * SCORE_SCALE
            )


def whole(shape):
    return pl.BlockSpec(shape, lambda s: (0,) * len(shape))


def attend_forward(query_low, pairs, query_pos, key_pos, heads):
    sequences, rows, width = query_low.shape
    shards, _, _, pair = pairs.shape
    stacked = query_pos.shape[0]
    row = pl.BlockSpec((1, rows, width), lambda s: (s, 0, 0))
    stack = lambda last: pl.BlockSpec((1, stacked, last), lambda s: (s, 0, 0))
    return pl.pallas_call(
        functools.partial(attend_forward_kernel, heads, min(shards, 16)),
        grid=(sequences,),
        in_specs=[
            row,
            pl.BlockSpec((shards, 1, rows, pair), lambda s: (0, s, 0, 0)),
            whole(query_pos.shape),
            whole(key_pos.shape),
        ],
        out_specs=[row, stack(pair // 2), stack(128)],
        out_shape=[
            jax.ShapeDtypeStruct((sequences, rows, width), BF16),
            jax.ShapeDtypeStruct((sequences, stacked, pair // 2), F32),
            jax.ShapeDtypeStruct((sequences, stacked, 128), F32),
        ],
        name="attend_forward",
    )(query_low, pairs, query_pos, key_pos)


def attend_backward(query_low, pairs, grad_mixed, mixed, totals, query_pos, key_pos, heads):
    sequences, rows, width = query_low.shape
    shards, _, _, pair = pairs.shape
    stacked = query_pos.shape[0]
    row = pl.BlockSpec((1, rows, width), lambda s: (s, 0, 0))
    stack = lambda last: pl.BlockSpec((1, stacked, last), lambda s: (s, 0, 0))
    pairs_spec = pl.BlockSpec((shards, 1, rows, pair), lambda s: (0, s, 0, 0))
    return pl.pallas_call(
        functools.partial(attend_backward_kernel, heads, min(shards, 16)),
        grid=(sequences,),
        in_specs=[
            row,
            pairs_spec,
            row,
            stack(pair // 2),
            stack(128),
            whole(query_pos.shape),
            whole(key_pos.shape),
        ],
        out_specs=[row, pairs_spec],
        out_shape=[
            jax.ShapeDtypeStruct((sequences, rows, width), F32),
            jax.ShapeDtypeStruct(pairs.shape, BF16),
        ],
        name="attend_backward",
    )(query_low, pairs, grad_mixed, mixed, totals, query_pos, key_pos)


class Ring:
    def __init__(self, devices):
        self.chips = devices // 2
        me = lax.axis_index("ctx")
        self.core = me % 2
        chip = me // 2
        across = chip % 2
        deep = chip // 2
        self.place = deep + across * (self.chips - 1 - 2 * deep)
        self.partner = me + 1 - 2 * self.core
        self.right = self.device((self.place + 1) % self.chips, self.core)
        self.left = self.device((self.place + self.chips - 1) % self.chips, self.core)

    def device(self, place, core):
        side = place // (self.chips // 2)
        return 2 * (2 * (place + side * (self.chips - 1 - 2 * place)) + side) + core

    def enter(self, across=False):
        barrier = pltpu.get_barrier_semaphore()
        targets = [{"ctx": other} for other in (self.left, self.right, self.partner)]
        if across:
            targets.append({"wsh": 1 - lax.axis_index("wsh")})
        for target in targets:
            pl.semaphore_signal(barrier, inc=1, device_id=target, device_id_type=MESH)
        pl.semaphore_wait(barrier, len(targets))


def ring_sum_kernel(devices, pieces, arrays, ahead, *refs):
    parts, outs = refs[:arrays], refs[arrays : 2 * arrays]
    own, other, flow = (refs[(2 + i) * arrays : (3 + i) * arrays] for i in range(3))
    own_sem, put_sem, got_sem, send_sem, recv_sem = refs[5 * arrays :]
    ring = Ring(devices)
    chips = ring.chips

    def region(p):
        array, _, first, rows, start, cols = pieces[p]
        return array, pl.ds(first, rows), pl.ds(start, cols)

    def chunk(p, step):
        way = pieces[p][1]
        return (ring.place + 2 * chips + way * (-1 - step)) % chips

    def load(p, step):
        array, rows, cols = region(p)
        source = ring.device(chunk(p, step), ring.core)
        return pltpu.make_async_copy(
            parts[array].at[source, rows, cols],
            own[array].at[step, rows, cols],
            own_sem.at[p, step],
        )

    def give(p, step):
        array, rows, cols = region(p)
        source = ring.device(chunk(p, step), 1 - ring.core)
        return pltpu.make_async_remote_copy(
            src_ref=parts[array].at[source, rows, cols],
            dst_ref=other[array].at[step, rows, cols],
            send_sem=put_sem.at[p, step],
            recv_sem=got_sem.at[p, step],
            device_id={"ctx": ring.partner},
            device_id_type=MESH,
        )

    def pass_on(p, step):
        array, rows, cols = region(p)
        way = pieces[p][1]
        return pltpu.make_async_remote_copy(
            src_ref=flow[array].at[step, rows, cols],
            dst_ref=flow[array].at[step + 1, rows, cols],
            send_sem=send_sem.at[p, step],
            recv_sem=recv_sem.at[p, step],
            device_id={"ctx": ring.right if way > 0 else ring.left},
            device_id_type=MESH,
        )

    def fetch(step):
        for p in range(len(pieces)):
            load(p, step).start()
            give(p, step).start()

    def add(p, step, first, last):
        array, _, row, rows, start, cols = pieces[p]
        width = 128 if cols % 128 == 0 else cols
        while width < 512 and cols % (2 * width) == 0:
            width *= 2
        rows = pl.ds(row, rows)

        def group(i, carry):
            at = start + i * width
            if cols > width:
                at = pl.multiple_of(at, 128)
            where = pl.ds(at, width)
            total = own[array][step, rows, where].astype(F32) + other[array][
                step, rows, where
            ].astype(F32)
            if not first:
                total += flow[array][step, rows, where].astype(F32)
            if last:
                outs[array][rows, where] = total.astype(outs[array].dtype)
            else:
                flow[array][step, rows, where] = total.astype(flow[array].dtype)
            return carry

        if cols == width:
            group(0, 0)
        else:
            lax.fori_loop(0, cols // width, group, 0)

    def work(step, first=False, last=False):
        for p in range(len(pieces)):
            load(p, step).wait()
            give(p, step).wait_recv()
            if not first:
                pass_on(p, step - 1).wait_recv()
            add(p, step, first, last)
            if not last:
                pass_on(p, step).start()

    for p in range(len(pieces)):
        load(p, 0).start()
    ring.enter()
    for p in range(len(pieces)):
        give(p, 0).start()
    for step in range(1, min(ahead, chips)):
        fetch(step)
    work(0, first=True)

    def middle(step, carry):
        @pl.when(step + ahead - 1 < chips)
        def _():
            fetch(step + ahead - 1)

        work(step)
        return carry

    lax.fori_loop(1, chips - 1, middle, 0)
    work(chips - 1, last=True)

    def drain(step, carry):
        for p in range(len(pieces)):
            give(p, step).wait_send()

            @pl.when(step < chips - 1)
            def _():
                pass_on(p, step).wait_send()

        return carry

    lax.fori_loop(0, chips, drain, 0)


def ring_sum(parts, pieces, devices, collective_id, ahead=3, name="ring_sum"):
    chips, count, arrays = devices // 2, len(pieces), len(parts)
    slots = [pltpu.VMEM((chips,) + p.shape[1:], p.dtype) for p in parts]
    return pl.pallas_call(
        functools.partial(ring_sum_kernel, devices, pieces, arrays, ahead),
        out_shape=[jax.ShapeDtypeStruct(p.shape[1:], F32) for p in parts],
        in_specs=[pl.BlockSpec(memory_space=pl.ANY)] * arrays,
        out_specs=[pl.BlockSpec(memory_space=pltpu.VMEM)] * arrays,
        scratch_shapes=slots * 3
        + [pltpu.SemaphoreType.DMA((count, chips))] * 3
        + [pltpu.SemaphoreType.DMA((count, chips - 1))] * 2,
        compiler_params=pltpu.CompilerParams(
            collective_id=collective_id, has_side_effects=True, vmem_limit_bytes=64000 * 1024
        ),
        name=name,
    )(*parts)


def split_ways(parts):
    pieces, lead = [], 1
    for i, p in enumerate(parts):
        _, rows, cols = p.shape
        tiles = cols // 128
        if cols % 128 == 0 and tiles > 1:
            left = (tiles + (1 if lead > 0 else 0)) // 2 * 128
            if tiles % 2:
                lead = -lead
            pieces.append((i, 1, 0, rows, 0, left))
            pieces.append((i, -1, 0, rows, left, cols - left))
        elif rows % 32 == 0:
            pieces.append((i, 1, 0, rows // 2, 0, cols))
            pieces.append((i, -1, rows // 2, rows // 2, 0, cols))
        else:
            pieces.append((i, 1, 0, rows, 0, cols))
    return tuple(pieces)


def sum_over_ctx(parts, pieces, devices, collective_id):
    if all(p.shape[1] % 8 == 0 for p in parts):
        return ring_sum(parts, pieces, devices, collective_id)
    return [
        lax.psum_scatter(p, "ctx", scatter_dimension=0, tiled=False).astype(F32) for p in parts
    ]


def front_kernel(
    devices,
    tokens_ref,
    gains_ref,
    cos_ref,
    sin_ref,
    key_weight,
    value_weight,
    query_weight,
    out_weight,
    pairs_ref,
    normed_ref,
    key_ref,
    all_gains_ref,
    key_other,
    value_other,
    query_other,
    out_other,
    gains_other,
    cross_send,
    cross_recv,
    side_send,
    side_recv,
    flow_send,
    flow_recv,
    twin_send,
    twin_recv,
):
    ring = Ring(devices)
    chips, far = ring.chips, ring.chips // 2
    me = lax.axis_index("ctx")
    mine = lax.axis_index("wsh")
    sequences, rows, width = tokens_ref.shape
    count = sequences * rows
    weights = (
        (key_weight, key_other),
        (value_weight, value_other),
        (query_weight, query_other),
        (out_weight, out_other),
    )

    def cross(i):
        if i == len(weights):
            source, target = gains_ref, gains_other
        else:
            local, other = weights[i]
            half = local.shape[0] // 2
            part = pl.ds(pl.multiple_of(ring.core * half, 16), half)
            source, target = local.at[part], other.at[part]
        return pltpu.make_async_remote_copy(
            src_ref=source,
            dst_ref=target,
            send_sem=cross_send.at[i],
            recv_sem=cross_recv.at[i],
            device_id={"wsh": 1 - mine},
            device_id_type=MESH,
        )

    def side(i):
        other = weights[i][1]
        half = other.shape[0] // 2
        part = pl.ds(pl.multiple_of(ring.core * half, 16), half)
        return pltpu.make_async_remote_copy(
            src_ref=other.at[part],
            dst_ref=other.at[part],
            send_sem=side_send.at[i],
            recv_sem=side_recv.at[i],
            device_id={"ctx": ring.partner},
            device_id_type=MESH,
        )

    def flow(way, seq, hop):
        stream = (1 if way < 0 else 0) * sequences + seq
        place = (ring.place + chips - way * hop) % chips
        block = pairs_ref.at[ring.device(place, ring.core), seq]
        return pltpu.make_async_remote_copy(
            src_ref=block,
            dst_ref=block,
            send_sem=flow_send.at[stream, hop],
            recv_sem=flow_recv.at[stream, hop],
            device_id={"ctx": ring.right if way > 0 else ring.left},
            device_id_type=MESH,
        )

    def twin(way, seq, hop):
        stream = (1 if way < 0 else 0) * sequences + seq
        place = (ring.place + chips - way * hop) % chips
        block = pairs_ref.at[ring.device(place, ring.core), seq]
        return pltpu.make_async_remote_copy(
            src_ref=block,
            dst_ref=block,
            send_sem=twin_send.at[stream, hop],
            recv_sem=twin_recv.at[stream, hop],
            device_id={"ctx": ring.partner},
            device_id_type=MESH,
        )

    def hops(way, seq):
        return far if (seq % 2 == 0) == (way > 0) else far - 1

    ring.enter(across=True)
    order = (len(weights), 0, 1, 2, 3)
    for i in order:
        cross(i).start()
    inputs = tokens_ref[...].reshape(count, width).astype(F32)
    scale = lax.rsqrt(jnp.mean(inputs * inputs, -1, keepdims=True) + EPS)
    cross(len(weights)).wait_recv()
    all_gains_ref[...] = gains_ref[...] + gains_other[...]
    normed_ref[...] = (inputs * scale * all_gains_ref[0:1, :]).astype(BF16)
    for i in (0, 1):
        cross(i).wait_recv()
        side(i).start()
    key_here = dot(normed_ref[...], key_weight[...], ((1,), (0,)))
    value_here = dot(normed_ref[...], value_weight[...], ((1,), (0,)))
    for i in (0, 1):
        side(i).wait_recv()
    key_there = dot(normed_ref[...], key_other[...], ((1,), (0,)))
    value_there = dot(normed_ref[...], value_other[...], ((1,), (0,)))
    lower = mine == 0
    first = jnp.where(lower, key_here, key_there)
    second = jnp.where(lower, key_there, key_here)
    middle = first.shape[1]
    key_ref[:, :middle] = first
    key_ref[:, middle:] = second
    power = jnp.sum(first * first, -1, keepdims=True) + jnp.sum(second * second, -1, keepdims=True)
    scale = lax.rsqrt(power / (2 * middle) + EPS)
    gain = all_gains_ref[4:5, 2 * middle : 4 * middle]
    first = first * scale * gain[:, :middle]
    second = second * scale * gain[:, middle:]
    cosine, sine = cos_ref[...], sin_ref[...]
    value_first = jnp.where(lower, value_here, value_there).astype(BF16)
    value_second = jnp.where(lower, value_there, value_here).astype(BF16)
    for seq in range(sequences):
        span = slice(seq * rows, (seq + 1) * rows)
        head, tail = first[span], second[span]
        pairs_ref[me, seq, :, 0 * middle : 1 * middle] = (head * cosine - tail * sine).astype(BF16)
        pairs_ref[me, seq, :, 1 * middle : 2 * middle] = (tail * cosine + head * sine).astype(BF16)
        pairs_ref[me, seq, :, 2 * middle : 3 * middle] = value_first[span]
        pairs_ref[me, seq, :, 3 * middle : 4 * middle] = value_second[span]
    streams = [(way, seq) for seq in range(sequences) for way in (1, -1)]
    for hop in range(far + 1):
        for way, seq in streams:
            if hop > hops(way, seq):
                continue
            if hop > 0:
                flow(way, seq, hop - 1).wait_recv()
            if hop < hops(way, seq):
                flow(way, seq, hop).start()
            if hop > 0 or way > 0:
                twin(way, seq, hop).start()
    for i in (2, 3):
        cross(i).wait_recv()
        side(i).start()
    for hop in range(far + 1):
        for way, seq in streams:
            if hop > hops(way, seq):
                continue
            if hop > 0 or way > 0:
                twin(way, seq, hop).wait()
            if hop < hops(way, seq):
                flow(way, seq, hop).wait_send()
    for i in order:
        cross(i).wait_send()
    for i in (2, 3):
        side(i).wait()
    for i in (0, 1):
        side(i).wait_send()


def front(tokens, gains, cosine, sine, weights, devices, collective_id):
    sequences, rows, width = tokens.shape
    size = 2 * cosine.shape[1]
    far = devices // 4
    here, there = pl.BlockSpec(memory_space=pltpu.VMEM), pl.BlockSpec(memory_space=pl.ANY)
    streams = pltpu.SemaphoreType.DMA((2 * sequences, far + 1))
    like = lambda a: jax.ShapeDtypeStruct(a.shape, a.dtype)
    return pl.pallas_call(
        functools.partial(front_kernel, devices),
        in_specs=[here] * 6 + [there] * 2,
        out_specs=[here] * 6 + [there] * 2,
        out_shape=[
            jax.ShapeDtypeStruct((devices, sequences, rows, 2 * size), BF16),
            jax.ShapeDtypeStruct((sequences * rows, width), BF16),
            jax.ShapeDtypeStruct((sequences * rows, size), F32),
            like(gains),
        ]
        + [like(w) for w in weights],
        scratch_shapes=[pltpu.VMEM(gains.shape, gains.dtype)]
        + [pltpu.SemaphoreType.DMA((5,))] * 2
        + [pltpu.SemaphoreType.DMA((4,))] * 2
        + [streams] * 4,
        compiler_params=pltpu.CompilerParams(
            collective_id=collective_id, has_side_effects=True, vmem_limit_bytes=60000 * 1024
        ),
        name="front",
    )(tokens, gains, cosine, sine, *weights)


class RingSum:
    def __init__(self, ring, pieces, parts, own, other, flow, outs, sems):
        self.ring, self.pieces, self.parts, self.own = ring, pieces, parts, own
        self.other, self.flow, self.outs = other, flow, outs
        self.put_sem, self.got_sem, self.send_sem, self.recv_sem = sems[:4]
        self.own_sem = sems[4] if own is not None else None
        self.last = ring.chips - 1

    def region(self, p):
        array, _, first, rows, start, cols = self.pieces[p]
        return array, pl.ds(first, rows), pl.ds(start, cols)

    def owner(self, p, step, core):
        way = self.pieces[p][1]
        chips = self.ring.chips
        return self.ring.device((self.ring.place + 2 * chips + way * (-1 - step)) % chips, core)

    def load(self, p, step):
        array, rows, cols = self.region(p)
        slot = step % self.own[array].shape[0]
        return pltpu.make_async_copy(
            self.parts[array].at[self.owner(p, step, self.ring.core), rows, cols],
            self.own[array].at[slot, rows, cols],
            self.own_sem.at[p, step],
        )

    def give(self, p, step):
        array, rows, cols = self.region(p)
        return pltpu.make_async_remote_copy(
            src_ref=self.parts[array].at[self.owner(p, step, 1 - self.ring.core), rows, cols],
            dst_ref=self.other[array].at[step, rows, cols],
            send_sem=self.put_sem.at[p, step],
            recv_sem=self.got_sem.at[p, step],
            device_id={"ctx": self.ring.partner},
            device_id_type=MESH,
        )

    def hop(self, p, step):
        array, rows, cols = self.region(p)
        way = self.pieces[p][1]
        return pltpu.make_async_remote_copy(
            src_ref=self.flow[array].at[step, rows, cols],
            dst_ref=self.flow[array].at[step + 1, rows, cols],
            send_sem=self.send_sem.at[p, step],
            recv_sem=self.recv_sem.at[p, step],
            device_id={"ctx": self.ring.right if way > 0 else self.ring.left},
            device_id_type=MESH,
        )

    def load_all(self, step):
        for p in range(len(self.pieces)):
            self.load(p, step).start()

    def give_all(self, step):
        for p in range(len(self.pieces)):
            self.give(p, step).start()

    def work(self, p, step):
        array, _, row, rows, start, cols = self.pieces[p]
        if self.own is not None:
            self.load(p, step).wait()
            mine, at_mine = self.own[array], step % self.own[array].shape[0]
        else:
            mine, at_mine = self.parts[array], self.owner(p, step, self.ring.core)
        self.give(p, step).wait_recv()
        if step > 0:
            self.hop(p, step - 1).wait_recv()
        width = 128 if cols % 128 == 0 else cols
        while width < 512 and cols % (2 * width) == 0:
            width *= 2
        rows = pl.ds(row, rows)

        def group(i, carry):
            at = start + i * width
            if cols > width:
                at = pl.multiple_of(at, 128)
            where = pl.ds(at, width)
            total = mine[at_mine, rows, where].astype(F32)
            total += self.other[array][step, rows, where].astype(F32)
            if step > 0:
                total += self.flow[array][step, rows, where].astype(F32)
            if step == self.last:
                self.outs[array][rows, where] = total.astype(self.outs[array].dtype)
            else:
                self.flow[array][step, rows, where] = total.astype(self.flow[array].dtype)
            return carry

        if cols == width:
            group(0, 0)
        else:
            lax.fori_loop(0, cols // width, group, 0)
        if step < self.last:
            self.hop(p, step).start()

    def drain(self):
        for p in range(len(self.pieces)):
            for step in range(self.last + 1):
                self.give(p, step).wait_send()
                if step < self.last:
                    self.hop(p, step).wait_send()


def norm_back(upstream, vector, gain):
    scale = lax.rsqrt(jnp.mean(vector * vector, -1, keepdims=True) + EPS)
    normal = vector * scale
    weighted = upstream * gain
    back = scale * (weighted - normal * jnp.mean(weighted * normal, -1, keepdims=True))
    return back, jnp.sum(upstream * normal, 0, keepdims=True)


def turn_back(upstream, cosine, sine):
    middle = upstream.shape[-1] // 2
    first, second = upstream[:, :middle], upstream[:, middle:]
    return jnp.concatenate([first * cosine + second * sine, second * cosine - first * sine], -1)


def back_kernel(devices, heads, ff_pieces, kv_pieces, attn_pieces, names, *refs):
    r = dict(zip(names, refs))
    ring = Ring(devices)
    chips = ring.chips
    mine = lax.axis_index("wsh")
    sequences, rows, _ = r["query"].shape
    size = r["key_raw"].shape[1]
    count = sequences * rows
    block = rows // 2
    stacked = heads * block

    ff = RingSum(
        ring,
        ff_pieces,
        [r["part_down"], r["part_gate"], r["part_up"]],
        [r[f"ff_own{i}"] for i in range(3)],
        [r[f"ff_other{i}"] for i in range(3)],
        [r[f"ff_flow{i}"] for i in range(3)],
        [r["grad_down"], r["grad_gate"], r["grad_up"]],
        [r["ff_put"], r["ff_got"], r["ff_send"], r["ff_recv"], r["ff_load"]],
    )
    kv = RingSum(
        ring,
        kv_pieces,
        [r["pairs"]],
        None,
        [r["kv_other"]],
        [r["kv_flow"]],
        [r["kv_sum"]],
        [r["kv_put"], r["kv_got"], r["kv_send"], r["kv_recv"]],
    )
    attn = RingSum(
        ring,
        attn_pieces,
        [r["qkv_part"], r["out_part"]],
        None,
        [r["qkv_other"], r["out_other"]],
        [r["qkv_flow"], r["out_flow"]],
        [r["grad_qkv"], r["grad_out"]],
        [r["at_put"], r["at_got"], r["at_send"], r["at_recv"]],
    )

    def brought(i):
        name = BROUGHT[i]
        return pltpu.make_async_copy(r["in_" + name], r[name], r["bring"].at[i])

    def need(*wanted):
        for name in wanted:
            brought(BROUGHT.index(name)).wait()

    def across(i, source, target):
        return pltpu.make_async_remote_copy(
            src_ref=source,
            dst_ref=target,
            send_sem=r["cross_send"].at[i],
            recv_sem=r["cross_recv"].at[i],
            device_id={"wsh": 1 - mine},
            device_id_type=MESH,
        )

    out_swap = across(0, r["att_send"], r["att_across"])
    col_swap = across(1, r["col_send"], r["col_rows"].at[pl.ds(count, count)])
    gain_swap = across(2, r["gain_own"], r["gain_across"])
    gain_twin = pltpu.make_async_remote_copy(
        src_ref=r["gain_pair"],
        dst_ref=r["gain_twin"],
        send_sem=r["twin_send"].at[0],
        recv_sem=r["twin_recv"].at[0],
        device_id={"ctx": ring.partner},
        device_id_type=MESH,
    )

    def gain_hop(way, step):
        return pltpu.make_async_remote_copy(
            src_ref=r["gain_flow"].at[way, step],
            dst_ref=r["gain_flow"].at[way, step + 1],
            send_sem=r["gain_send"].at[way, step],
            recv_sem=r["gain_recv"].at[way, step],
            device_id={"ctx": ring.right if way == 0 else ring.left},
            device_id_type=MESH,
        )

    gain_hops = (chips // 2, chips - 1 - chips // 2)

    def attention(seq):
        queries, scaled, correction = [], [], []
        for half in range(2):
            span = slice(half * stacked, (half + 1) * stacked)
            lines = slice(half * block, (half + 1) * block)
            cut = lambda ref: jnp.concatenate(
                [ref[seq, lines, h * size : (h + 1) * size] for h in range(heads)], 0
            )
            queries.append(cut(r["query"]))
            grad = cut(r["grad_mixed"]).astype(F32)
            total = r["totals"][seq, span, :1]
            delta = jnp.sum(grad * r["mixed"][seq, span, :], -1, keepdims=True)
            scaled.append((grad / total).astype(BF16))
            correction.append(delta / total)
        grad_query = [jnp.zeros((stacked, size), F32) for _ in range(2)]
        for key_half in range(2):
            lines = pl.ds(seq * rows + key_half * block, block)
            part = r["pairs"][:, lines, :].reshape(devices * block, 2 * size)
            keys, values = part[:, :size], part[:, size:]
            grad_keys = jnp.zeros((devices * block, size), F32)
            grad_values = jnp.zeros((devices * block, size), F32)
            for half in range(key_half, 2):
                weights = jnp.exp(dot(queries[half], keys, ((1,), (1,))) * SCORE_SCALE)
                if half == key_half:
                    allowed = (
                        r["key_pos"][key_half : key_half + 1, :]
                        <= r["query_pos"][half * stacked : (half + 1) * stacked, :]
                    )
                    weights = jnp.where(allowed, weights, 0.0)
                low = weights.astype(BF16)
                grad_weights = dot(scaled[half], values, ((1,), (1,)))
                grad_scores = (weights * (grad_weights - correction[half])).astype(BF16)
                grad_query[half] += dot(grad_scores, keys, ((1,), (0,)))
                grad_keys += dot(grad_scores, queries[half], ((0,), (0,)))
                grad_values += dot(low, scaled[half], ((0,), (0,)))
            both = jnp.concatenate([grad_keys * SCORE_SCALE, grad_values], -1).astype(BF16)
            r["pairs"][:, lines, :] = both.reshape(devices, block, 2 * size)
        for half in range(2):
            lines = pl.ds(seq * rows + half * block, block)
            for h in range(heads):
                r["grad_query"][lines, h * size : (h + 1) * size] = (
                    grad_query[half][h * block : (h + 1) * block] * SCORE_SCALE
                )

    def pick(value, which):
        middle = value.shape[1] // 2
        return jnp.where(which == 0, value[:, :middle], value[:, middle:])

    def projections():
        need("query_raw", "key_raw", "cosine", "sine", "gains")
        cosine, sine = r["cosine"][...], r["sine"][...]
        gain = r["gains"][4:5, :size]
        total = jnp.zeros((1, size), F32)
        lows = []
        for h in range(heads):
            cols = slice(h * size, (h + 1) * size)
            back, part = norm_back(
                turn_back(r["grad_query"][:, cols], cosine, sine), r["query_raw"][:, cols], gain
            )
            total += part
            r["query_low"][:, cols] = back.astype(BF16)
        back, key_total = norm_back(
            turn_back(r["kv_sum"][:, :size], cosine, sine),
            r["key_raw"][...],
            r["gains"][4:5, size : 2 * size],
        )
        r["pair_low"][:, :size] = back.astype(BF16)
        r["pair_low"][:, size:] = r["kv_sum"][:, size:].astype(BF16)
        first = 0
        for value in (
            r["query_low"][...],
            r["pair_low"][:, :size],
            r["pair_low"][:, size:],
        ):
            cols = slice(first, first + value.shape[1] // 2)
            r["col_rows"][:count, cols] = pick(value, mine)
            r["col_send"][:, cols] = pick(value, 1 - mine)
            first += value.shape[1] // 2
        col_swap.start()
        need("weight_query", "weight_pair", "tokens", "grad_hidden", "gain_part")
        grad_normed = dot(r["query_low"][...], r["weight_query"][...], ((1,), (1,)))
        grad_normed += dot(r["pair_low"][...], r["weight_pair"][...], ((1,), (1,)))
        back, part = norm_back(grad_normed, r["tokens"][...].astype(F32), r["gains"][0:1, :])
        r["grad_tokens"][...] = back + r["grad_hidden"][...]
        r["gain_own"][...] = r["gain_part"][...]
        r["gain_own"][0:1, :] = part
        r["gain_own"][4:5, :size] = total
        r["gain_own"][4:5, size : 2 * size] = key_total
        gain_swap.start()

    def out_part():
        need("mixed_turned", "att_own")
        out_swap.wait_recv()
        _, lines, cols = r["out_part"].shape
        value = dot(r["mixed_turned"][:, :count], r["att_own"][...], ((1,), (0,)))
        value += dot(r["mixed_turned"][:, count:], r["att_across"][...], ((1,), (0,)))
        r["out_part"][...] = value.reshape(devices, lines, cols).astype(BF16)

    def qkv_part():
        need("normed_turned")
        col_swap.wait_recv()
        _, lines, cols = r["qkv_part"].shape
        width = 256
        for first in range(0, cols, width):
            value = dot(
                r["normed_turned"][...], r["col_rows"][:, first : first + width], ((1,), (0,))
            )
            r["qkv_part"][:, :, first : first + width] = value.reshape(
                devices, lines, width
            ).astype(BF16)

    def gains_step(step):
        if step == 0:
            gain_swap.wait_recv()
            r["gain_pair"][...] = r["gain_own"][...] + r["gain_across"][...]
            gain_twin.start()
        elif step == 1:
            gain_twin.wait_recv()
            both = r["gain_pair"][...] + r["gain_twin"][...]
            r["gain_flow"][0, 0] = both
            r["gain_flow"][1, 0] = both
            r["gain_sum"][...] = both
            for way in range(2):
                gain_hop(way, 0).start()
        else:
            for way in range(2):
                if step - 2 < gain_hops[way]:
                    gain_hop(way, step - 2).wait_recv()
                    if step - 1 < gain_hops[way]:
                        gain_hop(way, step - 1).start()
                    r["gain_sum"][...] += r["gain_flow"][way, step - 1]

    def ff_step(step, extra=()):
        extra = list(extra)
        if step + 1 < chips:
            ff.load_all(step + 1)
        if step + 2 < chips:
            ff.give_all(step + 2)
        for p in range(len(ff_pieces)):
            ff.work(p, step)
            if p % 2 == 1 and extra:
                extra.pop(0)()
        for left in extra:
            left()

    def kv_step(step):
        def run():
            for p in range(len(kv_pieces)):
                kv.work(p, step)

        return run

    def attn_step(step):
        def run():
            gains_step(step)
            for p in range(len(attn_pieces)):
                attn.work(p, step)

        return run

    ff.load_all(0)
    for i in range(len(BROUGHT)):
        brought(i).start()
    ring.enter(across=True)
    ff.give_all(0)
    ff.give_all(1)
    need("att_send")
    out_swap.start()
    ff_step(0)
    need("pairs", "query", "grad_mixed", "mixed", "totals", "query_pos", "key_pos")
    for seq in range(sequences):
        attention(seq)
    for step in range(chips):
        kv.give_all(step)
    ff_step(1, [kv_step(0), kv_step(1), kv_step(2)])
    ff_step(2, [kv_step(3), kv_step(4), kv_step(5)])
    ff_step(3, [kv_step(6), kv_step(7), out_part])
    projections()
    ff_step(4)
    qkv_part()
    for step in range(chips):
        attn.give_all(step)
    ff_step(5, [attn_step(0), attn_step(1), attn_step(2)])
    ff_step(6, [attn_step(3), attn_step(4), attn_step(5)])
    ff_step(7, [attn_step(6), attn_step(7)])
    r["gains_total"][...] = r["gain_sum"][...]
    for copy in (out_swap, col_swap, gain_swap, gain_twin):
        copy.wait_send()
    for way in range(2):
        for step in range(gain_hops[way]):
            gain_hop(way, step).wait_send()
    ff.drain()
    kv.drain()
    attn.drain()


BROUGHT = (
    "att_send",
    "pairs",
    "query",
    "grad_mixed",
    "mixed",
    "totals",
    "query_pos",
    "key_pos",
    "att_own",
    "mixed_turned",
    "query_raw",
    "key_raw",
    "cosine",
    "sine",
    "gains",
    "weight_query",
    "weight_pair",
    "tokens",
    "grad_hidden",
    "gain_part",
    "normed_turned",
)


def back(given, ff_parts, heads, devices, collective_id):
    chips = devices // 2
    count, width = given["tokens"].shape
    size = given["key_raw"].shape[1]
    out_cols = given["att_send"].shape[1]
    out_lines = given["mixed_turned"].shape[0] // devices
    lines = width // devices
    cols = (heads * size + 2 * size) // 2
    slots = lambda n, p: pltpu.VMEM((n,) + tuple(p.shape[1:]), p.dtype)
    ff_pieces = split_ways(ff_parts)
    pair_rows = given["pairs"].shape[1]
    kv_pieces = tuple(
        (0, 1 - 2 * i, i * pair_rows // 2, pair_rows // 2, 0, 2 * size) for i in range(2)
    )
    attn_pieces = (
        (0, 1, 0, lines, 0, cols // 2),
        (0, -1, 0, lines, cols // 2, cols // 2),
        (1, 1, 0, out_lines // 2, 0, out_cols),
        (1, -1, out_lines // 2, out_lines // 2, 0, out_cols),
    )
    dma = lambda *shape: pltpu.SemaphoreType.DMA(shape)
    names, specs, operands = [], [], []
    for name, array in zip(("part_down", "part_gate", "part_up"), ff_parts):
        names.append(name)
        operands.append(array)
    for name in BROUGHT:
        names.append("in_" + name)
        operands.append(given[name])
    outs = {
        "grad_tokens": ((count, width), F32),
        "grad_down": (ff_parts[0].shape[1:], BF16),
        "grad_gate": (ff_parts[1].shape[1:], BF16),
        "grad_up": (ff_parts[2].shape[1:], BF16),
        "grad_qkv": ((lines, cols), F32),
        "grad_out": ((out_lines, out_cols), F32),
        "gains_total": (given["gains"].shape, F32),
    }
    scratch = {}
    for name in BROUGHT:
        shape = given[name].shape
        scratch[name] = pltpu.VMEM(shape, given[name].dtype)
    for i, p in enumerate(ff_parts):
        scratch[f"ff_own{i}"] = slots(2, p)
        scratch[f"ff_other{i}"] = slots(chips, p)
        scratch[f"ff_flow{i}"] = slots(chips, p)
    for kind, pieces in (("ff", ff_pieces), ("kv", kv_pieces), ("at", attn_pieces)):
        for name, steps in (("put", chips), ("got", chips), ("send", chips - 1), ("recv", chips - 1)):
            scratch[f"{kind}_{name}"] = dma(len(pieces), steps)
    scratch["ff_load"] = dma(len(ff_pieces), chips)
    scratch["kv_other"] = slots(chips, given["pairs"])
    scratch["kv_flow"] = slots(chips, given["pairs"])
    scratch["kv_sum"] = pltpu.VMEM((pair_rows, 2 * size), F32)
    scratch["att_across"] = pltpu.VMEM((count, out_cols), BF16)
    scratch["grad_query"] = pltpu.VMEM((count, heads * size), F32)
    scratch["query_low"] = pltpu.VMEM((count, heads * size), BF16)
    scratch["pair_low"] = pltpu.VMEM((count, 2 * size), BF16)
    scratch["col_rows"] = pltpu.VMEM((2 * count, cols), BF16)
    scratch["col_send"] = pltpu.VMEM((count, cols), BF16)
    for name, shape in (("qkv", (lines, cols)), ("out", (out_lines, out_cols))):
        scratch[f"{name}_part"] = pltpu.VMEM((devices,) + shape, BF16)
        scratch[f"{name}_other"] = pltpu.VMEM((chips,) + shape, BF16)
        scratch[f"{name}_flow"] = pltpu.VMEM((chips,) + shape, BF16)
    for name in ("gain_own", "gain_across", "gain_pair", "gain_twin", "gain_sum"):
        scratch[name] = pltpu.VMEM(given["gains"].shape, F32)
    scratch["gain_flow"] = pltpu.VMEM((2, chips // 2 + 1) + given["gains"].shape, F32)
    scratch["bring"] = dma(len(BROUGHT))
    for name, n in (("cross_send", 3), ("cross_recv", 3), ("twin_send", 1), ("twin_recv", 1)):
        scratch[name] = dma(n)
    scratch["gain_send"] = dma(2, chips // 2)
    scratch["gain_recv"] = dma(2, chips // 2)
    names += list(outs) + list(scratch)
    return pl.pallas_call(
        functools.partial(
            back_kernel, devices, heads, ff_pieces, kv_pieces, attn_pieces, tuple(names)
        ),
        in_specs=[pl.BlockSpec(memory_space=pl.ANY)] * len(operands),
        out_specs=[pl.BlockSpec(memory_space=pltpu.VMEM)] * len(outs),
        out_shape=[jax.ShapeDtypeStruct(shape, kind) for shape, kind in outs.values()],
        scratch_shapes=list(scratch.values()),
        compiler_params=pltpu.CompilerParams(
            collective_id=collective_id, has_side_effects=True, vmem_limit_bytes=67043328
        ),
        name="back",
    )(*operands)


def body(
    tokens,
    block_order,
    gain_attn_pre,
    gain_query,
    gain_key,
    gain_attn_post,
    gain_ff_pre,
    gain_ff_post,
    weight_query,
    weight_key,
    weight_value,
    weight_out,
    weight_gate,
    weight_up,
    weight_down,
    cotangent,
):
    sequences, rows, width = tokens.shape
    count = sequences * rows
    block = rows // 2
    devices = lax.axis_size("ctx")
    me = lax.axis_index("ctx")
    mine = lax.axis_index("wsh")

    head_size = 2 * gain_key.shape[0]
    heads = 2 * weight_query.shape[1] // head_size

    lane = jnp.arange(block, dtype=jnp.int32)
    late_order = 2 * devices - 1 - block_order
    early_pos = (block_order[:, None] * block + lane[None]).reshape(-1)
    late_pos = (late_order[:, None] * block + lane[None]).reshape(-1)
    key_pos = jnp.stack([early_pos, late_pos], 0)
    own_first = lax.dynamic_slice_in_dim(block_order, me, 1)[0]
    own_early = own_first * block + lane
    own_late = (2 * devices - 1 - own_first) * block + lane
    own_pos = jnp.concatenate([own_early, own_late])
    query_pos = jnp.concatenate([jnp.tile(own_early, heads), jnp.tile(own_late, heads)])[:, None]

    cosine, sine = angle_tables(own_pos, head_size)

    def placed(gain):
        zeros = jnp.zeros_like(gain)
        return jnp.where(
            mine == 0, jnp.concatenate([gain, zeros]), jnp.concatenate([zeros, gain])
        ).astype(F32)

    own_gains = [placed(g) for g in (gain_attn_pre, gain_attn_post, gain_ff_pre, gain_ff_post)]
    small = [placed(gain_query), placed(gain_key)]
    own_gains.append(jnp.concatenate(small + [jnp.zeros((width - 2 * head_size,), F32)]))
    own_gains = jnp.stack(own_gains + [jnp.zeros((width,), F32)] * 3)
    pairs, normed_low, key_raw, all_gains, key_other, value_other, query_other, out_other = front(
        tokens,
        own_gains,
        cosine,
        sine,
        (weight_key, weight_value, weight_query, weight_out),
        devices,
        2,
    )
    attn_pre, attn_post, ff_pre, ff_post = (all_gains[i] for i in range(4))
    query_gain = all_gains[4, :head_size]
    key_gain = all_gains[4, head_size : 2 * head_size]
    normed_low = normed_low.reshape(sequences, rows, width)
    key_raw = key_raw.reshape(sequences, rows, head_size)
    pair_weight = jnp.concatenate(
        [join_halves(mine, weight_key, key_other), join_halves(mine, weight_value, value_other)], 1
    )
    weight_query = join_halves(mine, weight_query, query_other)
    weight_out = join_halves(mine, weight_out, out_other)
    local_size = weight_key.shape[1]
    inputs = tokens.astype(F32)

    def key_path(key_in, key_scale):
        return rotate(norm_gain(key_in, key_scale), cosine[None], sine[None])

    def query_path(query_in, query_scale):
        return rotate(
            norm_gain(query_in, query_scale), cosine[None, :, None, :], sine[None, :, None, :]
        )

    query_raw = jnp.einsum(
        "srd,de->sre", normed_low, weight_query, preferred_element_type=F32
    ).reshape(sequences, rows, heads, head_size)
    query_rot, query_back = jax.vjp(query_path, query_raw, query_gain)
    query_low = query_rot.astype(BF16).reshape(sequences, rows, heads * head_size)

    mixed_low, mixed, totals = attend_forward(query_low, pairs, query_pos, key_pos, heads)
    attended = jnp.einsum("sre,ed->srd", mixed_low, weight_out, preferred_element_type=F32)
    post_attn, post_attn_back = jax.vjp(norm_gain, attended, attn_post)
    hidden_state = inputs + post_attn
    ff_input, ff_pre_back = jax.vjp(norm_gain, hidden_state, ff_pre)
    ff_own = ff_input.astype(BF16).reshape(count, width)
    ff_other = swap(ff_own)

    def ff_forward(rows_in):
        gate = dot(rows_in, weight_gate, ((1,), (0,)))
        upward = dot(rows_in, weight_up, ((1,), (0,)))
        activated, gelu_back = jax.vjp(gate_up, gate, upward)
        activated_low = activated.astype(BF16)
        return activated_low, gelu_back, dot(activated_low, weight_down, ((1,), (1,)))

    act_own, gelu_own, lowered_own = ff_forward(ff_own)
    act_other, gelu_other, lowered_other = ff_forward(ff_other)
    lowered = lowered_own + swap(lowered_other.astype(BF16)).astype(F32)
    lowered = lowered.reshape(sequences, rows, width)
    post_ff, post_ff_back = jax.vjp(norm_gain, lowered, ff_post)
    output = (hidden_state + post_ff).astype(BF16)

    grad_output = cotangent.astype(F32)
    grad_lowered, grad_ff_post = post_ff_back(grad_output)
    low_own = grad_lowered.astype(BF16).reshape(count, width)
    low_other = swap(low_own)

    def ff_backward(rows_in, gelu_back):
        grad_gate, grad_up = gelu_back(dot(rows_in, weight_down, ((1,), (0,))))
        grad_gate, grad_up = grad_gate.astype(BF16), grad_up.astype(BF16)
        back = dot(grad_gate, weight_gate, ((1,), (1,))) + dot(grad_up, weight_up, ((1,), (1,)))
        return grad_gate, grad_up, back

    gate_own, up_own, back_own = ff_backward(low_own, gelu_own)
    gate_other, up_other, back_other = ff_backward(low_other, gelu_other)
    grad_ff_input = back_own + swap(back_other.astype(BF16)).astype(F32)
    grad_ff_input = grad_ff_input.reshape(sequences, rows, width)

    def both(own, other):
        return jnp.concatenate([own, other], 0)

    def weight_grad(left, right):
        return dot(left, right, ((0,), (0,))).astype(BF16)

    ff_rows = both(ff_own, ff_other)
    part_down = weight_grad(both(low_own, low_other), both(act_own, act_other))
    part_gate = weight_grad(ff_rows, both(gate_own, gate_other))
    part_up = weight_grad(ff_rows, both(up_own, up_other))

    grad_hidden, grad_ff_pre = ff_pre_back(grad_ff_input)
    grad_hidden = grad_hidden + grad_output
    grad_attended, grad_attn_post = post_attn_back(grad_hidden)
    attended_low = grad_attended.astype(BF16)
    grad_mixed = jnp.einsum(
        "srd,ed->sre", attended_low, weight_out, preferred_element_type=F32
    ).astype(BF16)
    attended_low = attended_low.reshape(count, width)
    mixed_rows = mixed_low.reshape(count, heads * head_size)
    normed_rows = normed_low.reshape(count, width)
    given = {
        "att_send": half_of(attended_low, 1 - mine),
        "att_own": half_of(attended_low, mine),
        "pairs": pairs.reshape(devices, count, 2 * head_size),
        "query": query_low,
        "grad_mixed": grad_mixed,
        "mixed": mixed,
        "totals": totals,
        "query_pos": query_pos,
        "key_pos": key_pos,
        "mixed_turned": both(mixed_rows, swap(mixed_rows)).T,
        "query_raw": query_raw.reshape(count, heads * head_size),
        "key_raw": key_raw.reshape(count, head_size),
        "cosine": jnp.tile(cosine, (sequences, 1)),
        "sine": jnp.tile(sine, (sequences, 1)),
        "gains": all_gains,
        "weight_query": weight_query,
        "weight_pair": pair_weight,
        "tokens": tokens.reshape(count, width),
        "grad_hidden": grad_hidden.reshape(count, width),
        "gain_part": jnp.stack(
            [jnp.zeros((width,), F32), grad_attn_post, grad_ff_pre, grad_ff_post]
            + [jnp.zeros((width,), F32)] * 4
        ),
        "normed_turned": both(normed_rows, swap(normed_rows)).T,
    }
    if width % (8 * devices) == 0 and mixed_rows.shape[1] % (32 * devices) == 0:
        ff_parts = [
            p.reshape(devices, p.shape[0] // devices, p.shape[1])
            for p in (part_down, part_gate, part_up)
        ]
        grad_tokens, grad_down_w, grad_gate_w, grad_up_w, grad_qkv, grad_out_w, gain_sums = back(
            given, ff_parts, heads, devices, 0
        )
        grad_tokens = grad_tokens.reshape(sequences, rows, width)
        place = me * 2 + mine

        def share(row, first, size):
            part = size // (2 * devices)
            return lax.dynamic_slice(gain_sums, (row, first + place * part), (1, part))[0]

        outs = [
            share(0, 0, width),
            share(4, 0, head_size),
            share(4, head_size, head_size),
            share(1, 0, width),
            share(2, 0, width),
            share(3, 0, width),
        ]
    else:
        part_out = weight_grad(
            both(mixed_rows, swap(mixed_rows)),
            both(half_of(attended_low, mine), swap(half_of(attended_low, 1 - mine))),
        )
        grad_query, grad_pairs = attend_backward(
            query_low, pairs, grad_mixed, mixed, totals, query_pos, key_pos, heads
        )
        pair_rows = sequences * rows
        slots = grad_pairs.reshape(devices, pair_rows, 2 * head_size)
        share = pair_rows // 8
        pieces = tuple((0, 1 - 2 * (i % 2), i * share, share, 0, 2 * head_size) for i in range(8))
        own_grads = sum_over_ctx([slots], pieces, devices, 0)[0]
        own_grads = own_grads.reshape(sequences, rows, 2 * head_size)
        grad_key_raw, grad_key_gain = jax.vjp(key_path, key_raw, key_gain)[1](own_grads[..., :head_size])
        value_grad_low = own_grads[..., head_size:].astype(BF16)
        grad_query_raw, grad_query_gain = query_back(
            grad_query.reshape(sequences, rows, heads, head_size)
        )
        query_grad_low = grad_query_raw.reshape(count, heads * head_size).astype(BF16)
        key_grad_low = grad_key_raw.astype(BF16).reshape(count, head_size)
        value_grad_low = value_grad_low.reshape(count, head_size)
        grad_normed = (
            dot(query_grad_low, weight_query, ((1,), (1,)))
            + dot(jnp.concatenate([key_grad_low, value_grad_low], -1), pair_weight, ((1,), (1,)))
        ).reshape(sequences, rows, width)
        grad_inputs, grad_attn_pre = jax.vjp(norm_gain, inputs, attn_pre)[1](grad_normed)
        grad_tokens = grad_inputs + grad_hidden

        def columns(which):
            return jnp.concatenate(
                [half_of(v, which) for v in (query_grad_low, key_grad_low, value_grad_low)], -1
            )

        part_qkv = weight_grad(
            both(normed_rows, swap(normed_rows)), both(columns(mine), swap(columns(1 - mine)))
        )

        gain_grads = [
            grad_attn_pre,
            grad_query_gain,
            grad_key_gain,
            grad_attn_post,
            grad_ff_pre,
            grad_ff_post,
        ]
        packed = jnp.concatenate([g.reshape(devices, 2, -1) for g in gain_grads], -1)
        keep = jnp.where(mine == 0, packed[:, 0], packed[:, 1])
        send = jnp.where(mine == 0, packed[:, 1], packed[:, 0])
        packed = keep + swap(send)
        gain_size = packed.shape[-1]
        packed = jnp.pad(packed, ((0, 0), (0, 1024 - gain_size))).reshape(devices, 8, 128)
        parts = [
            p.reshape(devices, p.shape[0] // devices, p.shape[1])
            for p in (part_down, part_gate, part_up, part_qkv, part_out)
        ] + [packed]
        grad_down_w, grad_gate_w, grad_up_w, grad_qkv, grad_out_w, packed = sum_over_ctx(
            parts, split_ways(parts), devices, 1
        )
        packed = packed.reshape(-1)
        outs, first = [], 0
        for g in gain_grads:
            size = g.shape[0] // (2 * devices)
            outs.append(packed[first : first + size])
            first += size
    query_cols = grad_qkv.shape[1] - 2 * local_size
    grad_query_w = grad_qkv[:, :query_cols]
    grad_key_w = grad_qkv[:, query_cols : query_cols + local_size]
    grad_value_w = grad_qkv[:, query_cols + local_size :]
    grad_down_w, grad_gate_w, grad_up_w = (
        g.astype(F32) for g in (grad_down_w, grad_gate_w, grad_up_w)
    )
    return (
        output,
        grad_tokens,
        *outs,
        grad_query_w,
        grad_key_w,
        grad_value_w,
        grad_out_w,
        grad_gate_w,
        grad_up_w,
        grad_down_w,
    )


def solution(mesh):
    rows, vector, matrix = P("wsh", "ctx", None), P("wsh"), P(None, "wsh")
    in_specs = (rows, P()) + (vector,) * 6 + (matrix,) * 7 + (rows,)
    out_specs = (rows, rows) + (P(("ctx", "wsh")),) * 6 + (P("ctx", "wsh"),) * 7
    return jax.shard_map(body, mesh=mesh, in_specs=in_specs, out_specs=out_specs, check_vma=False)
```

```python
import functools
import math

import jax
import jax.numpy as jnp
from jax import lax
from jax.experimental import pallas as pl
from jax.experimental.pallas import tpu as pltpu
from jax.sharding import PartitionSpec as P

EPS = 1e-06
ROPE_BASE = 1000000.0
SCORE_SCALE = 0.0625
F32 = jnp.float32
BF16 = jnp.bfloat16
MESH = pl.DeviceIdType.MESH


def norm_gain(vector, gain):
    return vector * lax.rsqrt(jnp.mean(vector * vector, -1, keepdims=True) + EPS) * gain


def rotate(vector, cosine, sine):
    middle = vector.shape[-1] // 2
    first = vector[..., :middle]
    second = vector[..., middle:]
    return jnp.concatenate([first * cosine - second * sine, second * cosine + first * sine], -1)


def angle_tables(positions, head_size):
    middle = head_size // 2
    inverse = jnp.exp(
        jnp.arange(middle, dtype=F32) * (-2.0 * math.log(ROPE_BASE) / head_size)
    )
    theta = positions.astype(F32)[:, None] * inverse[None, :]
    return (jnp.cos(theta), jnp.sin(theta))


def swap(value):
    return lax.ppermute(value, "wsh", [(0, 1), (1, 0)])


def join_halves(mine, local, other):
    return jnp.where(
        mine == 0,
        jnp.concatenate([local, other], -1),
        jnp.concatenate([other, local], -1),
    )


def half_of(value, which):
    middle = value.shape[-1] // 2
    return jnp.where(which == 0, value[..., :middle], value[..., middle:])


def dot(left, right, dims):
    return lax.dot_general(left, right, (dims, ((), ())), preferred_element_type=F32)


def stack_heads(ref, half, block, heads, size):
    rows = slice(half * block, (half + 1) * block)
    return jnp.concatenate([ref[0, rows, h * size : (h + 1) * size] for h in range(heads)], 0)


def attend_forward_kernel(heads, chunk, q_ref, kv_ref, qpos_ref, kpos_ref, o_ref, mix_ref, tot_ref):
    shards, _, rows, pair = kv_ref.shape
    block, size = rows // 2, pair // 2
    queries = [stack_heads(q_ref, half, block, heads, size) for half in range(2)]
    stacked = heads * block
    sums = [jnp.zeros((stacked, size), F32) for _ in range(2)]
    totals = [jnp.zeros((stacked, 1), F32) for _ in range(2)]
    for first in range(0, shards, chunk):
        span = slice(first * block, (first + chunk) * block)
        for key_half in range(2):
            part = kv_ref[first : first + chunk, 0, key_half * block : (key_half + 1) * block, :]
            part = part.reshape(chunk * block, pair)
            keys, values = part[:, :size], part[:, size:]
            for half in range(key_half, 2):
                weights = jnp.exp(dot(queries[half], keys, ((1,), (1,))) * SCORE_SCALE)
                if half == key_half:
                    allowed = (
                        kpos_ref[key_half : key_half + 1, span]
                        <= qpos_ref[half * stacked : (half + 1) * stacked, :]
                    )
                    weights = jnp.where(allowed, weights, 0.0)
                low = weights.astype(BF16)
                totals[half] += jnp.sum(low.astype(F32), -1, keepdims=True)
                sums[half] += dot(low, values, ((1,), (0,)))
    for half in range(2):
        mixed = sums[half] / totals[half]
        mix_ref[0, half * stacked : (half + 1) * stacked, :] = mixed
        tot_ref[0, half * stacked : (half + 1) * stacked, :] = jnp.broadcast_to(
            totals[half], (stacked, tot_ref.shape[2])
        )
        for h in range(heads):
            o_ref[0, half * block : (half + 1) * block, h * size : (h + 1) * size] = mixed[
                h * block : (h + 1) * block
            ].astype(BF16)


def attend_backward_kernel(
    heads, chunk, q_ref, kv_ref, g_ref, mix_ref, tot_ref, qpos_ref, kpos_ref, dq_ref, dkv_ref
):
    shards, _, rows, pair = kv_ref.shape
    block, size = rows // 2, pair // 2
    stacked = heads * block
    queries, scaled, correction = [], [], []
    for half in range(2):
        queries.append(stack_heads(q_ref, half, block, heads, size))
        grad = stack_heads(g_ref, half, block, heads, size).astype(F32)
        span = slice(half * stacked, (half + 1) * stacked)
        total = tot_ref[0, span, :1]
        delta = jnp.sum(grad * mix_ref[0, span, :], -1, keepdims=True)
        scaled.append((grad / total).astype(BF16))
        correction.append(delta / total)
    grad_query = [jnp.zeros((stacked, size), F32) for _ in range(2)]
    for first in range(0, shards, chunk):
        span = slice(first * block, (first + chunk) * block)
        for key_half in range(2):
            part = kv_ref[first : first + chunk, 0, key_half * block : (key_half + 1) * block, :]
            part = part.reshape(chunk * block, pair)
            keys, values = part[:, :size], part[:, size:]
            grad_keys = jnp.zeros((chunk * block, size), F32)
            grad_values = jnp.zeros((chunk * block, size), F32)
            for half in range(key_half, 2):
                weights = jnp.exp(dot(queries[half], keys, ((1,), (1,))) * SCORE_SCALE)
                if half == key_half:
                    allowed = (
                        kpos_ref[key_half : key_half + 1, span]
                        <= qpos_ref[half * stacked : (half + 1) * stacked, :]
                    )
                    weights = jnp.where(allowed, weights, 0.0)
                low = weights.astype(BF16)
                grad_weights = dot(scaled[half], values, ((1,), (1,)))
                grad_scores = (weights * (grad_weights - correction[half])).astype(BF16)
                grad_query[half] += dot(grad_scores, keys, ((1,), (0,)))
                grad_keys += dot(grad_scores, queries[half], ((0,), (0,)))
                grad_values += dot(low, scaled[half], ((0,), (0,)))
            both = jnp.concatenate([grad_keys * SCORE_SCALE, grad_values], -1).astype(BF16)
            dkv_ref[first : first + chunk, 0, key_half * block : (key_half + 1) * block, :] = (
                both.reshape(chunk, block, pair)
            )
    for half in range(2):
        for h in range(heads):
            dq_ref[0, half * block : (half + 1) * block, h * size : (h + 1) * size] = (
                grad_query[half][h * block : (h + 1) * block] * SCORE_SCALE
            )


def whole(shape):
    return pl.BlockSpec(shape, lambda s: (0,) * len(shape))


def attend_forward(query_low, pairs, query_pos, key_pos, heads):
    sequences, rows, width = query_low.shape
    shards, _, _, pair = pairs.shape
    stacked = query_pos.shape[0]
    row = pl.BlockSpec((1, rows, width), lambda s: (s, 0, 0))
    stack = lambda last: pl.BlockSpec((1, stacked, last), lambda s: (s, 0, 0))
    return pl.pallas_call(
        functools.partial(attend_forward_kernel, heads, min(shards, 16)),
        grid=(sequences,),
        in_specs=[
            row,
            pl.BlockSpec((shards, 1, rows, pair), lambda s: (0, s, 0, 0)),
            whole(query_pos.shape),
            whole(key_pos.shape),
        ],
        out_specs=[row, stack(pair // 2), stack(128)],
        out_shape=[
            jax.ShapeDtypeStruct((sequences, rows, width), BF16),
            jax.ShapeDtypeStruct((sequences, stacked, pair // 2), F32),
            jax.ShapeDtypeStruct((sequences, stacked, 128), F32),
        ],
        name="attend_forward",
    )(query_low, pairs, query_pos, key_pos)


def attend_backward(query_low, pairs, grad_mixed, mixed, totals, query_pos, key_pos, heads):
    sequences, rows, width = query_low.shape
    shards, _, _, pair = pairs.shape
    stacked = query_pos.shape[0]
    row = pl.BlockSpec((1, rows, width), lambda s: (s, 0, 0))
    stack = lambda last: pl.BlockSpec((1, stacked, last), lambda s: (s, 0, 0))
    pairs_spec = pl.BlockSpec((shards, 1, rows, pair), lambda s: (0, s, 0, 0))
    return pl.pallas_call(
        functools.partial(attend_backward_kernel, heads, min(shards, 16)),
        grid=(sequences,),
        in_specs=[
            row,
            pairs_spec,
            row,
            stack(pair // 2),
            stack(128),
            whole(query_pos.shape),
            whole(key_pos.shape),
        ],
        out_specs=[row, pairs_spec],
        out_shape=[
            jax.ShapeDtypeStruct((sequences, rows, width), F32),
            jax.ShapeDtypeStruct(pairs.shape, BF16),
        ],
        name="attend_backward",
    )(query_low, pairs, grad_mixed, mixed, totals, query_pos, key_pos)


class Ring:
    def __init__(self, devices):
        self.chips = devices // 2
        me = lax.axis_index("ctx")
        self.core = me % 2
        chip = me // 2
        across = chip % 2
        deep = chip // 2
        self.place = deep + across * (self.chips - 1 - 2 * deep)
        self.partner = me + 1 - 2 * self.core
        self.right = self.device((self.place + 1) % self.chips, self.core)
        self.left = self.device((self.place + self.chips - 1) % self.chips, self.core)

    def device(self, place, core):
        side = place // (self.chips // 2)
        return 2 * (2 * (place + side * (self.chips - 1 - 2 * place)) + side) + core

    def enter(self, across=False):
        barrier = pltpu.get_barrier_semaphore()
        targets = [{"ctx": other} for other in (self.left, self.right, self.partner)]
        if across:
            targets.append({"wsh": 1 - lax.axis_index("wsh")})
        for target in targets:
            pl.semaphore_signal(barrier, inc=1, device_id=target, device_id_type=MESH)
        pl.semaphore_wait(barrier, len(targets))


def ring_sum_kernel(devices, pieces, arrays, ahead, *refs):
    parts, outs = refs[:arrays], refs[arrays : 2 * arrays]
    own, other, flow = (refs[(2 + i) * arrays : (3 + i) * arrays] for i in range(3))
    own_sem, put_sem, got_sem, send_sem, recv_sem = refs[5 * arrays :]
    ring = Ring(devices)
    chips = ring.chips

    def region(p):
        array, _, first, rows, start, cols = pieces[p]
        return array, pl.ds(first, rows), pl.ds(start, cols)

    def chunk(p, step):
        way = pieces[p][1]
        return (ring.place + 2 * chips + way * (-1 - step)) % chips

    def load(p, step):
        array, rows, cols = region(p)
        source = ring.device(chunk(p, step), ring.core)
        return pltpu.make_async_copy(
            parts[array].at[source, rows, cols],
            own[array].at[step, rows, cols],
            own_sem.at[p, step],
        )

    def give(p, step):
        array, rows, cols = region(p)
        source = ring.device(chunk(p, step), 1 - ring.core)
        return pltpu.make_async_remote_copy(
            src_ref=parts[array].at[source, rows, cols],
            dst_ref=other[array].at[step, rows, cols],
            send_sem=put_sem.at[p, step],
            recv_sem=got_sem.at[p, step],
            device_id={"ctx": ring.partner},
            device_id_type=MESH,
        )

    def pass_on(p, step):
        array, rows, cols = region(p)
        way = pieces[p][1]
        return pltpu.make_async_remote_copy(
            src_ref=flow[array].at[step, rows, cols],
            dst_ref=flow[array].at[step + 1, rows, cols],
            send_sem=send_sem.at[p, step],
            recv_sem=recv_sem.at[p, step],
            device_id={"ctx": ring.right if way > 0 else ring.left},
            device_id_type=MESH,
        )

    def fetch(step):
        for p in range(len(pieces)):
            load(p, step).start()
            give(p, step).start()

    def add(p, step, first, last):
        array, _, row, rows, start, cols = pieces[p]
        width = 128 if cols % 128 == 0 else cols
        while width < 512 and cols % (2 * width) == 0:
            width *= 2
        rows = pl.ds(row, rows)

        def group(i, carry):
            at = start + i * width
            if cols > width:
                at = pl.multiple_of(at, 128)
            where = pl.ds(at, width)
            total = own[array][step, rows, where].astype(F32) + other[array][
                step, rows, where
            ].astype(F32)
            if not first:
                total += flow[array][step, rows, where].astype(F32)
            if last:
                outs[array][rows, where] = total.astype(outs[array].dtype)
            else:
                flow[array][step, rows, where] = total.astype(flow[array].dtype)
            return carry

        if cols == width:
            group(0, 0)
        else:
            lax.fori_loop(0, cols // width, group, 0)

    def work(step, first=False, last=False):
        for p in range(len(pieces)):
            load(p, step).wait()
            give(p, step).wait_recv()
            if not first:
                pass_on(p, step - 1).wait_recv()
            add(p, step, first, last)
            if not last:
                pass_on(p, step).start()

    for p in range(len(pieces)):
        load(p, 0).start()
    ring.enter()
    for p in range(len(pieces)):
        give(p, 0).start()
    for step in range(1, min(ahead, chips)):
        fetch(step)
    work(0, first=True)

    def middle(step, carry):
        @pl.when(step + ahead - 1 < chips)
        def _():
            fetch(step + ahead - 1)

        work(step)
        return carry

    lax.fori_loop(1, chips - 1, middle, 0)
    work(chips - 1, last=True)

    def drain(step, carry):
        for p in range(len(pieces)):
            give(p, step).wait_send()

            @pl.when(step < chips - 1)
            def _():
                pass_on(p, step).wait_send()

        return carry

    lax.fori_loop(0, chips, drain, 0)


def ring_sum(parts, pieces, devices, collective_id, ahead=3, name="ring_sum"):
    chips, count, arrays = devices // 2, len(pieces), len(parts)
    slots = [pltpu.VMEM((chips,) + p.shape[1:], p.dtype) for p in parts]
    return pl.pallas_call(
        functools.partial(ring_sum_kernel, devices, pieces, arrays, ahead),
        out_shape=[jax.ShapeDtypeStruct(p.shape[1:], F32) for p in parts],
        in_specs=[pl.BlockSpec(memory_space=pl.ANY)] * arrays,
        out_specs=[pl.BlockSpec(memory_space=pltpu.VMEM)] * arrays,
        scratch_shapes=slots * 3
        + [pltpu.SemaphoreType.DMA((count, chips))] * 3
        + [pltpu.SemaphoreType.DMA((count, chips - 1))] * 2,
        compiler_params=pltpu.CompilerParams(
            collective_id=collective_id, has_side_effects=True, vmem_limit_bytes=64000 * 1024
        ),
        name=name,
    )(*parts)


def split_ways(parts):
    pieces, lead = [], 1
    for i, p in enumerate(parts):
        _, rows, cols = p.shape
        tiles = cols // 128
        if cols % 128 == 0 and tiles > 1:
            left = (tiles + (1 if lead > 0 else 0)) // 2 * 128
            if tiles % 2:
                lead = -lead
            pieces.append((i, 1, 0, rows, 0, left))
            pieces.append((i, -1, 0, rows, left, cols - left))
        elif rows % 32 == 0:
            pieces.append((i, 1, 0, rows // 2, 0, cols))
            pieces.append((i, -1, rows // 2, rows // 2, 0, cols))
        else:
            pieces.append((i, 1, 0, rows, 0, cols))
    return tuple(pieces)


def sum_over_ctx(parts, pieces, devices, collective_id):
    if all(p.shape[1] % 8 == 0 for p in parts):
        return ring_sum(parts, pieces, devices, collective_id)
    return [
        lax.psum_scatter(p, "ctx", scatter_dimension=0, tiled=False).astype(F32) for p in parts
    ]


def front_kernel(
    devices,
    tokens_ref,
    gains_ref,
    cos_ref,
    sin_ref,
    key_weight,
    value_weight,
    query_weight,
    out_weight,
    pairs_ref,
    normed_ref,
    key_ref,
    all_gains_ref,
    key_other,
    value_other,
    query_other,
    out_other,
    gains_other,
    cross_send,
    cross_recv,
    side_send,
    side_recv,
    flow_send,
    flow_recv,
    twin_send,
    twin_recv,
):
    ring = Ring(devices)
    chips, far = ring.chips, ring.chips // 2
    me = lax.axis_index("ctx")
    mine = lax.axis_index("wsh")
    sequences, rows, width = tokens_ref.shape
    count = sequences * rows
    weights = (
        (key_weight, key_other),
        (value_weight, value_other),
        (query_weight, query_other),
        (out_weight, out_other),
    )

    def cross(i):
        if i == len(weights):
            source, target = gains_ref, gains_other
        else:
            local, other = weights[i]
            half = local.shape[0] // 2
            part = pl.ds(pl.multiple_of(ring.core * half, 16), half)
            source, target = local.at[part], other.at[part]
        return pltpu.make_async_remote_copy(
            src_ref=source,
            dst_ref=target,
            send_sem=cross_send.at[i],
            recv_sem=cross_recv.at[i],
            device_id={"wsh": 1 - mine},
            device_id_type=MESH,
        )

    def side(i):
        other = weights[i][1]
        half = other.shape[0] // 2
        part = pl.ds(pl.multiple_of(ring.core * half, 16), half)
        return pltpu.make_async_remote_copy(
            src_ref=other.at[part],
            dst_ref=other.at[part],
            send_sem=side_send.at[i],
            recv_sem=side_recv.at[i],
            device_id={"ctx": ring.partner},
            device_id_type=MESH,
        )

    def flow(way, seq, hop):
        stream = (1 if way < 0 else 0) * sequences + seq
        place = (ring.place + chips - way * hop) % chips
        block = pairs_ref.at[ring.device(place, ring.core), seq]
        return pltpu.make_async_remote_copy(
            src_ref=block,
            dst_ref=block,
            send_sem=flow_send.at[stream, hop],
            recv_sem=flow_recv.at[stream, hop],
            device_id={"ctx": ring.right if way > 0 else ring.left},
            device_id_type=MESH,
        )

    def twin(way, seq, hop):
        stream = (1 if way < 0 else 0) * sequences + seq
        place = (ring.place + chips - way * hop) % chips
        block = pairs_ref.at[ring.device(place, ring.core), seq]
        return pltpu.make_async_remote_copy(
            src_ref=block,
            dst_ref=block,
            send_sem=twin_send.at[stream, hop],
            recv_sem=twin_recv.at[stream, hop],
            device_id={"ctx": ring.partner},
            device_id_type=MESH,
        )

    def hops(way, seq):
        return far if (seq % 2 == 0) == (way > 0) else far - 1

    ring.enter(across=True)
    order = (len(weights), 0, 1, 2, 3)
    for i in order:
        cross(i).start()
    inputs = tokens_ref[...].reshape(count, width).astype(F32)
    scale = lax.rsqrt(jnp.mean(inputs * inputs, -1, keepdims=True) + EPS)
    cross(len(weights)).wait_recv()
    all_gains_ref[...] = gains_ref[...] + gains_other[...]
    normed_ref[...] = (inputs * scale * all_gains_ref[0:1, :]).astype(BF16)
    for i in (0, 1):
        cross(i).wait_recv()
        side(i).start()
    key_here = dot(normed_ref[...], key_weight[...], ((1,), (0,)))
    value_here = dot(normed_ref[...], value_weight[...], ((1,), (0,)))
    for i in (0, 1):
        side(i).wait_recv()
    key_there = dot(normed_ref[...], key_other[...], ((1,), (0,)))
    value_there = dot(normed_ref[...], value_other[...], ((1,), (0,)))
    lower = mine == 0
    first = jnp.where(lower, key_here, key_there)
    second = jnp.where(lower, key_there, key_here)
    middle = first.shape[1]
    key_ref[:, :middle] = first
    key_ref[:, middle:] = second
    power = jnp.sum(first * first, -1, keepdims=True) + jnp.sum(second * second, -1, keepdims=True)
    scale = lax.rsqrt(power / (2 * middle) + EPS)
    gain = all_gains_ref[4:5, 2 * middle : 4 * middle]
    first = first * scale * gain[:, :middle]
    second = second * scale * gain[:, middle:]
    cosine, sine = cos_ref[...], sin_ref[...]
    value_first = jnp.where(lower, value_here, value_there).astype(BF16)
    value_second = jnp.where(lower, value_there, value_here).astype(BF16)
    for seq in range(sequences):
        span = slice(seq * rows, (seq + 1) * rows)
        head, tail = first[span], second[span]
        pairs_ref[me, seq, :, 0 * middle : 1 * middle] = (head * cosine - tail * sine).astype(BF16)
        pairs_ref[me, seq, :, 1 * middle : 2 * middle] = (tail * cosine + head * sine).astype(BF16)
        pairs_ref[me, seq, :, 2 * middle : 3 * middle] = value_first[span]
        pairs_ref[me, seq, :, 3 * middle : 4 * middle] = value_second[span]
    streams = [(way, seq) for seq in range(sequences) for way in (1, -1)]
    for hop in range(far + 1):
        for way, seq in streams:
            if hop > hops(way, seq):
                continue
            if hop > 0:
                flow(way, seq, hop - 1).wait_recv()
            if hop < hops(way, seq):
                flow(way, seq, hop).start()
            if hop > 0 or way > 0:
                twin(way, seq, hop).start()
    for i in (2, 3):
        cross(i).wait_recv()
        side(i).start()
    for hop in range(far + 1):
        for way, seq in streams:
            if hop > hops(way, seq):
                continue
            if hop > 0 or way > 0:
                twin(way, seq, hop).wait()
            if hop < hops(way, seq):
                flow(way, seq, hop).wait_send()
    for i in order:
        cross(i).wait_send()
    for i in (2, 3):
        side(i).wait()
    for i in (0, 1):
        side(i).wait_send()


def front(tokens, gains, cosine, sine, weights, devices, collective_id):
    sequences, rows, width = tokens.shape
    size = 2 * cosine.shape[1]
    far = devices // 4
    here, there = pl.BlockSpec(memory_space=pltpu.VMEM), pl.BlockSpec(memory_space=pl.ANY)
    streams = pltpu.SemaphoreType.DMA((2 * sequences, far + 1))
    like = lambda a: jax.ShapeDtypeStruct(a.shape, a.dtype)
    return pl.pallas_call(
        functools.partial(front_kernel, devices),
        in_specs=[here] * 6 + [there] * 2,
        out_specs=[here] * 6 + [there] * 2,
        out_shape=[
            jax.ShapeDtypeStruct((devices, sequences, rows, 2 * size), BF16),
            jax.ShapeDtypeStruct((sequences * rows, width), BF16),
            jax.ShapeDtypeStruct((sequences * rows, size), F32),
            like(gains),
        ]
        + [like(w) for w in weights],
        scratch_shapes=[pltpu.VMEM(gains.shape, gains.dtype)]
        + [pltpu.SemaphoreType.DMA((5,))] * 2
        + [pltpu.SemaphoreType.DMA((4,))] * 2
        + [streams] * 4,
        compiler_params=pltpu.CompilerParams(
            collective_id=collective_id, has_side_effects=True, vmem_limit_bytes=60000 * 1024
        ),
        name="front",
    )(tokens, gains, cosine, sine, *weights)


class RingSum:
    def __init__(self, ring, pieces, parts, own, other, flow, outs, sems):
        self.ring, self.pieces, self.parts, self.own = ring, pieces, parts, own
        self.other, self.flow, self.outs = other, flow, outs
        self.put_sem, self.got_sem, self.send_sem, self.recv_sem = sems[:4]
        self.own_sem = sems[4] if own is not None else None
        self.last = ring.chips - 1

    def region(self, p):
        array, _, first, rows, start, cols = self.pieces[p]
        return array, pl.ds(first, rows), pl.ds(start, cols)

    def owner(self, p, step, core):
        way = self.pieces[p][1]
        chips = self.ring.chips
        return self.ring.device((self.ring.place + 2 * chips + way * (-1 - step)) % chips, core)

    def load(self, p, step):
        array, rows, cols = self.region(p)
        slot = step % self.own[array].shape[0]
        return pltpu.make_async_copy(
            self.parts[array].at[self.owner(p, step, self.ring.core), rows, cols],
            self.own[array].at[slot, rows, cols],
            self.own_sem.at[p, step],
        )

    def give(self, p, step):
        array, rows, cols = self.region(p)
        return pltpu.make_async_remote_copy(
            src_ref=self.parts[array].at[self.owner(p, step, 1 - self.ring.core), rows, cols],
            dst_ref=self.other[array].at[step, rows, cols],
            send_sem=self.put_sem.at[p, step],
            recv_sem=self.got_sem.at[p, step],
            device_id={"ctx": self.ring.partner},
            device_id_type=MESH,
        )

    def hop(self, p, step):
        array, rows, cols = self.region(p)
        way = self.pieces[p][1]
        return pltpu.make_async_remote_copy(
            src_ref=self.flow[array].at[step, rows, cols],
            dst_ref=self.flow[array].at[step + 1, rows, cols],
            send_sem=self.send_sem.at[p, step],
            recv_sem=self.recv_sem.at[p, step],
            device_id={"ctx": self.ring.right if way > 0 else self.ring.left},
            device_id_type=MESH,
        )

    def load_all(self, step):
        for p in range(len(self.pieces)):
            self.load(p, step).start()

    def give_all(self, step):
        for p in range(len(self.pieces)):
            self.give(p, step).start()

    def work(self, p, step):
        array, _, row, rows, start, cols = self.pieces[p]
        if self.own is not None:
            self.load(p, step).wait()
            mine, at_mine = self.own[array], step % self.own[array].shape[0]
        else:
            mine, at_mine = self.parts[array], self.owner(p, step, self.ring.core)
        self.give(p, step).wait_recv()
        if step > 0:
            self.hop(p, step - 1).wait_recv()
        width = 128 if cols % 128 == 0 else cols
        while width < 512 and cols % (2 * width) == 0:
            width *= 2
        rows = pl.ds(row, rows)

        def group(i, carry):
            at = start + i * width
            if cols > width:
                at = pl.multiple_of(at, 128)
            where = pl.ds(at, width)
            total = mine[at_mine, rows, where].astype(F32)
            total += self.other[array][step, rows, where].astype(F32)
            if step > 0:
                total += self.flow[array][step, rows, where].astype(F32)
            if step == self.last:
                self.outs[array][rows, where] = total.astype(self.outs[array].dtype)
            else:
                self.flow[array][step, rows, where] = total.astype(self.flow[array].dtype)
            return carry

        if cols == width:
            group(0, 0)
        else:
            lax.fori_loop(0, cols // width, group, 0)
        if step < self.last:
            self.hop(p, step).start()

    def drain(self):
        for p in range(len(self.pieces)):
            for step in range(self.last + 1):
                self.give(p, step).wait_send()
                if step < self.last:
                    self.hop(p, step).wait_send()


def norm_back(upstream, vector, gain):
    scale = lax.rsqrt(jnp.mean(vector * vector, -1, keepdims=True) + EPS)
    normal = vector * scale
    weighted = upstream * gain
    back = scale * (weighted - normal * jnp.mean(weighted * normal, -1, keepdims=True))
    return back, jnp.sum(upstream * normal, 0, keepdims=True)


GELU_SCALE = math.sqrt(2.0 / math.pi)
GELU_CUBE = 0.044715


def feed_forward_kernel(
    attended_ref,
    tokens_ref,
    cotangent_ref,
    gains_ref,
    gate_hbm,
    up_hbm,
    down_hbm,
    output_ref,
    hidden_back_ref,
    attended_back_ref,
    gain_part_ref,
    down_grad_hbm,
    gate_grad_hbm,
    up_grad_hbm,
    gate_weight,
    up_weight,
    down_weight,
    ff_rows,
    low_rows,
    ff_turned,
    low_turned,
    gate,
    upward,
    activated,
    partial,
    part_send,
    part_recv,
    back_send,
    back_recv,
    hidden_ref,
    staging,
    load_sem,
    store_sem,
    cross_send,
    cross_recv,
):
    count, width = attended_ref.shape
    hidden_units = gate_weight.shape[1]
    block = part_send.shape[0] // 2
    chunk = staging.shape[2]
    whole_chunks = hidden_units // chunk
    rest = hidden_units - whole_chunks * chunk
    mine = lax.axis_index("wsh")
    weights = ((gate_hbm, gate_weight), (up_hbm, up_weight), (down_hbm, down_weight))

    def load(w, at, size, index):
        source, target = weights[w]
        cols = pl.ds(at, size)
        return pltpu.make_async_copy(source.at[:, cols], target.at[:, cols], load_sem.at[w, index])

    def chunks(work):
        def step(c, carry):
            work(pl.multiple_of(c * chunk, 128), chunk, c)
            return carry

        lax.fori_loop(0, whole_chunks, step, 0)
        if rest:
            work(whole_chunks * chunk, rest, whole_chunks)

    def across(kind, piece, source, target):
        return pltpu.make_async_remote_copy(
            src_ref=source,
            dst_ref=target,
            send_sem=cross_send.at[kind, piece],
            recv_sem=cross_recv.at[kind, piece],
            device_id={"wsh": 1 - mine},
            device_id_type=MESH,
        )

    def swap_rows(kind, ref, piece):
        first = pl.multiple_of(piece * block, block)
        return across(
            kind, piece, ref.at[pl.ds(first, block)], ref.at[pl.ds(count + first, block)]
        )

    def swap_parts(kind, source, target, piece):
        lines = pl.ds(pl.multiple_of(piece * block, block), block)
        return across(kind, piece, source.at[lines], target.at[lines])

    def start_load(at, size, index):
        for w in range(3):
            load(w, at, size, index).start()

    chunks(start_load)
    barrier = pltpu.get_barrier_semaphore()
    pl.semaphore_signal(barrier, inc=1, device_id={"wsh": 1 - mine}, device_id_type=MESH)

    attended = attended_ref[...]
    scale = lax.rsqrt(jnp.mean(attended * attended, -1, keepdims=True) + EPS)
    hidden = tokens_ref[...].astype(F32) + attended * scale * gains_ref[1:2, :]
    hidden_ref[...] = hidden
    scale = lax.rsqrt(jnp.mean(hidden * hidden, -1, keepdims=True) + EPS)
    ff_rows[:count, :] = (hidden * scale * gains_ref[2:3, :]).astype(BF16)
    pl.semaphore_wait(barrier, 1)
    for piece in range(2):
        swap_rows(0, ff_rows, piece).start()

    def forward(turn, carry):
        b = (2 * turn) % 5 - (2 * turn) % 5 // 4

        @pl.when(b >= 2)
        def _():
            swap_rows(0, ff_rows, b - 2).wait_recv()

        lines = pl.ds(pl.multiple_of(b * block, block), block)

        def columns(at, size, index):
            @pl.when(b == 0)
            def _():
                for w in range(3):
                    load(w, at, size, index).wait()

            cols = pl.ds(at, size)
            g = dot(ff_rows[lines, :], gate_weight[:, cols], ((1,), (0,)))
            u = dot(ff_rows[lines, :], up_weight[:, cols], ((1,), (0,)))
            t = jnp.tanh(GELU_SCALE * (g + GELU_CUBE * g * g * g))
            gate[lines, cols] = g.astype(BF16)
            upward[lines, cols] = u.astype(BF16)
            activated[lines, cols] = (0.5 * g * (1.0 + t) * u).astype(BF16)

        chunks(columns)
        value = dot(activated[lines, :], down_weight[...], ((1,), (1,)))

        @pl.when(b < 2)
        def _():
            partial[lines, :] = value

        @pl.when(b >= 2)
        def _():
            there = pl.ds(pl.multiple_of((b - 2) * block, block), block)
            part_send[there, :] = value.astype(BF16)
            swap_parts(1, part_send, part_recv, b - 2).start()

        return carry

    lax.fori_loop(0, 4, forward, 0)
    ff_turned[...] = ff_rows[...].T
    for piece in range(2):
        swap_parts(1, part_send, part_recv, piece).wait_recv()
    lowered = partial[...] + part_recv[...].astype(F32)
    cotangent = cotangent_ref[...].astype(F32)
    back, part = norm_back(cotangent, lowered, gains_ref[3:4, :])
    low_rows[:count, :] = back.astype(BF16)
    for piece in range(2):
        swap_rows(2, low_rows, piece).start()
    gain_part_ref[...] = jnp.zeros_like(gain_part_ref)
    gain_part_ref[3:4, :] = part
    scale = lax.rsqrt(jnp.mean(lowered * lowered, -1, keepdims=True) + EPS)
    output_ref[...] = (hidden_ref[...] + lowered * scale * gains_ref[3:4, :]).astype(BF16)

    def backward(turn, carry):
        b = (2 * turn) % 5 - (2 * turn) % 5 // 4

        @pl.when(b >= 2)
        def _():
            swap_rows(2, low_rows, b - 2).wait_recv()

        lines = pl.ds(pl.multiple_of(b * block, block), block)

        def columns(at, size, index):
            cols = pl.ds(at, size)
            d = dot(low_rows[lines, :], down_weight[:, cols], ((1,), (0,)))
            g = gate[lines, cols].astype(F32)
            u = upward[lines, cols].astype(F32)
            square = g * g
            t = jnp.tanh(GELU_SCALE * (g + GELU_CUBE * square * g))
            half = 0.5 * (1.0 + t)
            slope = half + 0.5 * g * (1.0 - t * t) * (
                GELU_SCALE * (1.0 + 3.0 * GELU_CUBE * square)
            )
            gate[lines, cols] = (d * u * slope).astype(BF16)
            upward[lines, cols] = (d * g * half).astype(BF16)

        chunks(columns)
        value = dot(gate[lines, :], gate_weight[...], ((1,), (1,)))
        value += dot(upward[lines, :], up_weight[...], ((1,), (1,)))

        @pl.when(b < 2)
        def _():
            partial[lines, :] = value

        @pl.when(b >= 2)
        def _():
            there = pl.ds(pl.multiple_of((b - 2) * block, block), block)
            back_send[there, :] = value.astype(BF16)
            swap_parts(3, back_send, back_recv, b - 2).start()

        return carry

    lax.fori_loop(0, 4, backward, 0)
    low_turned[...] = low_rows[...].T

    grads = (
        (low_turned, activated, down_grad_hbm),
        (ff_turned, gate, gate_grad_hbm),
        (ff_turned, upward, up_grad_hbm),
    )

    def store(m, at, size, index):
        cols = pl.ds(at, size)
        return pltpu.make_async_copy(
            staging.at[index % 2, :, pl.ds(0, size)], grads[m][2].at[:, cols], store_sem.at[m, index]
        )

    for m in range(3):
        left, right, _ = grads[m]

        def columns(at, size, index, m=m, left=left, right=right):
            @pl.when(index >= 2)
            def _():
                store(m, 0, chunk, index - 2).wait()

            for top in range(0, width, width // 2):
                lines = slice(top, top + width // 2)
                staging[index % 2, lines, :size] = dot(
                    left[lines, :], right[:, pl.ds(at, size)], ((1,), (0,))
                ).astype(BF16)
            store(m, at, size, index).start()

        chunks(columns)
        last = whole_chunks + (1 if rest else 0)
        for index in range(max(last - 2, 0), last):
            store(m, 0, rest if index == whole_chunks else chunk, index).wait()

    for piece in range(2):
        swap_parts(3, back_send, back_recv, piece).wait_recv()
    upstream = partial[...] + back_recv[...].astype(F32)
    back, part = norm_back(upstream, hidden_ref[...], gains_ref[2:3, :])
    gain_part_ref[2:3, :] = part
    back += cotangent_ref[...].astype(F32)
    hidden_back_ref[...] = back
    back, part = norm_back(back, attended_ref[...], gains_ref[1:2, :])
    gain_part_ref[1:2, :] = part
    attended_back_ref[...] = back.astype(BF16)
    for piece in range(2):
        swap_rows(0, ff_rows, piece).wait_send()
        swap_parts(1, part_send, part_recv, piece).wait_send()
        swap_rows(2, low_rows, piece).wait_send()
        swap_parts(3, back_send, back_recv, piece).wait_send()


def feed_forward(attended, tokens, cotangent, gains, weights, collective_id):
    count, width = attended.shape
    hidden_units = weights[0].shape[1]
    chunk = 512
    pieces = -(-hidden_units // chunk)
    here, there = pl.BlockSpec(memory_space=pltpu.VMEM), pl.BlockSpec(memory_space=pl.ANY)
    like = lambda shape, kind: jax.ShapeDtypeStruct(shape, kind)
    matrix = (width, hidden_units)
    return pl.pallas_call(
        feed_forward_kernel,
        in_specs=[here] * 4 + [there] * 3,
        out_specs=[here] * 4 + [there] * 3,
        out_shape=[
            like((count, width), BF16),
            like((count, width), F32),
            like((count, width), BF16),
            like(gains.shape, F32),
        ]
        + [like(matrix, BF16)] * 3,
        scratch_shapes=[pltpu.VMEM(matrix, BF16)] * 3
        + [pltpu.VMEM((2 * count, width), BF16)] * 2
        + [pltpu.VMEM((width, 2 * count), BF16)] * 2
        + [pltpu.VMEM((2 * count, hidden_units), BF16)] * 3
        + [pltpu.VMEM((count, width), F32)]
        + [pltpu.VMEM((count, width), BF16)] * 4
        + [
            pltpu.VMEM((count, width), F32),
            pltpu.VMEM((2, width, chunk), BF16),
            pltpu.SemaphoreType.DMA((3, pieces)),
            pltpu.SemaphoreType.DMA((3, pieces)),
            pltpu.SemaphoreType.DMA((4, 2)),
            pltpu.SemaphoreType.DMA((4, 2)),
        ],
        compiler_params=pltpu.CompilerParams(
            collective_id=collective_id, has_side_effects=True, vmem_limit_bytes=67043328
        ),
        name="feed_forward",
    )(attended, tokens, cotangent, gains, *weights)


def turn_back(upstream, cosine, sine):
    middle = upstream.shape[-1] // 2
    first, second = upstream[:, :middle], upstream[:, middle:]
    return jnp.concatenate([first * cosine + second * sine, second * cosine - first * sine], -1)


def back_kernel(devices, heads, ff_pieces, kv_pieces, attn_pieces, names, *refs):
    r = dict(zip(names, refs))
    ring = Ring(devices)
    chips = ring.chips
    mine = lax.axis_index("wsh")
    sequences, rows, _ = r["query"].shape
    size = r["key_raw"].shape[1]
    count = sequences * rows
    block = rows // 2
    stacked = heads * block

    ff = RingSum(
        ring,
        ff_pieces,
        [r["part_down"], r["part_gate"], r["part_up"]],
        [r[f"ff_own{i}"] for i in range(3)],
        [r[f"ff_other{i}"] for i in range(3)],
        [r[f"ff_flow{i}"] for i in range(3)],
        [r["grad_down"], r["grad_gate"], r["grad_up"]],
        [r["ff_put"], r["ff_got"], r["ff_send"], r["ff_recv"], r["ff_load"]],
    )
    kv = RingSum(
        ring,
        kv_pieces,
        [r["pairs"]],
        None,
        [r["kv_other"]],
        [r["kv_flow"]],
        [r["kv_sum"]],
        [r["kv_put"], r["kv_got"], r["kv_send"], r["kv_recv"]],
    )
    attn = RingSum(
        ring,
        attn_pieces,
        [r["qkv_part"], r["out_part"]],
        None,
        [r["qkv_other"], r["out_other"]],
        [r["qkv_flow"], r["out_flow"]],
        [r["grad_qkv"], r["grad_out"]],
        [r["at_put"], r["at_got"], r["at_send"], r["at_recv"]],
    )

    def brought(i):
        name = BROUGHT[i]
        return pltpu.make_async_copy(r["in_" + name], r[name], r["bring"].at[i])

    def need(*wanted):
        for name in wanted:
            brought(BROUGHT.index(name)).wait()

    def across(i, source, target):
        return pltpu.make_async_remote_copy(
            src_ref=source,
            dst_ref=target,
            send_sem=r["cross_send"].at[i],
            recv_sem=r["cross_recv"].at[i],
            device_id={"wsh": 1 - mine},
            device_id_type=MESH,
        )

    out_swap = across(0, r["att_send"], r["att_across"])
    col_swap = across(1, r["col_send"], r["col_rows"].at[pl.ds(count, count)])
    gain_swap = across(2, r["gain_own"], r["gain_across"])
    gain_twin = pltpu.make_async_remote_copy(
        src_ref=r["gain_pair"],
        dst_ref=r["gain_twin"],
        send_sem=r["twin_send"].at[0],
        recv_sem=r["twin_recv"].at[0],
        device_id={"ctx": ring.partner},
        device_id_type=MESH,
    )

    def gain_hop(way, step):
        return pltpu.make_async_remote_copy(
            src_ref=r["gain_flow"].at[way, step],
            dst_ref=r["gain_flow"].at[way, step + 1],
            send_sem=r["gain_send"].at[way, step],
            recv_sem=r["gain_recv"].at[way, step],
            device_id={"ctx": ring.right if way == 0 else ring.left},
            device_id_type=MESH,
        )

    gain_hops = (chips // 2, chips - 1 - chips // 2)

    def attention(seq):
        queries, scaled, correction = [], [], []
        for half in range(2):
            span = slice(half * stacked, (half + 1) * stacked)
            lines = slice(half * block, (half + 1) * block)
            cut = lambda ref: jnp.concatenate(
                [ref[seq, lines, h * size : (h + 1) * size] for h in range(heads)], 0
            )
            queries.append(cut(r["query"]))
            grad = cut(r["grad_mixed"]).astype(F32)
            total = r["totals"][seq, span, :1]
            delta = jnp.sum(grad * r["mixed"][seq, span, :], -1, keepdims=True)
            scaled.append((grad / total).astype(BF16))
            correction.append(delta / total)
        grad_query = [jnp.zeros((stacked, size), F32) for _ in range(2)]
        for key_half in range(2):
            lines = pl.ds(seq * rows + key_half * block, block)
            part = r["pairs"][:, lines, :].reshape(devices * block, 2 * size)
            keys, values = part[:, :size], part[:, size:]
            grad_keys = jnp.zeros((devices * block, size), F32)
            grad_values = jnp.zeros((devices * block, size), F32)
            for half in range(key_half, 2):
                weights = jnp.exp(dot(queries[half], keys, ((1,), (1,))) * SCORE_SCALE)
                if half == key_half:
                    allowed = (
                        r["key_pos"][key_half : key_half + 1, :]
                        <= r["query_pos"][half * stacked : (half + 1) * stacked, :]
                    )
                    weights = jnp.where(allowed, weights, 0.0)
                low = weights.astype(BF16)
                grad_weights = dot(scaled[half], values, ((1,), (1,)))
                grad_scores = (weights * (grad_weights - correction[half])).astype(BF16)
                grad_query[half] += dot(grad_scores, keys, ((1,), (0,)))
                grad_keys += dot(grad_scores, queries[half], ((0,), (0,)))
                grad_values += dot(low, scaled[half], ((0,), (0,)))
            both = jnp.concatenate([grad_keys * SCORE_SCALE, grad_values], -1).astype(BF16)
            r["pairs"][:, lines, :] = both.reshape(devices, block, 2 * size)
        for half in range(2):
            lines = pl.ds(seq * rows + half * block, block)
            for h in range(heads):
                r["grad_query"][lines, h * size : (h + 1) * size] = (
                    grad_query[half][h * block : (h + 1) * block] * SCORE_SCALE
                )

    def pick(value, which):
        middle = value.shape[1] // 2
        return jnp.where(which == 0, value[:, :middle], value[:, middle:])

    def projections():
        need("query_raw", "key_raw", "cosine", "sine", "gains")
        cosine, sine = r["cosine"][...], r["sine"][...]
        gain = r["gains"][4:5, :size]
        total = jnp.zeros((1, size), F32)
        lows = []
        for h in range(heads):
            cols = slice(h * size, (h + 1) * size)
            back, part = norm_back(
                turn_back(r["grad_query"][:, cols], cosine, sine), r["query_raw"][:, cols], gain
            )
            total += part
            r["query_low"][:, cols] = back.astype(BF16)
        back, key_total = norm_back(
            turn_back(r["kv_sum"][:, :size], cosine, sine),
            r["key_raw"][...],
            r["gains"][4:5, size : 2 * size],
        )
        r["pair_low"][:, :size] = back.astype(BF16)
        r["pair_low"][:, size:] = r["kv_sum"][:, size:].astype(BF16)
        first = 0
        for value in (
            r["query_low"][...],
            r["pair_low"][:, :size],
            r["pair_low"][:, size:],
        ):
            cols = slice(first, first + value.shape[1] // 2)
            r["col_rows"][:count, cols] = pick(value, mine)
            r["col_send"][:, cols] = pick(value, 1 - mine)
            first += value.shape[1] // 2
        col_swap.start()
        need("weight_query", "weight_pair", "tokens", "grad_hidden", "gain_part")
        grad_normed = dot(r["query_low"][...], r["weight_query"][...], ((1,), (1,)))
        grad_normed += dot(r["pair_low"][...], r["weight_pair"][...], ((1,), (1,)))
        back, part = norm_back(grad_normed, r["tokens"][...].astype(F32), r["gains"][0:1, :])
        r["grad_tokens"][...] = back + r["grad_hidden"][...]
        r["gain_own"][...] = r["gain_part"][...]
        r["gain_own"][0:1, :] = part
        r["gain_own"][4:5, :size] = total
        r["gain_own"][4:5, size : 2 * size] = key_total
        gain_swap.start()

    def out_part():
        need("mixed_turned", "att_own")
        out_swap.wait_recv()
        _, lines, cols = r["out_part"].shape
        value = dot(r["mixed_turned"][:, :count], r["att_own"][...], ((1,), (0,)))
        value += dot(r["mixed_turned"][:, count:], r["att_across"][...], ((1,), (0,)))
        r["out_part"][...] = value.reshape(devices, lines, cols).astype(BF16)

    def qkv_part():
        need("normed_turned")
        col_swap.wait_recv()
        _, lines, cols = r["qkv_part"].shape
        width = 256
        for first in range(0, cols, width):
            value = dot(
                r["normed_turned"][...], r["col_rows"][:, first : first + width], ((1,), (0,))
            )
            r["qkv_part"][:, :, first : first + width] = value.reshape(
                devices, lines, width
            ).astype(BF16)

    def gains_step(step):
        if step == 0:
            gain_swap.wait_recv()
            r["gain_pair"][...] = r["gain_own"][...] + r["gain_across"][...]
            gain_twin.start()
        elif step == 1:
            gain_twin.wait_recv()
            both = r["gain_pair"][...] + r["gain_twin"][...]
            r["gain_flow"][0, 0] = both
            r["gain_flow"][1, 0] = both
            r["gain_sum"][...] = both
            for way in range(2):
                gain_hop(way, 0).start()
        else:
            for way in range(2):
                if step - 2 < gain_hops[way]:
                    gain_hop(way, step - 2).wait_recv()
                    if step - 1 < gain_hops[way]:
                        gain_hop(way, step - 1).start()
                    r["gain_sum"][...] += r["gain_flow"][way, step - 1]

    def ff_step(step, extra=()):
        extra = list(extra)
        if step + 1 < chips:
            ff.load_all(step + 1)
        if step + 2 < chips:
            ff.give_all(step + 2)
        for p in range(len(ff_pieces)):
            ff.work(p, step)
            if p % 2 == 1 and extra:
                extra.pop(0)()
        for left in extra:
            left()

    def kv_step(step):
        def run():
            for p in range(len(kv_pieces)):
                kv.work(p, step)

        return run

    def attn_step(step):
        def run():
            gains_step(step)
            for p in range(len(attn_pieces)):
                attn.work(p, step)

        return run

    ff.load_all(0)
    for i in range(len(BROUGHT)):
        brought(i).start()
    ring.enter(across=True)
    ff.give_all(0)
    ff.give_all(1)
    need("att_send")
    out_swap.start()
    ff_step(0)
    need("pairs", "query", "grad_mixed", "mixed", "totals", "query_pos", "key_pos")
    for seq in range(sequences):
        attention(seq)
    for step in range(chips):
        kv.give_all(step)
    ff_step(1, [kv_step(0), kv_step(1), kv_step(2)])
    ff_step(2, [kv_step(3), kv_step(4), kv_step(5)])
    ff_step(3, [kv_step(6), kv_step(7), out_part])
    projections()
    ff_step(4)
    qkv_part()
    for step in range(chips):
        attn.give_all(step)
    ff_step(5, [attn_step(0), attn_step(1), attn_step(2)])
    ff_step(6, [attn_step(3), attn_step(4), attn_step(5)])
    ff_step(7, [attn_step(6), attn_step(7)])
    r["gains_total"][...] = r["gain_sum"][...]
    for copy in (out_swap, col_swap, gain_swap, gain_twin):
        copy.wait_send()
    for way in range(2):
        for step in range(gain_hops[way]):
            gain_hop(way, step).wait_send()
    ff.drain()
    kv.drain()
    attn.drain()


BROUGHT = (
    "att_send",
    "pairs",
    "query",
    "grad_mixed",
    "mixed",
    "totals",
    "query_pos",
    "key_pos",
    "att_own",
    "mixed_turned",
    "query_raw",
    "key_raw",
    "cosine",
    "sine",
    "gains",
    "weight_query",
    "weight_pair",
    "tokens",
    "grad_hidden",
    "gain_part",
    "normed_turned",
)


def back(given, ff_parts, heads, devices, collective_id):
    chips = devices // 2
    count, width = given["tokens"].shape
    size = given["key_raw"].shape[1]
    out_cols = given["att_send"].shape[1]
    out_lines = given["mixed_turned"].shape[0] // devices
    lines = width // devices
    cols = (heads * size + 2 * size) // 2
    slots = lambda n, p: pltpu.VMEM((n,) + tuple(p.shape[1:]), p.dtype)
    ff_pieces = split_ways(ff_parts)
    pair_rows = given["pairs"].shape[1]
    kv_pieces = tuple(
        (0, 1 - 2 * i, i * pair_rows // 2, pair_rows // 2, 0, 2 * size) for i in range(2)
    )
    attn_pieces = (
        (0, 1, 0, lines, 0, cols // 2),
        (0, -1, 0, lines, cols // 2, cols // 2),
        (1, 1, 0, out_lines // 2, 0, out_cols),
        (1, -1, out_lines // 2, out_lines // 2, 0, out_cols),
    )
    dma = lambda *shape: pltpu.SemaphoreType.DMA(shape)
    names, specs, operands = [], [], []
    for name, array in zip(("part_down", "part_gate", "part_up"), ff_parts):
        names.append(name)
        operands.append(array)
    for name in BROUGHT:
        names.append("in_" + name)
        operands.append(given[name])
    outs = {
        "grad_tokens": ((count, width), F32),
        "grad_down": (ff_parts[0].shape[1:], BF16),
        "grad_gate": (ff_parts[1].shape[1:], BF16),
        "grad_up": (ff_parts[2].shape[1:], BF16),
        "grad_qkv": ((lines, cols), F32),
        "grad_out": ((out_lines, out_cols), F32),
        "gains_total": (given["gains"].shape, F32),
    }
    scratch = {}
    for name in BROUGHT:
        shape = given[name].shape
        scratch[name] = pltpu.VMEM(shape, given[name].dtype)
    for i, p in enumerate(ff_parts):
        scratch[f"ff_own{i}"] = slots(2, p)
        scratch[f"ff_other{i}"] = slots(chips, p)
        scratch[f"ff_flow{i}"] = slots(chips, p)
    for kind, pieces in (("ff", ff_pieces), ("kv", kv_pieces), ("at", attn_pieces)):
        for name, steps in (("put", chips), ("got", chips), ("send", chips - 1), ("recv", chips - 1)):
            scratch[f"{kind}_{name}"] = dma(len(pieces), steps)
    scratch["ff_load"] = dma(len(ff_pieces), chips)
    scratch["kv_other"] = slots(chips, given["pairs"])
    scratch["kv_flow"] = slots(chips, given["pairs"])
    scratch["kv_sum"] = pltpu.VMEM((pair_rows, 2 * size), F32)
    scratch["att_across"] = pltpu.VMEM((count, out_cols), BF16)
    scratch["grad_query"] = pltpu.VMEM((count, heads * size), F32)
    scratch["query_low"] = pltpu.VMEM((count, heads * size), BF16)
    scratch["pair_low"] = pltpu.VMEM((count, 2 * size), BF16)
    scratch["col_rows"] = pltpu.VMEM((2 * count, cols), BF16)
    scratch["col_send"] = pltpu.VMEM((count, cols), BF16)
    for name, shape in (("qkv", (lines, cols)), ("out", (out_lines, out_cols))):
        scratch[f"{name}_part"] = pltpu.VMEM((devices,) + shape, BF16)
        scratch[f"{name}_other"] = pltpu.VMEM((chips,) + shape, BF16)
        scratch[f"{name}_flow"] = pltpu.VMEM((chips,) + shape, BF16)
    for name in ("gain_own", "gain_across", "gain_pair", "gain_twin", "gain_sum"):
        scratch[name] = pltpu.VMEM(given["gains"].shape, F32)
    scratch["gain_flow"] = pltpu.VMEM((2, chips // 2 + 1) + given["gains"].shape, F32)
    scratch["bring"] = dma(len(BROUGHT))
    for name, n in (("cross_send", 3), ("cross_recv", 3), ("twin_send", 1), ("twin_recv", 1)):
        scratch[name] = dma(n)
    scratch["gain_send"] = dma(2, chips // 2)
    scratch["gain_recv"] = dma(2, chips // 2)
    names += list(outs) + list(scratch)
    return pl.pallas_call(
        functools.partial(
            back_kernel, devices, heads, ff_pieces, kv_pieces, attn_pieces, tuple(names)
        ),
        in_specs=[pl.BlockSpec(memory_space=pl.ANY)] * len(operands),
        out_specs=[pl.BlockSpec(memory_space=pltpu.VMEM)] * len(outs),
        out_shape=[jax.ShapeDtypeStruct(shape, kind) for shape, kind in outs.values()],
        scratch_shapes=list(scratch.values()),
        compiler_params=pltpu.CompilerParams(
            collective_id=collective_id, has_side_effects=True, vmem_limit_bytes=67043328
        ),
        name="back",
    )(*operands)


def body(
    tokens,
    block_order,
    gain_attn_pre,
    gain_query,
    gain_key,
    gain_attn_post,
    gain_ff_pre,
    gain_ff_post,
    weight_query,
    weight_key,
    weight_value,
    weight_out,
    weight_gate,
    weight_up,
    weight_down,
    cotangent,
):
    sequences, rows, width = tokens.shape
    count = sequences * rows
    block = rows // 2
    devices = lax.axis_size("ctx")
    me = lax.axis_index("ctx")
    mine = lax.axis_index("wsh")

    head_size = 2 * gain_key.shape[0]
    heads = 2 * weight_query.shape[1] // head_size

    lane = jnp.arange(block, dtype=jnp.int32)
    late_order = 2 * devices - 1 - block_order
    early_pos = (block_order[:, None] * block + lane[None]).reshape(-1)
    late_pos = (late_order[:, None] * block + lane[None]).reshape(-1)
    key_pos = jnp.stack([early_pos, late_pos], 0)
    own_first = lax.dynamic_slice_in_dim(block_order, me, 1)[0]
    own_early = own_first * block + lane
    own_late = (2 * devices - 1 - own_first) * block + lane
    own_pos = jnp.concatenate([own_early, own_late])
    query_pos = jnp.concatenate([jnp.tile(own_early, heads), jnp.tile(own_late, heads)])[:, None]

    cosine, sine = angle_tables(own_pos, head_size)

    def placed(gain):
        zeros = jnp.zeros_like(gain)
        return jnp.where(
            mine == 0, jnp.concatenate([gain, zeros]), jnp.concatenate([zeros, gain])
        ).astype(F32)

    own_gains = [placed(g) for g in (gain_attn_pre, gain_attn_post, gain_ff_pre, gain_ff_post)]
    small = [placed(gain_query), placed(gain_key)]
    own_gains.append(jnp.concatenate(small + [jnp.zeros((width - 2 * head_size,), F32)]))
    own_gains = jnp.stack(own_gains + [jnp.zeros((width,), F32)] * 3)
    pairs, normed_low, key_raw, all_gains, key_other, value_other, query_other, out_other = front(
        tokens,
        own_gains,
        cosine,
        sine,
        (weight_key, weight_value, weight_query, weight_out),
        devices,
        2,
    )
    attn_pre = all_gains[0]
    query_gain = all_gains[4, :head_size]
    key_gain = all_gains[4, head_size : 2 * head_size]
    normed_low = normed_low.reshape(sequences, rows, width)
    key_raw = key_raw.reshape(sequences, rows, head_size)
    pair_weight = jnp.concatenate(
        [join_halves(mine, weight_key, key_other), join_halves(mine, weight_value, value_other)], 1
    )
    weight_query = join_halves(mine, weight_query, query_other)
    weight_out = join_halves(mine, weight_out, out_other)
    local_size = weight_key.shape[1]
    inputs = tokens.astype(F32)

    def key_path(key_in, key_scale):
        return rotate(norm_gain(key_in, key_scale), cosine[None], sine[None])

    def query_path(query_in, query_scale):
        return rotate(
            norm_gain(query_in, query_scale), cosine[None, :, None, :], sine[None, :, None, :]
        )

    query_raw = jnp.einsum(
        "srd,de->sre", normed_low, weight_query, preferred_element_type=F32
    ).reshape(sequences, rows, heads, head_size)
    query_rot, query_back = jax.vjp(query_path, query_raw, query_gain)
    query_low = query_rot.astype(BF16).reshape(sequences, rows, heads * head_size)

    mixed_low, mixed, totals = attend_forward(query_low, pairs, query_pos, key_pos, heads)
    attended = jnp.einsum("sre,ed->srd", mixed_low, weight_out, preferred_element_type=F32)
    (
        output,
        grad_hidden,
        attended_low,
        gain_part,
        part_down,
        part_gate,
        part_up,
    ) = feed_forward(
        attended.reshape(count, width),
        tokens.reshape(count, width),
        cotangent.reshape(count, width),
        all_gains,
        (weight_gate, weight_up, weight_down),
        3,
    )
    output = output.reshape(sequences, rows, width)

    def both(own, other):
        return jnp.concatenate([own, other], 0)

    def weight_grad(left, right):
        return dot(left, right, ((0,), (0,))).astype(BF16)

    attended_low = attended_low.reshape(sequences, rows, width)
    grad_mixed = jnp.einsum(
        "srd,ed->sre", attended_low, weight_out, preferred_element_type=F32
    ).astype(BF16)
    attended_low = attended_low.reshape(count, width)
    mixed_rows = mixed_low.reshape(count, heads * head_size)
    normed_rows = normed_low.reshape(count, width)
    given = {
        "att_send": half_of(attended_low, 1 - mine),
        "att_own": half_of(attended_low, mine),
        "pairs": pairs.reshape(devices, count, 2 * head_size),
        "query": query_low,
        "grad_mixed": grad_mixed,
        "mixed": mixed,
        "totals": totals,
        "query_pos": query_pos,
        "key_pos": key_pos,
        "mixed_turned": both(mixed_rows, swap(mixed_rows)).T,
        "query_raw": query_raw.reshape(count, heads * head_size),
        "key_raw": key_raw.reshape(count, head_size),
        "cosine": jnp.tile(cosine, (sequences, 1)),
        "sine": jnp.tile(sine, (sequences, 1)),
        "gains": all_gains,
        "weight_query": weight_query,
        "weight_pair": pair_weight,
        "tokens": tokens.reshape(count, width),
        "grad_hidden": grad_hidden.reshape(count, width),
        "gain_part": gain_part,
        "normed_turned": both(normed_rows, swap(normed_rows)).T,
    }
    if width % (8 * devices) == 0 and mixed_rows.shape[1] % (32 * devices) == 0:
        ff_parts = [
            p.reshape(devices, p.shape[0] // devices, p.shape[1])
            for p in (part_down, part_gate, part_up)
        ]
        grad_tokens, grad_down_w, grad_gate_w, grad_up_w, grad_qkv, grad_out_w, gain_sums = back(
            given, ff_parts, heads, devices, 0
        )
        grad_tokens = grad_tokens.reshape(sequences, rows, width)
        place = me * 2 + mine

        def share(row, first, size):
            part = size // (2 * devices)
            return lax.dynamic_slice(gain_sums, (row, first + place * part), (1, part))[0]

        outs = [
            share(0, 0, width),
            share(4, 0, head_size),
            share(4, head_size, head_size),
            share(1, 0, width),
            share(2, 0, width),
            share(3, 0, width),
        ]
    else:
        part_out = weight_grad(
            both(mixed_rows, swap(mixed_rows)),
            both(half_of(attended_low, mine), swap(half_of(attended_low, 1 - mine))),
        )
        grad_query, grad_pairs = attend_backward(
            query_low, pairs, grad_mixed, mixed, totals, query_pos, key_pos, heads
        )
        pair_rows = sequences * rows
        slots = grad_pairs.reshape(devices, pair_rows, 2 * head_size)
        share = pair_rows // 8
        pieces = tuple((0, 1 - 2 * (i % 2), i * share, share, 0, 2 * head_size) for i in range(8))
        own_grads = sum_over_ctx([slots], pieces, devices, 0)[0]
        own_grads = own_grads.reshape(sequences, rows, 2 * head_size)
        grad_key_raw, grad_key_gain = jax.vjp(key_path, key_raw, key_gain)[1](own_grads[..., :head_size])
        value_grad_low = own_grads[..., head_size:].astype(BF16)
        grad_query_raw, grad_query_gain = query_back(
            grad_query.reshape(sequences, rows, heads, head_size)
        )
        query_grad_low = grad_query_raw.reshape(count, heads * head_size).astype(BF16)
        key_grad_low = grad_key_raw.astype(BF16).reshape(count, head_size)
        value_grad_low = value_grad_low.reshape(count, head_size)
        grad_normed = (
            dot(query_grad_low, weight_query, ((1,), (1,)))
            + dot(jnp.concatenate([key_grad_low, value_grad_low], -1), pair_weight, ((1,), (1,)))
        ).reshape(sequences, rows, width)
        grad_inputs, grad_attn_pre = jax.vjp(norm_gain, inputs, attn_pre)[1](grad_normed)
        grad_tokens = grad_inputs + grad_hidden.reshape(sequences, rows, width)

        def columns(which):
            return jnp.concatenate(
                [half_of(v, which) for v in (query_grad_low, key_grad_low, value_grad_low)], -1
            )

        part_qkv = weight_grad(
            both(normed_rows, swap(normed_rows)), both(columns(mine), swap(columns(1 - mine)))
        )

        gain_grads = [
            grad_attn_pre,
            grad_query_gain,
            grad_key_gain,
            gain_part[1],
            gain_part[2],
            gain_part[3],
        ]
        packed = jnp.concatenate([g.reshape(devices, 2, -1) for g in gain_grads], -1)
        keep = jnp.where(mine == 0, packed[:, 0], packed[:, 1])
        send = jnp.where(mine == 0, packed[:, 1], packed[:, 0])
        packed = keep + swap(send)
        gain_size = packed.shape[-1]
        packed = jnp.pad(packed, ((0, 0), (0, 1024 - gain_size))).reshape(devices, 8, 128)
        parts = [
            p.reshape(devices, p.shape[0] // devices, p.shape[1])
            for p in (part_down, part_gate, part_up, part_qkv, part_out)
        ] + [packed]
        grad_down_w, grad_gate_w, grad_up_w, grad_qkv, grad_out_w, packed = sum_over_ctx(
            parts, split_ways(parts), devices, 1
        )
        packed = packed.reshape(-1)
        outs, first = [], 0
        for g in gain_grads:
            size = g.shape[0] // (2 * devices)
            outs.append(packed[first : first + size])
            first += size
    query_cols = grad_qkv.shape[1] - 2 * local_size
    grad_query_w = grad_qkv[:, :query_cols]
    grad_key_w = grad_qkv[:, query_cols : query_cols + local_size]
    grad_value_w = grad_qkv[:, query_cols + local_size :]
    grad_down_w, grad_gate_w, grad_up_w = (
        g.astype(F32) for g in (grad_down_w, grad_gate_w, grad_up_w)
    )
    return (
        output,
        grad_tokens,
        *outs,
        grad_query_w,
        grad_key_w,
        grad_value_w,
        grad_out_w,
        grad_gate_w,
        grad_up_w,
        grad_down_w,
    )


def solution(mesh):
    rows, vector, matrix = P("wsh", "ctx", None), P("wsh"), P(None, "wsh")
    in_specs = (rows, P()) + (vector,) * 6 + (matrix,) * 7 + (rows,)
    out_specs = (rows, rows) + (P(("ctx", "wsh")),) * 6 + (P("ctx", "wsh"),) * 7
    return jax.shard_map(body, mesh=mesh, in_specs=in_specs, out_specs=out_specs, check_vma=False)
```

```python
import functools
import math

import jax
import jax.numpy as jnp
from jax import lax
from jax.experimental import pallas as pl
from jax.experimental.pallas import tpu as pltpu
from jax.sharding import PartitionSpec as P

EPS = 1e-06
ROPE_BASE = 1000000.0
SCORE_SCALE = 0.0625
F32 = jnp.float32
BF16 = jnp.bfloat16
MESH = pl.DeviceIdType.MESH


def norm_gain(vector, gain):
    return vector * lax.rsqrt(jnp.mean(vector * vector, -1, keepdims=True) + EPS) * gain


def rotate(vector, cosine, sine):
    middle = vector.shape[-1] // 2
    first = vector[..., :middle]
    second = vector[..., middle:]
    return jnp.concatenate([first * cosine - second * sine, second * cosine + first * sine], -1)


def angle_tables(positions, head_size):
    middle = head_size // 2
    inverse = jnp.exp(
        jnp.arange(middle, dtype=F32) * (-2.0 * math.log(ROPE_BASE) / head_size)
    )
    theta = positions.astype(F32)[:, None] * inverse[None, :]
    return (jnp.cos(theta), jnp.sin(theta))


def swap(value):
    return lax.ppermute(value, "wsh", [(0, 1), (1, 0)])


def half_of(value, which):
    middle = value.shape[-1] // 2
    return jnp.where(which == 0, value[..., :middle], value[..., middle:])


def dot(left, right, dims):
    return lax.dot_general(left, right, (dims, ((), ())), preferred_element_type=F32)


def stack_heads(ref, half, block, heads, size):
    rows = slice(half * block, (half + 1) * block)
    return jnp.concatenate([ref[0, rows, h * size : (h + 1) * size] for h in range(heads)], 0)


def attend_backward_kernel(
    heads, chunk, q_ref, kv_ref, g_ref, mix_ref, tot_ref, qpos_ref, kpos_ref, dq_ref, dkv_ref
):
    shards, _, rows, pair = kv_ref.shape
    block, size = rows // 2, pair // 2
    stacked = heads * block
    queries, scaled, correction = [], [], []
    for half in range(2):
        queries.append(stack_heads(q_ref, half, block, heads, size))
        grad = stack_heads(g_ref, half, block, heads, size).astype(F32)
        span = slice(half * stacked, (half + 1) * stacked)
        total = tot_ref[0, span, :1]
        delta = jnp.sum(grad * mix_ref[0, span, :], -1, keepdims=True)
        scaled.append((grad / total).astype(BF16))
        correction.append(delta / total)
    grad_query = [jnp.zeros((stacked, size), F32) for _ in range(2)]
    for first in range(0, shards, chunk):
        span = slice(first * block, (first + chunk) * block)
        for key_half in range(2):
            part = kv_ref[first : first + chunk, 0, key_half * block : (key_half + 1) * block, :]
            part = part.reshape(chunk * block, pair)
            keys, values = part[:, :size], part[:, size:]
            grad_keys = jnp.zeros((chunk * block, size), F32)
            grad_values = jnp.zeros((chunk * block, size), F32)
            for half in range(key_half, 2):
                weights = jnp.exp(dot(queries[half], keys, ((1,), (1,))) * SCORE_SCALE)
                if half == key_half:
                    allowed = (
                        kpos_ref[key_half : key_half + 1, span]
                        <= qpos_ref[half * stacked : (half + 1) * stacked, :]
                    )
                    weights = jnp.where(allowed, weights, 0.0)
                low = weights.astype(BF16)
                grad_weights = dot(scaled[half], values, ((1,), (1,)))
                grad_scores = (weights * (grad_weights - correction[half])).astype(BF16)
                grad_query[half] += dot(grad_scores, keys, ((1,), (0,)))
                grad_keys += dot(grad_scores, queries[half], ((0,), (0,)))
                grad_values += dot(low, scaled[half], ((0,), (0,)))
            both = jnp.concatenate([grad_keys * SCORE_SCALE, grad_values], -1).astype(BF16)
            dkv_ref[first : first + chunk, 0, key_half * block : (key_half + 1) * block, :] = (
                both.reshape(chunk, block, pair)
            )
    for half in range(2):
        for h in range(heads):
            dq_ref[0, half * block : (half + 1) * block, h * size : (h + 1) * size] = (
                grad_query[half][h * block : (h + 1) * block] * SCORE_SCALE
            )


def whole(shape):
    return pl.BlockSpec(shape, lambda s: (0,) * len(shape))


def attend_backward(query_low, pairs, grad_mixed, mixed, totals, query_pos, key_pos, heads):
    sequences, rows, width = query_low.shape
    shards, _, _, pair = pairs.shape
    stacked = query_pos.shape[0]
    row = pl.BlockSpec((1, rows, width), lambda s: (s, 0, 0))
    stack = lambda last: pl.BlockSpec((1, stacked, last), lambda s: (s, 0, 0))
    pairs_spec = pl.BlockSpec((shards, 1, rows, pair), lambda s: (0, s, 0, 0))
    return pl.pallas_call(
        functools.partial(attend_backward_kernel, heads, min(shards, 16)),
        grid=(sequences,),
        in_specs=[
            row,
            pairs_spec,
            row,
            stack(pair // 2),
            stack(128),
            whole(query_pos.shape),
            whole(key_pos.shape),
        ],
        out_specs=[row, pairs_spec],
        out_shape=[
            jax.ShapeDtypeStruct((sequences, rows, width), F32),
            jax.ShapeDtypeStruct(pairs.shape, BF16),
        ],
        name="attend_backward",
    )(query_low, pairs, grad_mixed, mixed, totals, query_pos, key_pos)


class Ring:
    def __init__(self, devices):
        self.chips = devices // 2
        me = lax.axis_index("ctx")
        self.core = me % 2
        chip = me // 2
        across = chip % 2
        deep = chip // 2
        self.place = deep + across * (self.chips - 1 - 2 * deep)
        self.partner = me + 1 - 2 * self.core
        self.right = self.device((self.place + 1) % self.chips, self.core)
        self.left = self.device((self.place + self.chips - 1) % self.chips, self.core)

    def device(self, place, core):
        side = place // (self.chips // 2)
        return 2 * (2 * (place + side * (self.chips - 1 - 2 * place)) + side) + core

    def enter(self, across=False):
        barrier = pltpu.get_barrier_semaphore()
        targets = [{"ctx": other} for other in (self.left, self.right, self.partner)]
        if across:
            targets.append({"wsh": 1 - lax.axis_index("wsh")})
        for target in targets:
            pl.semaphore_signal(barrier, inc=1, device_id=target, device_id_type=MESH)
        pl.semaphore_wait(barrier, len(targets))


def ring_sum_kernel(devices, pieces, arrays, ahead, *refs):
    parts, outs = refs[:arrays], refs[arrays : 2 * arrays]
    own, other, flow = (refs[(2 + i) * arrays : (3 + i) * arrays] for i in range(3))
    own_sem, put_sem, got_sem, send_sem, recv_sem = refs[5 * arrays :]
    ring = Ring(devices)
    chips = ring.chips

    def region(p):
        array, _, first, rows, start, cols = pieces[p]
        return array, pl.ds(first, rows), pl.ds(start, cols)

    def chunk(p, step):
        way = pieces[p][1]
        return (ring.place + 2 * chips + way * (-1 - step)) % chips

    def load(p, step):
        array, rows, cols = region(p)
        source = ring.device(chunk(p, step), ring.core)
        return pltpu.make_async_copy(
            parts[array].at[source, rows, cols],
            own[array].at[step, rows, cols],
            own_sem.at[p, step],
        )

    def give(p, step):
        array, rows, cols = region(p)
        source = ring.device(chunk(p, step), 1 - ring.core)
        return pltpu.make_async_remote_copy(
            src_ref=parts[array].at[source, rows, cols],
            dst_ref=other[array].at[step, rows, cols],
            send_sem=put_sem.at[p, step],
            recv_sem=got_sem.at[p, step],
            device_id={"ctx": ring.partner},
            device_id_type=MESH,
        )

    def pass_on(p, step):
        array, rows, cols = region(p)
        way = pieces[p][1]
        return pltpu.make_async_remote_copy(
            src_ref=flow[array].at[step, rows, cols],
            dst_ref=flow[array].at[step + 1, rows, cols],
            send_sem=send_sem.at[p, step],
            recv_sem=recv_sem.at[p, step],
            device_id={"ctx": ring.right if way > 0 else ring.left},
            device_id_type=MESH,
        )

    def fetch(step):
        for p in range(len(pieces)):
            load(p, step).start()
            give(p, step).start()

    def add(p, step, first, last):
        array, _, row, rows, start, cols = pieces[p]
        width = 128 if cols % 128 == 0 else cols
        while width < 512 and cols % (2 * width) == 0:
            width *= 2
        rows = pl.ds(row, rows)

        def group(i, carry):
            at = start + i * width
            if cols > width:
                at = pl.multiple_of(at, 128)
            where = pl.ds(at, width)
            total = own[array][step, rows, where].astype(F32) + other[array][
                step, rows, where
            ].astype(F32)
            if not first:
                total += flow[array][step, rows, where].astype(F32)
            if last:
                outs[array][rows, where] = total.astype(outs[array].dtype)
            else:
                flow[array][step, rows, where] = total.astype(flow[array].dtype)
            return carry

        if cols == width:
            group(0, 0)
        else:
            lax.fori_loop(0, cols // width, group, 0)

    def work(step, first=False, last=False):
        for p in range(len(pieces)):
            load(p, step).wait()
            give(p, step).wait_recv()
            if not first:
                pass_on(p, step - 1).wait_recv()
            add(p, step, first, last)
            if not last:
                pass_on(p, step).start()

    for p in range(len(pieces)):
        load(p, 0).start()
    ring.enter()
    for p in range(len(pieces)):
        give(p, 0).start()
    for step in range(1, min(ahead, chips)):
        fetch(step)
    work(0, first=True)

    def middle(step, carry):
        @pl.when(step + ahead - 1 < chips)
        def _():
            fetch(step + ahead - 1)

        work(step)
        return carry

    lax.fori_loop(1, chips - 1, middle, 0)
    work(chips - 1, last=True)

    def drain(step, carry):
        for p in range(len(pieces)):
            give(p, step).wait_send()

            @pl.when(step < chips - 1)
            def _():
                pass_on(p, step).wait_send()

        return carry

    lax.fori_loop(0, chips, drain, 0)


def ring_sum(parts, pieces, devices, collective_id, ahead=3, name="ring_sum"):
    chips, count, arrays = devices // 2, len(pieces), len(parts)
    slots = [pltpu.VMEM((chips,) + p.shape[1:], p.dtype) for p in parts]
    return pl.pallas_call(
        functools.partial(ring_sum_kernel, devices, pieces, arrays, ahead),
        out_shape=[jax.ShapeDtypeStruct(p.shape[1:], F32) for p in parts],
        in_specs=[pl.BlockSpec(memory_space=pl.ANY)] * arrays,
        out_specs=[pl.BlockSpec(memory_space=pltpu.VMEM)] * arrays,
        scratch_shapes=slots * 3
        + [pltpu.SemaphoreType.DMA((count, chips))] * 3
        + [pltpu.SemaphoreType.DMA((count, chips - 1))] * 2,
        compiler_params=pltpu.CompilerParams(
            collective_id=collective_id, has_side_effects=True, vmem_limit_bytes=64000 * 1024
        ),
        name=name,
    )(*parts)


def split_ways(parts):
    pieces, lead = [], 1
    for i, p in enumerate(parts):
        _, rows, cols = p.shape
        tiles = cols // 128
        if cols % 128 == 0 and tiles > 1:
            left = (tiles + (1 if lead > 0 else 0)) // 2 * 128
            if tiles % 2:
                lead = -lead
            pieces.append((i, 1, 0, rows, 0, left))
            pieces.append((i, -1, 0, rows, left, cols - left))
        elif rows % 32 == 0:
            pieces.append((i, 1, 0, rows // 2, 0, cols))
            pieces.append((i, -1, rows // 2, rows // 2, 0, cols))
        else:
            pieces.append((i, 1, 0, rows, 0, cols))
    return tuple(pieces)


def sum_over_ctx(parts, pieces, devices, collective_id):
    if all(p.shape[1] % 8 == 0 for p in parts):
        return ring_sum(parts, pieces, devices, collective_id)
    return [
        lax.psum_scatter(p, "ctx", scatter_dimension=0, tiled=False).astype(F32) for p in parts
    ]


def front_kernel(
    devices,
    heads,
    tokens_ref,
    gains_ref,
    cos_ref,
    sin_ref,
    query_pos_ref,
    key_pos_ref,
    key_weight,
    value_weight,
    query_weight,
    out_weight,
    pairs_ref,
    normed_ref,
    key_ref,
    query_ref,
    query_low_ref,
    mixed_low_ref,
    mixed_ref,
    totals_ref,
    all_gains_ref,
    pair_whole,
    query_whole,
    out_whole,
    gains_other,
    own_sem,
    cross_send,
    cross_recv,
    side_send,
    side_recv,
    flow_send,
    flow_recv,
    twin_send,
    twin_recv,
):
    ring = Ring(devices)
    chips, far = ring.chips, ring.chips // 2
    me = lax.axis_index("ctx")
    mine = lax.axis_index("wsh")
    sequences, rows, width = tokens_ref.shape
    count = sequences * rows
    size = key_ref.shape[1]
    block = rows // 2
    stacked = heads * block
    weights = (key_weight, value_weight, query_weight, out_weight)

    def region(i, side, first, lines):
        if i == 3:
            start = side * out_weight.shape[0] + first
            return out_whole.at[pl.ds(pl.multiple_of(start, 16), lines)]
        cols = weights[i].shape[1]
        start = side * cols + (size if i == 1 else 0)
        target = query_whole if i == 2 else pair_whole
        return target.at[pl.ds(pl.multiple_of(first, 16), lines), pl.ds(pl.multiple_of(start, 128), cols)]

    def own(i):
        return pltpu.make_async_copy(
            weights[i], region(i, mine, 0, weights[i].shape[0]), own_sem.at[i]
        )

    def cross(i):
        if i == len(weights):
            source, target = gains_ref, gains_other
        else:
            half = weights[i].shape[0] // 2
            first = pl.multiple_of(ring.core * half, 16)
            source, target = weights[i].at[pl.ds(first, half)], region(i, mine, first, half)
        return pltpu.make_async_remote_copy(
            src_ref=source,
            dst_ref=target,
            send_sem=cross_send.at[i],
            recv_sem=cross_recv.at[i],
            device_id={"wsh": 1 - mine},
            device_id_type=MESH,
        )

    def side(i):
        half = weights[i].shape[0] // 2
        part = region(i, 1 - mine, ring.core * half, half)
        return pltpu.make_async_remote_copy(
            src_ref=part,
            dst_ref=part,
            send_sem=side_send.at[i],
            recv_sem=side_recv.at[i],
            device_id={"ctx": ring.partner},
            device_id_type=MESH,
        )

    def block_copy(way, seq, hop, target, send_sem, recv_sem):
        stream = (1 if way < 0 else 0) * sequences + seq
        place = (ring.place + chips - way * hop) % chips
        part = pairs_ref.at[ring.device(place, ring.core), seq]
        return pltpu.make_async_remote_copy(
            src_ref=part,
            dst_ref=part,
            send_sem=send_sem.at[stream, hop],
            recv_sem=recv_sem.at[stream, hop],
            device_id={"ctx": target},
            device_id_type=MESH,
        )

    def flow(way, seq, hop):
        target = ring.right if way > 0 else ring.left
        return block_copy(way, seq, hop, target, flow_send, flow_recv)

    def twin(way, seq, hop):
        return block_copy(way, seq, hop, ring.partner, twin_send, twin_recv)

    def hops(way, seq):
        return far if (seq % 2 == 0) == (way > 0) else far - 1

    streams = [(way, seq) for seq in range(sequences) for way in (1, -1)]

    def pass_on(hop):
        for way, seq in streams:
            if hop > hops(way, seq):
                continue
            if hop > 0:
                flow(way, seq, hop - 1).wait_recv()
            if hop < hops(way, seq):
                flow(way, seq, hop).start()
            if hop > 0 or way > 0:
                twin(way, seq, hop).start()

    def turned(value, gain):
        scale = lax.rsqrt(jnp.mean(value * value, -1, keepdims=True) + EPS)
        value = value * scale * gain
        first, second = value[:, : size // 2], value[:, size // 2 :]
        cosine, sine = cos_ref[...], sin_ref[...]
        return jnp.concatenate(
            [first * cosine - second * sine, second * cosine + first * sine], -1
        ).astype(BF16)

    def queries():
        gain = all_gains_ref[4:5, :size]
        for h in range(heads):
            cols = slice(h * size, (h + 1) * size)
            value = dot(normed_ref[...], query_whole[:, cols], ((1,), (0,)))
            query_ref[:, cols] = value
            query_low_ref[:, :, cols] = turned(value, gain).reshape(sequences, rows, size)

    def attention(seq, carry):
        chunk = min(devices, 16)
        asked, sums, totals = [], [], []
        for half in range(2):
            lines = slice(half * block, (half + 1) * block)
            asked.append(
                jnp.concatenate(
                    [query_low_ref[seq, lines, h * size : (h + 1) * size] for h in range(heads)], 0
                )
            )
            sums.append(jnp.zeros((stacked, size), F32))
            totals.append(jnp.zeros((stacked, 1), F32))
        for first in range(0, devices, chunk):
            span = slice(first * block, (first + chunk) * block)
            for key_half in range(2):
                part = pairs_ref[
                    first : first + chunk, seq, key_half * block : (key_half + 1) * block, :
                ].reshape(chunk * block, 2 * size)
                keys, values = part[:, :size], part[:, size:]
                for half in range(key_half, 2):
                    weights = jnp.exp(dot(asked[half], keys, ((1,), (1,))) * SCORE_SCALE)
                    if half == key_half:
                        allowed = (
                            key_pos_ref[key_half : key_half + 1, span]
                            <= query_pos_ref[half * stacked : (half + 1) * stacked, :]
                        )
                        weights = jnp.where(allowed, weights, 0.0)
                    low = weights.astype(BF16)
                    totals[half] += jnp.sum(low.astype(F32), -1, keepdims=True)
                    sums[half] += dot(low, values, ((1,), (0,)))
        for half in range(2):
            mixed = sums[half] / totals[half]
            span = slice(half * stacked, (half + 1) * stacked)
            mixed_ref[seq, span, :] = mixed
            totals_ref[seq, span, :] = jnp.broadcast_to(
                totals[half], (stacked, totals_ref.shape[2])
            )
            for h in range(heads):
                mixed_low_ref[
                    seq, half * block : (half + 1) * block, h * size : (h + 1) * size
                ] = mixed[h * block : (h + 1) * block].astype(BF16)
        return carry

    for i in range(len(weights)):
        own(i).start()
    ring.enter(across=True)
    order = (len(weights), 0, 1, 2, 3)
    for i in order:
        cross(i).start()
    inputs = tokens_ref[...].reshape(count, width).astype(F32)
    scale = lax.rsqrt(jnp.mean(inputs * inputs, -1, keepdims=True) + EPS)
    cross(len(weights)).wait_recv()
    all_gains_ref[...] = gains_ref[...] + gains_other[...]
    normed_ref[...] = (inputs * scale * all_gains_ref[0:1, :]).astype(BF16)
    for i in (0, 1):
        cross(i).wait_recv()
        side(i).start()
    for i in (0, 1):
        own(i).wait()
        side(i).wait_recv()
    value = dot(normed_ref[...], pair_whole[...], ((1,), (0,)))
    key_ref[...] = value[:, :size]
    key_low = turned(value[:, :size], all_gains_ref[4:5, size : 2 * size])
    pairs_ref[me, :, :, :size] = key_low.reshape(sequences, rows, size)
    pairs_ref[me, :, :, size:] = value[:, size:].astype(BF16).reshape(sequences, rows, size)
    pass_on(0)
    pass_on(1)
    cross(2).wait_recv()
    side(2).start()
    for hop in range(2, far + 1):
        pass_on(hop)
        if hop == 2:
            own(2).wait()
            side(2).wait_recv()
            queries()
    cross(3).wait_recv()
    side(3).start()
    for hop in range(far + 1):
        for way, seq in streams:
            if hop <= hops(way, seq) and (hop > 0 or way > 0):
                twin(way, seq, hop).wait_recv()
    lax.fori_loop(0, sequences, attention, 0)
    for hop in range(far + 1):
        for way, seq in streams:
            if hop > hops(way, seq):
                continue
            if hop > 0 or way > 0:
                twin(way, seq, hop).wait_send()
            if hop < hops(way, seq):
                flow(way, seq, hop).wait_send()
    own(3).wait()
    side(3).wait_recv()
    for i in order:
        cross(i).wait_send()
    for i in range(len(weights)):
        side(i).wait_send()


def front(tokens, gains, cosine, sine, query_pos, key_pos, weights, heads, devices, collective_id):
    sequences, rows, width = tokens.shape
    size = 2 * cosine.shape[1]
    count = sequences * rows
    far = devices // 4
    stacked = query_pos.shape[0]
    here, there = pl.BlockSpec(memory_space=pltpu.VMEM), pl.BlockSpec(memory_space=pl.ANY)
    streams = pltpu.SemaphoreType.DMA((2 * sequences, far + 1))
    outs = [
        ((devices, sequences, rows, 2 * size), BF16),
        ((count, width), BF16),
        ((count, size), F32),
        ((count, heads * size), F32),
        ((sequences, rows, heads * size), BF16),
        ((sequences, rows, heads * size), BF16),
        ((sequences, stacked, size), F32),
        ((sequences, stacked, 128), F32),
        (gains.shape, F32),
        ((width, 2 * size), BF16),
        ((width, heads * size), BF16),
        ((width, heads * size), BF16),
    ]
    return pl.pallas_call(
        functools.partial(front_kernel, devices, heads),
        in_specs=[here] * 6 + [there] * 4,
        out_specs=[here] * len(outs),
        out_shape=[jax.ShapeDtypeStruct(shape, kind) for shape, kind in outs],
        scratch_shapes=[pltpu.VMEM(gains.shape, gains.dtype)]
        + [pltpu.SemaphoreType.DMA((4,))]
        + [pltpu.SemaphoreType.DMA((5,))] * 2
        + [pltpu.SemaphoreType.DMA((4,))] * 2
        + [streams] * 4,
        compiler_params=pltpu.CompilerParams(
            collective_id=collective_id, has_side_effects=True, vmem_limit_bytes=67043328
        ),
        name="front",
    )(tokens, gains, cosine, sine, query_pos, key_pos, *weights)


class RingSum:
    def __init__(self, ring, pieces, parts, own, other, flow, outs, sems):
        self.ring, self.pieces, self.parts, self.own = ring, pieces, parts, own
        self.other, self.flow, self.outs = other, flow, outs
        self.put_sem, self.got_sem, self.send_sem, self.recv_sem = sems[:4]
        self.own_sem = sems[4] if own is not None else None
        self.last = ring.chips - 1

    def region(self, p):
        array, _, first, rows, start, cols = self.pieces[p]
        return array, pl.ds(first, rows), pl.ds(start, cols)

    def owner(self, p, step, core):
        way = self.pieces[p][1]
        chips = self.ring.chips
        return self.ring.device((self.ring.place + 2 * chips + way * (-1 - step)) % chips, core)

    def load(self, p, step):
        array, rows, cols = self.region(p)
        slot = step % self.own[array].shape[0]
        return pltpu.make_async_copy(
            self.parts[array].at[self.owner(p, step, self.ring.core), rows, cols],
            self.own[array].at[slot, rows, cols],
            self.own_sem.at[p, step],
        )

    def give(self, p, step):
        array, rows, cols = self.region(p)
        return pltpu.make_async_remote_copy(
            src_ref=self.parts[array].at[self.owner(p, step, 1 - self.ring.core), rows, cols],
            dst_ref=self.other[array].at[step, rows, cols],
            send_sem=self.put_sem.at[p, step],
            recv_sem=self.got_sem.at[p, step],
            device_id={"ctx": self.ring.partner},
            device_id_type=MESH,
        )

    def hop(self, p, step):
        array, rows, cols = self.region(p)
        way = self.pieces[p][1]
        return pltpu.make_async_remote_copy(
            src_ref=self.flow[array].at[step, rows, cols],
            dst_ref=self.flow[array].at[step + 1, rows, cols],
            send_sem=self.send_sem.at[p, step],
            recv_sem=self.recv_sem.at[p, step],
            device_id={"ctx": self.ring.right if way > 0 else self.ring.left},
            device_id_type=MESH,
        )

    def load_all(self, step):
        for p in range(len(self.pieces)):
            self.load(p, step).start()

    def give_all(self, step):
        for p in range(len(self.pieces)):
            self.give(p, step).start()

    def work(self, p, step):
        array, _, row, rows, start, cols = self.pieces[p]
        if self.own is not None:
            self.load(p, step).wait()
            mine, at_mine = self.own[array], step % self.own[array].shape[0]
        else:
            mine, at_mine = self.parts[array], self.owner(p, step, self.ring.core)
        self.give(p, step).wait_recv()
        if step > 0:
            self.hop(p, step - 1).wait_recv()
        width = 128 if cols % 128 == 0 else cols
        while width < 512 and cols % (2 * width) == 0:
            width *= 2
        rows = pl.ds(row, rows)

        def group(i, carry):
            at = start + i * width
            if cols > width:
                at = pl.multiple_of(at, 128)
            where = pl.ds(at, width)
            total = mine[at_mine, rows, where].astype(F32)
            total += self.other[array][step, rows, where].astype(F32)
            if step > 0:
                total += self.flow[array][step, rows, where].astype(F32)
            if step == self.last:
                self.outs[array][rows, where] = total.astype(self.outs[array].dtype)
            else:
                self.flow[array][step, rows, where] = total.astype(self.flow[array].dtype)
            return carry

        if cols == width:
            group(0, 0)
        else:
            lax.fori_loop(0, cols // width, group, 0)
        if step < self.last:
            self.hop(p, step).start()

    def drain(self):
        for p in range(len(self.pieces)):
            for step in range(self.last + 1):
                self.give(p, step).wait_send()
                if step < self.last:
                    self.hop(p, step).wait_send()


def norm_back(upstream, vector, gain):
    scale = lax.rsqrt(jnp.mean(vector * vector, -1, keepdims=True) + EPS)
    normal = vector * scale
    weighted = upstream * gain
    back = scale * (weighted - normal * jnp.mean(weighted * normal, -1, keepdims=True))
    return back, jnp.sum(upstream * normal, 0, keepdims=True)


GELU_SCALE = math.sqrt(2.0 / math.pi)
GELU_CUBE = 0.044715


def feed_forward_kernel(
    mixed_ref,
    tokens_ref,
    cotangent_ref,
    gains_ref,
    out_hbm,
    gate_hbm,
    up_hbm,
    down_hbm,
    output_ref,
    hidden_back_ref,
    mixed_back_ref,
    attended_own_ref,
    attended_send_ref,
    gain_part_ref,
    down_grad_hbm,
    gate_grad_hbm,
    up_grad_hbm,
    gate_weight,
    up_weight,
    down_weight,
    out_weight,
    attended_ref,
    ff_rows,
    low_rows,
    ff_turned,
    low_turned,
    gate,
    upward,
    activated,
    partial,
    part_send,
    part_recv,
    back_send,
    back_recv,
    hidden_ref,
    staging,
    load_sem,
    out_sem,
    store_sem,
    cross_send,
    cross_recv,
):
    count, width = attended_ref.shape
    hidden_units = gate_weight.shape[1]
    block = part_send.shape[0] // 2
    chunk = staging.shape[2]
    whole_chunks = hidden_units // chunk
    rest = hidden_units - whole_chunks * chunk
    mine = lax.axis_index("wsh")
    weights = ((gate_hbm, gate_weight), (up_hbm, up_weight), (down_hbm, down_weight))

    def load(w, at, size, index):
        source, target = weights[w]
        cols = pl.ds(at, size)
        return pltpu.make_async_copy(source.at[:, cols], target.at[:, cols], load_sem.at[w, index])

    def chunks(work):
        def step(c, carry):
            work(pl.multiple_of(c * chunk, 128), chunk, c)
            return carry

        lax.fori_loop(0, whole_chunks, step, 0)
        if rest:
            work(whole_chunks * chunk, rest, whole_chunks)

    def across(kind, piece, source, target):
        return pltpu.make_async_remote_copy(
            src_ref=source,
            dst_ref=target,
            send_sem=cross_send.at[kind, piece],
            recv_sem=cross_recv.at[kind, piece],
            device_id={"wsh": 1 - mine},
            device_id_type=MESH,
        )

    def swap_rows(kind, ref, piece):
        first = pl.multiple_of(piece * block, block)
        return across(
            kind, piece, ref.at[pl.ds(first, block)], ref.at[pl.ds(count + first, block)]
        )

    def swap_parts(kind, source, target, piece):
        lines = pl.ds(pl.multiple_of(piece * block, block), block)
        return across(kind, piece, source.at[lines], target.at[lines])

    def start_load(at, size, index):
        for w in range(3):
            load(w, at, size, index).start()

    bring_out = pltpu.make_async_copy(out_hbm, out_weight, out_sem.at[0])
    bring_out.start()
    chunks(start_load)
    barrier = pltpu.get_barrier_semaphore()
    pl.semaphore_signal(barrier, inc=1, device_id={"wsh": 1 - mine}, device_id_type=MESH)

    bring_out.wait()
    attended = dot(mixed_ref[...], out_weight[...], ((1,), (1,)))
    attended_ref[...] = attended
    scale = lax.rsqrt(jnp.mean(attended * attended, -1, keepdims=True) + EPS)
    hidden = tokens_ref[...].astype(F32) + attended * scale * gains_ref[1:2, :]
    hidden_ref[...] = hidden
    scale = lax.rsqrt(jnp.mean(hidden * hidden, -1, keepdims=True) + EPS)
    ff_rows[:count, :] = (hidden * scale * gains_ref[2:3, :]).astype(BF16)
    pl.semaphore_wait(barrier, 1)
    for piece in range(2):
        swap_rows(0, ff_rows, piece).start()

    def forward(turn, carry):
        b = (2 * turn) % 5 - (2 * turn) % 5 // 4

        @pl.when(b >= 2)
        def _():
            swap_rows(0, ff_rows, b - 2).wait_recv()

        lines = pl.ds(pl.multiple_of(b * block, block), block)

        def columns(at, size, index):
            @pl.when(b == 0)
            def _():
                for w in range(3):
                    load(w, at, size, index).wait()

            cols = pl.ds(at, size)
            g = dot(ff_rows[lines, :], gate_weight[:, cols], ((1,), (0,)))
            u = dot(ff_rows[lines, :], up_weight[:, cols], ((1,), (0,)))
            t = jnp.tanh(GELU_SCALE * (g + GELU_CUBE * g * g * g))
            gate[lines, cols] = g.astype(BF16)
            upward[lines, cols] = u.astype(BF16)
            activated[lines, cols] = (0.5 * g * (1.0 + t) * u).astype(BF16)

        chunks(columns)
        value = dot(activated[lines, :], down_weight[...], ((1,), (1,)))

        @pl.when(b < 2)
        def _():
            partial[lines, :] = value

        @pl.when(b >= 2)
        def _():
            there = pl.ds(pl.multiple_of((b - 2) * block, block), block)
            part_send[there, :] = value.astype(BF16)
            swap_parts(1, part_send, part_recv, b - 2).start()

        return carry

    lax.fori_loop(0, 4, forward, 0)
    ff_turned[...] = ff_rows[...].T
    for piece in range(2):
        swap_parts(1, part_send, part_recv, piece).wait_recv()
    lowered = partial[...] + part_recv[...].astype(F32)
    cotangent = cotangent_ref[...].astype(F32)
    back, part = norm_back(cotangent, lowered, gains_ref[3:4, :])
    low_rows[:count, :] = back.astype(BF16)
    for piece in range(2):
        swap_rows(2, low_rows, piece).start()
    gain_part_ref[...] = jnp.zeros_like(gain_part_ref)
    gain_part_ref[3:4, :] = part
    scale = lax.rsqrt(jnp.mean(lowered * lowered, -1, keepdims=True) + EPS)
    output_ref[...] = (hidden_ref[...] + lowered * scale * gains_ref[3:4, :]).astype(BF16)

    def backward(turn, carry):
        b = (2 * turn) % 5 - (2 * turn) % 5 // 4

        @pl.when(b >= 2)
        def _():
            swap_rows(2, low_rows, b - 2).wait_recv()

        lines = pl.ds(pl.multiple_of(b * block, block), block)

        def columns(at, size, index):
            cols = pl.ds(at, size)
            d = dot(low_rows[lines, :], down_weight[:, cols], ((1,), (0,)))
            g = gate[lines, cols].astype(F32)
            u = upward[lines, cols].astype(F32)
            square = g * g
            t = jnp.tanh(GELU_SCALE * (g + GELU_CUBE * square * g))
            half = 0.5 * (1.0 + t)
            slope = half + 0.5 * g * (1.0 - t * t) * (
                GELU_SCALE * (1.0 + 3.0 * GELU_CUBE * square)
            )
            gate[lines, cols] = (d * u * slope).astype(BF16)
            upward[lines, cols] = (d * g * half).astype(BF16)

        chunks(columns)
        value = dot(gate[lines, :], gate_weight[...], ((1,), (1,)))
        value += dot(upward[lines, :], up_weight[...], ((1,), (1,)))

        @pl.when(b < 2)
        def _():
            partial[lines, :] = value

        @pl.when(b >= 2)
        def _():
            there = pl.ds(pl.multiple_of((b - 2) * block, block), block)
            back_send[there, :] = value.astype(BF16)
            swap_parts(3, back_send, back_recv, b - 2).start()

        return carry

    lax.fori_loop(0, 4, backward, 0)
    low_turned[...] = low_rows[...].T

    grads = (
        (low_turned, activated, down_grad_hbm),
        (ff_turned, gate, gate_grad_hbm),
        (ff_turned, upward, up_grad_hbm),
    )

    def store(m, at, size, index):
        cols = pl.ds(at, size)
        return pltpu.make_async_copy(
            staging.at[index % 2, :, pl.ds(0, size)], grads[m][2].at[:, cols], store_sem.at[m, index]
        )

    for m in range(3):
        left, right, _ = grads[m]

        def columns(at, size, index, m=m, left=left, right=right):
            @pl.when(index >= 2)
            def _():
                store(m, 0, chunk, index - 2).wait()

            for top in range(0, width, width // 2):
                lines = slice(top, top + width // 2)
                staging[index % 2, lines, :size] = dot(
                    left[lines, :], right[:, pl.ds(at, size)], ((1,), (0,))
                ).astype(BF16)
            store(m, at, size, index).start()

        chunks(columns)
        last = whole_chunks + (1 if rest else 0)
        for index in range(max(last - 2, 0), last):
            store(m, 0, rest if index == whole_chunks else chunk, index).wait()

    for piece in range(2):
        swap_parts(3, back_send, back_recv, piece).wait_recv()
    upstream = partial[...] + back_recv[...].astype(F32)
    back, part = norm_back(upstream, hidden_ref[...], gains_ref[2:3, :])
    gain_part_ref[2:3, :] = part
    back += cotangent_ref[...].astype(F32)
    hidden_back_ref[...] = back
    back, part = norm_back(back, attended_ref[...], gains_ref[1:2, :])
    gain_part_ref[1:2, :] = part
    mixed_back_ref[...] = dot(back.astype(BF16), out_weight[...], ((1,), (0,))).astype(BF16)
    first, second = back[:, : width // 2].astype(BF16), back[:, width // 2 :].astype(BF16)
    attended_own_ref[...] = jnp.where(mine == 0, first, second)
    attended_send_ref[...] = jnp.where(mine == 0, second, first)
    for piece in range(2):
        swap_rows(0, ff_rows, piece).wait_send()
        swap_parts(1, part_send, part_recv, piece).wait_send()
        swap_rows(2, low_rows, piece).wait_send()
        swap_parts(3, back_send, back_recv, piece).wait_send()


def feed_forward(mixed, tokens, cotangent, gains, weights, collective_id):
    count, width = tokens.shape
    hidden_units = weights[1].shape[1]
    chunk = 512
    pieces = -(-hidden_units // chunk)
    here, there = pl.BlockSpec(memory_space=pltpu.VMEM), pl.BlockSpec(memory_space=pl.ANY)
    like = lambda shape, kind: jax.ShapeDtypeStruct(shape, kind)
    matrix = (width, hidden_units)
    return pl.pallas_call(
        feed_forward_kernel,
        in_specs=[here] * 4 + [there] * 4,
        out_specs=[here] * 6 + [there] * 3,
        out_shape=[
            like((count, width), BF16),
            like((count, width), F32),
            like(mixed.shape, BF16),
            like((count, width // 2), BF16),
            like((count, width // 2), BF16),
            like(gains.shape, F32),
        ]
        + [like(matrix, BF16)] * 3,
        scratch_shapes=[pltpu.VMEM(matrix, BF16)] * 3
        + [pltpu.VMEM(weights[0].shape, BF16), pltpu.VMEM((count, width), F32)]
        + [pltpu.VMEM((2 * count, width), BF16)] * 2
        + [pltpu.VMEM((width, 2 * count), BF16)] * 2
        + [pltpu.VMEM((2 * count, hidden_units), BF16)] * 3
        + [pltpu.VMEM((count, width), F32)]
        + [pltpu.VMEM((count, width), BF16)] * 4
        + [
            pltpu.VMEM((count, width), F32),
            pltpu.VMEM((2, width, chunk), BF16),
            pltpu.SemaphoreType.DMA((3, pieces)),
            pltpu.SemaphoreType.DMA((1,)),
            pltpu.SemaphoreType.DMA((3, pieces)),
            pltpu.SemaphoreType.DMA((4, 2)),
            pltpu.SemaphoreType.DMA((4, 2)),
        ],
        compiler_params=pltpu.CompilerParams(
            collective_id=collective_id, has_side_effects=True, vmem_limit_bytes=67043328
        ),
        name="feed_forward",
    )(mixed, tokens, cotangent, gains, *weights)


def turn_back(upstream, cosine, sine):
    middle = upstream.shape[-1] // 2
    first, second = upstream[:, :middle], upstream[:, middle:]
    return jnp.concatenate([first * cosine + second * sine, second * cosine - first * sine], -1)


def back_kernel(devices, heads, ff_pieces, kv_pieces, attn_pieces, names, *refs):
    r = dict(zip(names, refs))
    ring = Ring(devices)
    chips = ring.chips
    mine = lax.axis_index("wsh")
    sequences, rows, _ = r["query"].shape
    size = r["key_raw"].shape[1]
    count = sequences * rows
    block = rows // 2
    stacked = heads * block

    ff = RingSum(
        ring,
        ff_pieces,
        [r["part_down"], r["part_gate"], r["part_up"]],
        [r[f"ff_own{i}"] for i in range(3)],
        [r[f"ff_other{i}"] for i in range(3)],
        [r[f"ff_flow{i}"] for i in range(3)],
        [r["grad_down"], r["grad_gate"], r["grad_up"]],
        [r["ff_put"], r["ff_got"], r["ff_send"], r["ff_recv"], r["ff_load"]],
    )
    kv = RingSum(
        ring,
        kv_pieces,
        [r["pairs"]],
        None,
        [r["kv_other"]],
        [r["kv_flow"]],
        [r["kv_sum"]],
        [r["kv_put"], r["kv_got"], r["kv_send"], r["kv_recv"]],
    )
    attn = RingSum(
        ring,
        attn_pieces,
        [r["qkv_part"], r["out_part"]],
        None,
        [r["qkv_other"], r["out_other"]],
        [r["qkv_flow"], r["out_flow"]],
        [r["grad_qkv"], r["grad_out"]],
        [r["at_put"], r["at_got"], r["at_send"], r["at_recv"]],
    )

    def brought(i):
        name = BROUGHT[i]
        return pltpu.make_async_copy(r["in_" + name], r[name], r["bring"].at[i])

    def need(*wanted):
        for name in wanted:
            brought(BROUGHT.index(name)).wait()

    def across(i, source, target):
        return pltpu.make_async_remote_copy(
            src_ref=source,
            dst_ref=target,
            send_sem=r["cross_send"].at[i],
            recv_sem=r["cross_recv"].at[i],
            device_id={"wsh": 1 - mine},
            device_id_type=MESH,
        )

    out_swap = across(0, r["att_send"], r["att_across"])
    col_swap = across(1, r["col_send"], r["col_rows"].at[pl.ds(count, count)])
    gain_swap = across(2, r["gain_own"], r["gain_across"])
    gain_twin = pltpu.make_async_remote_copy(
        src_ref=r["gain_pair"],
        dst_ref=r["gain_twin"],
        send_sem=r["twin_send"].at[0],
        recv_sem=r["twin_recv"].at[0],
        device_id={"ctx": ring.partner},
        device_id_type=MESH,
    )

    def gain_hop(way, step):
        return pltpu.make_async_remote_copy(
            src_ref=r["gain_flow"].at[way, step],
            dst_ref=r["gain_flow"].at[way, step + 1],
            send_sem=r["gain_send"].at[way, step],
            recv_sem=r["gain_recv"].at[way, step],
            device_id={"ctx": ring.right if way == 0 else ring.left},
            device_id_type=MESH,
        )

    gain_hops = (chips // 2, chips - 1 - chips // 2)

    def attention(seq, carry):
        queries, scaled, correction = [], [], []
        for half in range(2):
            span = slice(half * stacked, (half + 1) * stacked)
            lines = slice(half * block, (half + 1) * block)
            cut = lambda ref: jnp.concatenate(
                [ref[seq, lines, h * size : (h + 1) * size] for h in range(heads)], 0
            )
            queries.append(cut(r["query"]))
            grad = cut(r["grad_mixed"]).astype(F32)
            total = r["totals"][seq, span, :1]
            delta = jnp.sum(grad * r["mixed"][seq, span, :], -1, keepdims=True)
            scaled.append((grad / total).astype(BF16))
            correction.append(delta / total)
        grad_query = [jnp.zeros((stacked, size), F32) for _ in range(2)]
        for key_half in range(2):
            lines = pl.ds(pl.multiple_of(seq * rows + key_half * block, block), block)
            part = r["pairs"][:, lines, :].reshape(devices * block, 2 * size)
            keys, values = part[:, :size], part[:, size:]
            grad_keys = jnp.zeros((devices * block, size), F32)
            grad_values = jnp.zeros((devices * block, size), F32)
            for half in range(key_half, 2):
                weights = jnp.exp(dot(queries[half], keys, ((1,), (1,))) * SCORE_SCALE)
                if half == key_half:
                    allowed = (
                        r["key_pos"][key_half : key_half + 1, :]
                        <= r["query_pos"][half * stacked : (half + 1) * stacked, :]
                    )
                    weights = jnp.where(allowed, weights, 0.0)
                low = weights.astype(BF16)
                grad_weights = dot(scaled[half], values, ((1,), (1,)))
                grad_scores = (weights * (grad_weights - correction[half])).astype(BF16)
                grad_query[half] += dot(grad_scores, keys, ((1,), (0,)))
                grad_keys += dot(grad_scores, queries[half], ((0,), (0,)))
                grad_values += dot(low, scaled[half], ((0,), (0,)))
            both = jnp.concatenate([grad_keys * SCORE_SCALE, grad_values], -1).astype(BF16)
            r["pairs"][:, lines, :] = both.reshape(devices, block, 2 * size)
        for half in range(2):
            r["mixed"][seq, half * stacked : (half + 1) * stacked, :] = grad_query[half] * SCORE_SCALE
        return carry

    def pick(value, which):
        middle = value.shape[1] // 2
        return jnp.where(which == 0, value[:, :middle], value[:, middle:])

    def projections():
        need("query_raw", "key_raw", "cosine", "sine", "gains")
        cosine, sine = r["cosine"][...], r["sine"][...]
        gain = r["gains"][4:5, :size]
        total = jnp.zeros((1, size), F32)
        lows = []
        for h in range(heads):
            cols = slice(h * size, (h + 1) * size)
            grad = jnp.concatenate(
                [
                    r["mixed"][seq, half * stacked + h * block : half * stacked + (h + 1) * block, :]
                    for seq in range(sequences)
                    for half in range(2)
                ],
                0,
            )
            back, part = norm_back(
                turn_back(grad, cosine, sine), r["query_raw"][:, cols], gain
            )
            total += part
            r["query_low"][:, cols] = back.astype(BF16)
        back, key_total = norm_back(
            turn_back(r["kv_sum"][:, :size], cosine, sine),
            r["key_raw"][...],
            r["gains"][4:5, size : 2 * size],
        )
        r["pair_low"][:, :size] = back.astype(BF16)
        r["pair_low"][:, size:] = r["kv_sum"][:, size:].astype(BF16)
        first = 0
        for value in (
            r["query_low"][...],
            r["pair_low"][:, :size],
            r["pair_low"][:, size:],
        ):
            cols = slice(first, first + value.shape[1] // 2)
            r["col_rows"][:count, cols] = pick(value, mine)
            r["col_send"][:, cols] = pick(value, 1 - mine)
            first += value.shape[1] // 2
        col_swap.start()
        need("weight_query", "weight_pair", "tokens", "grad_hidden", "gain_part")
        grad_normed = dot(r["query_low"][...], r["weight_query"][...], ((1,), (1,)))
        grad_normed += dot(r["pair_low"][...], r["weight_pair"][...], ((1,), (1,)))
        back, part = norm_back(grad_normed, r["tokens"][...].astype(F32), r["gains"][0:1, :])
        r["grad_tokens"][...] = back + r["grad_hidden"][...]
        r["gain_own"][...] = r["gain_part"][...]
        r["gain_own"][0:1, :] = part
        r["gain_own"][4:5, :size] = total
        r["gain_own"][4:5, size : 2 * size] = key_total
        gain_swap.start()

    def out_part():
        need("mixed_own", "mixed_other", "att_own")
        out_swap.wait_recv()
        _, lines, cols = r["out_part"].shape
        value = dot(r["mixed_own"][...], r["att_own"][...], ((0,), (0,)))
        value += dot(r["mixed_other"][...], r["att_across"][...], ((0,), (0,)))
        r["out_part"][...] = value.reshape(devices, lines, cols).astype(BF16)

    def turn_rows():
        need("normed_own", "normed_other")
        r["weight_pair"][:, :count] = r["normed_own"][...].T
        r["weight_pair"][:, count:] = r["normed_other"][...].T

    def qkv_part():
        col_swap.wait_recv()
        _, lines, cols = r["qkv_part"].shape
        width = 256
        for first in range(0, cols, width):
            value = dot(
                r["weight_pair"][...], r["col_rows"][:, first : first + width], ((1,), (0,))
            )
            r["qkv_part"][:, :, first : first + width] = value.reshape(
                devices, lines, width
            ).astype(BF16)

    def gains_step(step):
        if step == 0:
            gain_swap.wait_recv()
            r["gain_pair"][...] = r["gain_own"][...] + r["gain_across"][...]
            gain_twin.start()
        elif step == 1:
            gain_twin.wait_recv()
            both = r["gain_pair"][...] + r["gain_twin"][...]
            r["gain_flow"][0, 0] = both
            r["gain_flow"][1, 0] = both
            r["gain_sum"][...] = both
            for way in range(2):
                gain_hop(way, 0).start()
        else:
            for way in range(2):
                if step - 2 < gain_hops[way]:
                    gain_hop(way, step - 2).wait_recv()
                    if step - 1 < gain_hops[way]:
                        gain_hop(way, step - 1).start()
                    r["gain_sum"][...] += r["gain_flow"][way, step - 1]

    def ff_step(step, extra=()):
        extra = list(extra)
        if step + 1 < chips:
            ff.load_all(step + 1)
        if step + 2 < chips:
            ff.give_all(step + 2)
        for p in range(len(ff_pieces)):
            ff.work(p, step)
            if p % 2 == 1 and extra:
                extra.pop(0)()
        for left in extra:
            left()

    def kv_step(step):
        def run():
            for p in range(len(kv_pieces)):
                kv.work(p, step)

        return run

    def attn_step(step):
        def run():
            gains_step(step)
            for p in range(len(attn_pieces)):
                attn.work(p, step)

        return run

    ff.load_all(0)
    for i in range(len(BROUGHT)):
        brought(i).start()
    ring.enter(across=True)
    ff.give_all(0)
    ff.give_all(1)
    need("att_send")
    out_swap.start()
    ff_step(0)
    need("pairs", "query", "grad_mixed", "mixed", "totals", "query_pos", "key_pos")
    lax.fori_loop(0, sequences, attention, 0)
    for step in range(chips):
        kv.give_all(step)
    ff_step(1, [kv_step(0), kv_step(1), kv_step(2)])
    ff_step(2, [kv_step(3), kv_step(4), kv_step(5)])
    ff_step(3, [kv_step(6), kv_step(7), out_part])
    projections()
    ff_step(4, [turn_rows])
    qkv_part()
    for step in range(chips):
        attn.give_all(step)
    ff_step(5, [attn_step(0), attn_step(1), attn_step(2)])
    ff_step(6, [attn_step(3), attn_step(4), attn_step(5)])
    ff_step(7, [attn_step(6), attn_step(7)])
    r["gains_total"][...] = r["gain_sum"][...]
    for copy in (out_swap, col_swap, gain_swap, gain_twin):
        copy.wait_send()
    for way in range(2):
        for step in range(gain_hops[way]):
            gain_hop(way, step).wait_send()
    ff.drain()
    kv.drain()
    attn.drain()


BROUGHT = (
    "att_send",
    "pairs",
    "query",
    "grad_mixed",
    "mixed",
    "totals",
    "query_pos",
    "key_pos",
    "att_own",
    "mixed_own",
    "mixed_other",
    "query_raw",
    "key_raw",
    "cosine",
    "sine",
    "gains",
    "weight_query",
    "weight_pair",
    "tokens",
    "grad_hidden",
    "gain_part",
    "normed_own",
    "normed_other",
)


def back(given, ff_parts, heads, devices, collective_id):
    chips = devices // 2
    count, width = given["tokens"].shape
    size = given["key_raw"].shape[1]
    out_cols = given["att_send"].shape[1]
    out_lines = given["mixed_own"].shape[1] // devices
    lines = width // devices
    cols = (heads * size + 2 * size) // 2
    slots = lambda n, p: pltpu.VMEM((n,) + tuple(p.shape[1:]), p.dtype)
    ff_pieces = split_ways(ff_parts)
    pair_rows = given["pairs"].shape[1]
    kv_pieces = tuple(
        (0, 1 - 2 * i, i * pair_rows // 2, pair_rows // 2, 0, 2 * size) for i in range(2)
    )
    attn_pieces = (
        (0, 1, 0, lines, 0, cols // 2),
        (0, -1, 0, lines, cols // 2, cols // 2),
        (1, 1, 0, out_lines // 2, 0, out_cols),
        (1, -1, out_lines // 2, out_lines // 2, 0, out_cols),
    )
    dma = lambda *shape: pltpu.SemaphoreType.DMA(shape)
    names, specs, operands = [], [], []
    for name, array in zip(("part_down", "part_gate", "part_up"), ff_parts):
        names.append(name)
        operands.append(array)
    for name in BROUGHT:
        names.append("in_" + name)
        operands.append(given[name])
    outs = {
        "grad_tokens": ((count, width), F32),
        "grad_down": (ff_parts[0].shape[1:], BF16),
        "grad_gate": (ff_parts[1].shape[1:], BF16),
        "grad_up": (ff_parts[2].shape[1:], BF16),
        "grad_qkv": ((lines, cols), F32),
        "grad_out": ((out_lines, out_cols), F32),
        "gains_total": (given["gains"].shape, F32),
    }
    scratch = {}
    for name in BROUGHT:
        shape = given[name].shape
        scratch[name] = pltpu.VMEM(shape, given[name].dtype)
    for i, p in enumerate(ff_parts):
        scratch[f"ff_own{i}"] = slots(2, p)
        scratch[f"ff_other{i}"] = slots(chips, p)
        scratch[f"ff_flow{i}"] = slots(chips, p)
    for kind, pieces in (("ff", ff_pieces), ("kv", kv_pieces), ("at", attn_pieces)):
        for name, steps in (("put", chips), ("got", chips), ("send", chips - 1), ("recv", chips - 1)):
            scratch[f"{kind}_{name}"] = dma(len(pieces), steps)
    scratch["ff_load"] = dma(len(ff_pieces), chips)
    scratch["kv_other"] = slots(chips, given["pairs"])
    scratch["kv_flow"] = slots(chips, given["pairs"])
    scratch["kv_sum"] = pltpu.VMEM((pair_rows, 2 * size), F32)
    scratch["att_across"] = pltpu.VMEM((count, out_cols), BF16)
    scratch["query_low"] = pltpu.VMEM((count, heads * size), BF16)
    scratch["pair_low"] = pltpu.VMEM((count, 2 * size), BF16)
    scratch["col_rows"] = pltpu.VMEM((2 * count, cols), BF16)
    scratch["col_send"] = pltpu.VMEM((count, cols), BF16)
    for name, shape in (("qkv", (lines, cols)), ("out", (out_lines, out_cols))):
        scratch[f"{name}_part"] = pltpu.VMEM((devices,) + shape, BF16)
        scratch[f"{name}_other"] = pltpu.VMEM((chips,) + shape, BF16)
        scratch[f"{name}_flow"] = pltpu.VMEM((chips,) + shape, BF16)
    for name in ("gain_own", "gain_across", "gain_pair", "gain_twin", "gain_sum"):
        scratch[name] = pltpu.VMEM(given["gains"].shape, F32)
    scratch["gain_flow"] = pltpu.VMEM((2, chips // 2 + 1) + given["gains"].shape, F32)
    scratch["bring"] = dma(len(BROUGHT))
    for name, n in (("cross_send", 3), ("cross_recv", 3), ("twin_send", 1), ("twin_recv", 1)):
        scratch[name] = dma(n)
    scratch["gain_send"] = dma(2, chips // 2)
    scratch["gain_recv"] = dma(2, chips // 2)
    names += list(outs) + list(scratch)
    return pl.pallas_call(
        functools.partial(
            back_kernel, devices, heads, ff_pieces, kv_pieces, attn_pieces, tuple(names)
        ),
        in_specs=[pl.BlockSpec(memory_space=pl.ANY)] * len(operands),
        out_specs=[pl.BlockSpec(memory_space=pltpu.VMEM)] * len(outs),
        out_shape=[jax.ShapeDtypeStruct(shape, kind) for shape, kind in outs.values()],
        scratch_shapes=list(scratch.values()),
        compiler_params=pltpu.CompilerParams(
            collective_id=collective_id, has_side_effects=True, vmem_limit_bytes=67043328
        ),
        name="back",
    )(*operands)


def body(
    tokens,
    block_order,
    gain_attn_pre,
    gain_query,
    gain_key,
    gain_attn_post,
    gain_ff_pre,
    gain_ff_post,
    weight_query,
    weight_key,
    weight_value,
    weight_out,
    weight_gate,
    weight_up,
    weight_down,
    cotangent,
):
    sequences, rows, width = tokens.shape
    count = sequences * rows
    block = rows // 2
    devices = lax.axis_size("ctx")
    me = lax.axis_index("ctx")
    mine = lax.axis_index("wsh")

    head_size = 2 * gain_key.shape[0]
    heads = 2 * weight_query.shape[1] // head_size

    lane = jnp.arange(block, dtype=jnp.int32)
    late_order = 2 * devices - 1 - block_order
    early_pos = (block_order[:, None] * block + lane[None]).reshape(-1)
    late_pos = (late_order[:, None] * block + lane[None]).reshape(-1)
    key_pos = jnp.stack([early_pos, late_pos], 0)
    own_first = lax.dynamic_slice_in_dim(block_order, me, 1)[0]
    own_early = own_first * block + lane
    own_late = (2 * devices - 1 - own_first) * block + lane
    own_pos = jnp.concatenate([own_early, own_late])
    query_pos = jnp.concatenate([jnp.tile(own_early, heads), jnp.tile(own_late, heads)])[:, None]

    cosine, sine = angle_tables(own_pos, head_size)

    def placed(gain):
        zeros = jnp.zeros_like(gain)
        return jnp.where(
            mine == 0, jnp.concatenate([gain, zeros]), jnp.concatenate([zeros, gain])
        ).astype(F32)

    own_gains = [placed(g) for g in (gain_attn_pre, gain_attn_post, gain_ff_pre, gain_ff_post)]
    small = [placed(gain_query), placed(gain_key)]
    own_gains.append(jnp.concatenate(small + [jnp.zeros((width - 2 * head_size,), F32)]))
    own_gains = jnp.stack(own_gains + [jnp.zeros((width,), F32)] * 3)
    (
        pairs,
        normed_rows,
        key_raw,
        query_raw,
        query_low,
        mixed_low,
        mixed,
        totals,
        all_gains,
        pair_weight,
        query_weight,
        out_weight,
    ) = front(
        tokens,
        own_gains,
        jnp.tile(cosine, (sequences, 1)),
        jnp.tile(sine, (sequences, 1)),
        query_pos,
        key_pos,
        (weight_key, weight_value, weight_query, weight_out.T),
        heads,
        devices,
        2,
    )
    attn_pre = all_gains[0]
    query_gain = all_gains[4, :head_size]
    key_gain = all_gains[4, head_size : 2 * head_size]
    mixed_rows = mixed_low.reshape(count, heads * head_size)
    local_size = weight_key.shape[1]
    inputs = tokens.astype(F32)

    def key_path(key_in, key_scale):
        return rotate(norm_gain(key_in, key_scale), cosine[None], sine[None])

    def query_path(query_in, query_scale):
        return rotate(
            norm_gain(query_in, query_scale), cosine[None, :, None, :], sine[None, :, None, :]
        )

    (
        output,
        grad_hidden,
        grad_mixed,
        attended_own,
        attended_send,
        gain_part,
        part_down,
        part_gate,
        part_up,
    ) = feed_forward(
        mixed_rows,
        tokens.reshape(count, width),
        cotangent.reshape(count, width),
        all_gains,
        (out_weight, weight_gate, weight_up, weight_down),
        3,
    )
    output = output.reshape(sequences, rows, width)

    def both(own, other):
        return jnp.concatenate([own, other], 0)

    def weight_grad(left, right):
        return dot(left, right, ((0,), (0,))).astype(BF16)

    grad_mixed = grad_mixed.reshape(query_low.shape)
    given = {
        "att_send": attended_send,
        "att_own": attended_own,
        "pairs": pairs.reshape(devices, count, 2 * head_size),
        "query": query_low,
        "grad_mixed": grad_mixed,
        "mixed": mixed,
        "totals": totals,
        "query_pos": query_pos,
        "key_pos": key_pos,
        "mixed_own": mixed_rows,
        "mixed_other": swap(mixed_rows),
        "query_raw": query_raw,
        "key_raw": key_raw,
        "cosine": jnp.tile(cosine, (sequences, 1)),
        "sine": jnp.tile(sine, (sequences, 1)),
        "gains": all_gains,
        "weight_query": query_weight,
        "weight_pair": pair_weight,
        "tokens": tokens.reshape(count, width),
        "grad_hidden": grad_hidden.reshape(count, width),
        "gain_part": gain_part,
        "normed_own": normed_rows,
        "normed_other": swap(normed_rows),
    }
    aligned = width % (8 * devices) == 0 and mixed_rows.shape[1] % (32 * devices) == 0
    if aligned and count == head_size:
        ff_parts = [
            p.reshape(devices, p.shape[0] // devices, p.shape[1])
            for p in (part_down, part_gate, part_up)
        ]
        grad_tokens, grad_down_w, grad_gate_w, grad_up_w, grad_qkv, grad_out_w, gain_sums = back(
            given, ff_parts, heads, devices, 0
        )
        grad_tokens = grad_tokens.reshape(sequences, rows, width)
        place = me * 2 + mine

        def share(row, first, size):
            part = size // (2 * devices)
            return lax.dynamic_slice(gain_sums, (row, first + place * part), (1, part))[0]

        outs = [
            share(0, 0, width),
            share(4, 0, head_size),
            share(4, head_size, head_size),
            share(1, 0, width),
            share(2, 0, width),
            share(3, 0, width),
        ]
    else:
        part_out = weight_grad(
            both(mixed_rows, swap(mixed_rows)),
            both(attended_own, swap(attended_send)),
        )
        grad_query, grad_pairs = attend_backward(
            query_low, pairs, grad_mixed, mixed, totals, query_pos, key_pos, heads
        )
        pair_rows = sequences * rows
        slots = grad_pairs.reshape(devices, pair_rows, 2 * head_size)
        share = pair_rows // 8
        pieces = tuple((0, 1 - 2 * (i % 2), i * share, share, 0, 2 * head_size) for i in range(8))
        own_grads = sum_over_ctx([slots], pieces, devices, 0)[0]
        own_grads = own_grads.reshape(sequences, rows, 2 * head_size)
        grad_key_raw, grad_key_gain = jax.vjp(
            key_path, key_raw.reshape(sequences, rows, head_size), key_gain
        )[1](own_grads[..., :head_size])
        value_grad_low = own_grads[..., head_size:].astype(BF16)
        grad_query_raw, grad_query_gain = jax.vjp(
            query_path, query_raw.reshape(sequences, rows, heads, head_size), query_gain
        )[1](
            grad_query.reshape(sequences, rows, heads, head_size)
        )
        query_grad_low = grad_query_raw.reshape(count, heads * head_size).astype(BF16)
        key_grad_low = grad_key_raw.astype(BF16).reshape(count, head_size)
        value_grad_low = value_grad_low.reshape(count, head_size)
        grad_normed = (
            dot(query_grad_low, query_weight, ((1,), (1,)))
            + dot(jnp.concatenate([key_grad_low, value_grad_low], -1), pair_weight, ((1,), (1,)))
        ).reshape(sequences, rows, width)
        grad_inputs, grad_attn_pre = jax.vjp(norm_gain, inputs, attn_pre)[1](grad_normed)
        grad_tokens = grad_inputs + grad_hidden.reshape(sequences, rows, width)

        def columns(which):
            return jnp.concatenate(
                [half_of(v, which) for v in (query_grad_low, key_grad_low, value_grad_low)], -1
            )

        part_qkv = weight_grad(
            both(normed_rows, swap(normed_rows)), both(columns(mine), swap(columns(1 - mine)))
        )

        gain_grads = [
            grad_attn_pre,
            grad_query_gain,
            grad_key_gain,
            gain_part[1],
            gain_part[2],
            gain_part[3],
        ]
        packed = jnp.concatenate([g.reshape(devices, 2, -1) for g in gain_grads], -1)
        keep = jnp.where(mine == 0, packed[:, 0], packed[:, 1])
        send = jnp.where(mine == 0, packed[:, 1], packed[:, 0])
        packed = keep + swap(send)
        gain_size = packed.shape[-1]
        packed = jnp.pad(packed, ((0, 0), (0, 1024 - gain_size))).reshape(devices, 8, 128)
        parts = [
            p.reshape(devices, p.shape[0] // devices, p.shape[1])
            for p in (part_down, part_gate, part_up, part_qkv, part_out)
        ] + [packed]
        grad_down_w, grad_gate_w, grad_up_w, grad_qkv, grad_out_w, packed = sum_over_ctx(
            parts, split_ways(parts), devices, 1
        )
        packed = packed.reshape(-1)
        outs, first = [], 0
        for g in gain_grads:
            size = g.shape[0] // (2 * devices)
            outs.append(packed[first : first + size])
            first += size
    query_cols = grad_qkv.shape[1] - 2 * local_size
    grad_query_w = grad_qkv[:, :query_cols]
    grad_key_w = grad_qkv[:, query_cols : query_cols + local_size]
    grad_value_w = grad_qkv[:, query_cols + local_size :]
    grad_down_w, grad_gate_w, grad_up_w = (
        g.astype(F32) for g in (grad_down_w, grad_gate_w, grad_up_w)
    )
    return (
        output,
        grad_tokens,
        *outs,
        grad_query_w,
        grad_key_w,
        grad_value_w,
        grad_out_w,
        grad_gate_w,
        grad_up_w,
        grad_down_w,
    )


def solution(mesh):
    rows, vector, matrix = P("wsh", "ctx", None), P("wsh"), P(None, "wsh")
    in_specs = (rows, P()) + (vector,) * 6 + (matrix,) * 7 + (rows,)
    out_specs = (rows, rows) + (P(("ctx", "wsh")),) * 6 + (P("ctx", "wsh"),) * 7
    return jax.shard_map(body, mesh=mesh, in_specs=in_specs, out_specs=out_specs, check_vma=False)
```

```python
import functools
import math

import jax
import jax.numpy as jnp
from jax import lax
from jax.experimental import pallas as pl
from jax.experimental.pallas import tpu as pltpu
from jax.sharding import PartitionSpec as P

EPS = 1e-06
ROPE_BASE = 1000000.0
SCORE_SCALE = 0.0625
F32 = jnp.float32
BF16 = jnp.bfloat16
MESH = pl.DeviceIdType.MESH


def norm_gain(vector, gain):
    return vector * lax.rsqrt(jnp.mean(vector * vector, -1, keepdims=True) + EPS) * gain


def rotate(vector, cosine, sine):
    middle = vector.shape[-1] // 2
    first = vector[..., :middle]
    second = vector[..., middle:]
    return jnp.concatenate([first * cosine - second * sine, second * cosine + first * sine], -1)


def angle_tables(positions, head_size):
    middle = head_size // 2
    inverse = jnp.exp(
        jnp.arange(middle, dtype=F32) * (-2.0 * math.log(ROPE_BASE) / head_size)
    )
    theta = positions.astype(F32)[:, None] * inverse[None, :]
    return (jnp.cos(theta), jnp.sin(theta))


def swap(value):
    return lax.ppermute(value, "wsh", [(0, 1), (1, 0)])


def half_of(value, which):
    middle = value.shape[-1] // 2
    return jnp.where(which == 0, value[..., :middle], value[..., middle:])


def dot(left, right, dims):
    return lax.dot_general(left, right, (dims, ((), ())), preferred_element_type=F32)


def stack_heads(ref, half, block, heads, size):
    rows = slice(half * block, (half + 1) * block)
    return jnp.concatenate([ref[0, rows, h * size : (h + 1) * size] for h in range(heads)], 0)


def attend_backward_kernel(
    heads, chunk, q_ref, kv_ref, g_ref, mix_ref, tot_ref, qpos_ref, kpos_ref, dq_ref, dkv_ref
):
    shards, _, rows, pair = kv_ref.shape
    block, size = rows // 2, pair // 2
    stacked = heads * block
    queries, scaled, correction = [], [], []
    for half in range(2):
        queries.append(stack_heads(q_ref, half, block, heads, size))
        grad = stack_heads(g_ref, half, block, heads, size).astype(F32)
        span = slice(half * stacked, (half + 1) * stacked)
        total = tot_ref[0, span, :1]
        delta = jnp.sum(grad * mix_ref[0, span, :], -1, keepdims=True)
        scaled.append((grad / total).astype(BF16))
        correction.append(delta / total)
    grad_query = [jnp.zeros((stacked, size), F32) for _ in range(2)]
    for first in range(0, shards, chunk):
        span = slice(first * block, (first + chunk) * block)
        for key_half in range(2):
            part = kv_ref[first : first + chunk, 0, key_half * block : (key_half + 1) * block, :]
            part = part.reshape(chunk * block, pair)
            keys, values = part[:, :size], part[:, size:]
            grad_keys = jnp.zeros((chunk * block, size), F32)
            grad_values = jnp.zeros((chunk * block, size), F32)
            for half in range(key_half, 2):
                weights = jnp.exp(dot(queries[half], keys, ((1,), (1,))) * SCORE_SCALE)
                if half == key_half:
                    allowed = (
                        kpos_ref[key_half : key_half + 1, span]
                        <= qpos_ref[half * stacked : (half + 1) * stacked, :]
                    )
                    weights = jnp.where(allowed, weights, 0.0)
                low = weights.astype(BF16)
                grad_weights = dot(scaled[half], values, ((1,), (1,)))
                grad_scores = (weights * (grad_weights - correction[half])).astype(BF16)
                grad_query[half] += dot(grad_scores, keys, ((1,), (0,)))
                grad_keys += dot(grad_scores, queries[half], ((0,), (0,)))
                grad_values += dot(low, scaled[half], ((0,), (0,)))
            both = jnp.concatenate([grad_keys * SCORE_SCALE, grad_values], -1).astype(BF16)
            dkv_ref[first : first + chunk, 0, key_half * block : (key_half + 1) * block, :] = (
                both.reshape(chunk, block, pair)
            )
    for half in range(2):
        for h in range(heads):
            dq_ref[0, half * block : (half + 1) * block, h * size : (h + 1) * size] = (
                grad_query[half][h * block : (h + 1) * block] * SCORE_SCALE
            )


def whole(shape):
    return pl.BlockSpec(shape, lambda s: (0,) * len(shape))


def attend_backward(query_low, pairs, grad_mixed, mixed, totals, query_pos, key_pos, heads):
    sequences, rows, width = query_low.shape
    shards, _, _, pair = pairs.shape
    stacked = query_pos.shape[0]
    row = pl.BlockSpec((1, rows, width), lambda s: (s, 0, 0))
    stack = lambda last: pl.BlockSpec((1, stacked, last), lambda s: (s, 0, 0))
    pairs_spec = pl.BlockSpec((shards, 1, rows, pair), lambda s: (0, s, 0, 0))
    return pl.pallas_call(
        functools.partial(attend_backward_kernel, heads, min(shards, 16)),
        grid=(sequences,),
        in_specs=[
            row,
            pairs_spec,
            row,
            stack(pair // 2),
            stack(128),
            whole(query_pos.shape),
            whole(key_pos.shape),
        ],
        out_specs=[row, pairs_spec],
        out_shape=[
            jax.ShapeDtypeStruct((sequences, rows, width), F32),
            jax.ShapeDtypeStruct(pairs.shape, BF16),
        ],
        name="attend_backward",
    )(query_low, pairs, grad_mixed, mixed, totals, query_pos, key_pos)


class Ring:
    def __init__(self, devices):
        self.chips = devices // 2
        me = lax.axis_index("ctx")
        self.core = me % 2
        chip = me // 2
        across = chip % 2
        deep = chip // 2
        self.place = deep + across * (self.chips - 1 - 2 * deep)
        self.partner = me + 1 - 2 * self.core
        self.right = self.device((self.place + 1) % self.chips, self.core)
        self.left = self.device((self.place + self.chips - 1) % self.chips, self.core)

    def device(self, place, core):
        side = place // (self.chips // 2)
        return 2 * (2 * (place + side * (self.chips - 1 - 2 * place)) + side) + core

    def enter(self, across=False):
        barrier = pltpu.get_barrier_semaphore()
        targets = [{"ctx": other} for other in (self.left, self.right, self.partner)]
        if across:
            targets.append({"wsh": 1 - lax.axis_index("wsh")})
        for target in targets:
            pl.semaphore_signal(barrier, inc=1, device_id=target, device_id_type=MESH)
        pl.semaphore_wait(barrier, len(targets))


def ring_sum_kernel(devices, pieces, arrays, ahead, *refs):
    parts, outs = refs[:arrays], refs[arrays : 2 * arrays]
    own, other, flow = (refs[(2 + i) * arrays : (3 + i) * arrays] for i in range(3))
    own_sem, put_sem, got_sem, send_sem, recv_sem = refs[5 * arrays :]
    ring = Ring(devices)
    chips = ring.chips

    def region(p):
        array, _, first, rows, start, cols = pieces[p]
        return array, pl.ds(first, rows), pl.ds(start, cols)

    def chunk(p, step):
        way = pieces[p][1]
        return (ring.place + 2 * chips + way * (-1 - step)) % chips

    def load(p, step):
        array, rows, cols = region(p)
        source = ring.device(chunk(p, step), ring.core)
        return pltpu.make_async_copy(
            parts[array].at[source, rows, cols],
            own[array].at[step, rows, cols],
            own_sem.at[p, step],
        )

    def give(p, step):
        array, rows, cols = region(p)
        source = ring.device(chunk(p, step), 1 - ring.core)
        return pltpu.make_async_remote_copy(
            src_ref=parts[array].at[source, rows, cols],
            dst_ref=other[array].at[step, rows, cols],
            send_sem=put_sem.at[p, step],
            recv_sem=got_sem.at[p, step],
            device_id={"ctx": ring.partner},
            device_id_type=MESH,
        )

    def pass_on(p, step):
        array, rows, cols = region(p)
        way = pieces[p][1]
        return pltpu.make_async_remote_copy(
            src_ref=flow[array].at[step, rows, cols],
            dst_ref=flow[array].at[step + 1, rows, cols],
            send_sem=send_sem.at[p, step],
            recv_sem=recv_sem.at[p, step],
            device_id={"ctx": ring.right if way > 0 else ring.left},
            device_id_type=MESH,
        )

    def fetch(step):
        for p in range(len(pieces)):
            load(p, step).start()
            give(p, step).start()

    def add(p, step, first, last):
        array, _, row, rows, start, cols = pieces[p]
        width = 128 if cols % 128 == 0 else cols
        while width < 512 and cols % (2 * width) == 0:
            width *= 2
        rows = pl.ds(row, rows)

        def group(i, carry):
            at = start + i * width
            if cols > width:
                at = pl.multiple_of(at, 128)
            where = pl.ds(at, width)
            total = own[array][step, rows, where].astype(F32) + other[array][
                step, rows, where
            ].astype(F32)
            if not first:
                total += flow[array][step, rows, where].astype(F32)
            if last:
                outs[array][rows, where] = total.astype(outs[array].dtype)
            else:
                flow[array][step, rows, where] = total.astype(flow[array].dtype)
            return carry

        if cols == width:
            group(0, 0)
        else:
            lax.fori_loop(0, cols // width, group, 0)

    def work(step, first=False, last=False):
        for p in range(len(pieces)):
            load(p, step).wait()
            give(p, step).wait_recv()
            if not first:
                pass_on(p, step - 1).wait_recv()
            add(p, step, first, last)
            if not last:
                pass_on(p, step).start()

    for p in range(len(pieces)):
        load(p, 0).start()
    ring.enter()
    for p in range(len(pieces)):
        give(p, 0).start()
    for step in range(1, min(ahead, chips)):
        fetch(step)
    work(0, first=True)

    def middle(step, carry):
        @pl.when(step + ahead - 1 < chips)
        def _():
            fetch(step + ahead - 1)

        work(step)
        return carry

    lax.fori_loop(1, chips - 1, middle, 0)
    work(chips - 1, last=True)

    def drain(step, carry):
        for p in range(len(pieces)):
            give(p, step).wait_send()

            @pl.when(step < chips - 1)
            def _():
                pass_on(p, step).wait_send()

        return carry

    lax.fori_loop(0, chips, drain, 0)


def ring_sum(parts, pieces, devices, collective_id, ahead=3, name="ring_sum"):
    chips, count, arrays = devices // 2, len(pieces), len(parts)
    slots = [pltpu.VMEM((chips,) + p.shape[1:], p.dtype) for p in parts]
    return pl.pallas_call(
        functools.partial(ring_sum_kernel, devices, pieces, arrays, ahead),
        out_shape=[jax.ShapeDtypeStruct(p.shape[1:], F32) for p in parts],
        in_specs=[pl.BlockSpec(memory_space=pl.ANY)] * arrays,
        out_specs=[pl.BlockSpec(memory_space=pltpu.VMEM)] * arrays,
        scratch_shapes=slots * 3
        + [pltpu.SemaphoreType.DMA((count, chips))] * 3
        + [pltpu.SemaphoreType.DMA((count, chips - 1))] * 2,
        compiler_params=pltpu.CompilerParams(
            collective_id=collective_id, has_side_effects=True, vmem_limit_bytes=64000 * 1024
        ),
        name=name,
    )(*parts)


def split_ways(parts):
    pieces, lead = [], 1
    for i, p in enumerate(parts):
        _, rows, cols = p.shape
        tiles = cols // 128
        if cols % 128 == 0 and tiles > 1:
            left = (tiles + (1 if lead > 0 else 0)) // 2 * 128
            if tiles % 2:
                lead = -lead
            pieces.append((i, 1, 0, rows, 0, left))
            pieces.append((i, -1, 0, rows, left, cols - left))
        elif rows % 32 == 0:
            pieces.append((i, 1, 0, rows // 2, 0, cols))
            pieces.append((i, -1, rows // 2, rows // 2, 0, cols))
        else:
            pieces.append((i, 1, 0, rows, 0, cols))
    return tuple(pieces)


def sum_over_ctx(parts, pieces, devices, collective_id):
    if all(p.shape[1] % 8 == 0 for p in parts):
        return ring_sum(parts, pieces, devices, collective_id)
    return [
        lax.psum_scatter(p, "ctx", scatter_dimension=0, tiled=False).astype(F32) for p in parts
    ]


def front_kernel(
    devices,
    heads,
    tokens_ref,
    gains_ref,
    cos_ref,
    sin_ref,
    query_pos_ref,
    key_pos_ref,
    key_weight,
    value_weight,
    query_weight,
    out_weight,
    pairs_ref,
    normed_ref,
    key_ref,
    query_ref,
    query_low_ref,
    mixed_low_ref,
    mixed_ref,
    totals_ref,
    all_gains_ref,
    pair_whole,
    query_whole,
    out_whole,
    gains_other,
    own_sem,
    cross_send,
    cross_recv,
    side_send,
    side_recv,
    flow_send,
    flow_recv,
    twin_send,
    twin_recv,
):
    ring = Ring(devices)
    chips, far = ring.chips, ring.chips // 2
    me = lax.axis_index("ctx")
    mine = lax.axis_index("wsh")
    sequences, rows, width = tokens_ref.shape
    count = sequences * rows
    size = key_ref.shape[1]
    block = rows // 2
    stacked = heads * block
    weights = (key_weight, value_weight, query_weight, out_weight)

    def region(i, side, first, lines):
        if i == 3:
            start = side * out_weight.shape[0] + first
            return out_whole.at[pl.ds(pl.multiple_of(start, 16), lines)]
        cols = weights[i].shape[1]
        start = side * cols + (size if i == 1 else 0)
        target = query_whole if i == 2 else pair_whole
        return target.at[pl.ds(pl.multiple_of(first, 16), lines), pl.ds(pl.multiple_of(start, 128), cols)]

    def own(i):
        return pltpu.make_async_copy(
            weights[i], region(i, mine, 0, weights[i].shape[0]), own_sem.at[i]
        )

    def cross(i):
        if i == len(weights):
            source, target = gains_ref, gains_other
        else:
            half = weights[i].shape[0] // 2
            first = pl.multiple_of(ring.core * half, 16)
            source, target = weights[i].at[pl.ds(first, half)], region(i, mine, first, half)
        return pltpu.make_async_remote_copy(
            src_ref=source,
            dst_ref=target,
            send_sem=cross_send.at[i],
            recv_sem=cross_recv.at[i],
            device_id={"wsh": 1 - mine},
            device_id_type=MESH,
        )

    def side(i):
        half = weights[i].shape[0] // 2
        part = region(i, 1 - mine, ring.core * half, half)
        return pltpu.make_async_remote_copy(
            src_ref=part,
            dst_ref=part,
            send_sem=side_send.at[i],
            recv_sem=side_recv.at[i],
            device_id={"ctx": ring.partner},
            device_id_type=MESH,
        )

    def block_copy(way, seq, hop, target, send_sem, recv_sem):
        stream = (1 if way < 0 else 0) * sequences + seq
        place = (ring.place + chips - way * hop) % chips
        part = pairs_ref.at[ring.device(place, ring.core), seq]
        return pltpu.make_async_remote_copy(
            src_ref=part,
            dst_ref=part,
            send_sem=send_sem.at[stream, hop],
            recv_sem=recv_sem.at[stream, hop],
            device_id={"ctx": target},
            device_id_type=MESH,
        )

    def flow(way, seq, hop):
        target = ring.right if way > 0 else ring.left
        return block_copy(way, seq, hop, target, flow_send, flow_recv)

    def twin(way, seq, hop):
        return block_copy(way, seq, hop, ring.partner, twin_send, twin_recv)

    def hops(way, seq):
        return far if (seq % 2 == 0) == (way > 0) else far - 1

    streams = [(way, seq) for seq in range(sequences) for way in (1, -1)]

    def pass_on(hop):
        for way, seq in streams:
            if hop > hops(way, seq):
                continue
            if hop > 0:
                flow(way, seq, hop - 1).wait_recv()
            if hop < hops(way, seq):
                flow(way, seq, hop).start()
            if hop > 0 or way > 0:
                twin(way, seq, hop).start()

    def turned(value, gain):
        scale = lax.rsqrt(jnp.mean(value * value, -1, keepdims=True) + EPS)
        value = value * scale * gain
        first, second = value[:, : size // 2], value[:, size // 2 :]
        cosine = jnp.concatenate([cos_ref[...]] * sequences, 0)
        sine = jnp.concatenate([sin_ref[...]] * sequences, 0)
        return jnp.concatenate(
            [first * cosine - second * sine, second * cosine + first * sine], -1
        ).astype(BF16)

    def queries():
        gain = all_gains_ref[4:5, :size]
        for h in range(heads):
            cols = slice(h * size, (h + 1) * size)
            value = dot(normed_ref[...], query_whole[:, cols], ((1,), (0,)))
            query_ref[:, cols] = value
            query_low_ref[:, :, cols] = turned(value, gain).reshape(sequences, rows, size)

    def attention(seq, carry):
        chunk = min(devices, 16)
        asked, sums, totals = [], [], []
        for half in range(2):
            lines = slice(half * block, (half + 1) * block)
            asked.append(
                jnp.concatenate(
                    [query_low_ref[seq, lines, h * size : (h + 1) * size] for h in range(heads)], 0
                )
            )
            sums.append(jnp.zeros((stacked, size), F32))
            totals.append(jnp.zeros((stacked, 1), F32))
        for first in range(0, devices, chunk):
            span = slice(first * block, (first + chunk) * block)
            for key_half in range(2):
                part = pairs_ref[
                    first : first + chunk, seq, key_half * block : (key_half + 1) * block, :
                ].reshape(chunk * block, 2 * size)
                keys, values = part[:, :size], part[:, size:]
                for half in range(key_half, 2):
                    weights = jnp.exp(dot(asked[half], keys, ((1,), (1,))) * SCORE_SCALE)
                    if half == key_half:
                        allowed = (
                            key_pos_ref[key_half : key_half + 1, span]
                            <= query_pos_ref[half * stacked : (half + 1) * stacked, :]
                        )
                        weights = jnp.where(allowed, weights, 0.0)
                    low = weights.astype(BF16)
                    totals[half] += jnp.sum(low.astype(F32), -1, keepdims=True)
                    sums[half] += dot(low, values, ((1,), (0,)))
        for half in range(2):
            mixed = sums[half] / totals[half]
            span = slice(half * stacked, (half + 1) * stacked)
            mixed_ref[seq, span, :] = mixed
            totals_ref[seq, span, :] = jnp.broadcast_to(
                totals[half], (stacked, totals_ref.shape[2])
            )
            for h in range(heads):
                mixed_low_ref[
                    seq, half * block : (half + 1) * block, h * size : (h + 1) * size
                ] = mixed[h * block : (h + 1) * block].astype(BF16)
        return carry

    for i in range(len(weights)):
        own(i).start()
    ring.enter(across=True)
    order = (len(weights), 0, 1, 2, 3)
    for i in order:
        cross(i).start()
    inputs = tokens_ref[...].reshape(count, width).astype(F32)
    scale = lax.rsqrt(jnp.mean(inputs * inputs, -1, keepdims=True) + EPS)
    cross(len(weights)).wait_recv()
    all_gains_ref[...] = gains_ref[...] + gains_other[...]
    normed_ref[...] = (inputs * scale * all_gains_ref[0:1, :]).astype(BF16)
    for i in (0, 1):
        cross(i).wait_recv()
        side(i).start()
    for i in (0, 1):
        own(i).wait()
        side(i).wait_recv()
    value = dot(normed_ref[...], pair_whole[...], ((1,), (0,)))
    key_ref[...] = value[:, :size]
    key_low = turned(value[:, :size], all_gains_ref[4:5, size : 2 * size])
    pairs_ref[me, :, :, :size] = key_low.reshape(sequences, rows, size)
    pairs_ref[me, :, :, size:] = value[:, size:].astype(BF16).reshape(sequences, rows, size)
    pass_on(0)
    pass_on(1)
    cross(2).wait_recv()
    side(2).start()
    for hop in range(2, far + 1):
        pass_on(hop)
        if hop == 2:
            own(2).wait()
            side(2).wait_recv()
            queries()
    cross(3).wait_recv()
    side(3).start()
    for hop in range(far + 1):
        for way, seq in streams:
            if hop <= hops(way, seq) and (hop > 0 or way > 0):
                twin(way, seq, hop).wait_recv()
    lax.fori_loop(0, sequences, attention, 0)
    for hop in range(far + 1):
        for way, seq in streams:
            if hop > hops(way, seq):
                continue
            if hop > 0 or way > 0:
                twin(way, seq, hop).wait_send()
            if hop < hops(way, seq):
                flow(way, seq, hop).wait_send()
    own(3).wait()
    side(3).wait_recv()
    for i in order:
        cross(i).wait_send()
    for i in range(len(weights)):
        side(i).wait_send()


def front(tokens, gains, cosine, sine, query_pos, key_pos, weights, heads, devices, collective_id):
    sequences, rows, width = tokens.shape
    size = 2 * cosine.shape[1]
    count = sequences * rows
    far = devices // 4
    stacked = query_pos.shape[0]
    here, there = pl.BlockSpec(memory_space=pltpu.VMEM), pl.BlockSpec(memory_space=pl.ANY)
    streams = pltpu.SemaphoreType.DMA((2 * sequences, far + 1))
    outs = [
        ((devices, sequences, rows, 2 * size), BF16),
        ((count, width), BF16),
        ((count, size), F32),
        ((count, heads * size), F32),
        ((sequences, rows, heads * size), BF16),
        ((sequences, rows, heads * size), BF16),
        ((sequences, stacked, size), F32),
        ((sequences, stacked, 128), F32),
        (gains.shape, F32),
        ((width, 2 * size), BF16),
        ((width, heads * size), BF16),
        ((width, heads * size), BF16),
    ]
    return pl.pallas_call(
        functools.partial(front_kernel, devices, heads),
        in_specs=[here] * 6 + [there] * 4,
        out_specs=[here] * len(outs),
        out_shape=[jax.ShapeDtypeStruct(shape, kind) for shape, kind in outs],
        scratch_shapes=[pltpu.VMEM(gains.shape, gains.dtype)]
        + [pltpu.SemaphoreType.DMA((4,))]
        + [pltpu.SemaphoreType.DMA((5,))] * 2
        + [pltpu.SemaphoreType.DMA((4,))] * 2
        + [streams] * 4,
        compiler_params=pltpu.CompilerParams(
            collective_id=collective_id, has_side_effects=True, vmem_limit_bytes=67043328
        ),
        name="front",
    )(tokens, gains, cosine, sine, query_pos, key_pos, *weights)


class RingSum:
    def __init__(self, ring, pieces, parts, own, other, flow, outs, sems):
        self.ring, self.pieces, self.parts, self.own = ring, pieces, parts, own
        self.other, self.flow, self.outs = other, flow, outs
        self.put_sem, self.got_sem, self.send_sem, self.recv_sem = sems[:4]
        self.own_sem = sems[4] if own is not None else None
        self.last = ring.chips - 1

    def region(self, p):
        array, _, first, rows, start, cols = self.pieces[p]
        return array, pl.ds(first, rows), pl.ds(start, cols)

    def owner(self, p, step, core):
        way = self.pieces[p][1]
        chips = self.ring.chips
        return self.ring.device((self.ring.place + 2 * chips + way * (-1 - step)) % chips, core)

    def load(self, p, step):
        array, rows, cols = self.region(p)
        slot = step % self.own[array].shape[0]
        return pltpu.make_async_copy(
            self.parts[array].at[self.owner(p, step, self.ring.core), rows, cols],
            self.own[array].at[slot, rows, cols],
            self.own_sem.at[p, step],
        )

    def give(self, p, step):
        array, rows, cols = self.region(p)
        return pltpu.make_async_remote_copy(
            src_ref=self.parts[array].at[self.owner(p, step, 1 - self.ring.core), rows, cols],
            dst_ref=self.other[array].at[step, rows, cols],
            send_sem=self.put_sem.at[p, step],
            recv_sem=self.got_sem.at[p, step],
            device_id={"ctx": self.ring.partner},
            device_id_type=MESH,
        )

    def hop(self, p, step):
        array, rows, cols = self.region(p)
        way = self.pieces[p][1]
        return pltpu.make_async_remote_copy(
            src_ref=self.flow[array].at[step, rows, cols],
            dst_ref=self.flow[array].at[step + 1, rows, cols],
            send_sem=self.send_sem.at[p, step],
            recv_sem=self.recv_sem.at[p, step],
            device_id={"ctx": self.ring.right if way > 0 else self.ring.left},
            device_id_type=MESH,
        )

    def load_all(self, step):
        for p in range(len(self.pieces)):
            self.load(p, step).start()

    def give_all(self, step):
        for p in range(len(self.pieces)):
            self.give(p, step).start()

    def work(self, p, step):
        array, _, row, rows, start, cols = self.pieces[p]
        if self.own is not None:
            self.load(p, step).wait()
            mine, at_mine = self.own[array], step % self.own[array].shape[0]
        else:
            mine, at_mine = self.parts[array], self.owner(p, step, self.ring.core)
        self.give(p, step).wait_recv()
        if step > 0:
            self.hop(p, step - 1).wait_recv()
        width = 128 if cols % 128 == 0 else cols
        while width < 512 and cols % (2 * width) == 0:
            width *= 2
        rows = pl.ds(row, rows)

        def group(i, carry):
            at = start + i * width
            if cols > width:
                at = pl.multiple_of(at, 128)
            where = pl.ds(at, width)
            total = mine[at_mine, rows, where].astype(F32)
            total += self.other[array][step, rows, where].astype(F32)
            if step > 0:
                total += self.flow[array][step, rows, where].astype(F32)
            if step == self.last:
                self.outs[array][rows, where] = total.astype(self.outs[array].dtype)
            else:
                self.flow[array][step, rows, where] = total.astype(self.flow[array].dtype)
            return carry

        if cols == width:
            group(0, 0)
        else:
            lax.fori_loop(0, cols // width, group, 0)
        if step < self.last:
            self.hop(p, step).start()

    def drain(self):
        for p in range(len(self.pieces)):
            for step in range(self.last + 1):
                self.give(p, step).wait_send()
                if step < self.last:
                    self.hop(p, step).wait_send()


def norm_back(upstream, vector, gain):
    scale = lax.rsqrt(jnp.mean(vector * vector, -1, keepdims=True) + EPS)
    normal = vector * scale
    weighted = upstream * gain
    back = scale * (weighted - normal * jnp.mean(weighted * normal, -1, keepdims=True))
    return back, jnp.sum(upstream * normal, 0, keepdims=True)


GELU_SCALE = math.sqrt(2.0 / math.pi)
GELU_CUBE = 0.044715


def feed_forward_kernel(
    mixed_ref,
    tokens_ref,
    cotangent_ref,
    gains_ref,
    out_hbm,
    gate_hbm,
    up_hbm,
    down_hbm,
    output_ref,
    hidden_back_ref,
    mixed_back_ref,
    attended_own_ref,
    attended_send_ref,
    gain_part_ref,
    down_grad_hbm,
    gate_grad_hbm,
    up_grad_hbm,
    gate_weight,
    up_weight,
    down_weight,
    out_weight,
    attended_ref,
    ff_rows,
    low_rows,
    ff_turned,
    low_turned,
    gate,
    upward,
    activated,
    partial,
    part_send,
    part_recv,
    back_send,
    back_recv,
    hidden_ref,
    staging,
    load_sem,
    out_sem,
    store_sem,
    cross_send,
    cross_recv,
):
    count, width = attended_ref.shape
    hidden_units = gate_weight.shape[1]
    block = part_send.shape[0] // 2
    chunk = staging.shape[2]
    whole_chunks = hidden_units // chunk
    rest = hidden_units - whole_chunks * chunk
    mine = lax.axis_index("wsh")
    weights = ((gate_hbm, gate_weight), (up_hbm, up_weight), (down_hbm, down_weight))

    def load(w, at, size, index):
        source, target = weights[w]
        cols = pl.ds(at, size)
        return pltpu.make_async_copy(source.at[:, cols], target.at[:, cols], load_sem.at[w, index])

    def chunks(work):
        def step(c, carry):
            work(pl.multiple_of(c * chunk, 128), chunk, c)
            return carry

        lax.fori_loop(0, whole_chunks, step, 0)
        if rest:
            work(whole_chunks * chunk, rest, whole_chunks)

    def across(kind, piece, source, target):
        return pltpu.make_async_remote_copy(
            src_ref=source,
            dst_ref=target,
            send_sem=cross_send.at[kind, piece],
            recv_sem=cross_recv.at[kind, piece],
            device_id={"wsh": 1 - mine},
            device_id_type=MESH,
        )

    def swap_rows(kind, ref, piece):
        first = piece * block
        return across(
            kind, piece, ref.at[pl.ds(first, block)], ref.at[pl.ds(count + first, block)]
        )

    def swap_parts(kind, source, target, piece):
        lines = pl.ds(piece * block, block)
        return across(kind, piece, source.at[lines], target.at[lines])

    def start_load(at, size, index):
        for w in range(3):
            load(w, at, size, index).start()

    bring_out = pltpu.make_async_copy(out_hbm, out_weight, out_sem.at[0])
    bring_out.start()
    chunks(start_load)
    barrier = pltpu.get_barrier_semaphore()
    pl.semaphore_signal(barrier, inc=1, device_id={"wsh": 1 - mine}, device_id_type=MESH)

    bring_out.wait()
    attended = dot(mixed_ref[...], out_weight[...], ((1,), (1,)))
    attended_ref[...] = attended
    scale = lax.rsqrt(jnp.mean(attended * attended, -1, keepdims=True) + EPS)
    hidden = tokens_ref[...].astype(F32) + attended * scale * gains_ref[1:2, :]
    hidden_ref[...] = hidden
    scale = lax.rsqrt(jnp.mean(hidden * hidden, -1, keepdims=True) + EPS)
    ff_rows[:count, :] = (hidden * scale * gains_ref[2:3, :]).astype(BF16)
    pl.semaphore_wait(barrier, 1)
    for piece in range(2):
        swap_rows(0, ff_rows, piece).start()

    def forward(first, rows, fresh=False):
        lines = pl.ds(first, rows)

        def columns(at, size, index):
            if fresh:
                for w in range(3):
                    load(w, at, size, index).wait()
            cols = pl.ds(at, size)
            g = dot(ff_rows[lines, :], gate_weight[:, cols], ((1,), (0,)))
            u = dot(ff_rows[lines, :], up_weight[:, cols], ((1,), (0,)))
            square = g * g
            t = jnp.tanh(g * (GELU_SCALE + GELU_SCALE * GELU_CUBE * square))
            half = 0.5 + 0.5 * t
            gelu = g * half
            slope = half + gelu * (1.0 - t) * (GELU_SCALE + 3.0 * GELU_SCALE * GELU_CUBE * square)
            gate[lines, cols] = (u * slope).astype(BF16)
            upward[lines, cols] = gelu.astype(BF16)
            activated[lines, cols] = (gelu * u).astype(BF16)

        chunks(columns)
        return dot(activated[lines, :], down_weight[...], ((1,), (1,)))

    partial[...] = forward(0, count, fresh=True)
    for piece in range(2):
        swap_rows(0, ff_rows, piece).wait_recv()
        there = pl.ds(piece * block, block)
        part_send[there, :] = forward(count + piece * block, block).astype(BF16)
        swap_parts(1, part_send, part_recv, piece).start()
    ff_turned[...] = ff_rows[...].T
    for piece in range(2):
        swap_parts(1, part_send, part_recv, piece).wait_recv()
    lowered = partial[...] + part_recv[...].astype(F32)
    cotangent = cotangent_ref[...].astype(F32)
    back, part = norm_back(cotangent, lowered, gains_ref[3:4, :])
    low_rows[:count, :] = back.astype(BF16)
    for piece in range(2):
        swap_rows(2, low_rows, piece).start()
    gain_part_ref[...] = jnp.zeros_like(gain_part_ref)
    gain_part_ref[3:4, :] = part
    scale = lax.rsqrt(jnp.mean(lowered * lowered, -1, keepdims=True) + EPS)
    output_ref[...] = (hidden_ref[...] + lowered * scale * gains_ref[3:4, :]).astype(BF16)

    def backward(first, rows):
        lines = pl.ds(first, rows)

        def columns(at, size, index):
            cols = pl.ds(at, size)
            d = dot(low_rows[lines, :], down_weight[:, cols], ((1,), (0,)))
            gate[lines, cols] = (d * gate[lines, cols].astype(F32)).astype(BF16)
            upward[lines, cols] = (d * upward[lines, cols].astype(F32)).astype(BF16)

        chunks(columns)

    def inputs_back(first):
        lines = pl.ds(first, count)
        value = dot(gate[lines, :], gate_weight[...], ((1,), (1,)))
        return value + dot(upward[lines, :], up_weight[...], ((1,), (1,)))

    backward(0, count)
    partial[...] = inputs_back(0)
    for piece in range(2):
        swap_rows(2, low_rows, piece).wait_recv()
        backward(count + piece * block, block)
    back_send[...] = inputs_back(count).astype(BF16)
    for piece in range(2):
        swap_parts(3, back_send, back_recv, piece).start()
    low_turned[...] = low_rows[...].T

    grads = (
        (low_turned, activated, down_grad_hbm),
        (ff_turned, gate, gate_grad_hbm),
        (ff_turned, upward, up_grad_hbm),
    )

    def store(m, at, size, index):
        cols = pl.ds(at, size)
        return pltpu.make_async_copy(
            staging.at[index % 2, :, pl.ds(0, size)], grads[m][2].at[:, cols], store_sem.at[m, index]
        )

    for m in range(3):
        left, right, _ = grads[m]

        def columns(at, size, index, m=m, left=left, right=right):
            @pl.when(index >= 2)
            def _():
                store(m, 0, chunk, index - 2).wait()

            for top in range(0, width, width // 2):
                lines = slice(top, top + width // 2)
                staging[index % 2, lines, :size] = dot(
                    left[lines, :], right[:, pl.ds(at, size)], ((1,), (0,))
                ).astype(BF16)
            store(m, at, size, index).start()

        chunks(columns)
        last = whole_chunks + (1 if rest else 0)
        for index in range(max(last - 2, 0), last):
            store(m, 0, rest if index == whole_chunks else chunk, index).wait()

    for piece in range(2):
        swap_parts(3, back_send, back_recv, piece).wait_recv()
    upstream = partial[...] + back_recv[...].astype(F32)
    back, part = norm_back(upstream, hidden_ref[...], gains_ref[2:3, :])
    gain_part_ref[2:3, :] = part
    back += cotangent_ref[...].astype(F32)
    hidden_back_ref[...] = back
    back, part = norm_back(back, attended_ref[...], gains_ref[1:2, :])
    gain_part_ref[1:2, :] = part
    mixed_back_ref[...] = dot(back.astype(BF16), out_weight[...], ((1,), (0,))).astype(BF16)
    first, second = back[:, : width // 2].astype(BF16), back[:, width // 2 :].astype(BF16)
    attended_own_ref[...] = jnp.where(mine == 0, first, second)
    attended_send_ref[...] = jnp.where(mine == 0, second, first)
    for piece in range(2):
        swap_rows(0, ff_rows, piece).wait_send()
        swap_parts(1, part_send, part_recv, piece).wait_send()
        swap_rows(2, low_rows, piece).wait_send()
        swap_parts(3, back_send, back_recv, piece).wait_send()


def feed_forward(mixed, tokens, cotangent, gains, weights, collective_id):
    count, width = tokens.shape
    hidden_units = weights[1].shape[1]
    chunk = 512
    pieces = -(-hidden_units // chunk)
    here, there = pl.BlockSpec(memory_space=pltpu.VMEM), pl.BlockSpec(memory_space=pl.ANY)
    like = lambda shape, kind: jax.ShapeDtypeStruct(shape, kind)
    matrix = (width, hidden_units)
    return pl.pallas_call(
        feed_forward_kernel,
        in_specs=[here] * 4 + [there] * 4,
        out_specs=[here] * 6 + [there] * 3,
        out_shape=[
            like((count, width), BF16),
            like((count, width), F32),
            like(mixed.shape, BF16),
            like((count, width // 2), BF16),
            like((count, width // 2), BF16),
            like(gains.shape, F32),
        ]
        + [like(matrix, BF16)] * 3,
        scratch_shapes=[pltpu.VMEM(matrix, BF16)] * 3
        + [pltpu.VMEM(weights[0].shape, BF16), pltpu.VMEM((count, width), F32)]
        + [pltpu.VMEM((2 * count, width), BF16)] * 2
        + [pltpu.VMEM((width, 2 * count), BF16)] * 2
        + [pltpu.VMEM((2 * count, hidden_units), BF16)] * 3
        + [pltpu.VMEM((count, width), F32)]
        + [pltpu.VMEM((count, width), BF16)] * 4
        + [
            pltpu.VMEM((count, width), F32),
            pltpu.VMEM((2, width, chunk), BF16),
            pltpu.SemaphoreType.DMA((3, pieces)),
            pltpu.SemaphoreType.DMA((1,)),
            pltpu.SemaphoreType.DMA((3, pieces)),
            pltpu.SemaphoreType.DMA((4, 2)),
            pltpu.SemaphoreType.DMA((4, 2)),
        ],
        compiler_params=pltpu.CompilerParams(
            collective_id=collective_id, has_side_effects=True, vmem_limit_bytes=67043328
        ),
        name="feed_forward",
    )(mixed, tokens, cotangent, gains, *weights)


def turn_back(upstream, cosine, sine):
    middle = upstream.shape[-1] // 2
    first, second = upstream[:, :middle], upstream[:, middle:]
    return jnp.concatenate([first * cosine + second * sine, second * cosine - first * sine], -1)


def back_kernel(devices, heads, ff_pieces, kv_pieces, attn_pieces, names, *refs):
    r = dict(zip(names, refs))
    ring = Ring(devices)
    chips = ring.chips
    mine = lax.axis_index("wsh")
    sequences, rows, _ = r["query"].shape
    size = r["key_raw"].shape[1]
    count = sequences * rows
    block = rows // 2
    stacked = heads * block

    ff = RingSum(
        ring,
        ff_pieces,
        [r["part_down"], r["part_gate"], r["part_up"]],
        [r[f"ff_own{i}"] for i in range(3)],
        [r[f"ff_other{i}"] for i in range(3)],
        [r[f"ff_flow{i}"] for i in range(3)],
        [r["grad_down"], r["grad_gate"], r["grad_up"]],
        [r["ff_put"], r["ff_got"], r["ff_send"], r["ff_recv"], r["ff_load"]],
    )
    kv = RingSum(
        ring,
        kv_pieces,
        [r["pairs"]],
        None,
        [r["kv_other"]],
        [r["kv_flow"]],
        [r["kv_sum"]],
        [r["kv_put"], r["kv_got"], r["kv_send"], r["kv_recv"]],
    )
    attn = RingSum(
        ring,
        attn_pieces,
        [r["qkv_part"], r["out_part"]],
        None,
        [r["qkv_other"], r["out_other"]],
        [r["qkv_flow"], r["out_flow"]],
        [r["grad_qkv"], r["grad_out"]],
        [r["at_put"], r["at_got"], r["at_send"], r["at_recv"]],
    )

    def brought(i):
        name = BROUGHT[i]
        return pltpu.make_async_copy(r["in_" + name], r[name], r["bring"].at[i])

    def need(*wanted):
        for name in wanted:
            brought(BROUGHT.index(name)).wait()

    def across(i, source, target):
        return pltpu.make_async_remote_copy(
            src_ref=source,
            dst_ref=target,
            send_sem=r["cross_send"].at[i],
            recv_sem=r["cross_recv"].at[i],
            device_id={"wsh": 1 - mine},
            device_id_type=MESH,
        )

    out_swap = across(0, r["att_send"], r["att_across"])
    col_swap = across(1, r["col_send"], r["col_rows"].at[pl.ds(count, count)])
    gain_swap = across(2, r["gain_own"], r["gain_across"])
    gain_twin = pltpu.make_async_remote_copy(
        src_ref=r["gain_pair"],
        dst_ref=r["gain_twin"],
        send_sem=r["twin_send"].at[0],
        recv_sem=r["twin_recv"].at[0],
        device_id={"ctx": ring.partner},
        device_id_type=MESH,
    )

    def gain_hop(way, step):
        return pltpu.make_async_remote_copy(
            src_ref=r["gain_flow"].at[way, step],
            dst_ref=r["gain_flow"].at[way, step + 1],
            send_sem=r["gain_send"].at[way, step],
            recv_sem=r["gain_recv"].at[way, step],
            device_id={"ctx": ring.right if way == 0 else ring.left},
            device_id_type=MESH,
        )

    gain_hops = (chips // 2, chips - 1 - chips // 2)

    def attention(seq, carry):
        queries, scaled, correction = [], [], []
        for half in range(2):
            span = slice(half * stacked, (half + 1) * stacked)
            lines = slice(half * block, (half + 1) * block)
            cut = lambda ref: jnp.concatenate(
                [ref[seq, lines, h * size : (h + 1) * size] for h in range(heads)], 0
            )
            queries.append(cut(r["query"]))
            grad = cut(r["grad_mixed"]).astype(F32)
            total = r["totals"][seq, span, :1]
            delta = jnp.sum(grad * r["mixed"][seq, span, :], -1, keepdims=True)
            scaled.append((grad / total).astype(BF16))
            correction.append(delta / total)
        grad_query = [jnp.zeros((stacked, size), F32) for _ in range(2)]
        for key_half in range(2):
            lines = pl.ds(pl.multiple_of(seq * rows + key_half * block, block), block)
            part = r["pairs"][:, lines, :].reshape(devices * block, 2 * size)
            keys, values = part[:, :size], part[:, size:]
            grad_keys = jnp.zeros((devices * block, size), F32)
            grad_values = jnp.zeros((devices * block, size), F32)
            for half in range(key_half, 2):
                weights = jnp.exp(dot(queries[half], keys, ((1,), (1,))) * SCORE_SCALE)
                if half == key_half:
                    allowed = (
                        r["key_pos"][key_half : key_half + 1, :]
                        <= r["query_pos"][half * stacked : (half + 1) * stacked, :]
                    )
                    weights = jnp.where(allowed, weights, 0.0)
                low = weights.astype(BF16)
                grad_weights = dot(scaled[half], values, ((1,), (1,)))
                grad_scores = (weights * (grad_weights - correction[half])).astype(BF16)
                grad_query[half] += dot(grad_scores, keys, ((1,), (0,)))
                grad_keys += dot(grad_scores, queries[half], ((0,), (0,)))
                grad_values += dot(low, scaled[half], ((0,), (0,)))
            both = jnp.concatenate([grad_keys * SCORE_SCALE, grad_values], -1).astype(BF16)
            r["pairs"][:, lines, :] = both.reshape(devices, block, 2 * size)
        for half in range(2):
            r["mixed"][seq, half * stacked : (half + 1) * stacked, :] = grad_query[half] * SCORE_SCALE
        return carry

    def pick(value, which):
        middle = value.shape[1] // 2
        return jnp.where(which == 0, value[:, :middle], value[:, middle:])

    def projections():
        need("query_raw", "key_raw", "cosine", "sine", "gains")
        cosine = jnp.concatenate([r["cosine"][...]] * sequences, 0)
        sine = jnp.concatenate([r["sine"][...]] * sequences, 0)
        gain = r["gains"][4:5, :size]
        total = jnp.zeros((1, size), F32)
        lows = []
        for h in range(heads):
            cols = slice(h * size, (h + 1) * size)
            grad = jnp.concatenate(
                [
                    r["mixed"][seq, half * stacked + h * block : half * stacked + (h + 1) * block, :]
                    for seq in range(sequences)
                    for half in range(2)
                ],
                0,
            )
            back, part = norm_back(
                turn_back(grad, cosine, sine), r["query_raw"][:, cols], gain
            )
            total += part
            r["query_low"][:, cols] = back.astype(BF16)
        back, key_total = norm_back(
            turn_back(r["kv_sum"][:, :size], cosine, sine),
            r["key_raw"][...],
            r["gains"][4:5, size : 2 * size],
        )
        r["pair_low"][:, :size] = back.astype(BF16)
        r["pair_low"][:, size:] = r["kv_sum"][:, size:].astype(BF16)
        first = 0
        for value in (
            r["query_low"][...],
            r["pair_low"][:, :size],
            r["pair_low"][:, size:],
        ):
            cols = slice(first, first + value.shape[1] // 2)
            r["col_rows"][:count, cols] = pick(value, mine)
            r["col_send"][:, cols] = pick(value, 1 - mine)
            first += value.shape[1] // 2
        col_swap.start()
        need("weight_query", "weight_pair", "tokens", "grad_hidden", "gain_part")
        grad_normed = dot(r["query_low"][...], r["weight_query"][...], ((1,), (1,)))
        grad_normed += dot(r["pair_low"][...], r["weight_pair"][...], ((1,), (1,)))
        back, part = norm_back(grad_normed, r["tokens"][...].astype(F32), r["gains"][0:1, :])
        r["grad_tokens"][...] = back + r["grad_hidden"][...]
        r["gain_own"][...] = r["gain_part"][...]
        r["gain_own"][0:1, :] = part
        r["gain_own"][4:5, :size] = total
        r["gain_own"][4:5, size : 2 * size] = key_total
        gain_swap.start()

    def out_part():
        need("mixed_own", "mixed_other", "att_own")
        out_swap.wait_recv()
        _, lines, cols = r["out_part"].shape
        value = dot(r["mixed_own"][...], r["att_own"][...], ((0,), (0,)))
        value += dot(r["mixed_other"][...], r["att_across"][...], ((0,), (0,)))
        r["out_part"][...] = value.reshape(devices, lines, cols).astype(BF16)

    def turn_rows():
        need("normed_own", "normed_other")
        r["weight_pair"][:, :count] = r["normed_own"][...].T
        r["weight_pair"][:, count:] = r["normed_other"][...].T

    def qkv_part():
        col_swap.wait_recv()
        _, lines, cols = r["qkv_part"].shape
        width = 256
        for first in range(0, cols, width):
            value = dot(
                r["weight_pair"][...], r["col_rows"][:, first : first + width], ((1,), (0,))
            )
            r["qkv_part"][:, :, first : first + width] = value.reshape(
                devices, lines, width
            ).astype(BF16)

    def gains_step(step):
        if step == 0:
            gain_swap.wait_recv()
            r["gain_pair"][...] = r["gain_own"][...] + r["gain_across"][...]
            gain_twin.start()
        elif step == 1:
            gain_twin.wait_recv()
            both = r["gain_pair"][...] + r["gain_twin"][...]
            r["gain_flow"][0, 0] = both
            r["gain_flow"][1, 0] = both
            r["gain_sum"][...] = both
            for way in range(2):
                gain_hop(way, 0).start()
        else:
            for way in range(2):
                if step - 2 < gain_hops[way]:
                    gain_hop(way, step - 2).wait_recv()
                    if step - 1 < gain_hops[way]:
                        gain_hop(way, step - 1).start()
                    r["gain_sum"][...] += r["gain_flow"][way, step - 1]

    def ff_step(step, extra=()):
        extra = list(extra)
        if step + 1 < chips:
            ff.load_all(step + 1)
        if step + 2 < chips:
            ff.give_all(step + 2)
        for p in range(len(ff_pieces)):
            ff.work(p, step)
            if p % 2 == 1 and extra:
                extra.pop(0)()
        for left in extra:
            left()

    def kv_step(step):
        def run():
            for p in range(len(kv_pieces)):
                kv.work(p, step)

        return run

    def attn_step(step):
        def run():
            gains_step(step)
            for p in range(len(attn_pieces)):
                attn.work(p, step)

        return run

    def bring(first, last):
        for i in range(BROUGHT.index(first), BROUGHT.index(last) + 1):
            brought(i).start()

    ff.load_all(0)
    ring.enter(across=True)
    ff.give_all(0)
    bring("att_send", "key_pos")
    ff.give_all(1)
    ff_step(0)
    need("att_send")
    out_swap.start()
    bring("att_own", BROUGHT[-1])
    need("pairs", "query", "grad_mixed", "mixed", "totals", "query_pos", "key_pos")
    lax.fori_loop(0, sequences, attention, 0)
    for step in range(chips):
        kv.give_all(step)
    ff_step(1, [kv_step(0), kv_step(1), kv_step(2)])
    ff_step(2, [kv_step(3), kv_step(4), kv_step(5)])
    ff_step(3, [kv_step(6), kv_step(7), out_part])
    projections()
    ff_step(4, [turn_rows])
    qkv_part()
    for step in range(chips):
        attn.give_all(step)
    ff_step(5, [attn_step(0), attn_step(1), attn_step(2)])
    ff_step(6, [attn_step(3), attn_step(4), attn_step(5)])
    ff_step(7, [attn_step(6), attn_step(7)])
    r["gains_total"][...] = r["gain_sum"][...]
    for copy in (out_swap, col_swap, gain_swap, gain_twin):
        copy.wait_send()
    for way in range(2):
        for step in range(gain_hops[way]):
            gain_hop(way, step).wait_send()
    ff.drain()
    kv.drain()
    attn.drain()


BROUGHT = (
    "att_send",
    "pairs",
    "query",
    "grad_mixed",
    "mixed",
    "totals",
    "query_pos",
    "key_pos",
    "att_own",
    "mixed_own",
    "mixed_other",
    "query_raw",
    "key_raw",
    "cosine",
    "sine",
    "gains",
    "weight_query",
    "weight_pair",
    "tokens",
    "grad_hidden",
    "gain_part",
    "normed_own",
    "normed_other",
)


def back(given, ff_parts, heads, devices, collective_id):
    chips = devices // 2
    count, width = given["tokens"].shape
    size = given["key_raw"].shape[1]
    out_cols = given["att_send"].shape[1]
    out_lines = given["mixed_own"].shape[1] // devices
    lines = width // devices
    cols = (heads * size + 2 * size) // 2
    slots = lambda n, p: pltpu.VMEM((n,) + tuple(p.shape[1:]), p.dtype)
    ff_pieces = split_ways(ff_parts)
    pair_rows = given["pairs"].shape[1]
    kv_pieces = tuple(
        (0, 1 - 2 * i, i * pair_rows // 2, pair_rows // 2, 0, 2 * size) for i in range(2)
    )
    attn_pieces = (
        (0, 1, 0, lines, 0, cols // 2),
        (0, -1, 0, lines, cols // 2, cols // 2),
        (1, 1, 0, out_lines // 2, 0, out_cols),
        (1, -1, out_lines // 2, out_lines // 2, 0, out_cols),
    )
    dma = lambda *shape: pltpu.SemaphoreType.DMA(shape)
    names, specs, operands = [], [], []
    for name, array in zip(("part_down", "part_gate", "part_up"), ff_parts):
        names.append(name)
        operands.append(array)
    for name in BROUGHT:
        names.append("in_" + name)
        operands.append(given[name])
    outs = {
        "grad_tokens": ((count, width), F32),
        "grad_down": (ff_parts[0].shape[1:], BF16),
        "grad_gate": (ff_parts[1].shape[1:], BF16),
        "grad_up": (ff_parts[2].shape[1:], BF16),
        "grad_qkv": ((lines, cols), F32),
        "grad_out": ((out_lines, out_cols), F32),
        "gains_total": (given["gains"].shape, F32),
    }
    scratch = {}
    for name in BROUGHT:
        shape = given[name].shape
        scratch[name] = pltpu.VMEM(shape, given[name].dtype)
    for i, p in enumerate(ff_parts):
        scratch[f"ff_own{i}"] = slots(2, p)
        scratch[f"ff_other{i}"] = slots(chips, p)
        scratch[f"ff_flow{i}"] = slots(chips, p)
    for kind, pieces in (("ff", ff_pieces), ("kv", kv_pieces), ("at", attn_pieces)):
        for name, steps in (("put", chips), ("got", chips), ("send", chips - 1), ("recv", chips - 1)):
            scratch[f"{kind}_{name}"] = dma(len(pieces), steps)
    scratch["ff_load"] = dma(len(ff_pieces), chips)
    scratch["kv_other"] = slots(chips, given["pairs"])
    scratch["kv_flow"] = slots(chips, given["pairs"])
    scratch["kv_sum"] = pltpu.VMEM((pair_rows, 2 * size), F32)
    scratch["att_across"] = pltpu.VMEM((count, out_cols), BF16)
    scratch["query_low"] = pltpu.VMEM((count, heads * size), BF16)
    scratch["pair_low"] = pltpu.VMEM((count, 2 * size), BF16)
    scratch["col_rows"] = pltpu.VMEM((2 * count, cols), BF16)
    scratch["col_send"] = pltpu.VMEM((count, cols), BF16)
    for name, shape in (("qkv", (lines, cols)), ("out", (out_lines, out_cols))):
        scratch[f"{name}_part"] = pltpu.VMEM((devices,) + shape, BF16)
        scratch[f"{name}_other"] = pltpu.VMEM((chips,) + shape, BF16)
        scratch[f"{name}_flow"] = pltpu.VMEM((chips,) + shape, BF16)
    for name in ("gain_own", "gain_across", "gain_pair", "gain_twin", "gain_sum"):
        scratch[name] = pltpu.VMEM(given["gains"].shape, F32)
    scratch["gain_flow"] = pltpu.VMEM((2, chips // 2 + 1) + given["gains"].shape, F32)
    scratch["bring"] = dma(len(BROUGHT))
    for name, n in (("cross_send", 3), ("cross_recv", 3), ("twin_send", 1), ("twin_recv", 1)):
        scratch[name] = dma(n)
    scratch["gain_send"] = dma(2, chips // 2)
    scratch["gain_recv"] = dma(2, chips // 2)
    names += list(outs) + list(scratch)
    return pl.pallas_call(
        functools.partial(
            back_kernel, devices, heads, ff_pieces, kv_pieces, attn_pieces, tuple(names)
        ),
        in_specs=[pl.BlockSpec(memory_space=pl.ANY)] * len(operands),
        out_specs=[pl.BlockSpec(memory_space=pltpu.VMEM)] * len(outs),
        out_shape=[jax.ShapeDtypeStruct(shape, kind) for shape, kind in outs.values()],
        scratch_shapes=list(scratch.values()),
        compiler_params=pltpu.CompilerParams(
            collective_id=collective_id, has_side_effects=True, vmem_limit_bytes=67043328
        ),
        name="back",
    )(*operands)


def finish_kernel(count, *refs):
    sources, results = refs[:count], list(refs[count:])
    for source in sources:
        first = 0
        while first < source.shape[1]:
            result = results.pop(0)
            result[...] = source[:, first : first + result.shape[1]].astype(result.dtype)
            first += result.shape[1]


def finish(sources, columns):
    outs = [
        jax.ShapeDtypeStruct((source.shape[0], width), kind)
        for source, pieces in zip(sources, columns)
        for kind, width in pieces
    ]
    here = pl.BlockSpec(memory_space=pltpu.VMEM)
    return pl.pallas_call(
        functools.partial(finish_kernel, len(sources)),
        in_specs=[here] * len(sources),
        out_specs=[here] * len(outs),
        out_shape=outs,
        name="finish",
    )(*sources)


def body(
    tokens,
    block_order,
    gain_attn_pre,
    gain_query,
    gain_key,
    gain_attn_post,
    gain_ff_pre,
    gain_ff_post,
    weight_query,
    weight_key,
    weight_value,
    weight_out,
    weight_gate,
    weight_up,
    weight_down,
    cotangent,
):
    sequences, rows, width = tokens.shape
    count = sequences * rows
    block = rows // 2
    devices = lax.axis_size("ctx")
    me = lax.axis_index("ctx")
    mine = lax.axis_index("wsh")

    head_size = 2 * gain_key.shape[0]
    heads = 2 * weight_query.shape[1] // head_size

    lane = jnp.arange(block, dtype=jnp.int32)
    late_order = 2 * devices - 1 - block_order
    early_pos = (block_order[:, None] * block + lane[None]).reshape(-1)
    late_pos = (late_order[:, None] * block + lane[None]).reshape(-1)
    key_pos = jnp.stack([early_pos, late_pos], 0)
    own_first = lax.dynamic_slice_in_dim(block_order, me, 1)[0]
    own_early = own_first * block + lane
    own_late = (2 * devices - 1 - own_first) * block + lane
    own_pos = jnp.concatenate([own_early, own_late])
    query_pos = jnp.concatenate([jnp.tile(own_early, heads), jnp.tile(own_late, heads)])[:, None]

    cosine, sine = angle_tables(own_pos, head_size)

    def placed(gain):
        zeros = jnp.zeros_like(gain)
        return jnp.where(
            mine == 0, jnp.concatenate([gain, zeros]), jnp.concatenate([zeros, gain])
        ).astype(F32)

    own_gains = [placed(g) for g in (gain_attn_pre, gain_attn_post, gain_ff_pre, gain_ff_post)]
    small = [placed(gain_query), placed(gain_key)]
    own_gains.append(jnp.concatenate(small + [jnp.zeros((width - 2 * head_size,), F32)]))
    own_gains = jnp.stack(own_gains + [jnp.zeros((width,), F32)] * 3)
    (
        pairs,
        normed_rows,
        key_raw,
        query_raw,
        query_low,
        mixed_low,
        mixed,
        totals,
        all_gains,
        pair_weight,
        query_weight,
        out_weight,
    ) = front(
        tokens,
        own_gains,
        cosine,
        sine,
        query_pos,
        key_pos,
        (weight_key, weight_value, weight_query, weight_out.T),
        heads,
        devices,
        2,
    )
    attn_pre = all_gains[0]
    query_gain = all_gains[4, :head_size]
    key_gain = all_gains[4, head_size : 2 * head_size]
    mixed_rows = mixed_low.reshape(count, heads * head_size)
    local_size = weight_key.shape[1]
    inputs = tokens.astype(F32)

    def key_path(key_in, key_scale):
        return rotate(norm_gain(key_in, key_scale), cosine[None], sine[None])

    def query_path(query_in, query_scale):
        return rotate(
            norm_gain(query_in, query_scale), cosine[None, :, None, :], sine[None, :, None, :]
        )

    (
        output,
        grad_hidden,
        grad_mixed,
        attended_own,
        attended_send,
        gain_part,
        part_down,
        part_gate,
        part_up,
    ) = feed_forward(
        mixed_rows,
        tokens.reshape(count, width),
        cotangent.reshape(count, width),
        all_gains,
        (out_weight, weight_gate, weight_up, weight_down),
        3,
    )

    def both(own, other):
        return jnp.concatenate([own, other], 0)

    def weight_grad(left, right):
        return dot(left, right, ((0,), (0,))).astype(BF16)

    grad_mixed = grad_mixed.reshape(query_low.shape)
    given = {
        "att_send": attended_send,
        "att_own": attended_own,
        "pairs": pairs.reshape(devices, count, 2 * head_size),
        "query": query_low,
        "grad_mixed": grad_mixed,
        "mixed": mixed,
        "totals": totals,
        "query_pos": query_pos,
        "key_pos": key_pos,
        "mixed_own": mixed_rows,
        "mixed_other": swap(mixed_rows),
        "query_raw": query_raw,
        "key_raw": key_raw,
        "cosine": cosine,
        "sine": sine,
        "gains": all_gains,
        "weight_query": query_weight,
        "weight_pair": pair_weight,
        "tokens": tokens.reshape(count, width),
        "grad_hidden": grad_hidden.reshape(count, width),
        "gain_part": gain_part,
        "normed_own": normed_rows,
        "normed_other": swap(normed_rows),
    }
    aligned = width % (8 * devices) == 0 and mixed_rows.shape[1] % (32 * devices) == 0
    if aligned and count == head_size:
        ff_parts = [
            p.reshape(devices, p.shape[0] // devices, p.shape[1])
            for p in (part_down, part_gate, part_up)
        ]
        grad_tokens, grad_down_w, grad_gate_w, grad_up_w, grad_qkv, grad_out_w, gain_sums = back(
            given, ff_parts, heads, devices, 0
        )
        hidden_cols, query_cols = grad_gate_w.shape[1], heads * head_size // 2
        (
            output,
            grad_tokens,
            grad_down_w,
            grad_gate_w,
            grad_up_w,
            grad_query_w,
            grad_key_w,
            grad_value_w,
            grad_out_w,
        ) = finish(
            [output, grad_tokens, grad_down_w, grad_gate_w, grad_up_w, grad_qkv, grad_out_w],
            [[(BF16, width)], [(F32, width)]]
            + [[(F32, hidden_cols)]] * 3
            + [[(F32, query_cols), (F32, local_size), (F32, local_size)], [(F32, width // 2)]],
        )
        grad_tokens = grad_tokens.reshape(sequences, rows, width)
        place = me * 2 + mine

        def share(row, first, size):
            part = size // (2 * devices)
            return lax.dynamic_slice(gain_sums, (row, first + place * part), (1, part))[0]

        outs = [
            share(0, 0, width),
            share(4, 0, head_size),
            share(4, head_size, head_size),
            share(1, 0, width),
            share(2, 0, width),
            share(3, 0, width),
        ]
    else:
        part_out = weight_grad(
            both(mixed_rows, swap(mixed_rows)),
            both(attended_own, swap(attended_send)),
        )
        grad_query, grad_pairs = attend_backward(
            query_low, pairs, grad_mixed, mixed, totals, query_pos, key_pos, heads
        )
        pair_rows = sequences * rows
        slots = grad_pairs.reshape(devices, pair_rows, 2 * head_size)
        share = pair_rows // 8
        pieces = tuple((0, 1 - 2 * (i % 2), i * share, share, 0, 2 * head_size) for i in range(8))
        own_grads = sum_over_ctx([slots], pieces, devices, 0)[0]
        own_grads = own_grads.reshape(sequences, rows, 2 * head_size)
        grad_key_raw, grad_key_gain = jax.vjp(
            key_path, key_raw.reshape(sequences, rows, head_size), key_gain
        )[1](own_grads[..., :head_size])
        value_grad_low = own_grads[..., head_size:].astype(BF16)
        grad_query_raw, grad_query_gain = jax.vjp(
            query_path, query_raw.reshape(sequences, rows, heads, head_size), query_gain
        )[1](
            grad_query.reshape(sequences, rows, heads, head_size)
        )
        query_grad_low = grad_query_raw.reshape(count, heads * head_size).astype(BF16)
        key_grad_low = grad_key_raw.astype(BF16).reshape(count, head_size)
        value_grad_low = value_grad_low.reshape(count, head_size)
        grad_normed = (
            dot(query_grad_low, query_weight, ((1,), (1,)))
            + dot(jnp.concatenate([key_grad_low, value_grad_low], -1), pair_weight, ((1,), (1,)))
        ).reshape(sequences, rows, width)
        grad_inputs, grad_attn_pre = jax.vjp(norm_gain, inputs, attn_pre)[1](grad_normed)
        grad_tokens = grad_inputs + grad_hidden.reshape(sequences, rows, width)

        def columns(which):
            return jnp.concatenate(
                [half_of(v, which) for v in (query_grad_low, key_grad_low, value_grad_low)], -1
            )

        part_qkv = weight_grad(
            both(normed_rows, swap(normed_rows)), both(columns(mine), swap(columns(1 - mine)))
        )

        gain_grads = [
            grad_attn_pre,
            grad_query_gain,
            grad_key_gain,
            gain_part[1],
            gain_part[2],
            gain_part[3],
        ]
        packed = jnp.concatenate([g.reshape(devices, 2, -1) for g in gain_grads], -1)
        keep = jnp.where(mine == 0, packed[:, 0], packed[:, 1])
        send = jnp.where(mine == 0, packed[:, 1], packed[:, 0])
        packed = keep + swap(send)
        gain_size = packed.shape[-1]
        packed = jnp.pad(packed, ((0, 0), (0, 1024 - gain_size))).reshape(devices, 8, 128)
        parts = [
            p.reshape(devices, p.shape[0] // devices, p.shape[1])
            for p in (part_down, part_gate, part_up, part_qkv, part_out)
        ] + [packed]
        grad_down_w, grad_gate_w, grad_up_w, grad_qkv, grad_out_w, packed = sum_over_ctx(
            parts, split_ways(parts), devices, 1
        )
        packed = packed.reshape(-1)
        outs, first = [], 0
        for g in gain_grads:
            size = g.shape[0] // (2 * devices)
            outs.append(packed[first : first + size])
            first += size
        query_cols = grad_qkv.shape[1] - 2 * local_size
        grad_query_w = grad_qkv[:, :query_cols]
        grad_key_w = grad_qkv[:, query_cols : query_cols + local_size]
        grad_value_w = grad_qkv[:, query_cols + local_size :]
        grad_down_w, grad_gate_w, grad_up_w = (
            g.astype(F32) for g in (grad_down_w, grad_gate_w, grad_up_w)
        )
    output = output.reshape(sequences, rows, width)
    return (
        output,
        grad_tokens,
        *outs,
        grad_query_w,
        grad_key_w,
        grad_value_w,
        grad_out_w,
        grad_gate_w,
        grad_up_w,
        grad_down_w,
    )


def solution(mesh):
    rows, vector, matrix = P("wsh", "ctx", None), P("wsh"), P(None, "wsh")
    in_specs = (rows, P()) + (vector,) * 6 + (matrix,) * 7 + (rows,)
    out_specs = (rows, rows) + (P(("ctx", "wsh")),) * 6 + (P("ctx", "wsh"),) * 7
    return jax.shard_map(body, mesh=mesh, in_specs=in_specs, out_specs=out_specs, check_vma=False)
```

```python
import functools
import math

import jax
import jax.numpy as jnp
from jax import lax
from jax.experimental import pallas as pl
from jax.experimental.pallas import tpu as pltpu
from jax.sharding import PartitionSpec as P

EPS = 1e-06
ROPE_BASE = 1000000.0
SCORE_SCALE = 0.0625
F32 = jnp.float32
BF16 = jnp.bfloat16
MESH = pl.DeviceIdType.MESH


def norm_gain(vector, gain):
    return vector * lax.rsqrt(jnp.mean(vector * vector, -1, keepdims=True) + EPS) * gain


def rotate(vector, cosine, sine):
    middle = vector.shape[-1] // 2
    first = vector[..., :middle]
    second = vector[..., middle:]
    return jnp.concatenate([first * cosine - second * sine, second * cosine + first * sine], -1)


def angle_tables(positions, head_size):
    middle = head_size // 2
    inverse = jnp.exp(
        jnp.arange(middle, dtype=F32) * (-2.0 * math.log(ROPE_BASE) / head_size)
    )
    theta = positions.astype(F32)[:, None] * inverse[None, :]
    return (jnp.cos(theta), jnp.sin(theta))


def swap(value):
    return lax.ppermute(value, "wsh", [(0, 1), (1, 0)])


def half_of(value, which):
    middle = value.shape[-1] // 2
    return jnp.where(which == 0, value[..., :middle], value[..., middle:])


def dot(left, right, dims):
    return lax.dot_general(left, right, (dims, ((), ())), preferred_element_type=F32)


def stack_heads(ref, half, block, heads, size):
    rows = slice(half * block, (half + 1) * block)
    return jnp.concatenate([ref[0, rows, h * size : (h + 1) * size] for h in range(heads)], 0)


def attend_backward_kernel(
    heads, chunk, q_ref, kv_ref, g_ref, mix_ref, tot_ref, qpos_ref, kpos_ref, dq_ref, dkv_ref
):
    shards, _, rows, pair = kv_ref.shape
    block, size = rows // 2, pair // 2
    stacked = heads * block
    queries, scaled, correction = [], [], []
    for half in range(2):
        queries.append(stack_heads(q_ref, half, block, heads, size))
        grad = stack_heads(g_ref, half, block, heads, size).astype(F32)
        span = slice(half * stacked, (half + 1) * stacked)
        total = tot_ref[0, span, :1]
        delta = jnp.sum(grad * mix_ref[0, span, :], -1, keepdims=True)
        scaled.append((grad / total).astype(BF16))
        correction.append(delta / total)
    grad_query = [jnp.zeros((stacked, size), F32) for _ in range(2)]
    for first in range(0, shards, chunk):
        span = slice(first * block, (first + chunk) * block)
        for key_half in range(2):
            part = kv_ref[first : first + chunk, 0, key_half * block : (key_half + 1) * block, :]
            part = part.reshape(chunk * block, pair)
            keys, values = part[:, :size], part[:, size:]
            grad_keys = jnp.zeros((chunk * block, size), F32)
            grad_values = jnp.zeros((chunk * block, size), F32)
            for half in range(key_half, 2):
                weights = jnp.exp(dot(queries[half], keys, ((1,), (1,))) * SCORE_SCALE)
                if half == key_half:
                    allowed = (
                        kpos_ref[key_half : key_half + 1, span]
                        <= qpos_ref[half * stacked : (half + 1) * stacked, :]
                    )
                    weights = jnp.where(allowed, weights, 0.0)
                low = weights.astype(BF16)
                grad_weights = dot(scaled[half], values, ((1,), (1,)))
                grad_scores = (weights * (grad_weights - correction[half])).astype(BF16)
                grad_query[half] += dot(grad_scores, keys, ((1,), (0,)))
                grad_keys += dot(grad_scores, queries[half], ((0,), (0,)))
                grad_values += dot(low, scaled[half], ((0,), (0,)))
            both = jnp.concatenate([grad_keys * SCORE_SCALE, grad_values], -1).astype(BF16)
            dkv_ref[first : first + chunk, 0, key_half * block : (key_half + 1) * block, :] = (
                both.reshape(chunk, block, pair)
            )
    for half in range(2):
        for h in range(heads):
            dq_ref[0, half * block : (half + 1) * block, h * size : (h + 1) * size] = (
                grad_query[half][h * block : (h + 1) * block] * SCORE_SCALE
            )


def whole(shape):
    return pl.BlockSpec(shape, lambda s: (0,) * len(shape))


def attend_backward(query_low, pairs, grad_mixed, mixed, totals, query_pos, key_pos, heads):
    sequences, rows, width = query_low.shape
    shards, _, _, pair = pairs.shape
    stacked = query_pos.shape[0]
    row = pl.BlockSpec((1, rows, width), lambda s: (s, 0, 0))
    stack = lambda last: pl.BlockSpec((1, stacked, last), lambda s: (s, 0, 0))
    pairs_spec = pl.BlockSpec((shards, 1, rows, pair), lambda s: (0, s, 0, 0))
    return pl.pallas_call(
        functools.partial(attend_backward_kernel, heads, min(shards, 16)),
        grid=(sequences,),
        in_specs=[
            row,
            pairs_spec,
            row,
            stack(pair // 2),
            stack(128),
            whole(query_pos.shape),
            whole(key_pos.shape),
        ],
        out_specs=[row, pairs_spec],
        out_shape=[
            jax.ShapeDtypeStruct((sequences, rows, width), F32),
            jax.ShapeDtypeStruct(pairs.shape, BF16),
        ],
        name="attend_backward",
    )(query_low, pairs, grad_mixed, mixed, totals, query_pos, key_pos)


class Ring:
    def __init__(self, devices):
        self.chips = devices // 2
        me = lax.axis_index("ctx")
        self.core = me % 2
        chip = me // 2
        across = chip % 2
        deep = chip // 2
        self.place = deep + across * (self.chips - 1 - 2 * deep)
        self.partner = me + 1 - 2 * self.core
        self.right = self.device((self.place + 1) % self.chips, self.core)
        self.left = self.device((self.place + self.chips - 1) % self.chips, self.core)

    def device(self, place, core):
        side = place // (self.chips // 2)
        return 2 * (2 * (place + side * (self.chips - 1 - 2 * place)) + side) + core

    def enter(self, across=False):
        barrier = pltpu.get_barrier_semaphore()
        targets = [{"ctx": other} for other in (self.left, self.right, self.partner)]
        if across:
            targets.append({"wsh": 1 - lax.axis_index("wsh")})
        for target in targets:
            pl.semaphore_signal(barrier, inc=1, device_id=target, device_id_type=MESH)
        pl.semaphore_wait(barrier, len(targets))


def ring_sum_kernel(devices, pieces, arrays, ahead, *refs):
    parts, outs = refs[:arrays], refs[arrays : 2 * arrays]
    own, other, flow = (refs[(2 + i) * arrays : (3 + i) * arrays] for i in range(3))
    own_sem, put_sem, got_sem, send_sem, recv_sem = refs[5 * arrays :]
    ring = Ring(devices)
    chips = ring.chips

    def region(p):
        array, _, first, rows, start, cols = pieces[p]
        return array, pl.ds(first, rows), pl.ds(start, cols)

    def chunk(p, step):
        way = pieces[p][1]
        return (ring.place + 2 * chips + way * (-1 - step)) % chips

    def load(p, step):
        array, rows, cols = region(p)
        source = ring.device(chunk(p, step), ring.core)
        return pltpu.make_async_copy(
            parts[array].at[source, rows, cols],
            own[array].at[step, rows, cols],
            own_sem.at[p, step],
        )

    def give(p, step):
        array, rows, cols = region(p)
        source = ring.device(chunk(p, step), 1 - ring.core)
        return pltpu.make_async_remote_copy(
            src_ref=parts[array].at[source, rows, cols],
            dst_ref=other[array].at[step, rows, cols],
            send_sem=put_sem.at[p, step],
            recv_sem=got_sem.at[p, step],
            device_id={"ctx": ring.partner},
            device_id_type=MESH,
        )

    def pass_on(p, step):
        array, rows, cols = region(p)
        way = pieces[p][1]
        return pltpu.make_async_remote_copy(
            src_ref=flow[array].at[step, rows, cols],
            dst_ref=flow[array].at[step + 1, rows, cols],
            send_sem=send_sem.at[p, step],
            recv_sem=recv_sem.at[p, step],
            device_id={"ctx": ring.right if way > 0 else ring.left},
            device_id_type=MESH,
        )

    def fetch(step):
        for p in range(len(pieces)):
            load(p, step).start()
            give(p, step).start()

    def add(p, step, first, last):
        array, _, row, rows, start, cols = pieces[p]
        width = 128 if cols % 128 == 0 else cols
        while width < 512 and cols % (2 * width) == 0:
            width *= 2
        rows = pl.ds(row, rows)

        def group(i, carry):
            at = start + i * width
            if cols > width:
                at = pl.multiple_of(at, 128)
            where = pl.ds(at, width)
            total = own[array][step, rows, where].astype(F32) + other[array][
                step, rows, where
            ].astype(F32)
            if not first:
                total += flow[array][step, rows, where].astype(F32)
            if last:
                outs[array][rows, where] = total.astype(outs[array].dtype)
            else:
                flow[array][step, rows, where] = total.astype(flow[array].dtype)
            return carry

        if cols == width:
            group(0, 0)
        else:
            lax.fori_loop(0, cols // width, group, 0)

    def work(step, first=False, last=False):
        for p in range(len(pieces)):
            load(p, step).wait()
            give(p, step).wait_recv()
            if not first:
                pass_on(p, step - 1).wait_recv()
            add(p, step, first, last)
            if not last:
                pass_on(p, step).start()

    for p in range(len(pieces)):
        load(p, 0).start()
    ring.enter()
    for p in range(len(pieces)):
        give(p, 0).start()
    for step in range(1, min(ahead, chips)):
        fetch(step)
    work(0, first=True)

    def middle(step, carry):
        @pl.when(step + ahead - 1 < chips)
        def _():
            fetch(step + ahead - 1)

        work(step)
        return carry

    lax.fori_loop(1, chips - 1, middle, 0)
    work(chips - 1, last=True)

    def drain(step, carry):
        for p in range(len(pieces)):
            give(p, step).wait_send()

            @pl.when(step < chips - 1)
            def _():
                pass_on(p, step).wait_send()

        return carry

    lax.fori_loop(0, chips, drain, 0)


def ring_sum(parts, pieces, devices, collective_id, ahead=3, name="ring_sum"):
    chips, count, arrays = devices // 2, len(pieces), len(parts)
    slots = [pltpu.VMEM((chips,) + p.shape[1:], p.dtype) for p in parts]
    return pl.pallas_call(
        functools.partial(ring_sum_kernel, devices, pieces, arrays, ahead),
        out_shape=[jax.ShapeDtypeStruct(p.shape[1:], F32) for p in parts],
        in_specs=[pl.BlockSpec(memory_space=pl.ANY)] * arrays,
        out_specs=[pl.BlockSpec(memory_space=pltpu.VMEM)] * arrays,
        scratch_shapes=slots * 3
        + [pltpu.SemaphoreType.DMA((count, chips))] * 3
        + [pltpu.SemaphoreType.DMA((count, chips - 1))] * 2,
        compiler_params=pltpu.CompilerParams(
            collective_id=collective_id, has_side_effects=True, vmem_limit_bytes=64000 * 1024
        ),
        name=name,
    )(*parts)


def split_ways(parts):
    pieces, lead = [], 1
    for i, p in enumerate(parts):
        _, rows, cols = p.shape
        tiles = cols // 128
        if cols % 128 == 0 and tiles > 1:
            left = (tiles + (1 if lead > 0 else 0)) // 2 * 128
            if tiles % 2:
                lead = -lead
            pieces.append((i, 1, 0, rows, 0, left))
            pieces.append((i, -1, 0, rows, left, cols - left))
        elif rows % 32 == 0:
            pieces.append((i, 1, 0, rows // 2, 0, cols))
            pieces.append((i, -1, rows // 2, rows // 2, 0, cols))
        else:
            pieces.append((i, 1, 0, rows, 0, cols))
    return tuple(pieces)


def sum_over_ctx(parts, pieces, devices, collective_id):
    if all(p.shape[1] % 8 == 0 for p in parts):
        return ring_sum(parts, pieces, devices, collective_id)
    return [
        lax.psum_scatter(p, "ctx", scatter_dimension=0, tiled=False).astype(F32) for p in parts
    ]


def front_kernel(
    devices,
    heads,
    tokens_ref,
    gains_ref,
    cos_ref,
    sin_ref,
    query_pos_ref,
    key_pos_ref,
    key_weight,
    value_weight,
    query_weight,
    out_weight,
    normed_ref,
    key_ref,
    query_low_ref,
    mixed_low_ref,
    mixed_ref,
    totals_ref,
    all_gains_ref,
    pairs_hbm,
    query_hbm,
    pair_whole_hbm,
    query_whole_hbm,
    out_whole_hbm,
    pairs_ref,
    query_ref,
    pair_whole,
    query_whole,
    out_whole,
    gains_other,
    keep_sem,
    own_sem,
    cross_send,
    cross_recv,
    side_send,
    side_recv,
    flow_send,
    flow_recv,
    twin_send,
    twin_recv,
):
    ring = Ring(devices)
    chips, far = ring.chips, ring.chips // 2
    me = lax.axis_index("ctx")
    mine = lax.axis_index("wsh")
    sequences, rows, width = tokens_ref.shape
    count = sequences * rows
    size = key_ref.shape[1]
    block = rows // 2
    stacked = heads * block
    weights = (key_weight, value_weight, query_weight, out_weight)

    def region(i, side, first, lines):
        if i == 3:
            start = side * out_weight.shape[0] + first
            return out_whole.at[pl.ds(pl.multiple_of(start, 16), lines)]
        cols = weights[i].shape[1]
        start = side * cols + (size if i == 1 else 0)
        target = query_whole if i == 2 else pair_whole
        return target.at[pl.ds(pl.multiple_of(first, 16), lines), pl.ds(pl.multiple_of(start, 128), cols)]

    def keep(i):
        source, target = (
            (pairs_ref, pairs_hbm),
            (query_ref, query_hbm),
            (pair_whole, pair_whole_hbm),
            (query_whole, query_whole_hbm),
            (out_whole, out_whole_hbm),
        )[i]
        return pltpu.make_async_copy(source, target, keep_sem.at[i])

    def own(i):
        return pltpu.make_async_copy(
            weights[i], region(i, mine, 0, weights[i].shape[0]), own_sem.at[i]
        )

    def cross(i):
        if i == len(weights):
            source, target = gains_ref, gains_other
        else:
            half = weights[i].shape[0] // 2
            first = pl.multiple_of(ring.core * half, 16)
            source, target = weights[i].at[pl.ds(first, half)], region(i, mine, first, half)
        return pltpu.make_async_remote_copy(
            src_ref=source,
            dst_ref=target,
            send_sem=cross_send.at[i],
            recv_sem=cross_recv.at[i],
            device_id={"wsh": 1 - mine},
            device_id_type=MESH,
        )

    def side(i):
        half = weights[i].shape[0] // 2
        part = region(i, 1 - mine, ring.core * half, half)
        return pltpu.make_async_remote_copy(
            src_ref=part,
            dst_ref=part,
            send_sem=side_send.at[i],
            recv_sem=side_recv.at[i],
            device_id={"ctx": ring.partner},
            device_id_type=MESH,
        )

    def block_copy(way, seq, hop, target, send_sem, recv_sem):
        stream = (1 if way < 0 else 0) * sequences + seq
        place = (ring.place + chips - way * hop) % chips
        part = pairs_ref.at[ring.device(place, ring.core), seq]
        return pltpu.make_async_remote_copy(
            src_ref=part,
            dst_ref=part,
            send_sem=send_sem.at[stream, hop],
            recv_sem=recv_sem.at[stream, hop],
            device_id={"ctx": target},
            device_id_type=MESH,
        )

    def flow(way, seq, hop):
        target = ring.right if way > 0 else ring.left
        return block_copy(way, seq, hop, target, flow_send, flow_recv)

    def twin(way, seq, hop):
        return block_copy(way, seq, hop, ring.partner, twin_send, twin_recv)

    def hops(way, seq):
        return far if (seq % 2 == 0) == (way > 0) else far - 1

    streams = [(way, seq) for seq in range(sequences) for way in (1, -1)]

    def pass_on(hop):
        for way, seq in streams:
            if hop > hops(way, seq):
                continue
            if hop > 0:
                flow(way, seq, hop - 1).wait_recv()
            if hop < hops(way, seq):
                flow(way, seq, hop).start()
            if hop > 0 or way > 0:
                twin(way, seq, hop).start()

    def turned(value, gain):
        scale = lax.rsqrt(jnp.mean(value * value, -1, keepdims=True) + EPS)
        value = value * scale * gain
        first, second = value[:, : size // 2], value[:, size // 2 :]
        cosine = jnp.concatenate([cos_ref[...]] * sequences, 0)
        sine = jnp.concatenate([sin_ref[...]] * sequences, 0)
        return jnp.concatenate(
            [first * cosine - second * sine, second * cosine + first * sine], -1
        ).astype(BF16)

    def queries():
        gain = all_gains_ref[4:5, :size]
        for h in range(heads):
            cols = slice(h * size, (h + 1) * size)
            value = dot(normed_ref[...], query_whole[:, cols], ((1,), (0,)))
            query_ref[:, cols] = value
            query_low_ref[:, :, cols] = turned(value, gain).reshape(sequences, rows, size)

    def attention(seq, carry):
        chunk = min(devices, 16)
        asked, sums, totals = [], [], []
        for half in range(2):
            lines = slice(half * block, (half + 1) * block)
            asked.append(
                jnp.concatenate(
                    [query_low_ref[seq, lines, h * size : (h + 1) * size] for h in range(heads)], 0
                )
            )
            sums.append(jnp.zeros((stacked, size), F32))
            totals.append(jnp.zeros((stacked, 1), F32))
        for first in range(0, devices, chunk):
            span = slice(first * block, (first + chunk) * block)
            for key_half in range(2):
                part = pairs_ref[
                    first : first + chunk, seq, key_half * block : (key_half + 1) * block, :
                ].reshape(chunk * block, 2 * size)
                keys, values = part[:, :size], part[:, size:]
                for half in range(key_half, 2):
                    weights = jnp.exp(dot(asked[half], keys, ((1,), (1,))) * SCORE_SCALE)
                    if half == key_half:
                        allowed = (
                            key_pos_ref[key_half : key_half + 1, span]
                            <= query_pos_ref[half * stacked : (half + 1) * stacked, :]
                        )
                        weights = jnp.where(allowed, weights, 0.0)
                    low = weights.astype(BF16)
                    totals[half] += jnp.sum(low.astype(F32), -1, keepdims=True)
                    sums[half] += dot(low, values, ((1,), (0,)))
        for half in range(2):
            mixed = sums[half] / totals[half]
            span = slice(half * stacked, (half + 1) * stacked)
            mixed_ref[seq, span, :] = mixed
            totals_ref[seq, span, :] = jnp.broadcast_to(
                totals[half], (stacked, totals_ref.shape[2])
            )
            for h in range(heads):
                mixed_low_ref[
                    seq, half * block : (half + 1) * block, h * size : (h + 1) * size
                ] = mixed[h * block : (h + 1) * block].astype(BF16)
        return carry

    for i in range(len(weights)):
        own(i).start()
    ring.enter(across=True)
    order = (len(weights), 0, 1, 2, 3)
    for i in order:
        cross(i).start()
    inputs = tokens_ref[...].reshape(count, width).astype(F32)
    scale = lax.rsqrt(jnp.mean(inputs * inputs, -1, keepdims=True) + EPS)
    cross(len(weights)).wait_recv()
    all_gains_ref[...] = gains_ref[...] + gains_other[...]
    normed_ref[...] = (inputs * scale * all_gains_ref[0:1, :]).astype(BF16)
    for i in (0, 1):
        cross(i).wait_recv()
        side(i).start()
    for i in (0, 1):
        own(i).wait()
        side(i).wait_recv()
    keep(2).start()
    value = dot(normed_ref[...], pair_whole[...], ((1,), (0,)))
    key_ref[...] = value[:, :size]
    key_low = turned(value[:, :size], all_gains_ref[4:5, size : 2 * size])
    pairs_ref[me, :, :, :size] = key_low.reshape(sequences, rows, size)
    pairs_ref[me, :, :, size:] = value[:, size:].astype(BF16).reshape(sequences, rows, size)
    pass_on(0)
    pass_on(1)
    cross(2).wait_recv()
    side(2).start()
    for hop in range(2, far + 1):
        pass_on(hop)
        if hop == 2:
            own(2).wait()
            side(2).wait_recv()
            keep(3).start()
            queries()
            keep(1).start()
    cross(3).wait_recv()
    side(3).start()
    for hop in range(far + 1):
        for way, seq in streams:
            if hop <= hops(way, seq) and (hop > 0 or way > 0):
                twin(way, seq, hop).wait_recv()
    keep(0).start()
    own(3).wait()
    side(3).wait_recv()
    keep(4).start()
    lax.fori_loop(0, sequences, attention, 0)
    for hop in range(far + 1):
        for way, seq in streams:
            if hop > hops(way, seq):
                continue
            if hop > 0 or way > 0:
                twin(way, seq, hop).wait_send()
            if hop < hops(way, seq):
                flow(way, seq, hop).wait_send()
    for i in order:
        cross(i).wait_send()
    for i in range(len(weights)):
        side(i).wait_send()
    for i in range(5):
        keep(i).wait()


def front(tokens, gains, cosine, sine, query_pos, key_pos, weights, heads, devices, collective_id):
    sequences, rows, width = tokens.shape
    size = 2 * cosine.shape[1]
    count = sequences * rows
    far = devices // 4
    stacked = query_pos.shape[0]
    here, there = pl.BlockSpec(memory_space=pltpu.VMEM), pl.BlockSpec(memory_space=pl.ANY)
    streams = pltpu.SemaphoreType.DMA((2 * sequences, far + 1))
    outs = [
        ((count, width), BF16),
        ((count, size), F32),
        ((sequences, rows, heads * size), BF16),
        ((sequences, rows, heads * size), BF16),
        ((sequences, stacked, size), F32),
        ((sequences, stacked, 128), F32),
        (gains.shape, F32),
    ]
    kept = [
        ((devices, sequences, rows, 2 * size), BF16),
        ((count, heads * size), F32),
        ((width, 2 * size), BF16),
        ((width, heads * size), BF16),
        ((width, heads * size), BF16),
    ]
    return pl.pallas_call(
        functools.partial(front_kernel, devices, heads),
        in_specs=[here] * 6 + [there] * 4,
        out_specs=[here] * len(outs) + [there] * len(kept),
        out_shape=[jax.ShapeDtypeStruct(shape, kind) for shape, kind in outs + kept],
        scratch_shapes=[pltpu.VMEM(shape, kind) for shape, kind in kept]
        + [pltpu.VMEM(gains.shape, gains.dtype)]
        + [pltpu.SemaphoreType.DMA((5,))]
        + [pltpu.SemaphoreType.DMA((4,))]
        + [pltpu.SemaphoreType.DMA((5,))] * 2
        + [pltpu.SemaphoreType.DMA((4,))] * 2
        + [streams] * 4,
        compiler_params=pltpu.CompilerParams(
            collective_id=collective_id, has_side_effects=True, vmem_limit_bytes=67043328
        ),
        name="front",
    )(tokens, gains, cosine, sine, query_pos, key_pos, *weights)


class RingSum:
    def __init__(self, ring, pieces, parts, own, other, flow, outs, sems):
        self.ring, self.pieces, self.parts, self.own = ring, pieces, parts, own
        self.other, self.flow, self.outs = other, flow, outs
        self.put_sem, self.got_sem, self.send_sem, self.recv_sem = sems[:4]
        self.own_sem = sems[4] if own is not None else None
        self.last = ring.chips - 1

    def region(self, p):
        array, _, first, rows, start, cols = self.pieces[p]
        return array, pl.ds(first, rows), pl.ds(start, cols)

    def owner(self, p, step, core):
        way = self.pieces[p][1]
        chips = self.ring.chips
        return self.ring.device((self.ring.place + 2 * chips + way * (-1 - step)) % chips, core)

    def load(self, p, step):
        array, rows, cols = self.region(p)
        slot = step % self.own[array].shape[0]
        return pltpu.make_async_copy(
            self.parts[array].at[self.owner(p, step, self.ring.core), rows, cols],
            self.own[array].at[slot, rows, cols],
            self.own_sem.at[p, step],
        )

    def give(self, p, step):
        array, rows, cols = self.region(p)
        return pltpu.make_async_remote_copy(
            src_ref=self.parts[array].at[self.owner(p, step, 1 - self.ring.core), rows, cols],
            dst_ref=self.other[array].at[step, rows, cols],
            send_sem=self.put_sem.at[p, step],
            recv_sem=self.got_sem.at[p, step],
            device_id={"ctx": self.ring.partner},
            device_id_type=MESH,
        )

    def hop(self, p, step):
        array, rows, cols = self.region(p)
        way = self.pieces[p][1]
        return pltpu.make_async_remote_copy(
            src_ref=self.flow[array].at[step, rows, cols],
            dst_ref=self.flow[array].at[step + 1, rows, cols],
            send_sem=self.send_sem.at[p, step],
            recv_sem=self.recv_sem.at[p, step],
            device_id={"ctx": self.ring.right if way > 0 else self.ring.left},
            device_id_type=MESH,
        )

    def load_all(self, step):
        for p in range(len(self.pieces)):
            self.load(p, step).start()

    def give_all(self, step):
        for p in range(len(self.pieces)):
            self.give(p, step).start()

    def work(self, p, step):
        array, _, row, rows, start, cols = self.pieces[p]
        if self.own is not None:
            self.load(p, step).wait()
            mine, at_mine = self.own[array], step % self.own[array].shape[0]
        else:
            mine, at_mine = self.parts[array], self.owner(p, step, self.ring.core)
        self.give(p, step).wait_recv()
        if step > 0:
            self.hop(p, step - 1).wait_recv()
        width = 128 if cols % 128 == 0 else cols
        while width < 512 and cols % (2 * width) == 0:
            width *= 2
        rows = pl.ds(row, rows)

        def group(i, carry):
            at = start + i * width
            if cols > width:
                at = pl.multiple_of(at, 128)
            where = pl.ds(at, width)
            total = mine[at_mine, rows, where].astype(F32)
            total += self.other[array][step, rows, where].astype(F32)
            if step > 0:
                total += self.flow[array][step, rows, where].astype(F32)
            if step == self.last:
                self.outs[array][rows, where] = total.astype(self.outs[array].dtype)
            else:
                self.flow[array][step, rows, where] = total.astype(self.flow[array].dtype)
            return carry

        if cols == width:
            group(0, 0)
        else:
            lax.fori_loop(0, cols // width, group, 0)
        if step < self.last:
            self.hop(p, step).start()

    def drain(self):
        for p in range(len(self.pieces)):
            for step in range(self.last + 1):
                self.give(p, step).wait_send()
                if step < self.last:
                    self.hop(p, step).wait_send()


def norm_back(upstream, vector, gain):
    scale = lax.rsqrt(jnp.mean(vector * vector, -1, keepdims=True) + EPS)
    normal = vector * scale
    weighted = upstream * gain
    back = scale * (weighted - normal * jnp.mean(weighted * normal, -1, keepdims=True))
    return back, jnp.sum(upstream * normal, 0, keepdims=True)


GELU_SCALE = math.sqrt(2.0 / math.pi)
GELU_CUBE = 0.044715


def feed_forward_kernel(
    mixed_ref,
    tokens_ref,
    cotangent_ref,
    gains_ref,
    out_hbm,
    gate_hbm,
    up_hbm,
    down_hbm,
    output_ref,
    hidden_back_ref,
    mixed_back_ref,
    attended_own_ref,
    attended_send_ref,
    gain_part_ref,
    down_grad_hbm,
    gate_grad_hbm,
    up_grad_hbm,
    gate_weight,
    up_weight,
    down_weight,
    out_weight,
    attended_ref,
    ff_rows,
    low_rows,
    ff_turned,
    low_turned,
    gate,
    upward,
    activated,
    partial,
    part_send,
    part_recv,
    back_send,
    back_recv,
    hidden_ref,
    staging,
    load_sem,
    out_sem,
    store_sem,
    cross_send,
    cross_recv,
):
    count, width = attended_ref.shape
    hidden_units = gate_weight.shape[1]
    block = part_send.shape[0] // 2
    chunk = staging.shape[2]
    whole_chunks = hidden_units // chunk
    rest = hidden_units - whole_chunks * chunk
    mine = lax.axis_index("wsh")
    weights = ((gate_hbm, gate_weight), (up_hbm, up_weight), (down_hbm, down_weight))

    def load(w, at, size, index):
        source, target = weights[w]
        cols = pl.ds(at, size)
        return pltpu.make_async_copy(source.at[:, cols], target.at[:, cols], load_sem.at[w, index])

    def chunks(work):
        def step(c, carry):
            work(pl.multiple_of(c * chunk, 128), chunk, c)
            return carry

        lax.fori_loop(0, whole_chunks, step, 0)
        if rest:
            work(whole_chunks * chunk, rest, whole_chunks)

    def across(kind, piece, source, target):
        return pltpu.make_async_remote_copy(
            src_ref=source,
            dst_ref=target,
            send_sem=cross_send.at[kind, piece],
            recv_sem=cross_recv.at[kind, piece],
            device_id={"wsh": 1 - mine},
            device_id_type=MESH,
        )

    def swap_rows(kind, ref, piece):
        first = piece * block
        here, there = pl.multiple_of(first, block), pl.multiple_of(count + first, block)
        return across(kind, piece, ref.at[pl.ds(here, block)], ref.at[pl.ds(there, block)])

    def swap_parts(kind, source, target, piece):
        lines = pl.ds(pl.multiple_of(piece * block, block), block)
        return across(kind, piece, source.at[lines], target.at[lines])

    def start_load(at, size, index):
        for w in range(3):
            load(w, at, size, index).start()

    bring_out = pltpu.make_async_copy(out_hbm, out_weight, out_sem.at[0])
    bring_out.start()
    chunks(start_load)
    barrier = pltpu.get_barrier_semaphore()
    pl.semaphore_signal(barrier, inc=1, device_id={"wsh": 1 - mine}, device_id_type=MESH)

    bring_out.wait()
    attended = dot(mixed_ref[...], out_weight[...], ((1,), (1,)))
    attended_ref[...] = attended
    scale = lax.rsqrt(jnp.mean(attended * attended, -1, keepdims=True) + EPS)
    hidden = tokens_ref[...].astype(F32) + attended * scale * gains_ref[1:2, :]
    hidden_ref[...] = hidden
    scale = lax.rsqrt(jnp.mean(hidden * hidden, -1, keepdims=True) + EPS)
    ff_rows[:count, :] = (hidden * scale * gains_ref[2:3, :]).astype(BF16)
    pl.semaphore_wait(barrier, 1)
    for piece in range(2):
        swap_rows(0, ff_rows, piece).start()

    def forward(b, carry):
        @pl.when(b >= 2)
        def _():
            swap_rows(0, ff_rows, b - 2).wait_recv()

        lines = pl.ds(pl.multiple_of(b * block, block), block)

        def columns(at, size, index):
            @pl.when(b == 0)
            def _():
                for w in range(3):
                    load(w, at, size, index).wait()

            cols = pl.ds(at, size)
            g = dot(ff_rows[lines, :], gate_weight[:, cols], ((1,), (0,)))
            u = dot(ff_rows[lines, :], up_weight[:, cols], ((1,), (0,)))
            square = g * g
            t = jnp.tanh(g * (GELU_SCALE + GELU_SCALE * GELU_CUBE * square))
            half = 0.5 + 0.5 * t
            gelu = g * half
            slope = half + gelu * (1.0 - t) * (GELU_SCALE + 3.0 * GELU_SCALE * GELU_CUBE * square)
            gate[lines, cols] = (u * slope).astype(BF16)
            upward[lines, cols] = gelu.astype(BF16)
            activated[lines, cols] = (gelu * u).astype(BF16)

        chunks(columns)

        @pl.when(b == 1)
        def _():
            partial[...] = dot(activated[:count, :], down_weight[...], ((1,), (1,)))

        @pl.when(b >= 2)
        def _():
            there = pl.ds(pl.multiple_of((b - 2) * block, block), block)
            part_send[there, :] = dot(activated[lines, :], down_weight[...], ((1,), (1,))).astype(
                BF16
            )
            swap_parts(1, part_send, part_recv, b - 2).start()

        return carry

    lax.fori_loop(0, 4, forward, 0)
    ff_turned[...] = ff_rows[...].T
    for piece in range(2):
        swap_parts(1, part_send, part_recv, piece).wait_recv()
    lowered = partial[...] + part_recv[...].astype(F32)
    cotangent = cotangent_ref[...].astype(F32)
    back, part = norm_back(cotangent, lowered, gains_ref[3:4, :])
    low_rows[:count, :] = back.astype(BF16)
    for piece in range(2):
        swap_rows(2, low_rows, piece).start()
    gain_part_ref[...] = jnp.zeros_like(gain_part_ref)
    gain_part_ref[3:4, :] = part
    scale = lax.rsqrt(jnp.mean(lowered * lowered, -1, keepdims=True) + EPS)
    output_ref[...] = (hidden_ref[...] + lowered * scale * gains_ref[3:4, :]).astype(BF16)

    def backward(half, carry):
        def columns_of(piece, carry):
            @pl.when(half == 1)
            def _():
                swap_rows(2, low_rows, piece).wait_recv()

            lines = pl.ds(pl.multiple_of(half * count + piece * block, block), block)

            def columns(at, size, index):
                cols = pl.ds(at, size)
                d = dot(low_rows[lines, :], down_weight[:, cols], ((1,), (0,)))
                gate[lines, cols] = (d * gate[lines, cols].astype(F32)).astype(BF16)
                upward[lines, cols] = (d * upward[lines, cols].astype(F32)).astype(BF16)

            chunks(columns)
            return carry

        lax.fori_loop(0, 2, columns_of, 0)
        lines = pl.ds(pl.multiple_of(half * count, block), count)
        value = dot(gate[lines, :], gate_weight[...], ((1,), (1,)))
        value += dot(upward[lines, :], up_weight[...], ((1,), (1,)))

        @pl.when(half == 0)
        def _():
            partial[...] = value

        @pl.when(half == 1)
        def _():
            back_send[...] = value.astype(BF16)
            for piece in range(2):
                swap_parts(3, back_send, back_recv, piece).start()

        return carry

    lax.fori_loop(0, 2, backward, 0)
    low_turned[...] = low_rows[...].T

    grads = (
        (low_turned, activated, down_grad_hbm),
        (ff_turned, gate, gate_grad_hbm),
        (ff_turned, upward, up_grad_hbm),
    )

    def store(m, at, size, index):
        cols = pl.ds(at, size)
        return pltpu.make_async_copy(
            staging.at[index % 2, :, pl.ds(0, size)], grads[m][2].at[:, cols], store_sem.at[m, index]
        )

    for m in range(3):
        left, right, _ = grads[m]

        def columns(at, size, index, m=m, left=left, right=right):
            @pl.when(index >= 2)
            def _():
                store(m, 0, chunk, index - 2).wait()

            for top in range(0, width, width // 2):
                lines = slice(top, top + width // 2)
                staging[index % 2, lines, :size] = dot(
                    left[lines, :], right[:, pl.ds(at, size)], ((1,), (0,))
                ).astype(BF16)
            store(m, at, size, index).start()

        chunks(columns)
        last = whole_chunks + (1 if rest else 0)
        for index in range(max(last - 2, 0), last):
            store(m, 0, rest if index == whole_chunks else chunk, index).wait()

    for piece in range(2):
        swap_parts(3, back_send, back_recv, piece).wait_recv()
    upstream = partial[...] + back_recv[...].astype(F32)
    back, part = norm_back(upstream, hidden_ref[...], gains_ref[2:3, :])
    gain_part_ref[2:3, :] = part
    back += cotangent_ref[...].astype(F32)
    hidden_back_ref[...] = back
    back, part = norm_back(back, attended_ref[...], gains_ref[1:2, :])
    gain_part_ref[1:2, :] = part
    mixed_back_ref[...] = dot(back.astype(BF16), out_weight[...], ((1,), (0,))).astype(BF16)
    first, second = back[:, : width // 2].astype(BF16), back[:, width // 2 :].astype(BF16)
    attended_own_ref[...] = jnp.where(mine == 0, first, second)
    attended_send_ref[...] = jnp.where(mine == 0, second, first)
    for piece in range(2):
        swap_rows(0, ff_rows, piece).wait_send()
        swap_parts(1, part_send, part_recv, piece).wait_send()
        swap_rows(2, low_rows, piece).wait_send()
        swap_parts(3, back_send, back_recv, piece).wait_send()


def feed_forward(mixed, tokens, cotangent, gains, weights, collective_id):
    count, width = tokens.shape
    hidden_units = weights[1].shape[1]
    chunk = 512
    pieces = -(-hidden_units // chunk)
    here, there = pl.BlockSpec(memory_space=pltpu.VMEM), pl.BlockSpec(memory_space=pl.ANY)
    like = lambda shape, kind: jax.ShapeDtypeStruct(shape, kind)
    matrix = (width, hidden_units)
    return pl.pallas_call(
        feed_forward_kernel,
        in_specs=[here] * 4 + [there] * 4,
        out_specs=[here] * 6 + [there] * 3,
        out_shape=[
            like((count, width), BF16),
            like((count, width), F32),
            like(mixed.shape, BF16),
            like((count, width // 2), BF16),
            like((count, width // 2), BF16),
            like(gains.shape, F32),
        ]
        + [like(matrix, BF16)] * 3,
        scratch_shapes=[pltpu.VMEM(matrix, BF16)] * 3
        + [pltpu.VMEM(weights[0].shape, BF16), pltpu.VMEM((count, width), F32)]
        + [pltpu.VMEM((2 * count, width), BF16)] * 2
        + [pltpu.VMEM((width, 2 * count), BF16)] * 2
        + [pltpu.VMEM((2 * count, hidden_units), BF16)] * 3
        + [pltpu.VMEM((count, width), F32)]
        + [pltpu.VMEM((count, width), BF16)] * 4
        + [
            pltpu.VMEM((count, width), F32),
            pltpu.VMEM((2, width, chunk), BF16),
            pltpu.SemaphoreType.DMA((3, pieces)),
            pltpu.SemaphoreType.DMA((1,)),
            pltpu.SemaphoreType.DMA((3, pieces)),
            pltpu.SemaphoreType.DMA((4, 2)),
            pltpu.SemaphoreType.DMA((4, 2)),
        ],
        compiler_params=pltpu.CompilerParams(
            collective_id=collective_id, has_side_effects=True, vmem_limit_bytes=67043328
        ),
        name="feed_forward",
    )(mixed, tokens, cotangent, gains, *weights)


def turn_back(upstream, cosine, sine):
    middle = upstream.shape[-1] // 2
    first, second = upstream[:, :middle], upstream[:, middle:]
    return jnp.concatenate([first * cosine + second * sine, second * cosine - first * sine], -1)


def back_kernel(devices, heads, ff_pieces, kv_pieces, attn_pieces, names, *refs):
    r = dict(zip(names, refs))
    ring = Ring(devices)
    chips = ring.chips
    mine = lax.axis_index("wsh")
    sequences, rows, _ = r["query"].shape
    size = r["key_raw"].shape[1]
    count = sequences * rows
    block = rows // 2
    stacked = heads * block

    ff = RingSum(
        ring,
        ff_pieces,
        [r["part_down"], r["part_gate"], r["part_up"]],
        [r[f"ff_own{i}"] for i in range(3)],
        [r[f"ff_other{i}"] for i in range(3)],
        [r[f"ff_flow{i}"] for i in range(3)],
        [r["grad_down"], r["grad_gate"], r["grad_up"]],
        [r["ff_put"], r["ff_got"], r["ff_send"], r["ff_recv"], r["ff_load"]],
    )
    kv = RingSum(
        ring,
        kv_pieces,
        [r["pairs"]],
        None,
        [r["kv_other"]],
        [r["kv_flow"]],
        [r["kv_sum"]],
        [r["kv_put"], r["kv_got"], r["kv_send"], r["kv_recv"]],
    )
    attn = RingSum(
        ring,
        attn_pieces,
        [r["qkv_part"], r["out_part"]],
        None,
        [r["qkv_other"], r["out_other"]],
        [r["qkv_flow"], r["out_flow"]],
        [r["grad_qkv"], r["grad_out"]],
        [r["at_put"], r["at_got"], r["at_send"], r["at_recv"]],
    )

    def brought(i):
        name = BROUGHT[i]
        return pltpu.make_async_copy(r["in_" + name], r[name], r["bring"].at[i])

    def need(*wanted):
        for name in wanted:
            brought(BROUGHT.index(name)).wait()

    def across(i, source, target):
        return pltpu.make_async_remote_copy(
            src_ref=source,
            dst_ref=target,
            send_sem=r["cross_send"].at[i],
            recv_sem=r["cross_recv"].at[i],
            device_id={"wsh": 1 - mine},
            device_id_type=MESH,
        )

    out_swap = across(0, r["att_send"], r["att_across"])
    col_swap = across(1, r["col_send"], r["col_rows"].at[pl.ds(count, count)])
    gain_swap = across(2, r["gain_own"], r["gain_across"])
    mixed_swap = across(3, r["mixed_own"], r["mixed_other"])
    normed_swap = across(4, r["normed_own"], r["normed_other"])
    gain_twin = pltpu.make_async_remote_copy(
        src_ref=r["gain_pair"],
        dst_ref=r["gain_twin"],
        send_sem=r["twin_send"].at[0],
        recv_sem=r["twin_recv"].at[0],
        device_id={"ctx": ring.partner},
        device_id_type=MESH,
    )

    def gain_hop(way, step):
        return pltpu.make_async_remote_copy(
            src_ref=r["gain_flow"].at[way, step],
            dst_ref=r["gain_flow"].at[way, step + 1],
            send_sem=r["gain_send"].at[way, step],
            recv_sem=r["gain_recv"].at[way, step],
            device_id={"ctx": ring.right if way == 0 else ring.left},
            device_id_type=MESH,
        )

    gain_hops = (chips // 2, chips - 1 - chips // 2)

    def attention(seq, carry):
        queries, scaled, correction = [], [], []
        for half in range(2):
            span = slice(half * stacked, (half + 1) * stacked)
            lines = slice(half * block, (half + 1) * block)
            cut = lambda ref: jnp.concatenate(
                [ref[seq, lines, h * size : (h + 1) * size] for h in range(heads)], 0
            )
            queries.append(cut(r["query"]))
            grad = cut(r["grad_mixed"]).astype(F32)
            total = r["totals"][seq, span, :1]
            delta = jnp.sum(grad * r["mixed"][seq, span, :], -1, keepdims=True)
            scaled.append((grad / total).astype(BF16))
            correction.append(delta / total)
        grad_query = [jnp.zeros((stacked, size), F32) for _ in range(2)]
        for key_half in range(2):
            lines = pl.ds(pl.multiple_of(seq * rows + key_half * block, block), block)
            part = r["pairs"][:, lines, :].reshape(devices * block, 2 * size)
            keys, values = part[:, :size], part[:, size:]
            grad_keys = jnp.zeros((devices * block, size), F32)
            grad_values = jnp.zeros((devices * block, size), F32)
            for half in range(key_half, 2):
                weights = jnp.exp(dot(queries[half], keys, ((1,), (1,))) * SCORE_SCALE)
                if half == key_half:
                    allowed = (
                        r["key_pos"][key_half : key_half + 1, :]
                        <= r["query_pos"][half * stacked : (half + 1) * stacked, :]
                    )
                    weights = jnp.where(allowed, weights, 0.0)
                low = weights.astype(BF16)
                grad_weights = dot(scaled[half], values, ((1,), (1,)))
                grad_scores = (weights * (grad_weights - correction[half])).astype(BF16)
                grad_query[half] += dot(grad_scores, keys, ((1,), (0,)))
                grad_keys += dot(grad_scores, queries[half], ((0,), (0,)))
                grad_values += dot(low, scaled[half], ((0,), (0,)))
            both = jnp.concatenate([grad_keys * SCORE_SCALE, grad_values], -1).astype(BF16)
            r["pairs"][:, lines, :] = both.reshape(devices, block, 2 * size)
        for half in range(2):
            r["mixed"][seq, half * stacked : (half + 1) * stacked, :] = grad_query[half] * SCORE_SCALE
        return carry

    def pick(value, which):
        middle = value.shape[1] // 2
        return jnp.where(which == 0, value[:, :middle], value[:, middle:])

    def projections():
        need("query_raw", "key_raw", "cosine", "sine", "gains")
        cosine = jnp.concatenate([r["cosine"][...]] * sequences, 0)
        sine = jnp.concatenate([r["sine"][...]] * sequences, 0)
        gain = r["gains"][4:5, :size]
        total = jnp.zeros((1, size), F32)
        lows = []
        for h in range(heads):
            cols = slice(h * size, (h + 1) * size)
            grad = jnp.concatenate(
                [
                    r["mixed"][seq, half * stacked + h * block : half * stacked + (h + 1) * block, :]
                    for seq in range(sequences)
                    for half in range(2)
                ],
                0,
            )
            back, part = norm_back(
                turn_back(grad, cosine, sine), r["query_raw"][:, cols], gain
            )
            total += part
            r["query_low"][:, cols] = back.astype(BF16)
        back, key_total = norm_back(
            turn_back(r["kv_sum"][:, :size], cosine, sine),
            r["key_raw"][...],
            r["gains"][4:5, size : 2 * size],
        )
        r["pair_low"][:, :size] = back.astype(BF16)
        r["pair_low"][:, size:] = r["kv_sum"][:, size:].astype(BF16)
        first = 0
        for value in (
            r["query_low"][...],
            r["pair_low"][:, :size],
            r["pair_low"][:, size:],
        ):
            cols = slice(first, first + value.shape[1] // 2)
            r["col_rows"][:count, cols] = pick(value, mine)
            r["col_send"][:, cols] = pick(value, 1 - mine)
            first += value.shape[1] // 2
        col_swap.start()
        need("weight_query", "weight_pair", "tokens", "grad_hidden", "gain_part")
        grad_normed = dot(r["query_low"][...], r["weight_query"][...], ((1,), (1,)))
        grad_normed += dot(r["pair_low"][...], r["weight_pair"][...], ((1,), (1,)))
        back, part = norm_back(grad_normed, r["tokens"][...].astype(F32), r["gains"][0:1, :])
        r["grad_tokens"][...] = back + r["grad_hidden"][...]
        r["gain_own"][...] = r["gain_part"][...]
        r["gain_own"][0:1, :] = part
        r["gain_own"][4:5, :size] = total
        r["gain_own"][4:5, size : 2 * size] = key_total
        gain_swap.start()

    def out_part():
        need("att_own")
        out_swap.wait_recv()
        mixed_swap.wait_recv()
        _, lines, cols = r["out_part"].shape
        value = dot(r["mixed_own"][...], r["att_own"][...], ((0,), (0,)))
        value += dot(r["mixed_other"][...], r["att_across"][...], ((0,), (0,)))
        r["out_part"][...] = value.reshape(devices, lines, cols).astype(BF16)

    def turn_rows():
        normed_swap.wait_recv()
        r["weight_pair"][:, :count] = r["normed_own"][...].T
        r["weight_pair"][:, count:] = r["normed_other"][...].T

    def qkv_part():
        col_swap.wait_recv()
        _, lines, cols = r["qkv_part"].shape
        width = 256
        for first in range(0, cols, width):
            value = dot(
                r["weight_pair"][...], r["col_rows"][:, first : first + width], ((1,), (0,))
            )
            r["qkv_part"][:, :, first : first + width] = value.reshape(
                devices, lines, width
            ).astype(BF16)

    def gains_step(step):
        if step == 0:
            gain_swap.wait_recv()
            r["gain_pair"][...] = r["gain_own"][...] + r["gain_across"][...]
            gain_twin.start()
        elif step == 1:
            gain_twin.wait_recv()
            both = r["gain_pair"][...] + r["gain_twin"][...]
            r["gain_flow"][0, 0] = both
            r["gain_flow"][1, 0] = both
            r["gain_sum"][...] = both
            for way in range(2):
                gain_hop(way, 0).start()
        else:
            for way in range(2):
                if step - 2 < gain_hops[way]:
                    gain_hop(way, step - 2).wait_recv()
                    if step - 1 < gain_hops[way]:
                        gain_hop(way, step - 1).start()
                    r["gain_sum"][...] += r["gain_flow"][way, step - 1]

    def ff_step(step, extra=()):
        extra = list(extra)
        if step + 1 < chips:
            ff.load_all(step + 1)
        if step + 2 < chips:
            ff.give_all(step + 2)
        for p in range(len(ff_pieces)):
            ff.work(p, step)
            if p % 2 == 1 and extra:
                extra.pop(0)()
        for left in extra:
            left()

    def kv_step(step):
        def run():
            for p in range(len(kv_pieces)):
                kv.work(p, step)

        return run

    def attn_step(step):
        def run():
            gains_step(step)
            for p in range(len(attn_pieces)):
                attn.work(p, step)

        return run

    def bring(first, last):
        for i in range(BROUGHT.index(first), BROUGHT.index(last) + 1):
            brought(i).start()

    ff.load_all(0)
    ring.enter(across=True)
    ff.give_all(0)
    bring("att_send", "key_pos")
    ff.give_all(1)
    ff_step(0)
    need("att_send")
    out_swap.start()
    bring("mixed_own", BROUGHT[-1])
    need("mixed_own", "normed_own")
    mixed_swap.start()
    normed_swap.start()
    need("pairs", "query", "grad_mixed", "mixed", "totals", "query_pos", "key_pos")
    lax.fori_loop(0, sequences, attention, 0)
    for step in range(chips):
        kv.give_all(step)
    ff_step(1, [kv_step(0), kv_step(1), kv_step(2)])
    ff_step(2, [kv_step(3), kv_step(4), kv_step(5)])
    ff_step(3, [kv_step(6), kv_step(7), out_part])
    projections()
    ff_step(4, [turn_rows])
    qkv_part()
    for step in range(chips):
        attn.give_all(step)
    ff_step(5, [attn_step(0), attn_step(1), attn_step(2)])
    ff_step(6, [attn_step(3), attn_step(4), attn_step(5)])
    ff_step(7, [attn_step(6), attn_step(7)])
    r["gains_total"][...] = r["gain_sum"][...]
    for copy in (out_swap, col_swap, gain_swap, mixed_swap, normed_swap, gain_twin):
        copy.wait_send()
    for way in range(2):
        for step in range(gain_hops[way]):
            gain_hop(way, step).wait_send()
    ff.drain()
    kv.drain()
    attn.drain()


BROUGHT = (
    "att_send",
    "pairs",
    "query",
    "grad_mixed",
    "mixed",
    "totals",
    "query_pos",
    "key_pos",
    "mixed_own",
    "normed_own",
    "att_own",
    "query_raw",
    "key_raw",
    "cosine",
    "sine",
    "gains",
    "weight_query",
    "weight_pair",
    "tokens",
    "grad_hidden",
    "gain_part",
)


def back(given, ff_parts, heads, devices, collective_id):
    chips = devices // 2
    count, width = given["tokens"].shape
    size = given["key_raw"].shape[1]
    out_cols = given["att_send"].shape[1]
    out_lines = given["mixed_own"].shape[1] // devices
    lines = width // devices
    cols = (heads * size + 2 * size) // 2
    slots = lambda n, p: pltpu.VMEM((n,) + tuple(p.shape[1:]), p.dtype)
    ff_pieces = split_ways(ff_parts)
    pair_rows = given["pairs"].shape[1]
    kv_pieces = tuple(
        (0, 1 - 2 * i, i * pair_rows // 2, pair_rows // 2, 0, 2 * size) for i in range(2)
    )
    attn_pieces = (
        (0, 1, 0, lines, 0, cols // 2),
        (0, -1, 0, lines, cols // 2, cols // 2),
        (1, 1, 0, out_lines // 2, 0, out_cols),
        (1, -1, out_lines // 2, out_lines // 2, 0, out_cols),
    )
    dma = lambda *shape: pltpu.SemaphoreType.DMA(shape)
    names, specs, operands = [], [], []
    for name, array in zip(("part_down", "part_gate", "part_up"), ff_parts):
        names.append(name)
        operands.append(array)
    for name in BROUGHT:
        names.append("in_" + name)
        operands.append(given[name])
    outs = {
        "grad_tokens": ((count, width), F32),
        "grad_down": (ff_parts[0].shape[1:], BF16),
        "grad_gate": (ff_parts[1].shape[1:], BF16),
        "grad_up": (ff_parts[2].shape[1:], BF16),
        "grad_qkv": ((lines, cols), F32),
        "grad_out": ((out_lines, out_cols), F32),
        "gains_total": (given["gains"].shape, F32),
    }
    scratch = {}
    for name in BROUGHT:
        shape = given[name].shape
        scratch[name] = pltpu.VMEM(shape, given[name].dtype)
    for i, p in enumerate(ff_parts):
        scratch[f"ff_own{i}"] = slots(2, p)
        scratch[f"ff_other{i}"] = slots(chips, p)
        scratch[f"ff_flow{i}"] = slots(chips, p)
    for kind, pieces in (("ff", ff_pieces), ("kv", kv_pieces), ("at", attn_pieces)):
        for name, steps in (("put", chips), ("got", chips), ("send", chips - 1), ("recv", chips - 1)):
            scratch[f"{kind}_{name}"] = dma(len(pieces), steps)
    scratch["ff_load"] = dma(len(ff_pieces), chips)
    scratch["kv_other"] = slots(chips, given["pairs"])
    scratch["kv_flow"] = slots(chips, given["pairs"])
    scratch["kv_sum"] = pltpu.VMEM((pair_rows, 2 * size), F32)
    for name in ("mixed", "normed"):
        scratch[f"{name}_other"] = pltpu.VMEM(given[f"{name}_own"].shape, BF16)
    scratch["att_across"] = pltpu.VMEM((count, out_cols), BF16)
    scratch["query_low"] = pltpu.VMEM((count, heads * size), BF16)
    scratch["pair_low"] = pltpu.VMEM((count, 2 * size), BF16)
    scratch["col_rows"] = pltpu.VMEM((2 * count, cols), BF16)
    scratch["col_send"] = pltpu.VMEM((count, cols), BF16)
    for name, shape in (("qkv", (lines, cols)), ("out", (out_lines, out_cols))):
        scratch[f"{name}_part"] = pltpu.VMEM((devices,) + shape, BF16)
        scratch[f"{name}_other"] = pltpu.VMEM((chips,) + shape, BF16)
        scratch[f"{name}_flow"] = pltpu.VMEM((chips,) + shape, BF16)
    for name in ("gain_own", "gain_across", "gain_pair", "gain_twin", "gain_sum"):
        scratch[name] = pltpu.VMEM(given["gains"].shape, F32)
    scratch["gain_flow"] = pltpu.VMEM((2, chips // 2 + 1) + given["gains"].shape, F32)
    scratch["bring"] = dma(len(BROUGHT))
    for name, n in (("cross_send", 5), ("cross_recv", 5), ("twin_send", 1), ("twin_recv", 1)):
        scratch[name] = dma(n)
    scratch["gain_send"] = dma(2, chips // 2)
    scratch["gain_recv"] = dma(2, chips // 2)
    names += list(outs) + list(scratch)
    return pl.pallas_call(
        functools.partial(
            back_kernel, devices, heads, ff_pieces, kv_pieces, attn_pieces, tuple(names)
        ),
        in_specs=[pl.BlockSpec(memory_space=pl.ANY)] * len(operands),
        out_specs=[pl.BlockSpec(memory_space=pltpu.VMEM)] * len(outs),
        out_shape=[jax.ShapeDtypeStruct(shape, kind) for shape, kind in outs.values()],
        scratch_shapes=list(scratch.values()),
        compiler_params=pltpu.CompilerParams(
            collective_id=collective_id, has_side_effects=True, vmem_limit_bytes=67043328
        ),
        name="back",
    )(*operands)


def finish_kernel(count, *refs):
    sources, results = refs[:count], list(refs[count:])
    for source in sources:
        first = 0
        while first < source.shape[1]:
            result = results.pop(0)
            result[...] = source[:, first : first + result.shape[1]].astype(result.dtype)
            first += result.shape[1]


def finish(sources, columns):
    outs = [
        jax.ShapeDtypeStruct((source.shape[0], width), kind)
        for source, pieces in zip(sources, columns)
        for kind, width in pieces
    ]
    here = pl.BlockSpec(memory_space=pltpu.VMEM)
    return pl.pallas_call(
        functools.partial(finish_kernel, len(sources)),
        in_specs=[here] * len(sources),
        out_specs=[here] * len(outs),
        out_shape=outs,
        name="finish",
    )(*sources)


def body(
    tokens,
    block_order,
    gain_attn_pre,
    gain_query,
    gain_key,
    gain_attn_post,
    gain_ff_pre,
    gain_ff_post,
    weight_query,
    weight_key,
    weight_value,
    weight_out,
    weight_gate,
    weight_up,
    weight_down,
    cotangent,
):
    sequences, rows, width = tokens.shape
    count = sequences * rows
    block = rows // 2
    devices = lax.axis_size("ctx")
    me = lax.axis_index("ctx")
    mine = lax.axis_index("wsh")

    head_size = 2 * gain_key.shape[0]
    heads = 2 * weight_query.shape[1] // head_size

    lane = jnp.arange(block, dtype=jnp.int32)
    late_order = 2 * devices - 1 - block_order
    early_pos = (block_order[:, None] * block + lane[None]).reshape(-1)
    late_pos = (late_order[:, None] * block + lane[None]).reshape(-1)
    key_pos = jnp.stack([early_pos, late_pos], 0)
    own_first = lax.dynamic_slice_in_dim(block_order, me, 1)[0]
    own_early = own_first * block + lane
    own_late = (2 * devices - 1 - own_first) * block + lane
    own_pos = jnp.concatenate([own_early, own_late])
    query_pos = jnp.concatenate([jnp.tile(own_early, heads), jnp.tile(own_late, heads)])[:, None]

    cosine, sine = angle_tables(own_pos, head_size)

    def placed(gain):
        zeros = jnp.zeros_like(gain)
        return jnp.where(
            mine == 0, jnp.concatenate([gain, zeros]), jnp.concatenate([zeros, gain])
        ).astype(F32)

    own_gains = [placed(g) for g in (gain_attn_pre, gain_attn_post, gain_ff_pre, gain_ff_post)]
    small = [placed(gain_query), placed(gain_key)]
    own_gains.append(jnp.concatenate(small + [jnp.zeros((width - 2 * head_size,), F32)]))
    own_gains = jnp.stack(own_gains + [jnp.zeros((width,), F32)] * 3)
    (
        normed_rows,
        key_raw,
        query_low,
        mixed_low,
        mixed,
        totals,
        all_gains,
        pairs,
        query_raw,
        pair_weight,
        query_weight,
        out_weight,
    ) = front(
        tokens,
        own_gains,
        cosine,
        sine,
        query_pos,
        key_pos,
        (weight_key, weight_value, weight_query, weight_out.T),
        heads,
        devices,
        2,
    )
    attn_pre = all_gains[0]
    query_gain = all_gains[4, :head_size]
    key_gain = all_gains[4, head_size : 2 * head_size]
    mixed_rows = mixed_low.reshape(count, heads * head_size)
    local_size = weight_key.shape[1]
    inputs = tokens.astype(F32)

    def key_path(key_in, key_scale):
        return rotate(norm_gain(key_in, key_scale), cosine[None], sine[None])

    def query_path(query_in, query_scale):
        return rotate(
            norm_gain(query_in, query_scale), cosine[None, :, None, :], sine[None, :, None, :]
        )

    (
        output,
        grad_hidden,
        grad_mixed,
        attended_own,
        attended_send,
        gain_part,
        part_down,
        part_gate,
        part_up,
    ) = feed_forward(
        mixed_rows,
        tokens.reshape(count, width),
        cotangent.reshape(count, width),
        all_gains,
        (out_weight, weight_gate, weight_up, weight_down),
        3,
    )

    def both(own, other):
        return jnp.concatenate([own, other], 0)

    def weight_grad(left, right):
        return dot(left, right, ((0,), (0,))).astype(BF16)

    grad_mixed = grad_mixed.reshape(query_low.shape)
    given = {
        "att_send": attended_send,
        "att_own": attended_own,
        "pairs": pairs.reshape(devices, count, 2 * head_size),
        "query": query_low,
        "grad_mixed": grad_mixed,
        "mixed": mixed,
        "totals": totals,
        "query_pos": query_pos,
        "key_pos": key_pos,
        "mixed_own": mixed_rows,
        "query_raw": query_raw,
        "key_raw": key_raw,
        "cosine": cosine,
        "sine": sine,
        "gains": all_gains,
        "weight_query": query_weight,
        "weight_pair": pair_weight,
        "tokens": tokens.reshape(count, width),
        "grad_hidden": grad_hidden.reshape(count, width),
        "gain_part": gain_part,
        "normed_own": normed_rows,
    }
    aligned = width % (8 * devices) == 0 and mixed_rows.shape[1] % (32 * devices) == 0
    if aligned and count == head_size:
        ff_parts = [
            p.reshape(devices, p.shape[0] // devices, p.shape[1])
            for p in (part_down, part_gate, part_up)
        ]
        grad_tokens, grad_down_w, grad_gate_w, grad_up_w, grad_qkv, grad_out_w, gain_sums = back(
            given, ff_parts, heads, devices, 0
        )
        hidden_cols, query_cols = grad_gate_w.shape[1], heads * head_size // 2
        (
            output,
            grad_tokens,
            grad_down_w,
            grad_gate_w,
            grad_up_w,
            grad_query_w,
            grad_key_w,
            grad_value_w,
            grad_out_w,
        ) = finish(
            [output, grad_tokens, grad_down_w, grad_gate_w, grad_up_w, grad_qkv, grad_out_w],
            [[(BF16, width)], [(F32, width)]]
            + [[(F32, hidden_cols)]] * 3
            + [[(F32, query_cols), (F32, local_size), (F32, local_size)], [(F32, width // 2)]],
        )
        grad_tokens = grad_tokens.reshape(sequences, rows, width)
        place = me * 2 + mine

        def share(row, first, size):
            part = size // (2 * devices)
            return lax.dynamic_slice(gain_sums, (row, first + place * part), (1, part))[0]

        outs = [
            share(0, 0, width),
            share(4, 0, head_size),
            share(4, head_size, head_size),
            share(1, 0, width),
            share(2, 0, width),
            share(3, 0, width),
        ]
    else:
        part_out = weight_grad(
            both(mixed_rows, swap(mixed_rows)),
            both(attended_own, swap(attended_send)),
        )
        grad_query, grad_pairs = attend_backward(
            query_low, pairs, grad_mixed, mixed, totals, query_pos, key_pos, heads
        )
        pair_rows = sequences * rows
        slots = grad_pairs.reshape(devices, pair_rows, 2 * head_size)
        share = pair_rows // 8
        pieces = tuple((0, 1 - 2 * (i % 2), i * share, share, 0, 2 * head_size) for i in range(8))
        own_grads = sum_over_ctx([slots], pieces, devices, 0)[0]
        own_grads = own_grads.reshape(sequences, rows, 2 * head_size)
        grad_key_raw, grad_key_gain = jax.vjp(
            key_path, key_raw.reshape(sequences, rows, head_size), key_gain
        )[1](own_grads[..., :head_size])
        value_grad_low = own_grads[..., head_size:].astype(BF16)
        grad_query_raw, grad_query_gain = jax.vjp(
            query_path, query_raw.reshape(sequences, rows, heads, head_size), query_gain
        )[1](
            grad_query.reshape(sequences, rows, heads, head_size)
        )
        query_grad_low = grad_query_raw.reshape(count, heads * head_size).astype(BF16)
        key_grad_low = grad_key_raw.astype(BF16).reshape(count, head_size)
        value_grad_low = value_grad_low.reshape(count, head_size)
        grad_normed = (
            dot(query_grad_low, query_weight, ((1,), (1,)))
            + dot(jnp.concatenate([key_grad_low, value_grad_low], -1), pair_weight, ((1,), (1,)))
        ).reshape(sequences, rows, width)
        grad_inputs, grad_attn_pre = jax.vjp(norm_gain, inputs, attn_pre)[1](grad_normed)
        grad_tokens = grad_inputs + grad_hidden.reshape(sequences, rows, width)

        def columns(which):
            return jnp.concatenate(
                [half_of(v, which) for v in (query_grad_low, key_grad_low, value_grad_low)], -1
            )

        part_qkv = weight_grad(
            both(normed_rows, swap(normed_rows)), both(columns(mine), swap(columns(1 - mine)))
        )

        gain_grads = [
            grad_attn_pre,
            grad_query_gain,
            grad_key_gain,
            gain_part[1],
            gain_part[2],
            gain_part[3],
        ]
        packed = jnp.concatenate([g.reshape(devices, 2, -1) for g in gain_grads], -1)
        keep = jnp.where(mine == 0, packed[:, 0], packed[:, 1])
        send = jnp.where(mine == 0, packed[:, 1], packed[:, 0])
        packed = keep + swap(send)
        gain_size = packed.shape[-1]
        packed = jnp.pad(packed, ((0, 0), (0, 1024 - gain_size))).reshape(devices, 8, 128)
        parts = [
            p.reshape(devices, p.shape[0] // devices, p.shape[1])
            for p in (part_down, part_gate, part_up, part_qkv, part_out)
        ] + [packed]
        grad_down_w, grad_gate_w, grad_up_w, grad_qkv, grad_out_w, packed = sum_over_ctx(
            parts, split_ways(parts), devices, 1
        )
        packed = packed.reshape(-1)
        outs, first = [], 0
        for g in gain_grads:
            size = g.shape[0] // (2 * devices)
            outs.append(packed[first : first + size])
            first += size
        query_cols = grad_qkv.shape[1] - 2 * local_size
        grad_query_w = grad_qkv[:, :query_cols]
        grad_key_w = grad_qkv[:, query_cols : query_cols + local_size]
        grad_value_w = grad_qkv[:, query_cols + local_size :]
        grad_down_w, grad_gate_w, grad_up_w = (
            g.astype(F32) for g in (grad_down_w, grad_gate_w, grad_up_w)
        )
    output = output.reshape(sequences, rows, width)
    return (
        output,
        grad_tokens,
        *outs,
        grad_query_w,
        grad_key_w,
        grad_value_w,
        grad_out_w,
        grad_gate_w,
        grad_up_w,
        grad_down_w,
    )


def solution(mesh):
    rows, vector, matrix = P("wsh", "ctx", None), P("wsh"), P(None, "wsh")
    in_specs = (rows, P()) + (vector,) * 6 + (matrix,) * 7 + (rows,)
    out_specs = (rows, rows) + (P(("ctx", "wsh")),) * 6 + (P("ctx", "wsh"),) * 7
    return jax.shard_map(body, mesh=mesh, in_specs=in_specs, out_specs=out_specs, check_vma=False)
```

```python
import functools
import math

import jax
import jax.numpy as jnp
from jax import lax
from jax.experimental import pallas as pl
from jax.experimental.pallas import tpu as pltpu
from jax.sharding import PartitionSpec as P

EPS = 1e-06
ROPE_BASE = 1000000.0
SCORE_SCALE = 0.0625
F32 = jnp.float32
BF16 = jnp.bfloat16
MESH = pl.DeviceIdType.MESH


def norm_gain(vector, gain):
    return vector * lax.rsqrt(jnp.mean(vector * vector, -1, keepdims=True) + EPS) * gain


def rotate(vector, cosine, sine):
    middle = vector.shape[-1] // 2
    first = vector[..., :middle]
    second = vector[..., middle:]
    return jnp.concatenate([first * cosine - second * sine, second * cosine + first * sine], -1)


def angle_tables(positions, head_size):
    middle = head_size // 2
    inverse = jnp.exp(
        jnp.arange(middle, dtype=F32) * (-2.0 * math.log(ROPE_BASE) / head_size)
    )
    theta = positions.astype(F32)[:, None] * inverse[None, :]
    return (jnp.cos(theta), jnp.sin(theta))


def swap(value):
    return lax.ppermute(value, "wsh", [(0, 1), (1, 0)])


def half_of(value, which):
    middle = value.shape[-1] // 2
    return jnp.where(which == 0, value[..., :middle], value[..., middle:])


def dot(left, right, dims):
    return lax.dot_general(left, right, (dims, ((), ())), preferred_element_type=F32)


def stack_heads(ref, half, block, heads, size):
    rows = slice(half * block, (half + 1) * block)
    return jnp.concatenate([ref[0, rows, h * size : (h + 1) * size] for h in range(heads)], 0)


def attend_backward_kernel(
    heads, chunk, q_ref, kv_ref, g_ref, mix_ref, tot_ref, qpos_ref, kpos_ref, dq_ref, dkv_ref
):
    shards, _, rows, pair = kv_ref.shape
    block, size = rows // 2, pair // 2
    stacked = heads * block
    queries, scaled, correction = [], [], []
    for half in range(2):
        queries.append(stack_heads(q_ref, half, block, heads, size))
        grad = stack_heads(g_ref, half, block, heads, size).astype(F32)
        span = slice(half * stacked, (half + 1) * stacked)
        total = tot_ref[0, span, :1]
        delta = jnp.sum(grad * mix_ref[0, span, :], -1, keepdims=True)
        scaled.append((grad / total).astype(BF16))
        correction.append(delta / total)
    grad_query = [jnp.zeros((stacked, size), F32) for _ in range(2)]
    for first in range(0, shards, chunk):
        span = slice(first * block, (first + chunk) * block)
        for key_half in range(2):
            part = kv_ref[first : first + chunk, 0, key_half * block : (key_half + 1) * block, :]
            part = part.reshape(chunk * block, pair)
            keys, values = part[:, :size], part[:, size:]
            grad_keys = jnp.zeros((chunk * block, size), F32)
            grad_values = jnp.zeros((chunk * block, size), F32)
            for half in range(key_half, 2):
                weights = jnp.exp(dot(queries[half], keys, ((1,), (1,))) * SCORE_SCALE)
                if half == key_half:
                    allowed = (
                        kpos_ref[key_half : key_half + 1, span]
                        <= qpos_ref[half * stacked : (half + 1) * stacked, :]
                    )
                    weights = jnp.where(allowed, weights, 0.0)
                low = weights.astype(BF16)
                grad_weights = dot(scaled[half], values, ((1,), (1,)))
                grad_scores = (weights * (grad_weights - correction[half])).astype(BF16)
                grad_query[half] += dot(grad_scores, keys, ((1,), (0,)))
                grad_keys += dot(grad_scores, queries[half], ((0,), (0,)))
                grad_values += dot(low, scaled[half], ((0,), (0,)))
            both = jnp.concatenate([grad_keys * SCORE_SCALE, grad_values], -1).astype(BF16)
            dkv_ref[first : first + chunk, 0, key_half * block : (key_half + 1) * block, :] = (
                both.reshape(chunk, block, pair)
            )
    for half in range(2):
        for h in range(heads):
            dq_ref[0, half * block : (half + 1) * block, h * size : (h + 1) * size] = (
                grad_query[half][h * block : (h + 1) * block] * SCORE_SCALE
            )


def whole(shape):
    return pl.BlockSpec(shape, lambda s: (0,) * len(shape))


def attend_backward(query_low, pairs, grad_mixed, mixed, totals, query_pos, key_pos, heads):
    sequences, rows, width = query_low.shape
    shards, _, _, pair = pairs.shape
    stacked = query_pos.shape[0]
    row = pl.BlockSpec((1, rows, width), lambda s: (s, 0, 0))
    stack = lambda last: pl.BlockSpec((1, stacked, last), lambda s: (s, 0, 0))
    pairs_spec = pl.BlockSpec((shards, 1, rows, pair), lambda s: (0, s, 0, 0))
    return pl.pallas_call(
        functools.partial(attend_backward_kernel, heads, min(shards, 16)),
        grid=(sequences,),
        in_specs=[
            row,
            pairs_spec,
            row,
            stack(pair // 2),
            stack(128),
            whole(query_pos.shape),
            whole(key_pos.shape),
        ],
        out_specs=[row, pairs_spec],
        out_shape=[
            jax.ShapeDtypeStruct((sequences, rows, width), F32),
            jax.ShapeDtypeStruct(pairs.shape, BF16),
        ],
        name="attend_backward",
    )(query_low, pairs, grad_mixed, mixed, totals, query_pos, key_pos)


class Ring:
    def __init__(self, devices):
        self.chips = devices // 2
        me = lax.axis_index("ctx")
        self.core = me % 2
        chip = me // 2
        across = chip % 2
        deep = chip // 2
        self.place = deep + across * (self.chips - 1 - 2 * deep)
        self.partner = me + 1 - 2 * self.core
        self.right = self.device((self.place + 1) % self.chips, self.core)
        self.left = self.device((self.place + self.chips - 1) % self.chips, self.core)

    def device(self, place, core):
        side = place // (self.chips // 2)
        return 2 * (2 * (place + side * (self.chips - 1 - 2 * place)) + side) + core

    def enter(self, across=False):
        barrier = pltpu.get_barrier_semaphore()
        targets = [{"ctx": other} for other in (self.left, self.right, self.partner)]
        if across:
            targets.append({"wsh": 1 - lax.axis_index("wsh")})
        for target in targets:
            pl.semaphore_signal(barrier, inc=1, device_id=target, device_id_type=MESH)
        pl.semaphore_wait(barrier, len(targets))


def ring_sum_kernel(devices, pieces, arrays, ahead, *refs):
    parts, outs = refs[:arrays], refs[arrays : 2 * arrays]
    own, other, flow = (refs[(2 + i) * arrays : (3 + i) * arrays] for i in range(3))
    own_sem, put_sem, got_sem, send_sem, recv_sem = refs[5 * arrays :]
    ring = Ring(devices)
    chips = ring.chips

    def region(p):
        array, _, first, rows, start, cols = pieces[p]
        return array, pl.ds(first, rows), pl.ds(start, cols)

    def chunk(p, step):
        way = pieces[p][1]
        return (ring.place + 2 * chips + way * (-1 - step)) % chips

    def load(p, step):
        array, rows, cols = region(p)
        source = ring.device(chunk(p, step), ring.core)
        return pltpu.make_async_copy(
            parts[array].at[source, rows, cols],
            own[array].at[step, rows, cols],
            own_sem.at[p, step],
        )

    def give(p, step):
        array, rows, cols = region(p)
        source = ring.device(chunk(p, step), 1 - ring.core)
        return pltpu.make_async_remote_copy(
            src_ref=parts[array].at[source, rows, cols],
            dst_ref=other[array].at[step, rows, cols],
            send_sem=put_sem.at[p, step],
            recv_sem=got_sem.at[p, step],
            device_id={"ctx": ring.partner},
            device_id_type=MESH,
        )

    def pass_on(p, step):
        array, rows, cols = region(p)
        way = pieces[p][1]
        return pltpu.make_async_remote_copy(
            src_ref=flow[array].at[step, rows, cols],
            dst_ref=flow[array].at[step + 1, rows, cols],
            send_sem=send_sem.at[p, step],
            recv_sem=recv_sem.at[p, step],
            device_id={"ctx": ring.right if way > 0 else ring.left},
            device_id_type=MESH,
        )

    def fetch(step):
        for p in range(len(pieces)):
            load(p, step).start()
            give(p, step).start()

    def add(p, step, first, last):
        array, _, row, rows, start, cols = pieces[p]
        width = 128 if cols % 128 == 0 else cols
        while width < 512 and cols % (2 * width) == 0:
            width *= 2
        rows = pl.ds(row, rows)

        def group(i, carry):
            at = start + i * width
            if cols > width:
                at = pl.multiple_of(at, 128)
            where = pl.ds(at, width)
            total = own[array][step, rows, where].astype(F32) + other[array][
                step, rows, where
            ].astype(F32)
            if not first:
                total += flow[array][step, rows, where].astype(F32)
            if last:
                outs[array][rows, where] = total.astype(outs[array].dtype)
            else:
                flow[array][step, rows, where] = total.astype(flow[array].dtype)
            return carry

        if cols == width:
            group(0, 0)
        else:
            lax.fori_loop(0, cols // width, group, 0)

    def work(step, first=False, last=False):
        for p in range(len(pieces)):
            load(p, step).wait()
            give(p, step).wait_recv()
            if not first:
                pass_on(p, step - 1).wait_recv()
            add(p, step, first, last)
            if not last:
                pass_on(p, step).start()

    for p in range(len(pieces)):
        load(p, 0).start()
    ring.enter()
    for p in range(len(pieces)):
        give(p, 0).start()
    for step in range(1, min(ahead, chips)):
        fetch(step)
    work(0, first=True)

    def middle(step, carry):
        @pl.when(step + ahead - 1 < chips)
        def _():
            fetch(step + ahead - 1)

        work(step)
        return carry

    lax.fori_loop(1, chips - 1, middle, 0)
    work(chips - 1, last=True)

    def drain(step, carry):
        for p in range(len(pieces)):
            give(p, step).wait_send()

            @pl.when(step < chips - 1)
            def _():
                pass_on(p, step).wait_send()

        return carry

    lax.fori_loop(0, chips, drain, 0)


def ring_sum(parts, pieces, devices, collective_id, ahead=3, name="ring_sum"):
    chips, count, arrays = devices // 2, len(pieces), len(parts)
    slots = [pltpu.VMEM((chips,) + p.shape[1:], p.dtype) for p in parts]
    return pl.pallas_call(
        functools.partial(ring_sum_kernel, devices, pieces, arrays, ahead),
        out_shape=[jax.ShapeDtypeStruct(p.shape[1:], F32) for p in parts],
        in_specs=[pl.BlockSpec(memory_space=pl.ANY)] * arrays,
        out_specs=[pl.BlockSpec(memory_space=pltpu.VMEM)] * arrays,
        scratch_shapes=slots * 3
        + [pltpu.SemaphoreType.DMA((count, chips))] * 3
        + [pltpu.SemaphoreType.DMA((count, chips - 1))] * 2,
        compiler_params=pltpu.CompilerParams(
            collective_id=collective_id, has_side_effects=True, vmem_limit_bytes=64000 * 1024
        ),
        name=name,
    )(*parts)


def split_ways(parts):
    pieces, lead = [], 1
    for i, p in enumerate(parts):
        _, rows, cols = p.shape
        tiles = cols // 128
        if cols % 128 == 0 and tiles > 1:
            left = (tiles + (1 if lead > 0 else 0)) // 2 * 128
            if tiles % 2:
                lead = -lead
            pieces.append((i, 1, 0, rows, 0, left))
            pieces.append((i, -1, 0, rows, left, cols - left))
        elif rows % 32 == 0:
            pieces.append((i, 1, 0, rows // 2, 0, cols))
            pieces.append((i, -1, rows // 2, rows // 2, 0, cols))
        else:
            pieces.append((i, 1, 0, rows, 0, cols))
    return tuple(pieces)


def sum_over_ctx(parts, pieces, devices, collective_id):
    if all(p.shape[1] % 8 == 0 for p in parts):
        return ring_sum(parts, pieces, devices, collective_id)
    return [
        lax.psum_scatter(p, "ctx", scatter_dimension=0, tiled=False).astype(F32) for p in parts
    ]


def front_kernel(
    devices,
    heads,
    tokens_ref,
    gains_ref,
    cos_ref,
    sin_ref,
    query_pos_ref,
    key_pos_ref,
    key_weight,
    value_weight,
    query_weight,
    out_weight,
    normed_ref,
    key_ref,
    query_low_ref,
    mixed_low_ref,
    mixed_ref,
    totals_ref,
    all_gains_ref,
    pairs_hbm,
    query_hbm,
    pair_whole_hbm,
    query_whole_hbm,
    out_whole_hbm,
    pairs_ref,
    query_ref,
    pair_whole,
    query_whole,
    out_whole,
    gains_other,
    keep_sem,
    own_sem,
    cross_send,
    cross_recv,
    side_send,
    side_recv,
    flow_send,
    flow_recv,
    twin_send,
    twin_recv,
):
    ring = Ring(devices)
    chips, far = ring.chips, ring.chips // 2
    me = lax.axis_index("ctx")
    mine = lax.axis_index("wsh")
    sequences, rows, width = tokens_ref.shape
    count = sequences * rows
    size = key_ref.shape[1]
    block = rows // 2
    stacked = heads * block
    weights = (key_weight, value_weight, query_weight, out_weight)

    def region(i, side, first, lines):
        if i == 3:
            start = side * out_weight.shape[0] + first
            return out_whole.at[pl.ds(pl.multiple_of(start, 16), lines)]
        cols = weights[i].shape[1]
        start = side * cols + (size if i == 1 else 0)
        target = query_whole if i == 2 else pair_whole
        return target.at[pl.ds(pl.multiple_of(first, 16), lines), pl.ds(pl.multiple_of(start, 128), cols)]

    def keep(i):
        source, target = (
            (pairs_ref, pairs_hbm),
            (query_ref, query_hbm),
            (pair_whole, pair_whole_hbm),
            (query_whole, query_whole_hbm),
            (out_whole, out_whole_hbm),
        )[i]
        return pltpu.make_async_copy(source, target, keep_sem.at[i])

    def own(i):
        return pltpu.make_async_copy(
            weights[i], region(i, mine, 0, weights[i].shape[0]), own_sem.at[i]
        )

    def cross(i):
        if i == len(weights):
            source, target = gains_ref, gains_other
        else:
            half = weights[i].shape[0] // 2
            first = pl.multiple_of(ring.core * half, 16)
            source, target = weights[i].at[pl.ds(first, half)], region(i, mine, first, half)
        return pltpu.make_async_remote_copy(
            src_ref=source,
            dst_ref=target,
            send_sem=cross_send.at[i],
            recv_sem=cross_recv.at[i],
            device_id={"wsh": 1 - mine},
            device_id_type=MESH,
        )

    def side(i):
        half = weights[i].shape[0] // 2
        part = region(i, 1 - mine, ring.core * half, half)
        return pltpu.make_async_remote_copy(
            src_ref=part,
            dst_ref=part,
            send_sem=side_send.at[i],
            recv_sem=side_recv.at[i],
            device_id={"ctx": ring.partner},
            device_id_type=MESH,
        )

    def block_copy(way, seq, hop, target, send_sem, recv_sem):
        stream = (1 if way < 0 else 0) * sequences + seq
        place = (ring.place + chips - way * hop) % chips
        part = pairs_ref.at[ring.device(place, ring.core), seq]
        return pltpu.make_async_remote_copy(
            src_ref=part,
            dst_ref=part,
            send_sem=send_sem.at[stream, hop],
            recv_sem=recv_sem.at[stream, hop],
            device_id={"ctx": target},
            device_id_type=MESH,
        )

    def flow(way, seq, hop):
        target = ring.right if way > 0 else ring.left
        return block_copy(way, seq, hop, target, flow_send, flow_recv)

    def twin(way, seq, hop):
        return block_copy(way, seq, hop, ring.partner, twin_send, twin_recv)

    def hops(way, seq):
        return far if (seq % 2 == 0) == (way > 0) else far - 1

    streams = [(way, seq) for seq in range(sequences) for way in (1, -1)]

    def pass_on(hop):
        for way, seq in streams:
            if hop > hops(way, seq):
                continue
            if hop > 0:
                flow(way, seq, hop - 1).wait_recv()
            if hop < hops(way, seq):
                flow(way, seq, hop).start()
            if hop > 0 or way > 0:
                twin(way, seq, hop).start()

    def turned(value, gain):
        scale = lax.rsqrt(jnp.mean(value * value, -1, keepdims=True) + EPS)
        value = value * scale * gain
        first, second = value[:, : size // 2], value[:, size // 2 :]
        cosine = jnp.concatenate([cos_ref[...]] * sequences, 0)
        sine = jnp.concatenate([sin_ref[...]] * sequences, 0)
        return jnp.concatenate(
            [first * cosine - second * sine, second * cosine + first * sine], -1
        ).astype(BF16)

    def queries():
        gain = all_gains_ref[4:5, :size]
        for h in range(heads):
            cols = slice(h * size, (h + 1) * size)
            value = dot(normed_ref[...], query_whole[:, cols], ((1,), (0,)))
            query_ref[:, cols] = value
            query_low_ref[:, :, cols] = turned(value, gain).reshape(sequences, rows, size)

    def attention(seq, carry):
        chunk = min(devices, 16)
        asked, sums, totals = [], [], []
        for half in range(2):
            lines = slice(half * block, (half + 1) * block)
            asked.append(
                jnp.concatenate(
                    [query_low_ref[seq, lines, h * size : (h + 1) * size] for h in range(heads)], 0
                )
            )
            sums.append(jnp.zeros((stacked, size), F32))
            totals.append(jnp.zeros((stacked, 1), F32))
        for first in range(0, devices, chunk):
            span = slice(first * block, (first + chunk) * block)
            for key_half in range(2):
                part = pairs_ref[
                    first : first + chunk, seq, key_half * block : (key_half + 1) * block, :
                ].reshape(chunk * block, 2 * size)
                keys, values = part[:, :size], part[:, size:]
                for half in range(key_half, 2):
                    weights = jnp.exp(dot(asked[half], keys, ((1,), (1,))) * SCORE_SCALE)
                    if half == key_half:
                        allowed = (
                            key_pos_ref[key_half : key_half + 1, span]
                            <= query_pos_ref[half * stacked : (half + 1) * stacked, :]
                        )
                        weights = jnp.where(allowed, weights, 0.0)
                    low = weights.astype(BF16)
                    totals[half] += jnp.sum(low.astype(F32), -1, keepdims=True)
                    sums[half] += dot(low, values, ((1,), (0,)))
        for half in range(2):
            mixed = sums[half] / totals[half]
            span = slice(half * stacked, (half + 1) * stacked)
            mixed_ref[seq, span, :] = mixed
            totals_ref[seq, span, :] = jnp.broadcast_to(
                totals[half], (stacked, totals_ref.shape[2])
            )
            for h in range(heads):
                mixed_low_ref[
                    seq, half * block : (half + 1) * block, h * size : (h + 1) * size
                ] = mixed[h * block : (h + 1) * block].astype(BF16)
        return carry

    for i in range(len(weights)):
        own(i).start()
    ring.enter(across=True)
    order = (len(weights), 0, 1, 2, 3)
    for i in order:
        cross(i).start()
    inputs = tokens_ref[...].reshape(count, width).astype(F32)
    scale = lax.rsqrt(jnp.mean(inputs * inputs, -1, keepdims=True) + EPS)
    cross(len(weights)).wait_recv()
    all_gains_ref[...] = gains_ref[...] + gains_other[...]
    normed_ref[...] = (inputs * scale * all_gains_ref[0:1, :]).astype(BF16)
    for i in (0, 1):
        cross(i).wait_recv()
        side(i).start()
    for i in (0, 1):
        own(i).wait()
        side(i).wait_recv()
    keep(2).start()
    value = dot(normed_ref[...], pair_whole[...], ((1,), (0,)))
    key_ref[...] = value[:, :size]
    key_low = turned(value[:, :size], all_gains_ref[4:5, size : 2 * size])
    pairs_ref[me, :, :, :size] = key_low.reshape(sequences, rows, size)
    pairs_ref[me, :, :, size:] = value[:, size:].astype(BF16).reshape(sequences, rows, size)
    pass_on(0)
    pass_on(1)
    cross(2).wait_recv()
    side(2).start()
    for hop in range(2, far + 1):
        pass_on(hop)
        if hop == 2:
            own(2).wait()
            side(2).wait_recv()
            keep(3).start()
            queries()
            keep(1).start()
    cross(3).wait_recv()
    side(3).start()
    for hop in range(far + 1):
        for way, seq in streams:
            if hop <= hops(way, seq) and (hop > 0 or way > 0):
                twin(way, seq, hop).wait_recv()
    keep(0).start()
    own(3).wait()
    side(3).wait_recv()
    keep(4).start()
    lax.fori_loop(0, sequences, attention, 0)
    for hop in range(far + 1):
        for way, seq in streams:
            if hop > hops(way, seq):
                continue
            if hop > 0 or way > 0:
                twin(way, seq, hop).wait_send()
            if hop < hops(way, seq):
                flow(way, seq, hop).wait_send()
    for i in order:
        cross(i).wait_send()
    for i in range(len(weights)):
        side(i).wait_send()
    for i in range(5):
        keep(i).wait()


def front(tokens, gains, cosine, sine, query_pos, key_pos, weights, heads, devices, collective_id):
    sequences, rows, width = tokens.shape
    size = 2 * cosine.shape[1]
    count = sequences * rows
    far = devices // 4
    stacked = query_pos.shape[0]
    here, there = pl.BlockSpec(memory_space=pltpu.VMEM), pl.BlockSpec(memory_space=pl.ANY)
    streams = pltpu.SemaphoreType.DMA((2 * sequences, far + 1))
    outs = [
        ((count, width), BF16),
        ((count, size), F32),
        ((sequences, rows, heads * size), BF16),
        ((sequences, rows, heads * size), BF16),
        ((sequences, stacked, size), F32),
        ((sequences, stacked, 128), F32),
        (gains.shape, F32),
    ]
    kept = [
        ((devices, sequences, rows, 2 * size), BF16),
        ((count, heads * size), F32),
        ((width, 2 * size), BF16),
        ((width, heads * size), BF16),
        ((width, heads * size), BF16),
    ]
    return pl.pallas_call(
        functools.partial(front_kernel, devices, heads),
        in_specs=[here] * 6 + [there] * 4,
        out_specs=[here] * len(outs) + [there] * len(kept),
        out_shape=[jax.ShapeDtypeStruct(shape, kind) for shape, kind in outs + kept],
        scratch_shapes=[pltpu.VMEM(shape, kind) for shape, kind in kept]
        + [pltpu.VMEM(gains.shape, gains.dtype)]
        + [pltpu.SemaphoreType.DMA((5,))]
        + [pltpu.SemaphoreType.DMA((4,))]
        + [pltpu.SemaphoreType.DMA((5,))] * 2
        + [pltpu.SemaphoreType.DMA((4,))] * 2
        + [streams] * 4,
        compiler_params=pltpu.CompilerParams(
            collective_id=collective_id, has_side_effects=True, vmem_limit_bytes=67043328
        ),
        name="front",
    )(tokens, gains, cosine, sine, query_pos, key_pos, *weights)


class RingSum:
    def __init__(self, ring, pieces, parts, own, other, flow, outs, sems):
        self.ring, self.pieces, self.parts, self.own = ring, pieces, parts, own
        self.other, self.flow, self.outs = other, flow, outs
        self.put_sem, self.got_sem, self.send_sem, self.recv_sem = sems[:4]
        self.own_sem = sems[4] if own is not None else None
        self.last = ring.chips - 1

    def region(self, p):
        array, _, first, rows, start, cols = self.pieces[p]
        return array, pl.ds(first, rows), pl.ds(start, cols)

    def owner(self, p, step, core):
        way = self.pieces[p][1]
        chips = self.ring.chips
        return self.ring.device((self.ring.place + 2 * chips + way * (-1 - step)) % chips, core)

    def load(self, p, step):
        array, rows, cols = self.region(p)
        slot = step % self.own[array].shape[0]
        return pltpu.make_async_copy(
            self.parts[array].at[self.owner(p, step, self.ring.core), rows, cols],
            self.own[array].at[slot, rows, cols],
            self.own_sem.at[p, step],
        )

    def give(self, p, step):
        array, rows, cols = self.region(p)
        return pltpu.make_async_remote_copy(
            src_ref=self.parts[array].at[self.owner(p, step, 1 - self.ring.core), rows, cols],
            dst_ref=self.other[array].at[step, rows, cols],
            send_sem=self.put_sem.at[p, step],
            recv_sem=self.got_sem.at[p, step],
            device_id={"ctx": self.ring.partner},
            device_id_type=MESH,
        )

    def hop(self, p, step):
        array, rows, cols = self.region(p)
        way = self.pieces[p][1]
        return pltpu.make_async_remote_copy(
            src_ref=self.flow[array].at[step, rows, cols],
            dst_ref=self.flow[array].at[step + 1, rows, cols],
            send_sem=self.send_sem.at[p, step],
            recv_sem=self.recv_sem.at[p, step],
            device_id={"ctx": self.ring.right if way > 0 else self.ring.left},
            device_id_type=MESH,
        )

    def load_all(self, step):
        for p in range(len(self.pieces)):
            self.load(p, step).start()

    def give_all(self, step):
        for p in range(len(self.pieces)):
            self.give(p, step).start()

    def work(self, p, step):
        array, _, row, rows, start, cols = self.pieces[p]
        if self.own is not None:
            self.load(p, step).wait()
            mine, at_mine = self.own[array], step % self.own[array].shape[0]
        else:
            mine, at_mine = self.parts[array], self.owner(p, step, self.ring.core)
        self.give(p, step).wait_recv()
        if step > 0:
            self.hop(p, step - 1).wait_recv()
        width = 128 if cols % 128 == 0 else cols
        while width < 512 and cols % (2 * width) == 0:
            width *= 2
        rows = pl.ds(row, rows)

        def group(i, carry):
            at = start + i * width
            if cols > width:
                at = pl.multiple_of(at, 128)
            where = pl.ds(at, width)
            total = mine[at_mine, rows, where].astype(F32)
            total += self.other[array][step, rows, where].astype(F32)
            if step > 0:
                total += self.flow[array][step, rows, where].astype(F32)
            if step == self.last:
                self.outs[array][rows, where] = total.astype(self.outs[array].dtype)
            else:
                self.flow[array][step, rows, where] = total.astype(self.flow[array].dtype)
            return carry

        if cols == width:
            group(0, 0)
        else:
            lax.fori_loop(0, cols // width, group, 0)
        if step < self.last:
            self.hop(p, step).start()

    def drain(self):
        for p in range(len(self.pieces)):
            for step in range(self.last + 1):
                self.give(p, step).wait_send()
                if step < self.last:
                    self.hop(p, step).wait_send()


def norm_back(upstream, vector, gain):
    scale = lax.rsqrt(jnp.mean(vector * vector, -1, keepdims=True) + EPS)
    normal = vector * scale
    weighted = upstream * gain
    back = scale * (weighted - normal * jnp.mean(weighted * normal, -1, keepdims=True))
    return back, jnp.sum(upstream * normal, 0, keepdims=True)


GELU_SCALE = math.sqrt(2.0 / math.pi)
GELU_CUBE = 0.044715


def feed_forward_kernel(
    mixed_ref,
    tokens_ref,
    cotangent_ref,
    gains_ref,
    out_hbm,
    gate_hbm,
    up_hbm,
    down_hbm,
    output_ref,
    hidden_back_ref,
    mixed_back_ref,
    attended_own_ref,
    attended_send_ref,
    gain_part_ref,
    down_grad_hbm,
    gate_grad_hbm,
    up_grad_hbm,
    gate_weight,
    up_weight,
    down_weight,
    out_weight,
    attended_ref,
    ff_rows,
    low_rows,
    ff_turned,
    low_turned,
    gate,
    upward,
    activated,
    partial,
    part_send,
    part_recv,
    back_send,
    back_recv,
    hidden_ref,
    staging,
    load_sem,
    out_sem,
    store_sem,
    cross_send,
    cross_recv,
):
    count, width = attended_ref.shape
    hidden_units = gate_weight.shape[1]
    block = part_send.shape[0] // 2
    chunk = staging.shape[2]
    whole_chunks = hidden_units // chunk
    rest = hidden_units - whole_chunks * chunk
    mine = lax.axis_index("wsh")
    weights = ((gate_hbm, gate_weight), (up_hbm, up_weight), (down_hbm, down_weight))

    def load(w, at, size, index):
        source, target = weights[w]
        cols = pl.ds(at, size)
        return pltpu.make_async_copy(source.at[:, cols], target.at[:, cols], load_sem.at[w, index])

    def chunks(work):
        def step(c, carry):
            work(pl.multiple_of(c * chunk, 128), chunk, c)
            return carry

        lax.fori_loop(0, whole_chunks, step, 0)
        if rest:
            work(whole_chunks * chunk, rest, whole_chunks)

    def across(kind, piece, source, target):
        return pltpu.make_async_remote_copy(
            src_ref=source,
            dst_ref=target,
            send_sem=cross_send.at[kind, piece],
            recv_sem=cross_recv.at[kind, piece],
            device_id={"wsh": 1 - mine},
            device_id_type=MESH,
        )

    def swap_rows(kind, ref, piece):
        first = piece * block
        here, there = pl.multiple_of(first, block), pl.multiple_of(count + first, block)
        return across(kind, piece, ref.at[pl.ds(here, block)], ref.at[pl.ds(there, block)])

    def swap_parts(kind, source, target, piece):
        lines = pl.ds(pl.multiple_of(piece * block, block), block)
        return across(kind, piece, source.at[lines], target.at[lines])

    def start_load(at, size, index):
        for w in range(3):
            load(w, at, size, index).start()

    bring_out = pltpu.make_async_copy(out_hbm, out_weight, out_sem.at[0])
    bring_out.start()
    chunks(start_load)
    barrier = pltpu.get_barrier_semaphore()
    pl.semaphore_signal(barrier, inc=1, device_id={"wsh": 1 - mine}, device_id_type=MESH)

    bring_out.wait()
    attended = dot(mixed_ref[...], out_weight[...], ((1,), (1,)))
    attended_ref[...] = attended
    scale = lax.rsqrt(jnp.mean(attended * attended, -1, keepdims=True) + EPS)
    hidden = tokens_ref[...].astype(F32) + attended * scale * gains_ref[1:2, :]
    hidden_ref[...] = hidden
    scale = lax.rsqrt(jnp.mean(hidden * hidden, -1, keepdims=True) + EPS)
    ff_rows[:count, :] = (hidden * scale * gains_ref[2:3, :]).astype(BF16)
    pl.semaphore_wait(barrier, 1)
    for piece in range(2):
        swap_rows(0, ff_rows, piece).start()

    def forward(b, carry):
        @pl.when(b >= 2)
        def _():
            swap_rows(0, ff_rows, b - 2).wait_recv()

        lines = pl.ds(pl.multiple_of(b * block, block), block)

        def columns(at, size, index):
            @pl.when(b == 0)
            def _():
                for w in range(3):
                    load(w, at, size, index).wait()

            cols = pl.ds(at, size)
            g = dot(ff_rows[lines, :], gate_weight[:, cols], ((1,), (0,)))
            u = dot(ff_rows[lines, :], up_weight[:, cols], ((1,), (0,)))
            square = g * g
            t = jnp.tanh(g * (GELU_SCALE + GELU_SCALE * GELU_CUBE * square))
            half = 0.5 + 0.5 * t
            gelu = g * half
            slope = half + gelu * (1.0 - t) * (GELU_SCALE + 3.0 * GELU_SCALE * GELU_CUBE * square)
            gate[lines, cols] = (u * slope).astype(BF16)
            upward[lines, cols] = gelu.astype(BF16)
            activated[lines, cols] = (gelu * u).astype(BF16)

        chunks(columns)

        @pl.when(b == 1)
        def _():
            partial[...] = dot(activated[:count, :], down_weight[...], ((1,), (1,)))

        @pl.when(b >= 2)
        def _():
            there = pl.ds(pl.multiple_of((b - 2) * block, block), block)
            part_send[there, :] = dot(activated[lines, :], down_weight[...], ((1,), (1,))).astype(
                BF16
            )
            swap_parts(1, part_send, part_recv, b - 2).start()

        return carry

    lax.fori_loop(0, 4, forward, 0)
    ff_turned[...] = ff_rows[...].T
    for piece in range(2):
        swap_parts(1, part_send, part_recv, piece).wait_recv()
    lowered = partial[...] + part_recv[...].astype(F32)
    cotangent = cotangent_ref[...].astype(F32)
    back, part = norm_back(cotangent, lowered, gains_ref[3:4, :])
    low_rows[:count, :] = back.astype(BF16)
    for piece in range(2):
        swap_rows(2, low_rows, piece).start()
    gain_part_ref[...] = jnp.zeros_like(gain_part_ref)
    gain_part_ref[3:4, :] = part
    scale = lax.rsqrt(jnp.mean(lowered * lowered, -1, keepdims=True) + EPS)
    output_ref[...] = (hidden_ref[...] + lowered * scale * gains_ref[3:4, :]).astype(BF16)

    def backward(half, carry):
        def columns_of(piece, carry):
            @pl.when(half == 1)
            def _():
                swap_rows(2, low_rows, piece).wait_recv()

            lines = pl.ds(pl.multiple_of(half * count + piece * block, block), block)

            def columns(at, size, index):
                cols = pl.ds(at, size)
                d = dot(low_rows[lines, :], down_weight[:, cols], ((1,), (0,)))
                gate[lines, cols] = (d * gate[lines, cols].astype(F32)).astype(BF16)
                upward[lines, cols] = (d * upward[lines, cols].astype(F32)).astype(BF16)

            chunks(columns)
            return carry

        lax.fori_loop(0, 2, columns_of, 0)
        lines = pl.ds(pl.multiple_of(half * count, block), count)
        value = dot(gate[lines, :], gate_weight[...], ((1,), (1,)))
        value += dot(upward[lines, :], up_weight[...], ((1,), (1,)))

        @pl.when(half == 0)
        def _():
            partial[...] = value

        @pl.when(half == 1)
        def _():
            back_send[...] = value.astype(BF16)
            for piece in range(2):
                swap_parts(3, back_send, back_recv, piece).start()

        return carry

    lax.fori_loop(0, 2, backward, 0)
    low_turned[...] = low_rows[...].T

    grads = (
        (low_turned, activated, down_grad_hbm),
        (ff_turned, gate, gate_grad_hbm),
        (ff_turned, upward, up_grad_hbm),
    )

    def store(m, at, size, index):
        cols = pl.ds(at, size)
        return pltpu.make_async_copy(
            staging.at[index % 2, :, pl.ds(0, size)], grads[m][2].at[:, cols], store_sem.at[m, index]
        )

    for m in range(3):
        left, right, _ = grads[m]

        def columns(at, size, index, m=m, left=left, right=right):
            @pl.when(index >= 2)
            def _():
                store(m, 0, chunk, index - 2).wait()

            for top in range(0, width, width // 2):
                lines = slice(top, top + width // 2)
                staging[index % 2, lines, :size] = dot(
                    left[lines, :], right[:, pl.ds(at, size)], ((1,), (0,))
                ).astype(BF16)
            store(m, at, size, index).start()

        chunks(columns)
        last = whole_chunks + (1 if rest else 0)
        for index in range(max(last - 2, 0), last):
            store(m, 0, rest if index == whole_chunks else chunk, index).wait()

    for piece in range(2):
        swap_parts(3, back_send, back_recv, piece).wait_recv()
    upstream = partial[...] + back_recv[...].astype(F32)
    back, part = norm_back(upstream, hidden_ref[...], gains_ref[2:3, :])
    gain_part_ref[2:3, :] = part
    back += cotangent_ref[...].astype(F32)
    hidden_back_ref[...] = back
    back, part = norm_back(back, attended_ref[...], gains_ref[1:2, :])
    gain_part_ref[1:2, :] = part
    mixed_back_ref[...] = dot(back.astype(BF16), out_weight[...], ((1,), (0,))).astype(BF16)
    first, second = back[:, : width // 2].astype(BF16), back[:, width // 2 :].astype(BF16)
    attended_own_ref[...] = jnp.where(mine == 0, first, second)
    attended_send_ref[...] = jnp.where(mine == 0, second, first)
    for piece in range(2):
        swap_rows(0, ff_rows, piece).wait_send()
        swap_parts(1, part_send, part_recv, piece).wait_send()
        swap_rows(2, low_rows, piece).wait_send()
        swap_parts(3, back_send, back_recv, piece).wait_send()


def feed_forward(mixed, tokens, cotangent, gains, weights, collective_id):
    count, width = tokens.shape
    hidden_units = weights[1].shape[1]
    chunk = 512
    pieces = -(-hidden_units // chunk)
    here, there = pl.BlockSpec(memory_space=pltpu.VMEM), pl.BlockSpec(memory_space=pl.ANY)
    like = lambda shape, kind: jax.ShapeDtypeStruct(shape, kind)
    matrix = (width, hidden_units)
    return pl.pallas_call(
        feed_forward_kernel,
        in_specs=[here] * 4 + [there] * 4,
        out_specs=[here] * 6 + [there] * 3,
        out_shape=[
            like((count, width), BF16),
            like((count, width), F32),
            like(mixed.shape, BF16),
            like((count, width // 2), BF16),
            like((count, width // 2), BF16),
            like(gains.shape, F32),
        ]
        + [like(matrix, BF16)] * 3,
        scratch_shapes=[pltpu.VMEM(matrix, BF16)] * 3
        + [pltpu.VMEM(weights[0].shape, BF16), pltpu.VMEM((count, width), F32)]
        + [pltpu.VMEM((2 * count, width), BF16)] * 2
        + [pltpu.VMEM((width, 2 * count), BF16)] * 2
        + [pltpu.VMEM((2 * count, hidden_units), BF16)] * 3
        + [pltpu.VMEM((count, width), F32)]
        + [pltpu.VMEM((count, width), BF16)] * 4
        + [
            pltpu.VMEM((count, width), F32),
            pltpu.VMEM((2, width, chunk), BF16),
            pltpu.SemaphoreType.DMA((3, pieces)),
            pltpu.SemaphoreType.DMA((1,)),
            pltpu.SemaphoreType.DMA((3, pieces)),
            pltpu.SemaphoreType.DMA((4, 2)),
            pltpu.SemaphoreType.DMA((4, 2)),
        ],
        compiler_params=pltpu.CompilerParams(
            collective_id=collective_id, has_side_effects=True, vmem_limit_bytes=67043328
        ),
        name="feed_forward",
    )(mixed, tokens, cotangent, gains, *weights)


def turn_back(upstream, cosine, sine):
    middle = upstream.shape[-1] // 2
    first, second = upstream[:, :middle], upstream[:, middle:]
    return jnp.concatenate([first * cosine + second * sine, second * cosine - first * sine], -1)


def back_kernel(devices, heads, ff_pieces, kv_pieces, attn_pieces, names, *refs):
    r = dict(zip(names, refs))
    ring = Ring(devices)
    chips = ring.chips
    mine = lax.axis_index("wsh")
    sequences, rows, _ = r["query"].shape
    size = r["key_raw"].shape[1]
    count = sequences * rows
    block = rows // 2
    stacked = heads * block

    ff = RingSum(
        ring,
        ff_pieces,
        [r["part_down"], r["part_gate"], r["part_up"]],
        [r[f"ff_own{i}"] for i in range(3)],
        [r[f"ff_other{i}"] for i in range(3)],
        [r[f"ff_flow{i}"] for i in range(3)],
        [r["grad_down"], r["grad_gate"], r["grad_up"]],
        [r["ff_put"], r["ff_got"], r["ff_send"], r["ff_recv"], r["ff_load"]],
    )
    kv = RingSum(
        ring,
        kv_pieces,
        [r["pairs"]],
        None,
        [r["kv_other"]],
        [r["kv_flow"]],
        [r["kv_sum"]],
        [r["kv_put"], r["kv_got"], r["kv_send"], r["kv_recv"]],
    )
    attn = RingSum(
        ring,
        attn_pieces,
        [r["qkv_part"], r["out_part"]],
        None,
        [r["qkv_other"], r["out_other"]],
        [r["qkv_flow"], r["out_flow"]],
        [r["grad_qkv"], r["grad_out"]],
        [r["at_put"], r["at_got"], r["at_send"], r["at_recv"]],
    )

    def brought(i):
        name = BROUGHT[i]
        return pltpu.make_async_copy(r["in_" + name], r[name], r["bring"].at[i])

    def need(*wanted):
        for name in wanted:
            brought(BROUGHT.index(name)).wait()

    def across(i, source, target):
        return pltpu.make_async_remote_copy(
            src_ref=source,
            dst_ref=target,
            send_sem=r["cross_send"].at[i],
            recv_sem=r["cross_recv"].at[i],
            device_id={"wsh": 1 - mine},
            device_id_type=MESH,
        )

    out_swap = across(0, r["att_send"], r["att_across"])
    col_swap = across(1, r["col_send"], r["col_rows"].at[pl.ds(count, count)])
    gain_swap = across(2, r["gain_own"], r["gain_across"])
    mixed_swap = across(3, r["mixed_own"], r["mixed_other"])
    normed_swap = across(4, r["normed_own"], r["normed_other"])
    gain_twin = pltpu.make_async_remote_copy(
        src_ref=r["gain_pair"],
        dst_ref=r["gain_twin"],
        send_sem=r["twin_send"].at[0],
        recv_sem=r["twin_recv"].at[0],
        device_id={"ctx": ring.partner},
        device_id_type=MESH,
    )

    def gain_hop(way, step):
        return pltpu.make_async_remote_copy(
            src_ref=r["gain_flow"].at[way, step],
            dst_ref=r["gain_flow"].at[way, step + 1],
            send_sem=r["gain_send"].at[way, step],
            recv_sem=r["gain_recv"].at[way, step],
            device_id={"ctx": ring.right if way == 0 else ring.left},
            device_id_type=MESH,
        )

    gain_hops = (chips // 2, chips - 1 - chips // 2)

    def attention(seq, carry):
        queries, scaled, correction = [], [], []
        for half in range(2):
            span = slice(half * stacked, (half + 1) * stacked)
            lines = slice(half * block, (half + 1) * block)
            cut = lambda ref: jnp.concatenate(
                [ref[seq, lines, h * size : (h + 1) * size] for h in range(heads)], 0
            )
            queries.append(cut(r["query"]))
            grad = cut(r["grad_mixed"]).astype(F32)
            total = r["totals"][seq, span, :1]
            delta = jnp.sum(grad * r["mixed"][seq, span, :], -1, keepdims=True)
            scaled.append((grad / total).astype(BF16))
            correction.append(delta / total)
        grad_query = [jnp.zeros((stacked, size), F32) for _ in range(2)]
        for key_half in range(2):
            lines = pl.ds(pl.multiple_of(seq * rows + key_half * block, block), block)
            part = r["pairs"][:, lines, :].reshape(devices * block, 2 * size)
            keys, values = part[:, :size], part[:, size:]
            grad_keys = jnp.zeros((devices * block, size), F32)
            grad_values = jnp.zeros((devices * block, size), F32)
            for half in range(key_half, 2):
                weights = jnp.exp(dot(queries[half], keys, ((1,), (1,))) * SCORE_SCALE)
                if half == key_half:
                    allowed = (
                        r["key_pos"][key_half : key_half + 1, :]
                        <= r["query_pos"][half * stacked : (half + 1) * stacked, :]
                    )
                    weights = jnp.where(allowed, weights, 0.0)
                low = weights.astype(BF16)
                grad_weights = dot(scaled[half], values, ((1,), (1,)))
                grad_scores = (weights * (grad_weights - correction[half])).astype(BF16)
                grad_query[half] += dot(grad_scores, keys, ((1,), (0,)))
                grad_keys += dot(grad_scores, queries[half], ((0,), (0,)))
                grad_values += dot(low, scaled[half], ((0,), (0,)))
            both = jnp.concatenate([grad_keys * SCORE_SCALE, grad_values], -1).astype(BF16)
            r["pairs"][:, lines, :] = both.reshape(devices, block, 2 * size)
        for half in range(2):
            r["mixed"][seq, half * stacked : (half + 1) * stacked, :] = grad_query[half] * SCORE_SCALE
        return carry

    def pick(value, which):
        middle = value.shape[1] // 2
        return jnp.where(which == 0, value[:, :middle], value[:, middle:])

    def query_grads():
        need("query_raw", "cosine", "sine", "gains")
        cosine = jnp.concatenate([r["cosine"][...]] * sequences, 0)
        sine = jnp.concatenate([r["sine"][...]] * sequences, 0)
        gain = r["gains"][4:5, :size]
        total = jnp.zeros((1, size), F32)
        for h in range(heads):
            cols = slice(h * size, (h + 1) * size)
            grad = jnp.concatenate(
                [
                    r["mixed"][seq, half * stacked + h * block : half * stacked + (h + 1) * block, :]
                    for seq in range(sequences)
                    for half in range(2)
                ],
                0,
            )
            value, part = norm_back(
                turn_back(grad, cosine, sine), r["query_raw"][:, cols], gain
            )
            total += part
            r["query_low"][:, cols] = value.astype(BF16)
        r["gain_sum"][4:5, :size] = total

    def projections():
        need("key_raw")
        cosine = jnp.concatenate([r["cosine"][...]] * sequences, 0)
        sine = jnp.concatenate([r["sine"][...]] * sequences, 0)
        back, key_total = norm_back(
            turn_back(r["kv_sum"][:, :size], cosine, sine),
            r["key_raw"][...],
            r["gains"][4:5, size : 2 * size],
        )
        r["pair_low"][:, :size] = back.astype(BF16)
        r["pair_low"][:, size:] = r["kv_sum"][:, size:].astype(BF16)
        first = 0
        for value in (
            r["query_low"][...],
            r["pair_low"][:, :size],
            r["pair_low"][:, size:],
        ):
            cols = slice(first, first + value.shape[1] // 2)
            r["col_rows"][:count, cols] = pick(value, mine)
            r["col_send"][:, cols] = pick(value, 1 - mine)
            first += value.shape[1] // 2
        col_swap.start()
        need("weight_query", "weight_pair", "tokens", "grad_hidden", "gain_part")
        grad_normed = dot(r["query_low"][...], r["weight_query"][...], ((1,), (1,)))
        grad_normed += dot(r["pair_low"][...], r["weight_pair"][...], ((1,), (1,)))
        back, part = norm_back(grad_normed, r["tokens"][...].astype(F32), r["gains"][0:1, :])
        r["grad_tokens"][...] = back + r["grad_hidden"][...]
        r["gain_own"][...] = r["gain_part"][...]
        r["gain_own"][0:1, :] = part
        r["gain_own"][4:5, :size] = r["gain_sum"][4:5, :size]
        r["gain_own"][4:5, size : 2 * size] = key_total
        gain_swap.start()

    def out_part():
        need("att_own")
        out_swap.wait_recv()
        mixed_swap.wait_recv()
        _, lines, cols = r["out_part"].shape
        value = dot(r["mixed_own"][...], r["att_own"][...], ((0,), (0,)))
        value += dot(r["mixed_other"][...], r["att_across"][...], ((0,), (0,)))
        r["out_part"][...] = value.reshape(devices, lines, cols).astype(BF16)

    def turn_rows():
        normed_swap.wait_recv()
        r["weight_pair"][:, :count] = r["normed_own"][...].T
        r["weight_pair"][:, count:] = r["normed_other"][...].T

    def qkv_part():
        col_swap.wait_recv()
        _, lines, cols = r["qkv_part"].shape
        width = 256
        for first in range(0, cols, width):
            value = dot(
                r["weight_pair"][...], r["col_rows"][:, first : first + width], ((1,), (0,))
            )
            r["qkv_part"][:, :, first : first + width] = value.reshape(
                devices, lines, width
            ).astype(BF16)

    def gains_step(step):
        if step == 0:
            gain_swap.wait_recv()
            r["gain_pair"][...] = r["gain_own"][...] + r["gain_across"][...]
            gain_twin.start()
        elif step == 1:
            gain_twin.wait_recv()
            both = r["gain_pair"][...] + r["gain_twin"][...]
            r["gain_flow"][0, 0] = both
            r["gain_flow"][1, 0] = both
            r["gain_sum"][...] = both
            for way in range(2):
                gain_hop(way, 0).start()
        else:
            for way in range(2):
                if step - 2 < gain_hops[way]:
                    gain_hop(way, step - 2).wait_recv()
                    if step - 1 < gain_hops[way]:
                        gain_hop(way, step - 1).start()
                    r["gain_sum"][...] += r["gain_flow"][way, step - 1]

    def ff_step(step, extra=()):
        extra = list(extra)
        if step + 1 < chips:
            ff.load_all(step + 1)
        if step + 2 < chips:
            ff.give_all(step + 2)
        for p in range(len(ff_pieces)):
            ff.work(p, step)
            if p % 2 == 1 and extra:
                extra.pop(0)()
        for left in extra:
            left()

    def kv_step(step):
        def run():
            for p in range(len(kv_pieces)):
                kv.work(p, step)

        return run

    def attn_step(step):
        def run():
            gains_step(step)
            for p in range(len(attn_pieces)):
                attn.work(p, step)

        return run

    def bring(first, last):
        for i in range(BROUGHT.index(first), BROUGHT.index(last) + 1):
            brought(i).start()

    ff.load_all(0)
    ring.enter(across=True)
    ff.give_all(0)
    bring("att_send", "key_pos")
    ff.give_all(1)
    ff_step(0)
    need("att_send")
    out_swap.start()
    bring("mixed_own", BROUGHT[-1])
    need("mixed_own", "normed_own")
    mixed_swap.start()
    normed_swap.start()
    need("pairs", "query", "grad_mixed", "mixed", "totals", "query_pos", "key_pos")
    lax.fori_loop(0, sequences, attention, 0)
    for step in range(chips):
        kv.give_all(step)
    ff_step(1, [kv_step(0), kv_step(1), kv_step(2)])
    ff_step(2, [kv_step(3), kv_step(4), kv_step(5), query_grads])
    ff_step(3, [kv_step(6), kv_step(7), out_part])
    projections()
    ff_step(4, [turn_rows])
    qkv_part()
    for step in range(chips):
        attn.give_all(step)
    ff_step(5, [attn_step(0), attn_step(1), attn_step(2)])
    ff_step(6, [attn_step(3), attn_step(4), attn_step(5)])
    ff_step(7, [attn_step(6), attn_step(7)])
    r["gains_total"][...] = r["gain_sum"][...]
    for copy in (out_swap, col_swap, gain_swap, mixed_swap, normed_swap, gain_twin):
        copy.wait_send()
    for way in range(2):
        for step in range(gain_hops[way]):
            gain_hop(way, step).wait_send()
    ff.drain()
    kv.drain()
    attn.drain()


BROUGHT = (
    "att_send",
    "pairs",
    "query",
    "grad_mixed",
    "mixed",
    "totals",
    "query_pos",
    "key_pos",
    "mixed_own",
    "normed_own",
    "att_own",
    "query_raw",
    "key_raw",
    "cosine",
    "sine",
    "gains",
    "weight_query",
    "weight_pair",
    "tokens",
    "grad_hidden",
    "gain_part",
)


def back(given, ff_parts, heads, devices, collective_id):
    chips = devices // 2
    count, width = given["tokens"].shape
    size = given["key_raw"].shape[1]
    out_cols = given["att_send"].shape[1]
    out_lines = given["mixed_own"].shape[1] // devices
    lines = width // devices
    cols = (heads * size + 2 * size) // 2
    slots = lambda n, p: pltpu.VMEM((n,) + tuple(p.shape[1:]), p.dtype)
    ff_pieces = split_ways(ff_parts)
    pair_rows = given["pairs"].shape[1]
    kv_pieces = tuple(
        (0, 1 - 2 * i, i * pair_rows // 2, pair_rows // 2, 0, 2 * size) for i in range(2)
    )
    attn_pieces = (
        (0, 1, 0, lines, 0, cols // 2),
        (0, -1, 0, lines, cols // 2, cols // 2),
        (1, 1, 0, out_lines // 2, 0, out_cols),
        (1, -1, out_lines // 2, out_lines // 2, 0, out_cols),
    )
    dma = lambda *shape: pltpu.SemaphoreType.DMA(shape)
    names, specs, operands = [], [], []
    for name, array in zip(("part_down", "part_gate", "part_up"), ff_parts):
        names.append(name)
        operands.append(array)
    for name in BROUGHT:
        names.append("in_" + name)
        operands.append(given[name])
    outs = {
        "grad_tokens": ((count, width), F32),
        "grad_down": (ff_parts[0].shape[1:], BF16),
        "grad_gate": (ff_parts[1].shape[1:], BF16),
        "grad_up": (ff_parts[2].shape[1:], BF16),
        "grad_qkv": ((lines, cols), F32),
        "grad_out": ((out_lines, out_cols), F32),
        "gains_total": (given["gains"].shape, F32),
    }
    scratch = {}
    for name in BROUGHT:
        shape = given[name].shape
        scratch[name] = pltpu.VMEM(shape, given[name].dtype)
    for i, p in enumerate(ff_parts):
        scratch[f"ff_own{i}"] = slots(2, p)
        scratch[f"ff_other{i}"] = slots(chips, p)
        scratch[f"ff_flow{i}"] = slots(chips, p)
    for kind, pieces in (("ff", ff_pieces), ("kv", kv_pieces), ("at", attn_pieces)):
        for name, steps in (("put", chips), ("got", chips), ("send", chips - 1), ("recv", chips - 1)):
            scratch[f"{kind}_{name}"] = dma(len(pieces), steps)
    scratch["ff_load"] = dma(len(ff_pieces), chips)
    scratch["kv_other"] = slots(chips, given["pairs"])
    scratch["kv_flow"] = slots(chips, given["pairs"])
    scratch["kv_sum"] = pltpu.VMEM((pair_rows, 2 * size), F32)
    for name in ("mixed", "normed"):
        scratch[f"{name}_other"] = pltpu.VMEM(given[f"{name}_own"].shape, BF16)
    scratch["att_across"] = pltpu.VMEM((count, out_cols), BF16)
    scratch["query_low"] = pltpu.VMEM((count, heads * size), BF16)
    scratch["pair_low"] = pltpu.VMEM((count, 2 * size), BF16)
    scratch["col_rows"] = pltpu.VMEM((2 * count, cols), BF16)
    scratch["col_send"] = pltpu.VMEM((count, cols), BF16)
    for name, shape in (("qkv", (lines, cols)), ("out", (out_lines, out_cols))):
        scratch[f"{name}_part"] = pltpu.VMEM((devices,) + shape, BF16)
        scratch[f"{name}_other"] = pltpu.VMEM((chips,) + shape, BF16)
        scratch[f"{name}_flow"] = pltpu.VMEM((chips,) + shape, BF16)
    for name in ("gain_own", "gain_across", "gain_pair", "gain_twin", "gain_sum"):
        scratch[name] = pltpu.VMEM(given["gains"].shape, F32)
    scratch["gain_flow"] = pltpu.VMEM((2, chips // 2 + 1) + given["gains"].shape, F32)
    scratch["bring"] = dma(len(BROUGHT))
    for name, n in (("cross_send", 5), ("cross_recv", 5), ("twin_send", 1), ("twin_recv", 1)):
        scratch[name] = dma(n)
    scratch["gain_send"] = dma(2, chips // 2)
    scratch["gain_recv"] = dma(2, chips // 2)
    names += list(outs) + list(scratch)
    return pl.pallas_call(
        functools.partial(
            back_kernel, devices, heads, ff_pieces, kv_pieces, attn_pieces, tuple(names)
        ),
        in_specs=[pl.BlockSpec(memory_space=pl.ANY)] * len(operands),
        out_specs=[pl.BlockSpec(memory_space=pltpu.VMEM)] * len(outs),
        out_shape=[jax.ShapeDtypeStruct(shape, kind) for shape, kind in outs.values()],
        scratch_shapes=list(scratch.values()),
        compiler_params=pltpu.CompilerParams(
            collective_id=collective_id, has_side_effects=True, vmem_limit_bytes=67043328
        ),
        name="back",
    )(*operands)


def finish_kernel(count, *refs):
    sources, results = refs[:count], list(refs[count:])
    for source in sources:
        first = 0
        while first < source.shape[1]:
            result = results.pop(0)
            result[...] = source[:, first : first + result.shape[1]].astype(result.dtype)
            first += result.shape[1]


def finish(sources, columns):
    outs = [
        jax.ShapeDtypeStruct((source.shape[0], width), kind)
        for source, pieces in zip(sources, columns)
        for kind, width in pieces
    ]
    here = pl.BlockSpec(memory_space=pltpu.VMEM)
    return pl.pallas_call(
        functools.partial(finish_kernel, len(sources)),
        in_specs=[here] * len(sources),
        out_specs=[here] * len(outs),
        out_shape=outs,
        name="finish",
    )(*sources)


def body(
    tokens,
    block_order,
    gain_attn_pre,
    gain_query,
    gain_key,
    gain_attn_post,
    gain_ff_pre,
    gain_ff_post,
    weight_query,
    weight_key,
    weight_value,
    weight_out,
    weight_gate,
    weight_up,
    weight_down,
    cotangent,
):
    sequences, rows, width = tokens.shape
    count = sequences * rows
    block = rows // 2
    devices = lax.axis_size("ctx")
    me = lax.axis_index("ctx")
    mine = lax.axis_index("wsh")

    head_size = 2 * gain_key.shape[0]
    heads = 2 * weight_query.shape[1] // head_size

    lane = jnp.arange(block, dtype=jnp.int32)
    late_order = 2 * devices - 1 - block_order
    early_pos = (block_order[:, None] * block + lane[None]).reshape(-1)
    late_pos = (late_order[:, None] * block + lane[None]).reshape(-1)
    key_pos = jnp.stack([early_pos, late_pos], 0)
    own_first = lax.dynamic_slice_in_dim(block_order, me, 1)[0]
    own_early = own_first * block + lane
    own_late = (2 * devices - 1 - own_first) * block + lane
    own_pos = jnp.concatenate([own_early, own_late])
    query_pos = jnp.concatenate([jnp.tile(own_early, heads), jnp.tile(own_late, heads)])[:, None]

    cosine, sine = angle_tables(own_pos, head_size)

    def placed(gain):
        zeros = jnp.zeros_like(gain)
        return jnp.where(
            mine == 0, jnp.concatenate([gain, zeros]), jnp.concatenate([zeros, gain])
        ).astype(F32)

    own_gains = [placed(g) for g in (gain_attn_pre, gain_attn_post, gain_ff_pre, gain_ff_post)]
    small = [placed(gain_query), placed(gain_key)]
    own_gains.append(jnp.concatenate(small + [jnp.zeros((width - 2 * head_size,), F32)]))
    own_gains = jnp.stack(own_gains + [jnp.zeros((width,), F32)] * 3)
    (
        normed_rows,
        key_raw,
        query_low,
        mixed_low,
        mixed,
        totals,
        all_gains,
        pairs,
        query_raw,
        pair_weight,
        query_weight,
        out_weight,
    ) = front(
        tokens,
        own_gains,
        cosine,
        sine,
        query_pos,
        key_pos,
        (weight_key, weight_value, weight_query, weight_out.T),
        heads,
        devices,
        2,
    )
    attn_pre = all_gains[0]
    query_gain = all_gains[4, :head_size]
    key_gain = all_gains[4, head_size : 2 * head_size]
    mixed_rows = mixed_low.reshape(count, heads * head_size)
    local_size = weight_key.shape[1]
    inputs = tokens.astype(F32)

    def key_path(key_in, key_scale):
        return rotate(norm_gain(key_in, key_scale), cosine[None], sine[None])

    def query_path(query_in, query_scale):
        return rotate(
            norm_gain(query_in, query_scale), cosine[None, :, None, :], sine[None, :, None, :]
        )

    (
        output,
        grad_hidden,
        grad_mixed,
        attended_own,
        attended_send,
        gain_part,
        part_down,
        part_gate,
        part_up,
    ) = feed_forward(
        mixed_rows,
        tokens.reshape(count, width),
        cotangent.reshape(count, width),
        all_gains,
        (out_weight, weight_gate, weight_up, weight_down),
        3,
    )

    def both(own, other):
        return jnp.concatenate([own, other], 0)

    def weight_grad(left, right):
        return dot(left, right, ((0,), (0,))).astype(BF16)

    grad_mixed = grad_mixed.reshape(query_low.shape)
    given = {
        "att_send": attended_send,
        "att_own": attended_own,
        "pairs": pairs.reshape(devices, count, 2 * head_size),
        "query": query_low,
        "grad_mixed": grad_mixed,
        "mixed": mixed,
        "totals": totals,
        "query_pos": query_pos,
        "key_pos": key_pos,
        "mixed_own": mixed_rows,
        "query_raw": query_raw,
        "key_raw": key_raw,
        "cosine": cosine,
        "sine": sine,
        "gains": all_gains,
        "weight_query": query_weight,
        "weight_pair": pair_weight,
        "tokens": tokens.reshape(count, width),
        "grad_hidden": grad_hidden.reshape(count, width),
        "gain_part": gain_part,
        "normed_own": normed_rows,
    }
    aligned = width % (8 * devices) == 0 and mixed_rows.shape[1] % (32 * devices) == 0
    if aligned and count == head_size:
        ff_parts = [
            p.reshape(devices, p.shape[0] // devices, p.shape[1])
            for p in (part_down, part_gate, part_up)
        ]
        grad_tokens, grad_down_w, grad_gate_w, grad_up_w, grad_qkv, grad_out_w, gain_sums = back(
            given, ff_parts, heads, devices, 0
        )
        hidden_cols, query_cols = grad_gate_w.shape[1], heads * head_size // 2
        (
            output,
            grad_tokens,
            grad_down_w,
            grad_gate_w,
            grad_up_w,
            grad_query_w,
            grad_key_w,
            grad_value_w,
            grad_out_w,
        ) = finish(
            [output, grad_tokens, grad_down_w, grad_gate_w, grad_up_w, grad_qkv, grad_out_w],
            [[(BF16, width)], [(F32, width)]]
            + [[(F32, hidden_cols)]] * 3
            + [[(F32, query_cols), (F32, local_size), (F32, local_size)], [(F32, width // 2)]],
        )
        grad_tokens = grad_tokens.reshape(sequences, rows, width)
        place = me * 2 + mine

        def share(row, first, size):
            part = size // (2 * devices)
            return lax.dynamic_slice(gain_sums, (row, first + place * part), (1, part))[0]

        outs = [
            share(0, 0, width),
            share(4, 0, head_size),
            share(4, head_size, head_size),
            share(1, 0, width),
            share(2, 0, width),
            share(3, 0, width),
        ]
    else:
        part_out = weight_grad(
            both(mixed_rows, swap(mixed_rows)),
            both(attended_own, swap(attended_send)),
        )
        grad_query, grad_pairs = attend_backward(
            query_low, pairs, grad_mixed, mixed, totals, query_pos, key_pos, heads
        )
        pair_rows = sequences * rows
        slots = grad_pairs.reshape(devices, pair_rows, 2 * head_size)
        share = pair_rows // 8
        pieces = tuple((0, 1 - 2 * (i % 2), i * share, share, 0, 2 * head_size) for i in range(8))
        own_grads = sum_over_ctx([slots], pieces, devices, 0)[0]
        own_grads = own_grads.reshape(sequences, rows, 2 * head_size)
        grad_key_raw, grad_key_gain = jax.vjp(
            key_path, key_raw.reshape(sequences, rows, head_size), key_gain
        )[1](own_grads[..., :head_size])
        value_grad_low = own_grads[..., head_size:].astype(BF16)
        grad_query_raw, grad_query_gain = jax.vjp(
            query_path, query_raw.reshape(sequences, rows, heads, head_size), query_gain
        )[1](
            grad_query.reshape(sequences, rows, heads, head_size)
        )
        query_grad_low = grad_query_raw.reshape(count, heads * head_size).astype(BF16)
        key_grad_low = grad_key_raw.astype(BF16).reshape(count, head_size)
        value_grad_low = value_grad_low.reshape(count, head_size)
        grad_normed = (
            dot(query_grad_low, query_weight, ((1,), (1,)))
            + dot(jnp.concatenate([key_grad_low, value_grad_low], -1), pair_weight, ((1,), (1,)))
        ).reshape(sequences, rows, width)
        grad_inputs, grad_attn_pre = jax.vjp(norm_gain, inputs, attn_pre)[1](grad_normed)
        grad_tokens = grad_inputs + grad_hidden.reshape(sequences, rows, width)

        def columns(which):
            return jnp.concatenate(
                [half_of(v, which) for v in (query_grad_low, key_grad_low, value_grad_low)], -1
            )

        part_qkv = weight_grad(
            both(normed_rows, swap(normed_rows)), both(columns(mine), swap(columns(1 - mine)))
        )

        gain_grads = [
            grad_attn_pre,
            grad_query_gain,
            grad_key_gain,
            gain_part[1],
            gain_part[2],
            gain_part[3],
        ]
        packed = jnp.concatenate([g.reshape(devices, 2, -1) for g in gain_grads], -1)
        keep = jnp.where(mine == 0, packed[:, 0], packed[:, 1])
        send = jnp.where(mine == 0, packed[:, 1], packed[:, 0])
        packed = keep + swap(send)
        gain_size = packed.shape[-1]
        packed = jnp.pad(packed, ((0, 0), (0, 1024 - gain_size))).reshape(devices, 8, 128)
        parts = [
            p.reshape(devices, p.shape[0] // devices, p.shape[1])
            for p in (part_down, part_gate, part_up, part_qkv, part_out)
        ] + [packed]
        grad_down_w, grad_gate_w, grad_up_w, grad_qkv, grad_out_w, packed = sum_over_ctx(
            parts, split_ways(parts), devices, 1
        )
        packed = packed.reshape(-1)
        outs, first = [], 0
        for g in gain_grads:
            size = g.shape[0] // (2 * devices)
            outs.append(packed[first : first + size])
            first += size
        query_cols = grad_qkv.shape[1] - 2 * local_size
        grad_query_w = grad_qkv[:, :query_cols]
        grad_key_w = grad_qkv[:, query_cols : query_cols + local_size]
        grad_value_w = grad_qkv[:, query_cols + local_size :]
        grad_down_w, grad_gate_w, grad_up_w = (
            g.astype(F32) for g in (grad_down_w, grad_gate_w, grad_up_w)
        )
    output = output.reshape(sequences, rows, width)
    return (
        output,
        grad_tokens,
        *outs,
        grad_query_w,
        grad_key_w,
        grad_value_w,
        grad_out_w,
        grad_gate_w,
        grad_up_w,
        grad_down_w,
    )


def solution(mesh):
    rows, vector, matrix = P("wsh", "ctx", None), P("wsh"), P(None, "wsh")
    in_specs = (rows, P()) + (vector,) * 6 + (matrix,) * 7 + (rows,)
    out_specs = (rows, rows) + (P(("ctx", "wsh")),) * 6 + (P("ctx", "wsh"),) * 7
    return jax.shard_map(body, mesh=mesh, in_specs=in_specs, out_specs=out_specs, check_vma=False)
```

```python
import functools
import math

import jax
import jax.numpy as jnp
from jax import lax
from jax.experimental import pallas as pl
from jax.experimental.pallas import tpu as pltpu
from jax.sharding import PartitionSpec as P

EPS = 1e-06
ROPE_BASE = 1000000.0
SCORE_SCALE = 0.0625
F32 = jnp.float32
BF16 = jnp.bfloat16
MESH = pl.DeviceIdType.MESH


def norm_gain(vector, gain):
    return vector * lax.rsqrt(jnp.mean(vector * vector, -1, keepdims=True) + EPS) * gain


def rotate(vector, cosine, sine):
    middle = vector.shape[-1] // 2
    first = vector[..., :middle]
    second = vector[..., middle:]
    return jnp.concatenate([first * cosine - second * sine, second * cosine + first * sine], -1)


def angle_tables(positions, head_size):
    middle = head_size // 2
    inverse = jnp.exp(
        jnp.arange(middle, dtype=F32) * (-2.0 * math.log(ROPE_BASE) / head_size)
    )
    theta = positions.astype(F32)[:, None] * inverse[None, :]
    return (jnp.cos(theta), jnp.sin(theta))


def swap(value):
    return lax.ppermute(value, "wsh", [(0, 1), (1, 0)])


def half_of(value, which):
    middle = value.shape[-1] // 2
    return jnp.where(which == 0, value[..., :middle], value[..., middle:])


def dot(left, right, dims):
    return lax.dot_general(left, right, (dims, ((), ())), preferred_element_type=F32)


def stack_heads(ref, half, block, heads, size):
    rows = slice(half * block, (half + 1) * block)
    return jnp.concatenate([ref[0, rows, h * size : (h + 1) * size] for h in range(heads)], 0)


def attend_backward_kernel(
    heads, chunk, q_ref, kv_ref, g_ref, mix_ref, tot_ref, qpos_ref, kpos_ref, dq_ref, dkv_ref
):
    shards, _, rows, pair = kv_ref.shape
    block, size = rows // 2, pair // 2
    stacked = heads * block
    queries, scaled, correction = [], [], []
    for half in range(2):
        queries.append(stack_heads(q_ref, half, block, heads, size))
        grad = stack_heads(g_ref, half, block, heads, size).astype(F32)
        span = slice(half * stacked, (half + 1) * stacked)
        total = tot_ref[0, span, :1]
        delta = jnp.sum(grad * mix_ref[0, span, :], -1, keepdims=True)
        scaled.append((grad / total).astype(BF16))
        correction.append(delta / total)
    grad_query = [jnp.zeros((stacked, size), F32) for _ in range(2)]
    for first in range(0, shards, chunk):
        span = slice(first * block, (first + chunk) * block)
        for key_half in range(2):
            part = kv_ref[first : first + chunk, 0, key_half * block : (key_half + 1) * block, :]
            part = part.reshape(chunk * block, pair)
            keys, values = part[:, :size], part[:, size:]
            grad_keys = jnp.zeros((chunk * block, size), F32)
            grad_values = jnp.zeros((chunk * block, size), F32)
            for half in range(key_half, 2):
                weights = jnp.exp(dot(queries[half], keys, ((1,), (1,))) * SCORE_SCALE)
                if half == key_half:
                    allowed = (
                        kpos_ref[key_half : key_half + 1, span]
                        <= qpos_ref[half * stacked : (half + 1) * stacked, :]
                    )
                    weights = jnp.where(allowed, weights, 0.0)
                low = weights.astype(BF16)
                grad_weights = dot(scaled[half], values, ((1,), (1,)))
                grad_scores = (weights * (grad_weights - correction[half])).astype(BF16)
                grad_query[half] += dot(grad_scores, keys, ((1,), (0,)))
                grad_keys += dot(grad_scores, queries[half], ((0,), (0,)))
                grad_values += dot(low, scaled[half], ((0,), (0,)))
            both = jnp.concatenate([grad_keys * SCORE_SCALE, grad_values], -1).astype(BF16)
            dkv_ref[first : first + chunk, 0, key_half * block : (key_half + 1) * block, :] = (
                both.reshape(chunk, block, pair)
            )
    for half in range(2):
        for h in range(heads):
            dq_ref[0, half * block : (half + 1) * block, h * size : (h + 1) * size] = (
                grad_query[half][h * block : (h + 1) * block] * SCORE_SCALE
            )


def whole(shape):
    return pl.BlockSpec(shape, lambda s: (0,) * len(shape))


def attend_backward(query_low, pairs, grad_mixed, mixed, totals, query_pos, key_pos, heads):
    sequences, rows, width = query_low.shape
    shards, _, _, pair = pairs.shape
    stacked = query_pos.shape[0]
    row = pl.BlockSpec((1, rows, width), lambda s: (s, 0, 0))
    stack = lambda last: pl.BlockSpec((1, stacked, last), lambda s: (s, 0, 0))
    pairs_spec = pl.BlockSpec((shards, 1, rows, pair), lambda s: (0, s, 0, 0))
    return pl.pallas_call(
        functools.partial(attend_backward_kernel, heads, min(shards, 16)),
        grid=(sequences,),
        in_specs=[
            row,
            pairs_spec,
            row,
            stack(pair // 2),
            stack(128),
            whole(query_pos.shape),
            whole(key_pos.shape),
        ],
        out_specs=[row, pairs_spec],
        out_shape=[
            jax.ShapeDtypeStruct((sequences, rows, width), F32),
            jax.ShapeDtypeStruct(pairs.shape, BF16),
        ],
        name="attend_backward",
    )(query_low, pairs, grad_mixed, mixed, totals, query_pos, key_pos)


class Ring:
    def __init__(self, devices):
        self.chips = devices // 2
        me = lax.axis_index("ctx")
        self.core = me % 2
        chip = me // 2
        across = chip % 2
        deep = chip // 2
        self.place = deep + across * (self.chips - 1 - 2 * deep)
        self.partner = me + 1 - 2 * self.core
        self.right = self.device((self.place + 1) % self.chips, self.core)
        self.left = self.device((self.place + self.chips - 1) % self.chips, self.core)

    def device(self, place, core):
        side = place // (self.chips // 2)
        return 2 * (2 * (place + side * (self.chips - 1 - 2 * place)) + side) + core

    def enter(self, across=False):
        barrier = pltpu.get_barrier_semaphore()
        targets = [{"ctx": other} for other in (self.left, self.right, self.partner)]
        if across:
            targets.append({"wsh": 1 - lax.axis_index("wsh")})
        for target in targets:
            pl.semaphore_signal(barrier, inc=1, device_id=target, device_id_type=MESH)
        pl.semaphore_wait(barrier, len(targets))


def ring_sum_kernel(devices, pieces, arrays, ahead, *refs):
    parts, outs = refs[:arrays], refs[arrays : 2 * arrays]
    own, other, flow = (refs[(2 + i) * arrays : (3 + i) * arrays] for i in range(3))
    own_sem, put_sem, got_sem, send_sem, recv_sem = refs[5 * arrays :]
    ring = Ring(devices)
    chips = ring.chips

    def region(p):
        array, _, first, rows, start, cols = pieces[p]
        return array, pl.ds(first, rows), pl.ds(start, cols)

    def chunk(p, step):
        way = pieces[p][1]
        return (ring.place + 2 * chips + way * (-1 - step)) % chips

    def load(p, step):
        array, rows, cols = region(p)
        source = ring.device(chunk(p, step), ring.core)
        return pltpu.make_async_copy(
            parts[array].at[source, rows, cols],
            own[array].at[step, rows, cols],
            own_sem.at[p, step],
        )

    def give(p, step):
        array, rows, cols = region(p)
        source = ring.device(chunk(p, step), 1 - ring.core)
        return pltpu.make_async_remote_copy(
            src_ref=parts[array].at[source, rows, cols],
            dst_ref=other[array].at[step, rows, cols],
            send_sem=put_sem.at[p, step],
            recv_sem=got_sem.at[p, step],
            device_id={"ctx": ring.partner},
            device_id_type=MESH,
        )

    def pass_on(p, step):
        array, rows, cols = region(p)
        way = pieces[p][1]
        return pltpu.make_async_remote_copy(
            src_ref=flow[array].at[step, rows, cols],
            dst_ref=flow[array].at[step + 1, rows, cols],
            send_sem=send_sem.at[p, step],
            recv_sem=recv_sem.at[p, step],
            device_id={"ctx": ring.right if way > 0 else ring.left},
            device_id_type=MESH,
        )

    def fetch(step):
        for p in range(len(pieces)):
            load(p, step).start()
            give(p, step).start()

    def add(p, step, first, last):
        array, _, row, rows, start, cols = pieces[p]
        width = 128 if cols % 128 == 0 else cols
        while width < 512 and cols % (2 * width) == 0:
            width *= 2
        rows = pl.ds(row, rows)

        def group(i, carry):
            at = start + i * width
            if cols > width:
                at = pl.multiple_of(at, 128)
            where = pl.ds(at, width)
            total = own[array][step, rows, where].astype(F32) + other[array][
                step, rows, where
            ].astype(F32)
            if not first:
                total += flow[array][step, rows, where].astype(F32)
            if last:
                outs[array][rows, where] = total.astype(outs[array].dtype)
            else:
                flow[array][step, rows, where] = total.astype(flow[array].dtype)
            return carry

        if cols == width:
            group(0, 0)
        else:
            lax.fori_loop(0, cols // width, group, 0)

    def work(step, first=False, last=False):
        for p in range(len(pieces)):
            load(p, step).wait()
            give(p, step).wait_recv()
            if not first:
                pass_on(p, step - 1).wait_recv()
            add(p, step, first, last)
            if not last:
                pass_on(p, step).start()

    for p in range(len(pieces)):
        load(p, 0).start()
    ring.enter()
    for p in range(len(pieces)):
        give(p, 0).start()
    for step in range(1, min(ahead, chips)):
        fetch(step)
    work(0, first=True)

    def middle(step, carry):
        @pl.when(step + ahead - 1 < chips)
        def _():
            fetch(step + ahead - 1)

        work(step)
        return carry

    lax.fori_loop(1, chips - 1, middle, 0)
    work(chips - 1, last=True)

    def drain(step, carry):
        for p in range(len(pieces)):
            give(p, step).wait_send()

            @pl.when(step < chips - 1)
            def _():
                pass_on(p, step).wait_send()

        return carry

    lax.fori_loop(0, chips, drain, 0)


def ring_sum(parts, pieces, devices, collective_id, ahead=3, name="ring_sum"):
    chips, count, arrays = devices // 2, len(pieces), len(parts)
    slots = [pltpu.VMEM((chips,) + p.shape[1:], p.dtype) for p in parts]
    return pl.pallas_call(
        functools.partial(ring_sum_kernel, devices, pieces, arrays, ahead),
        out_shape=[jax.ShapeDtypeStruct(p.shape[1:], F32) for p in parts],
        in_specs=[pl.BlockSpec(memory_space=pl.ANY)] * arrays,
        out_specs=[pl.BlockSpec(memory_space=pltpu.VMEM)] * arrays,
        scratch_shapes=slots * 3
        + [pltpu.SemaphoreType.DMA((count, chips))] * 3
        + [pltpu.SemaphoreType.DMA((count, chips - 1))] * 2,
        compiler_params=pltpu.CompilerParams(
            collective_id=collective_id, has_side_effects=True, vmem_limit_bytes=64000 * 1024
        ),
        name=name,
    )(*parts)


def split_ways(parts):
    pieces, lead = [], 1
    for i, p in enumerate(parts):
        _, rows, cols = p.shape
        tiles = cols // 128
        if cols % 128 == 0 and tiles > 1:
            left = (tiles + (1 if lead > 0 else 0)) // 2 * 128
            if tiles % 2:
                lead = -lead
            pieces.append((i, 1, 0, rows, 0, left))
            pieces.append((i, -1, 0, rows, left, cols - left))
        elif rows % 32 == 0:
            pieces.append((i, 1, 0, rows // 2, 0, cols))
            pieces.append((i, -1, rows // 2, rows // 2, 0, cols))
        else:
            pieces.append((i, 1, 0, rows, 0, cols))
    return tuple(pieces)


def sum_over_ctx(parts, pieces, devices, collective_id):
    if all(p.shape[1] % 8 == 0 for p in parts):
        return ring_sum(parts, pieces, devices, collective_id)
    return [
        lax.psum_scatter(p, "ctx", scatter_dimension=0, tiled=False).astype(F32) for p in parts
    ]


def front_kernel(
    devices,
    heads,
    tokens_ref,
    gains_ref,
    cos_ref,
    sin_ref,
    query_pos_ref,
    key_pos_ref,
    key_weight,
    value_weight,
    query_weight,
    out_weight,
    normed_ref,
    key_ref,
    query_low_ref,
    mixed_low_ref,
    mixed_ref,
    totals_ref,
    all_gains_ref,
    pairs_hbm,
    query_hbm,
    pair_whole_hbm,
    query_whole_hbm,
    out_whole_hbm,
    pairs_ref,
    query_ref,
    pair_whole,
    query_whole,
    out_whole,
    gains_other,
    keep_sem,
    own_sem,
    cross_send,
    cross_recv,
    side_send,
    side_recv,
    flow_send,
    flow_recv,
    twin_send,
    twin_recv,
):
    ring = Ring(devices)
    chips, far = ring.chips, ring.chips // 2
    me = lax.axis_index("ctx")
    mine = lax.axis_index("wsh")
    sequences, rows, width = tokens_ref.shape
    count = sequences * rows
    size = key_ref.shape[1]
    block = rows // 2
    stacked = heads * block
    weights = (key_weight, value_weight, query_weight, out_weight)

    def region(i, side, first, lines):
        if i == 3:
            start = side * out_weight.shape[0] + first
            return out_whole.at[pl.ds(pl.multiple_of(start, 16), lines)]
        cols = weights[i].shape[1]
        start = side * cols + (size if i == 1 else 0)
        target = query_whole if i == 2 else pair_whole
        return target.at[pl.ds(pl.multiple_of(first, 16), lines), pl.ds(pl.multiple_of(start, 128), cols)]

    def keep(i):
        source, target = (
            (pairs_ref, pairs_hbm),
            (query_ref, query_hbm),
            (pair_whole, pair_whole_hbm),
            (query_whole, query_whole_hbm),
            (out_whole, out_whole_hbm),
        )[i]
        return pltpu.make_async_copy(source, target, keep_sem.at[i])

    def own(i):
        return pltpu.make_async_copy(
            weights[i], region(i, mine, 0, weights[i].shape[0]), own_sem.at[i]
        )

    def cross(i):
        if i == len(weights):
            source, target = gains_ref, gains_other
        else:
            half = weights[i].shape[0] // 2
            first = pl.multiple_of(ring.core * half, 16)
            source, target = weights[i].at[pl.ds(first, half)], region(i, mine, first, half)
        return pltpu.make_async_remote_copy(
            src_ref=source,
            dst_ref=target,
            send_sem=cross_send.at[i],
            recv_sem=cross_recv.at[i],
            device_id={"wsh": 1 - mine},
            device_id_type=MESH,
        )

    def side(i):
        half = weights[i].shape[0] // 2
        part = region(i, 1 - mine, ring.core * half, half)
        return pltpu.make_async_remote_copy(
            src_ref=part,
            dst_ref=part,
            send_sem=side_send.at[i],
            recv_sem=side_recv.at[i],
            device_id={"ctx": ring.partner},
            device_id_type=MESH,
        )

    def block_copy(way, seq, hop, target, send_sem, recv_sem):
        stream = (1 if way < 0 else 0) * sequences + seq
        place = (ring.place + chips - way * hop) % chips
        part = pairs_ref.at[ring.device(place, ring.core), seq]
        return pltpu.make_async_remote_copy(
            src_ref=part,
            dst_ref=part,
            send_sem=send_sem.at[stream, hop],
            recv_sem=recv_sem.at[stream, hop],
            device_id={"ctx": target},
            device_id_type=MESH,
        )

    def flow(way, seq, hop):
        target = ring.right if way > 0 else ring.left
        return block_copy(way, seq, hop, target, flow_send, flow_recv)

    def twin(way, seq, hop):
        return block_copy(way, seq, hop, ring.partner, twin_send, twin_recv)

    def hops(way, seq):
        return far if (seq % 2 == 0) == (way > 0) else far - 1

    streams = [(way, seq) for seq in range(sequences) for way in (1, -1)]

    def pass_on(hop):
        for way, seq in streams:
            if hop > hops(way, seq):
                continue
            if hop > 0:
                flow(way, seq, hop - 1).wait_recv()
            if hop < hops(way, seq):
                flow(way, seq, hop).start()
            if hop > 0 or way > 0:
                twin(way, seq, hop).start()

    def turned(value, gain):
        scale = lax.rsqrt(jnp.mean(value * value, -1, keepdims=True) + EPS)
        value = value * scale * gain
        first, second = value[:, : size // 2], value[:, size // 2 :]
        cosine = jnp.concatenate([cos_ref[...]] * sequences, 0)
        sine = jnp.concatenate([sin_ref[...]] * sequences, 0)
        return jnp.concatenate(
            [first * cosine - second * sine, second * cosine + first * sine], -1
        ).astype(BF16)

    def queries():
        gain = all_gains_ref[4:5, :size]
        for h in range(heads):
            cols = slice(h * size, (h + 1) * size)
            value = dot(normed_ref[...], query_whole[:, cols], ((1,), (0,)))
            query_ref[:, cols] = value
            query_low_ref[:, :, cols] = turned(value, gain).reshape(sequences, rows, size)

    def attention(seq, carry):
        chunk = min(devices, 16)
        asked, sums, totals = [], [], []
        for half in range(2):
            lines = slice(half * block, (half + 1) * block)
            asked.append(
                jnp.concatenate(
                    [query_low_ref[seq, lines, h * size : (h + 1) * size] for h in range(heads)], 0
                )
            )
            sums.append(jnp.zeros((stacked, size), F32))
            totals.append(jnp.zeros((stacked, 1), F32))
        for first in range(0, devices, chunk):
            span = slice(first * block, (first + chunk) * block)
            for key_half in range(2):
                part = pairs_ref[
                    first : first + chunk, seq, key_half * block : (key_half + 1) * block, :
                ].reshape(chunk * block, 2 * size)
                keys, values = part[:, :size], part[:, size:]
                for half in range(key_half, 2):
                    weights = jnp.exp(dot(asked[half], keys, ((1,), (1,))) * SCORE_SCALE)
                    if half == key_half:
                        allowed = (
                            key_pos_ref[key_half : key_half + 1, span]
                            <= query_pos_ref[half * stacked : (half + 1) * stacked, :]
                        )
                        weights = jnp.where(allowed, weights, 0.0)
                    low = weights.astype(BF16)
                    totals[half] += jnp.sum(low.astype(F32), -1, keepdims=True)
                    sums[half] += dot(low, values, ((1,), (0,)))
        for half in range(2):
            mixed = sums[half] / totals[half]
            span = slice(half * stacked, (half + 1) * stacked)
            mixed_ref[seq, span, :] = mixed
            totals_ref[seq, span, :] = jnp.broadcast_to(
                totals[half], (stacked, totals_ref.shape[2])
            )
            for h in range(heads):
                mixed_low_ref[
                    seq, half * block : (half + 1) * block, h * size : (h + 1) * size
                ] = mixed[h * block : (h + 1) * block].astype(BF16)
        return carry

    for i in range(len(weights)):
        own(i).start()
    ring.enter(across=True)
    order = (len(weights), 0, 1, 2, 3)
    for i in order:
        cross(i).start()
    inputs = tokens_ref[...].reshape(count, width).astype(F32)
    scale = lax.rsqrt(jnp.mean(inputs * inputs, -1, keepdims=True) + EPS)
    cross(len(weights)).wait_recv()
    all_gains_ref[...] = gains_ref[...] + gains_other[...]
    normed_ref[...] = (inputs * scale * all_gains_ref[0:1, :]).astype(BF16)
    for i in (0, 1):
        cross(i).wait_recv()
        side(i).start()
    for i in (0, 1):
        own(i).wait()
        side(i).wait_recv()
    keep(2).start()
    value = dot(normed_ref[...], pair_whole[...], ((1,), (0,)))
    key_ref[...] = value[:, :size]
    key_low = turned(value[:, :size], all_gains_ref[4:5, size : 2 * size])
    pairs_ref[me, :, :, :size] = key_low.reshape(sequences, rows, size)
    pairs_ref[me, :, :, size:] = value[:, size:].astype(BF16).reshape(sequences, rows, size)
    pass_on(0)
    pass_on(1)
    cross(2).wait_recv()
    side(2).start()
    for hop in range(2, far + 1):
        pass_on(hop)
        if hop == 2:
            own(2).wait()
            side(2).wait_recv()
            keep(3).start()
            queries()
            keep(1).start()
    cross(3).wait_recv()
    side(3).start()
    for hop in range(far + 1):
        for way, seq in streams:
            if hop <= hops(way, seq) and (hop > 0 or way > 0):
                twin(way, seq, hop).wait_recv()
    keep(0).start()
    own(3).wait()
    side(3).wait_recv()
    keep(4).start()
    lax.fori_loop(0, sequences, attention, 0)
    for hop in range(far + 1):
        for way, seq in streams:
            if hop > hops(way, seq):
                continue
            if hop > 0 or way > 0:
                twin(way, seq, hop).wait_send()
            if hop < hops(way, seq):
                flow(way, seq, hop).wait_send()
    for i in order:
        cross(i).wait_send()
    for i in range(len(weights)):
        side(i).wait_send()
    for i in range(5):
        keep(i).wait()


def front(tokens, gains, cosine, sine, query_pos, key_pos, weights, heads, devices, collective_id):
    sequences, rows, width = tokens.shape
    size = 2 * cosine.shape[1]
    count = sequences * rows
    far = devices // 4
    stacked = query_pos.shape[0]
    here, there = pl.BlockSpec(memory_space=pltpu.VMEM), pl.BlockSpec(memory_space=pl.ANY)
    streams = pltpu.SemaphoreType.DMA((2 * sequences, far + 1))
    outs = [
        ((count, width), BF16),
        ((count, size), F32),
        ((sequences, rows, heads * size), BF16),
        ((sequences, rows, heads * size), BF16),
        ((sequences, stacked, size), F32),
        ((sequences, stacked, 128), F32),
        (gains.shape, F32),
    ]
    kept = [
        ((devices, sequences, rows, 2 * size), BF16),
        ((count, heads * size), F32),
        ((width, 2 * size), BF16),
        ((width, heads * size), BF16),
        ((width, heads * size), BF16),
    ]
    return pl.pallas_call(
        functools.partial(front_kernel, devices, heads),
        in_specs=[here] * 6 + [there] * 4,
        out_specs=[here] * len(outs) + [there] * len(kept),
        out_shape=[jax.ShapeDtypeStruct(shape, kind) for shape, kind in outs + kept],
        scratch_shapes=[pltpu.VMEM(shape, kind) for shape, kind in kept]
        + [pltpu.VMEM(gains.shape, gains.dtype)]
        + [pltpu.SemaphoreType.DMA((5,))]
        + [pltpu.SemaphoreType.DMA((4,))]
        + [pltpu.SemaphoreType.DMA((5,))] * 2
        + [pltpu.SemaphoreType.DMA((4,))] * 2
        + [streams] * 4,
        compiler_params=pltpu.CompilerParams(
            collective_id=collective_id, has_side_effects=True, vmem_limit_bytes=67043328
        ),
        name="front",
    )(tokens, gains, cosine, sine, query_pos, key_pos, *weights)


class RingSum:
    def __init__(self, ring, pieces, parts, own, other, flow, outs, sems):
        self.ring, self.pieces, self.parts, self.own = ring, pieces, parts, own
        self.other, self.flow, self.outs = other, flow, outs
        self.put_sem, self.got_sem, self.send_sem, self.recv_sem = sems[:4]
        self.own_sem = sems[4] if own is not None else None
        self.last = ring.chips - 1

    def region(self, p):
        array, _, first, rows, start, cols = self.pieces[p]
        return array, pl.ds(first, rows), pl.ds(start, cols)

    def owner(self, p, step, core):
        way = self.pieces[p][1]
        chips = self.ring.chips
        return self.ring.device((self.ring.place + 2 * chips + way * (-1 - step)) % chips, core)

    def load(self, p, step):
        array, rows, cols = self.region(p)
        slot = step % self.own[array].shape[0]
        return pltpu.make_async_copy(
            self.parts[array].at[self.owner(p, step, self.ring.core), rows, cols],
            self.own[array].at[slot, rows, cols],
            self.own_sem.at[p, step],
        )

    def give(self, p, step):
        array, rows, cols = self.region(p)
        return pltpu.make_async_remote_copy(
            src_ref=self.parts[array].at[self.owner(p, step, 1 - self.ring.core), rows, cols],
            dst_ref=self.other[array].at[step, rows, cols],
            send_sem=self.put_sem.at[p, step],
            recv_sem=self.got_sem.at[p, step],
            device_id={"ctx": self.ring.partner},
            device_id_type=MESH,
        )

    def hop(self, p, step):
        array, rows, cols = self.region(p)
        way = self.pieces[p][1]
        return pltpu.make_async_remote_copy(
            src_ref=self.flow[array].at[step, rows, cols],
            dst_ref=self.flow[array].at[step + 1, rows, cols],
            send_sem=self.send_sem.at[p, step],
            recv_sem=self.recv_sem.at[p, step],
            device_id={"ctx": self.ring.right if way > 0 else self.ring.left},
            device_id_type=MESH,
        )

    def load_all(self, step):
        for p in range(len(self.pieces)):
            self.load(p, step).start()

    def give_all(self, step):
        for p in range(len(self.pieces)):
            self.give(p, step).start()

    def work(self, p, step):
        array, _, row, rows, start, cols = self.pieces[p]
        if self.own is not None:
            self.load(p, step).wait()
            mine, at_mine = self.own[array], step % self.own[array].shape[0]
        else:
            mine, at_mine = self.parts[array], self.owner(p, step, self.ring.core)
        self.give(p, step).wait_recv()
        if step > 0:
            self.hop(p, step - 1).wait_recv()
        width = 128 if cols % 128 == 0 else cols
        while width < 512 and cols % (2 * width) == 0:
            width *= 2
        rows = pl.ds(row, rows)

        def group(i, carry):
            at = start + i * width
            if cols > width:
                at = pl.multiple_of(at, 128)
            where = pl.ds(at, width)
            total = mine[at_mine, rows, where].astype(F32)
            total += self.other[array][step, rows, where].astype(F32)
            if step > 0:
                total += self.flow[array][step, rows, where].astype(F32)
            if step == self.last:
                self.outs[array][rows, where] = total.astype(self.outs[array].dtype)
            else:
                self.flow[array][step, rows, where] = total.astype(self.flow[array].dtype)
            return carry

        if cols == width:
            group(0, 0)
        else:
            lax.fori_loop(0, cols // width, group, 0)
        if step < self.last:
            self.hop(p, step).start()

    def drain(self):
        for p in range(len(self.pieces)):
            for step in range(self.last + 1):
                self.give(p, step).wait_send()
                if step < self.last:
                    self.hop(p, step).wait_send()


def norm_back(upstream, vector, gain):
    scale = lax.rsqrt(jnp.mean(vector * vector, -1, keepdims=True) + EPS)
    normal = vector * scale
    weighted = upstream * gain
    back = scale * (weighted - normal * jnp.mean(weighted * normal, -1, keepdims=True))
    return back, jnp.sum(upstream * normal, 0, keepdims=True)


GELU_SCALE = math.sqrt(2.0 / math.pi)
GELU_CUBE = 0.044715


def feed_forward_kernel(
    mixed_ref,
    tokens_ref,
    cotangent_ref,
    gains_ref,
    out_hbm,
    gate_hbm,
    up_hbm,
    down_hbm,
    output_ref,
    hidden_back_ref,
    mixed_back_ref,
    attended_own_ref,
    attended_send_ref,
    gain_part_ref,
    down_grad_hbm,
    gate_grad_hbm,
    up_grad_hbm,
    gate_weight,
    up_weight,
    down_weight,
    out_weight,
    attended_ref,
    ff_rows,
    low_rows,
    ff_turned,
    low_turned,
    gate,
    upward,
    activated,
    partial,
    part_send,
    part_recv,
    back_send,
    back_recv,
    hidden_ref,
    staging,
    load_sem,
    out_sem,
    store_sem,
    cross_send,
    cross_recv,
):
    count, width = attended_ref.shape
    hidden_units = gate_weight.shape[1]
    block = part_send.shape[0] // 2
    chunk = staging.shape[2]
    whole_chunks = hidden_units // chunk
    rest = hidden_units - whole_chunks * chunk
    mine = lax.axis_index("wsh")
    weights = ((gate_hbm, gate_weight), (up_hbm, up_weight), (down_hbm, down_weight))

    def load(w, at, size, index):
        source, target = weights[w]
        cols = pl.ds(at, size)
        return pltpu.make_async_copy(source.at[:, cols], target.at[:, cols], load_sem.at[w, index])

    def chunks(work):
        def step(c, carry):
            work(pl.multiple_of(c * chunk, 128), chunk, c)
            return carry

        lax.fori_loop(0, whole_chunks, step, 0)
        if rest:
            work(whole_chunks * chunk, rest, whole_chunks)

    def across(kind, piece, source, target):
        return pltpu.make_async_remote_copy(
            src_ref=source,
            dst_ref=target,
            send_sem=cross_send.at[kind, piece],
            recv_sem=cross_recv.at[kind, piece],
            device_id={"wsh": 1 - mine},
            device_id_type=MESH,
        )

    def swap_rows(kind, ref, piece):
        first = piece * block
        here, there = pl.multiple_of(first, block), pl.multiple_of(count + first, block)
        return across(kind, piece, ref.at[pl.ds(here, block)], ref.at[pl.ds(there, block)])

    def swap_parts(kind, source, target, piece):
        lines = pl.ds(pl.multiple_of(piece * block, block), block)
        return across(kind, piece, source.at[lines], target.at[lines])

    def start_load(at, size, index):
        for w in range(3):
            load(w, at, size, index).start()

    bring_out = pltpu.make_async_copy(out_hbm, out_weight, out_sem.at[0])
    bring_out.start()
    chunks(start_load)
    barrier = pltpu.get_barrier_semaphore()
    pl.semaphore_signal(barrier, inc=1, device_id={"wsh": 1 - mine}, device_id_type=MESH)

    bring_out.wait()
    attended = dot(mixed_ref[...], out_weight[...], ((1,), (1,)))
    attended_ref[...] = attended
    scale = lax.rsqrt(jnp.mean(attended * attended, -1, keepdims=True) + EPS)
    hidden = tokens_ref[...].astype(F32) + attended * scale * gains_ref[1:2, :]
    hidden_ref[...] = hidden
    scale = lax.rsqrt(jnp.mean(hidden * hidden, -1, keepdims=True) + EPS)
    ff_rows[:count, :] = (hidden * scale * gains_ref[2:3, :]).astype(BF16)
    pl.semaphore_wait(barrier, 1)
    for piece in range(2):
        swap_rows(0, ff_rows, piece).start()

    def forward(b, carry):
        @pl.when(b >= 2)
        def _():
            swap_rows(0, ff_rows, b - 2).wait_recv()

        lines = pl.ds(pl.multiple_of(b * block, block), block)

        def columns(at, size, index):
            @pl.when(b == 0)
            def _():
                for w in range(3):
                    load(w, at, size, index).wait()

            cols = pl.ds(at, size)
            g = dot(ff_rows[lines, :], gate_weight[:, cols], ((1,), (0,)))
            u = dot(ff_rows[lines, :], up_weight[:, cols], ((1,), (0,)))
            square = g * g
            t = jnp.tanh(g * (GELU_SCALE + GELU_SCALE * GELU_CUBE * square))
            half = 0.5 + 0.5 * t
            gelu = g * half
            slope = half + gelu * (1.0 - t) * (GELU_SCALE + 3.0 * GELU_SCALE * GELU_CUBE * square)
            gate[lines, cols] = (u * slope).astype(BF16)
            upward[lines, cols] = gelu.astype(BF16)
            activated[lines, cols] = (gelu * u).astype(BF16)

        chunks(columns)

        @pl.when(b == 1)
        def _():
            partial[...] = dot(activated[:count, :], down_weight[...], ((1,), (1,)))

        @pl.when(b >= 2)
        def _():
            there = pl.ds(pl.multiple_of((b - 2) * block, block), block)
            part_send[there, :] = dot(activated[lines, :], down_weight[...], ((1,), (1,))).astype(
                BF16
            )
            swap_parts(1, part_send, part_recv, b - 2).start()

        return carry

    lax.fori_loop(0, 4, forward, 0)
    ff_turned[...] = ff_rows[...].T
    for piece in range(2):
        swap_parts(1, part_send, part_recv, piece).wait_recv()
    lowered = partial[...] + part_recv[...].astype(F32)
    cotangent = cotangent_ref[...].astype(F32)
    back, part = norm_back(cotangent, lowered, gains_ref[3:4, :])
    low_rows[:count, :] = back.astype(BF16)
    for piece in range(2):
        swap_rows(2, low_rows, piece).start()
    gain_part_ref[...] = jnp.zeros_like(gain_part_ref)
    gain_part_ref[3:4, :] = part
    scale = lax.rsqrt(jnp.mean(lowered * lowered, -1, keepdims=True) + EPS)
    output_ref[...] = (hidden_ref[...] + lowered * scale * gains_ref[3:4, :]).astype(BF16)

    def backward(half, carry):
        def columns_of(piece, carry):
            @pl.when(half == 1)
            def _():
                swap_rows(2, low_rows, piece).wait_recv()

            lines = pl.ds(pl.multiple_of(half * count + piece * block, block), block)

            def columns(at, size, index):
                cols = pl.ds(at, size)
                d = dot(low_rows[lines, :], down_weight[:, cols], ((1,), (0,)))
                gate[lines, cols] = (d * gate[lines, cols].astype(F32)).astype(BF16)
                upward[lines, cols] = (d * upward[lines, cols].astype(F32)).astype(BF16)

            chunks(columns)
            return carry

        lax.fori_loop(0, 2, columns_of, 0)
        lines = pl.ds(pl.multiple_of(half * count, block), count)
        value = dot(gate[lines, :], gate_weight[...], ((1,), (1,)))
        value += dot(upward[lines, :], up_weight[...], ((1,), (1,)))

        @pl.when(half == 0)
        def _():
            partial[...] = value

        @pl.when(half == 1)
        def _():
            back_send[...] = value.astype(BF16)
            for piece in range(2):
                swap_parts(3, back_send, back_recv, piece).start()

        return carry

    lax.fori_loop(0, 2, backward, 0)
    low_turned[...] = low_rows[...].T

    grads = (
        (low_turned, activated, down_grad_hbm),
        (ff_turned, gate, gate_grad_hbm),
        (ff_turned, upward, up_grad_hbm),
    )

    def store(m, at, size, index):
        cols = pl.ds(at, size)
        return pltpu.make_async_copy(
            staging.at[index % 2, :, pl.ds(0, size)], grads[m][2].at[:, cols], store_sem.at[m, index]
        )

    for m in range(3):
        left, right, _ = grads[m]

        def columns(at, size, index, m=m, left=left, right=right):
            @pl.when(index >= 2)
            def _():
                store(m, 0, chunk, index - 2).wait()

            for top in range(0, width, width // 2):
                lines = slice(top, top + width // 2)
                staging[index % 2, lines, :size] = dot(
                    left[lines, :], right[:, pl.ds(at, size)], ((1,), (0,))
                ).astype(BF16)
            store(m, at, size, index).start()

        chunks(columns)
        last = whole_chunks + (1 if rest else 0)
        for index in range(max(last - 2, 0), last):
            store(m, 0, rest if index == whole_chunks else chunk, index).wait()

    for piece in range(2):
        swap_parts(3, back_send, back_recv, piece).wait_recv()
    upstream = partial[...] + back_recv[...].astype(F32)
    back, part = norm_back(upstream, hidden_ref[...], gains_ref[2:3, :])
    gain_part_ref[2:3, :] = part
    back += cotangent_ref[...].astype(F32)
    hidden_back_ref[...] = back
    back, part = norm_back(back, attended_ref[...], gains_ref[1:2, :])
    gain_part_ref[1:2, :] = part
    mixed_back_ref[...] = dot(back.astype(BF16), out_weight[...], ((1,), (0,))).astype(BF16)
    first, second = back[:, : width // 2].astype(BF16), back[:, width // 2 :].astype(BF16)
    attended_own_ref[...] = jnp.where(mine == 0, first, second)
    attended_send_ref[...] = jnp.where(mine == 0, second, first)
    for piece in range(2):
        swap_rows(0, ff_rows, piece).wait_send()
        swap_parts(1, part_send, part_recv, piece).wait_send()
        swap_rows(2, low_rows, piece).wait_send()
        swap_parts(3, back_send, back_recv, piece).wait_send()


def feed_forward(mixed, tokens, cotangent, gains, weights, collective_id):
    count, width = tokens.shape
    hidden_units = weights[1].shape[1]
    chunk = 512
    pieces = -(-hidden_units // chunk)
    here, there = pl.BlockSpec(memory_space=pltpu.VMEM), pl.BlockSpec(memory_space=pl.ANY)
    like = lambda shape, kind: jax.ShapeDtypeStruct(shape, kind)
    matrix = (width, hidden_units)
    return pl.pallas_call(
        feed_forward_kernel,
        in_specs=[here] * 4 + [there] * 4,
        out_specs=[here] * 6 + [there] * 3,
        out_shape=[
            like((count, width), BF16),
            like((count, width), F32),
            like(mixed.shape, BF16),
            like((count, width // 2), BF16),
            like((count, width // 2), BF16),
            like(gains.shape, F32),
        ]
        + [like(matrix, BF16)] * 3,
        scratch_shapes=[pltpu.VMEM(matrix, BF16)] * 3
        + [pltpu.VMEM(weights[0].shape, BF16), pltpu.VMEM((count, width), F32)]
        + [pltpu.VMEM((2 * count, width), BF16)] * 2
        + [pltpu.VMEM((width, 2 * count), BF16)] * 2
        + [pltpu.VMEM((2 * count, hidden_units), BF16)] * 3
        + [pltpu.VMEM((count, width), F32)]
        + [pltpu.VMEM((count, width), BF16)] * 4
        + [
            pltpu.VMEM((count, width), F32),
            pltpu.VMEM((2, width, chunk), BF16),
            pltpu.SemaphoreType.DMA((3, pieces)),
            pltpu.SemaphoreType.DMA((1,)),
            pltpu.SemaphoreType.DMA((3, pieces)),
            pltpu.SemaphoreType.DMA((4, 2)),
            pltpu.SemaphoreType.DMA((4, 2)),
        ],
        compiler_params=pltpu.CompilerParams(
            collective_id=collective_id, has_side_effects=True, vmem_limit_bytes=67043328
        ),
        name="feed_forward",
    )(mixed, tokens, cotangent, gains, *weights)


def turn_back(upstream, cosine, sine):
    middle = upstream.shape[-1] // 2
    first, second = upstream[:, :middle], upstream[:, middle:]
    return jnp.concatenate([first * cosine + second * sine, second * cosine - first * sine], -1)


def back_kernel(devices, heads, ff_pieces, kv_pieces, attn_pieces, names, *refs):
    r = dict(zip(names, refs))
    ring = Ring(devices)
    chips = ring.chips
    mine = lax.axis_index("wsh")
    sequences, rows, _ = r["query"].shape
    size = r["key_raw"].shape[1]
    count = sequences * rows
    block = rows // 2
    stacked = heads * block

    ff = RingSum(
        ring,
        ff_pieces,
        [r["part_down"], r["part_gate"], r["part_up"]],
        [r[f"ff_own{i}"] for i in range(3)],
        [r[f"ff_other{i}"] for i in range(3)],
        [r[f"ff_flow{i}"] for i in range(3)],
        [r["grad_down"], r["grad_gate"], r["grad_up"]],
        [r["ff_put"], r["ff_got"], r["ff_send"], r["ff_recv"], r["ff_load"]],
    )
    kv = RingSum(
        ring,
        kv_pieces,
        [r["pairs"]],
        None,
        [r["kv_other"]],
        [r["kv_flow"]],
        [r["kv_sum"]],
        [r["kv_put"], r["kv_got"], r["kv_send"], r["kv_recv"]],
    )
    attn = RingSum(
        ring,
        attn_pieces,
        [r["qkv_part"], r["out_part"]],
        None,
        [r["qkv_other"], r["out_other"]],
        [r["qkv_flow"], r["out_flow"]],
        [r["grad_qkv"], r["grad_out"]],
        [r["at_put"], r["at_got"], r["at_send"], r["at_recv"]],
    )

    def brought(i):
        name = BROUGHT[i]
        return pltpu.make_async_copy(r["in_" + name], r[name], r["bring"].at[i])

    def need(*wanted):
        for name in wanted:
            brought(BROUGHT.index(name)).wait()

    def across(i, source, target):
        return pltpu.make_async_remote_copy(
            src_ref=source,
            dst_ref=target,
            send_sem=r["cross_send"].at[i],
            recv_sem=r["cross_recv"].at[i],
            device_id={"wsh": 1 - mine},
            device_id_type=MESH,
        )

    out_swap = across(0, r["att_send"], r["att_across"])
    col_swap = across(1, r["col_send"], r["col_rows"].at[pl.ds(count, count)])
    gain_swap = across(2, r["gain_own"], r["gain_across"])
    mixed_swap = across(3, r["mixed_own"], r["mixed_other"])
    normed_swap = across(4, r["normed_own"], r["normed_other"])
    gain_twin = pltpu.make_async_remote_copy(
        src_ref=r["gain_pair"],
        dst_ref=r["gain_twin"],
        send_sem=r["twin_send"].at[0],
        recv_sem=r["twin_recv"].at[0],
        device_id={"ctx": ring.partner},
        device_id_type=MESH,
    )

    def gain_hop(way, step):
        return pltpu.make_async_remote_copy(
            src_ref=r["gain_flow"].at[way, step],
            dst_ref=r["gain_flow"].at[way, step + 1],
            send_sem=r["gain_send"].at[way, step],
            recv_sem=r["gain_recv"].at[way, step],
            device_id={"ctx": ring.right if way == 0 else ring.left},
            device_id_type=MESH,
        )

    gain_hops = (chips // 2, chips - 1 - chips // 2)

    def attention(seq, carry):
        queries, scaled, correction = [], [], []
        for half in range(2):
            span = slice(half * stacked, (half + 1) * stacked)
            lines = slice(half * block, (half + 1) * block)
            cut = lambda ref: jnp.concatenate(
                [ref[seq, lines, h * size : (h + 1) * size] for h in range(heads)], 0
            )
            queries.append(cut(r["query"]))
            grad = cut(r["grad_mixed"]).astype(F32)
            total = r["totals"][seq, span, :1]
            delta = jnp.sum(grad * r["mixed"][seq, span, :], -1, keepdims=True)
            scaled.append((grad / total).astype(BF16))
            correction.append(delta / total)
        grad_query = [jnp.zeros((stacked, size), F32) for _ in range(2)]
        for key_half in range(2):
            lines = pl.ds(pl.multiple_of(seq * rows + key_half * block, block), block)
            part = r["pairs"][:, lines, :].reshape(devices * block, 2 * size)
            keys, values = part[:, :size], part[:, size:]
            grad_keys = jnp.zeros((devices * block, size), F32)
            grad_values = jnp.zeros((devices * block, size), F32)
            for half in range(key_half, 2):
                weights = jnp.exp(dot(queries[half], keys, ((1,), (1,))) * SCORE_SCALE)
                if half == key_half:
                    allowed = (
                        r["key_pos"][key_half : key_half + 1, :]
                        <= r["query_pos"][half * stacked : (half + 1) * stacked, :]
                    )
                    weights = jnp.where(allowed, weights, 0.0)
                low = weights.astype(BF16)
                grad_weights = dot(scaled[half], values, ((1,), (1,)))
                grad_scores = (weights * (grad_weights - correction[half])).astype(BF16)
                grad_query[half] += dot(grad_scores, keys, ((1,), (0,)))
                grad_keys += dot(grad_scores, queries[half], ((0,), (0,)))
                grad_values += dot(low, scaled[half], ((0,), (0,)))
            both = jnp.concatenate([grad_keys * SCORE_SCALE, grad_values], -1).astype(BF16)
            r["pairs"][:, lines, :] = both.reshape(devices, block, 2 * size)
        for half in range(2):
            r["mixed"][seq, half * stacked : (half + 1) * stacked, :] = grad_query[half] * SCORE_SCALE
        return carry

    def pick(value, which):
        middle = value.shape[1] // 2
        return jnp.where(which == 0, value[:, :middle], value[:, middle:])

    def projections():
        need("query_raw", "key_raw", "cosine", "sine", "gains")
        cosine = jnp.concatenate([r["cosine"][...]] * sequences, 0)
        sine = jnp.concatenate([r["sine"][...]] * sequences, 0)
        gain = r["gains"][4:5, :size]
        total = jnp.zeros((1, size), F32)
        lows = []
        for h in range(heads):
            cols = slice(h * size, (h + 1) * size)
            grad = jnp.concatenate(
                [
                    r["mixed"][seq, half * stacked + h * block : half * stacked + (h + 1) * block, :]
                    for seq in range(sequences)
                    for half in range(2)
                ],
                0,
            )
            back, part = norm_back(
                turn_back(grad, cosine, sine), r["query_raw"][:, cols], gain
            )
            total += part
            r["query_low"][:, cols] = back.astype(BF16)
        back, key_total = norm_back(
            turn_back(r["kv_sum"][:, :size], cosine, sine),
            r["key_raw"][...],
            r["gains"][4:5, size : 2 * size],
        )
        r["pair_low"][:, :size] = back.astype(BF16)
        r["pair_low"][:, size:] = r["kv_sum"][:, size:].astype(BF16)
        first = 0
        for value in (
            r["query_low"][...],
            r["pair_low"][:, :size],
            r["pair_low"][:, size:],
        ):
            cols = slice(first, first + value.shape[1] // 2)
            r["col_rows"][:count, cols] = pick(value, mine)
            r["col_send"][:, cols] = pick(value, 1 - mine)
            first += value.shape[1] // 2
        col_swap.start()
        need("weight_query", "weight_pair", "tokens", "grad_hidden", "gain_part")
        grad_normed = dot(r["query_low"][...], r["weight_query"][...], ((1,), (1,)))
        grad_normed += dot(r["pair_low"][...], r["weight_pair"][...], ((1,), (1,)))
        back, part = norm_back(grad_normed, r["tokens"][...].astype(F32), r["gains"][0:1, :])
        r["grad_tokens"][...] = back + r["grad_hidden"][...]
        r["gain_own"][...] = r["gain_part"][...]
        r["gain_own"][0:1, :] = part
        r["gain_own"][4:5, :size] = total
        r["gain_own"][4:5, size : 2 * size] = key_total
        gain_swap.start()

    def out_part():
        need("att_own")
        out_swap.wait_recv()
        mixed_swap.wait_recv()
        _, lines, cols = r["out_part"].shape
        value = dot(r["mixed_own"][...], r["att_own"][...], ((0,), (0,)))
        value += dot(r["mixed_other"][...], r["att_across"][...], ((0,), (0,)))
        r["out_part"][...] = value.reshape(devices, lines, cols).astype(BF16)

    def turn_rows():
        normed_swap.wait_recv()
        r["weight_pair"][:, :count] = r["normed_own"][...].T
        r["weight_pair"][:, count:] = r["normed_other"][...].T

    def qkv_part():
        col_swap.wait_recv()
        _, lines, cols = r["qkv_part"].shape
        width = 256
        for first in range(0, cols, width):
            value = dot(
                r["weight_pair"][...], r["col_rows"][:, first : first + width], ((1,), (0,))
            )
            r["qkv_part"][:, :, first : first + width] = value.reshape(
                devices, lines, width
            ).astype(BF16)

    def gains_step(step):
        if step == 0:
            gain_swap.wait_recv()
            r["gain_pair"][...] = r["gain_own"][...] + r["gain_across"][...]
            gain_twin.start()
        elif step == 1:
            gain_twin.wait_recv()
            both = r["gain_pair"][...] + r["gain_twin"][...]
            r["gain_flow"][0, 0] = both
            r["gain_flow"][1, 0] = both
            r["gain_sum"][...] = both
            for way in range(2):
                gain_hop(way, 0).start()
        else:
            for way in range(2):
                if step - 2 < gain_hops[way]:
                    gain_hop(way, step - 2).wait_recv()
                    if step - 1 < gain_hops[way]:
                        gain_hop(way, step - 1).start()
                    r["gain_sum"][...] += r["gain_flow"][way, step - 1]

    def ff_step(step, extra=()):
        extra = list(extra)
        if step + 1 < chips:
            ff.load_all(step + 1)
        if step + 2 < chips:
            ff.give_all(step + 2)
        for p in range(len(ff_pieces)):
            ff.work(p, step)
            if p % 2 == 1 and extra:
                extra.pop(0)()
        for left in extra:
            left()

    def kv_step(step):
        def run():
            for p in range(len(kv_pieces)):
                kv.work(p, step)

        return run

    def attn_step(step):
        def run():
            gains_step(step)
            for p in range(len(attn_pieces)):
                attn.work(p, step)

        return run

    def bring(first, last):
        for i in range(BROUGHT.index(first), BROUGHT.index(last) + 1):
            brought(i).start()

    ff.load_all(0)
    ring.enter(across=True)
    ff.give_all(0)
    bring("att_send", "key_pos")
    ff.give_all(1)
    ff_step(0)
    need("att_send")
    out_swap.start()
    bring("mixed_own", BROUGHT[-1])
    need("mixed_own", "normed_own")
    mixed_swap.start()
    normed_swap.start()
    need("pairs", "query", "grad_mixed", "mixed", "totals", "query_pos", "key_pos")
    lax.fori_loop(0, sequences, attention, 0)
    for step in range(chips):
        kv.give_all(step)
    ff_step(1, [kv_step(0), kv_step(1), kv_step(2)])
    ff_step(2, [kv_step(3), kv_step(4), kv_step(5)])
    ff_step(3, [kv_step(6), kv_step(7), out_part])
    projections()
    ff_step(4, [turn_rows])
    qkv_part()
    for step in range(chips):
        attn.give_all(step)
    ff_step(5, [attn_step(0), attn_step(1), attn_step(2)])
    ff_step(6, [attn_step(3), attn_step(4), attn_step(5)])
    ff_step(7, [attn_step(6), attn_step(7)])
    r["gains_total"][...] = r["gain_sum"][...]
    for copy in (out_swap, col_swap, gain_swap, mixed_swap, normed_swap, gain_twin):
        copy.wait_send()
    for way in range(2):
        for step in range(gain_hops[way]):
            gain_hop(way, step).wait_send()
    ff.drain()
    kv.drain()
    attn.drain()


BROUGHT = (
    "att_send",
    "pairs",
    "query",
    "grad_mixed",
    "mixed",
    "totals",
    "query_pos",
    "key_pos",
    "mixed_own",
    "normed_own",
    "att_own",
    "query_raw",
    "key_raw",
    "cosine",
    "sine",
    "gains",
    "weight_query",
    "weight_pair",
    "tokens",
    "grad_hidden",
    "gain_part",
)


def back(given, ff_parts, heads, devices, collective_id):
    chips = devices // 2
    count, width = given["tokens"].shape
    size = given["key_raw"].shape[1]
    out_cols = given["att_send"].shape[1]
    out_lines = given["mixed_own"].shape[1] // devices
    lines = width // devices
    cols = (heads * size + 2 * size) // 2
    slots = lambda n, p: pltpu.VMEM((n,) + tuple(p.shape[1:]), p.dtype)
    ff_pieces = split_ways(ff_parts)
    pair_rows = given["pairs"].shape[1]
    kv_pieces = tuple(
        (0, 1 - 2 * (i % 2), i * pair_rows // 4, pair_rows // 4, 0, 2 * size) for i in range(4)
    )
    attn_pieces = (
        (0, 1, 0, lines, 0, cols // 2),
        (0, -1, 0, lines, cols // 2, cols // 2),
        (1, 1, 0, out_lines // 2, 0, out_cols),
        (1, -1, out_lines // 2, out_lines // 2, 0, out_cols),
    )
    dma = lambda *shape: pltpu.SemaphoreType.DMA(shape)
    names, specs, operands = [], [], []
    for name, array in zip(("part_down", "part_gate", "part_up"), ff_parts):
        names.append(name)
        operands.append(array)
    for name in BROUGHT:
        names.append("in_" + name)
        operands.append(given[name])
    outs = {
        "grad_tokens": ((count, width), F32),
        "grad_down": (ff_parts[0].shape[1:], BF16),
        "grad_gate": (ff_parts[1].shape[1:], BF16),
        "grad_up": (ff_parts[2].shape[1:], BF16),
        "grad_qkv": ((lines, cols), F32),
        "grad_out": ((out_lines, out_cols), F32),
        "gains_total": (given["gains"].shape, F32),
    }
    scratch = {}
    for name in BROUGHT:
        shape = given[name].shape
        scratch[name] = pltpu.VMEM(shape, given[name].dtype)
    for i, p in enumerate(ff_parts):
        scratch[f"ff_own{i}"] = slots(2, p)
        scratch[f"ff_other{i}"] = slots(chips, p)
        scratch[f"ff_flow{i}"] = slots(chips, p)
    for kind, pieces in (("ff", ff_pieces), ("kv", kv_pieces), ("at", attn_pieces)):
        for name, steps in (("put", chips), ("got", chips), ("send", chips - 1), ("recv", chips - 1)):
            scratch[f"{kind}_{name}"] = dma(len(pieces), steps)
    scratch["ff_load"] = dma(len(ff_pieces), chips)
    scratch["kv_other"] = slots(chips, given["pairs"])
    scratch["kv_flow"] = slots(chips, given["pairs"])
    scratch["kv_sum"] = pltpu.VMEM((pair_rows, 2 * size), F32)
    for name in ("mixed", "normed"):
        scratch[f"{name}_other"] = pltpu.VMEM(given[f"{name}_own"].shape, BF16)
    scratch["att_across"] = pltpu.VMEM((count, out_cols), BF16)
    scratch["query_low"] = pltpu.VMEM((count, heads * size), BF16)
    scratch["pair_low"] = pltpu.VMEM((count, 2 * size), BF16)
    scratch["col_rows"] = pltpu.VMEM((2 * count, cols), BF16)
    scratch["col_send"] = pltpu.VMEM((count, cols), BF16)
    for name, shape in (("qkv", (lines, cols)), ("out", (out_lines, out_cols))):
        scratch[f"{name}_part"] = pltpu.VMEM((devices,) + shape, BF16)
        scratch[f"{name}_other"] = pltpu.VMEM((chips,) + shape, BF16)
        scratch[f"{name}_flow"] = pltpu.VMEM((chips,) + shape, BF16)
    for name in ("gain_own", "gain_across", "gain_pair", "gain_twin", "gain_sum"):
        scratch[name] = pltpu.VMEM(given["gains"].shape, F32)
    scratch["gain_flow"] = pltpu.VMEM((2, chips // 2 + 1) + given["gains"].shape, F32)
    scratch["bring"] = dma(len(BROUGHT))
    for name, n in (("cross_send", 5), ("cross_recv", 5), ("twin_send", 1), ("twin_recv", 1)):
        scratch[name] = dma(n)
    scratch["gain_send"] = dma(2, chips // 2)
    scratch["gain_recv"] = dma(2, chips // 2)
    names += list(outs) + list(scratch)
    return pl.pallas_call(
        functools.partial(
            back_kernel, devices, heads, ff_pieces, kv_pieces, attn_pieces, tuple(names)
        ),
        in_specs=[pl.BlockSpec(memory_space=pl.ANY)] * len(operands),
        out_specs=[pl.BlockSpec(memory_space=pltpu.VMEM)] * len(outs),
        out_shape=[jax.ShapeDtypeStruct(shape, kind) for shape, kind in outs.values()],
        scratch_shapes=list(scratch.values()),
        compiler_params=pltpu.CompilerParams(
            collective_id=collective_id, has_side_effects=True, vmem_limit_bytes=67043328
        ),
        name="back",
    )(*operands)


def finish_kernel(count, *refs):
    sources, results = refs[:count], list(refs[count:])
    for source in sources:
        first = 0
        while first < source.shape[1]:
            result = results.pop(0)
            result[...] = source[:, first : first + result.shape[1]].astype(result.dtype)
            first += result.shape[1]


def finish(sources, columns):
    outs = [
        jax.ShapeDtypeStruct((source.shape[0], width), kind)
        for source, pieces in zip(sources, columns)
        for kind, width in pieces
    ]
    here = pl.BlockSpec(memory_space=pltpu.VMEM)
    return pl.pallas_call(
        functools.partial(finish_kernel, len(sources)),
        in_specs=[here] * len(sources),
        out_specs=[here] * len(outs),
        out_shape=outs,
        name="finish",
    )(*sources)


def body(
    tokens,
    block_order,
    gain_attn_pre,
    gain_query,
    gain_key,
    gain_attn_post,
    gain_ff_pre,
    gain_ff_post,
    weight_query,
    weight_key,
    weight_value,
    weight_out,
    weight_gate,
    weight_up,
    weight_down,
    cotangent,
):
    sequences, rows, width = tokens.shape
    count = sequences * rows
    block = rows // 2
    devices = lax.axis_size("ctx")
    me = lax.axis_index("ctx")
    mine = lax.axis_index("wsh")

    head_size = 2 * gain_key.shape[0]
    heads = 2 * weight_query.shape[1] // head_size

    lane = jnp.arange(block, dtype=jnp.int32)
    late_order = 2 * devices - 1 - block_order
    early_pos = (block_order[:, None] * block + lane[None]).reshape(-1)
    late_pos = (late_order[:, None] * block + lane[None]).reshape(-1)
    key_pos = jnp.stack([early_pos, late_pos], 0)
    own_first = lax.dynamic_slice_in_dim(block_order, me, 1)[0]
    own_early = own_first * block + lane
    own_late = (2 * devices - 1 - own_first) * block + lane
    own_pos = jnp.concatenate([own_early, own_late])
    query_pos = jnp.concatenate([jnp.tile(own_early, heads), jnp.tile(own_late, heads)])[:, None]

    cosine, sine = angle_tables(own_pos, head_size)

    def placed(gain):
        zeros = jnp.zeros_like(gain)
        return jnp.where(
            mine == 0, jnp.concatenate([gain, zeros]), jnp.concatenate([zeros, gain])
        ).astype(F32)

    own_gains = [placed(g) for g in (gain_attn_pre, gain_attn_post, gain_ff_pre, gain_ff_post)]
    small = [placed(gain_query), placed(gain_key)]
    own_gains.append(jnp.concatenate(small + [jnp.zeros((width - 2 * head_size,), F32)]))
    own_gains = jnp.stack(own_gains + [jnp.zeros((width,), F32)] * 3)
    (
        normed_rows,
        key_raw,
        query_low,
        mixed_low,
        mixed,
        totals,
        all_gains,
        pairs,
        query_raw,
        pair_weight,
        query_weight,
        out_weight,
    ) = front(
        tokens,
        own_gains,
        cosine,
        sine,
        query_pos,
        key_pos,
        (weight_key, weight_value, weight_query, weight_out.T),
        heads,
        devices,
        2,
    )
    attn_pre = all_gains[0]
    query_gain = all_gains[4, :head_size]
    key_gain = all_gains[4, head_size : 2 * head_size]
    mixed_rows = mixed_low.reshape(count, heads * head_size)
    local_size = weight_key.shape[1]
    inputs = tokens.astype(F32)

    def key_path(key_in, key_scale):
        return rotate(norm_gain(key_in, key_scale), cosine[None], sine[None])

    def query_path(query_in, query_scale):
        return rotate(
            norm_gain(query_in, query_scale), cosine[None, :, None, :], sine[None, :, None, :]
        )

    (
        output,
        grad_hidden,
        grad_mixed,
        attended_own,
        attended_send,
        gain_part,
        part_down,
        part_gate,
        part_up,
    ) = feed_forward(
        mixed_rows,
        tokens.reshape(count, width),
        cotangent.reshape(count, width),
        all_gains,
        (out_weight, weight_gate, weight_up, weight_down),
        3,
    )

    def both(own, other):
        return jnp.concatenate([own, other], 0)

    def weight_grad(left, right):
        return dot(left, right, ((0,), (0,))).astype(BF16)

    grad_mixed = grad_mixed.reshape(query_low.shape)
    given = {
        "att_send": attended_send,
        "att_own": attended_own,
        "pairs": pairs.reshape(devices, count, 2 * head_size),
        "query": query_low,
        "grad_mixed": grad_mixed,
        "mixed": mixed,
        "totals": totals,
        "query_pos": query_pos,
        "key_pos": key_pos,
        "mixed_own": mixed_rows,
        "query_raw": query_raw,
        "key_raw": key_raw,
        "cosine": cosine,
        "sine": sine,
        "gains": all_gains,
        "weight_query": query_weight,
        "weight_pair": pair_weight,
        "tokens": tokens.reshape(count, width),
        "grad_hidden": grad_hidden.reshape(count, width),
        "gain_part": gain_part,
        "normed_own": normed_rows,
    }
    aligned = width % (8 * devices) == 0 and mixed_rows.shape[1] % (32 * devices) == 0
    if aligned and count == head_size:
        ff_parts = [
            p.reshape(devices, p.shape[0] // devices, p.shape[1])
            for p in (part_down, part_gate, part_up)
        ]
        grad_tokens, grad_down_w, grad_gate_w, grad_up_w, grad_qkv, grad_out_w, gain_sums = back(
            given, ff_parts, heads, devices, 0
        )
        hidden_cols, query_cols = grad_gate_w.shape[1], heads * head_size // 2
        (
            output,
            grad_tokens,
            grad_down_w,
            grad_gate_w,
            grad_up_w,
            grad_query_w,
            grad_key_w,
            grad_value_w,
            grad_out_w,
        ) = finish(
            [output, grad_tokens, grad_down_w, grad_gate_w, grad_up_w, grad_qkv, grad_out_w],
            [[(BF16, width)], [(F32, width)]]
            + [[(F32, hidden_cols)]] * 3
            + [[(F32, query_cols), (F32, local_size), (F32, local_size)], [(F32, width // 2)]],
        )
        grad_tokens = grad_tokens.reshape(sequences, rows, width)
        place = me * 2 + mine

        def share(row, first, size):
            part = size // (2 * devices)
            return lax.dynamic_slice(gain_sums, (row, first + place * part), (1, part))[0]

        outs = [
            share(0, 0, width),
            share(4, 0, head_size),
            share(4, head_size, head_size),
            share(1, 0, width),
            share(2, 0, width),
            share(3, 0, width),
        ]
    else:
        part_out = weight_grad(
            both(mixed_rows, swap(mixed_rows)),
            both(attended_own, swap(attended_send)),
        )
        grad_query, grad_pairs = attend_backward(
            query_low, pairs, grad_mixed, mixed, totals, query_pos, key_pos, heads
        )
        pair_rows = sequences * rows
        slots = grad_pairs.reshape(devices, pair_rows, 2 * head_size)
        share = pair_rows // 8
        pieces = tuple((0, 1 - 2 * (i % 2), i * share, share, 0, 2 * head_size) for i in range(8))
        own_grads = sum_over_ctx([slots], pieces, devices, 0)[0]
        own_grads = own_grads.reshape(sequences, rows, 2 * head_size)
        grad_key_raw, grad_key_gain = jax.vjp(
            key_path, key_raw.reshape(sequences, rows, head_size), key_gain
        )[1](own_grads[..., :head_size])
        value_grad_low = own_grads[..., head_size:].astype(BF16)
        grad_query_raw, grad_query_gain = jax.vjp(
            query_path, query_raw.reshape(sequences, rows, heads, head_size), query_gain
        )[1](
            grad_query.reshape(sequences, rows, heads, head_size)
        )
        query_grad_low = grad_query_raw.reshape(count, heads * head_size).astype(BF16)
        key_grad_low = grad_key_raw.astype(BF16).reshape(count, head_size)
        value_grad_low = value_grad_low.reshape(count, head_size)
        grad_normed = (
            dot(query_grad_low, query_weight, ((1,), (1,)))
            + dot(jnp.concatenate([key_grad_low, value_grad_low], -1), pair_weight, ((1,), (1,)))
        ).reshape(sequences, rows, width)
        grad_inputs, grad_attn_pre = jax.vjp(norm_gain, inputs, attn_pre)[1](grad_normed)
        grad_tokens = grad_inputs + grad_hidden.reshape(sequences, rows, width)

        def columns(which):
            return jnp.concatenate(
                [half_of(v, which) for v in (query_grad_low, key_grad_low, value_grad_low)], -1
            )

        part_qkv = weight_grad(
            both(normed_rows, swap(normed_rows)), both(columns(mine), swap(columns(1 - mine)))
        )

        gain_grads = [
            grad_attn_pre,
            grad_query_gain,
            grad_key_gain,
            gain_part[1],
            gain_part[2],
            gain_part[3],
        ]
        packed = jnp.concatenate([g.reshape(devices, 2, -1) for g in gain_grads], -1)
        keep = jnp.where(mine == 0, packed[:, 0], packed[:, 1])
        send = jnp.where(mine == 0, packed[:, 1], packed[:, 0])
        packed = keep + swap(send)
        gain_size = packed.shape[-1]
        packed = jnp.pad(packed, ((0, 0), (0, 1024 - gain_size))).reshape(devices, 8, 128)
        parts = [
            p.reshape(devices, p.shape[0] // devices, p.shape[1])
            for p in (part_down, part_gate, part_up, part_qkv, part_out)
        ] + [packed]
        grad_down_w, grad_gate_w, grad_up_w, grad_qkv, grad_out_w, packed = sum_over_ctx(
            parts, split_ways(parts), devices, 1
        )
        packed = packed.reshape(-1)
        outs, first = [], 0
        for g in gain_grads:
            size = g.shape[0] // (2 * devices)
            outs.append(packed[first : first + size])
            first += size
        query_cols = grad_qkv.shape[1] - 2 * local_size
        grad_query_w = grad_qkv[:, :query_cols]
        grad_key_w = grad_qkv[:, query_cols : query_cols + local_size]
        grad_value_w = grad_qkv[:, query_cols + local_size :]
        grad_down_w, grad_gate_w, grad_up_w = (
            g.astype(F32) for g in (grad_down_w, grad_gate_w, grad_up_w)
        )
    output = output.reshape(sequences, rows, width)
    return (
        output,
        grad_tokens,
        *outs,
        grad_query_w,
        grad_key_w,
        grad_value_w,
        grad_out_w,
        grad_gate_w,
        grad_up_w,
        grad_down_w,
    )


def solution(mesh):
    rows, vector, matrix = P("wsh", "ctx", None), P("wsh"), P(None, "wsh")
    in_specs = (rows, P()) + (vector,) * 6 + (matrix,) * 7 + (rows,)
    out_specs = (rows, rows) + (P(("ctx", "wsh")),) * 6 + (P("ctx", "wsh"),) * 7
    return jax.shard_map(body, mesh=mesh, in_specs=in_specs, out_specs=out_specs, check_vma=False)
```
